128 devices in a mesh: cp: 32 (over x, y, core), tp: 4 (over z).
Axes of the slice: x: 4, y: 4, z: 4, core: 2. Of those that a mesh axis runs over, the one named last changes fastest.
Arguments:
- hidden: bfloat16 [8192, 4096], P('cp', 'tp'), may hold values from -120 to 120
- query_weight: bfloat16 [4096, 4096], P(None, 'tp'), may hold values from -0.1875 to 0.1875
- key_matrix: bfloat16 [4096, 512], P(None, 'tp'), may hold values from -0.09375 to 0.09375
- value_matrix: bfloat16 [4096, 512], P(None, 'tp'), may hold values from -0.09375 to 0.09375
- output_weight: bfloat16 [4096, 4096], P('tp'), may hold values from -0.1875 to 0.1875
- document_bounds: int32 [9], replicated, may hold values from 0 to 8192, as said below
- block_owner: int32 [64], replicated, may hold values from 0 to 31, as said below
Outputs:
- attended: bfloat16 [8192, 4096], P('cp', 'tp')
The draws below stay inside these ranges and needn't reach their ends.
Inputs may be any that keep to these rules, and one draw needn't show every extreme that they name: document_bounds[0] = 0, document_bounds[8] = 8192, strictly rising; document i holds the tokens from document_bounds[i] to document_bounds[i + 1] - 1. `block_owner`: every index of cp is named by exactly 2 blocks.
All inputs are finite; a program needn't handle non-finite values.
Results may differ from the reference program's by a relative error of at most 0.012.
The reference program's roundings to bfloat16 on the way (of `queries`, `values`, `heads_out` and `projected`) count: a program that leaves them out, or rounds other values in their place, can miss the bound.
Values may be sent and summed in bfloat16 or wider, within the bound.
A program may use at most 128 MiB of HBM per device.

```python
import math
import jax
import jax.numpy as jnp
from jax import lax

MODEL_WIDTH = 4096
QUERY_HEADS = 32
KEY_VALUE_HEADS = 4
HEAD_WIDTH = 128
BLOCK = 128
DOCS = 8
TOK_DEV = 256
PACKED_TOKENS = 8192
NBLK = 64


def draw_hidden(key, part):
    drawn = jax.random.normal(key, (PACKED_TOKENS, MODEL_WIDTH), jnp.float32)
    return jnp.clip(drawn, -6.0, 6.0).astype(jnp.bfloat16)


def draw_document_bounds(key, part):
    cut_points = jax.random.permutation(jax.random.fold_in(key, 21), PACKED_TOKENS - 1)[:DOCS - 1] + 1
    inner_cuts = jnp.sort(cut_points).astype(jnp.int32)
    return jnp.concatenate([jnp.zeros((1,), jnp.int32), inner_cuts, jnp.full((1,), PACKED_TOKENS, jnp.int32)])


def draw_block_owner(key, part):
    shuffled = jax.random.permutation(jax.random.fold_in(key, 31), NBLK)
    return (shuffled // (TOK_DEV // BLOCK)).astype(jnp.int32)


def steps_of(key, shape, pieces, low, largest):
    factor_of, own = 1.0, jax.random.fold_in(key, 6)
    for position, blocks in pieces:
        draws = jnp.exp(jax.random.uniform(jax.random.fold_in(own, position), (blocks,), jnp.float32, low / len(pieces), largest / len(pieces)))
        factor_of = factor_of * jnp.repeat(draws, shape[position] // blocks).reshape([-1 if axis == position else 1 for axis in range(len(shape))])
    return factor_of


def normal_values(own_key, shape, scale, most, shards=(), held_as=jnp.bfloat16):
    values = jax.random.normal(own_key, shape, jnp.float32) * scale
    if len(shards) > 0:
        values = steps_of(own_key, shape, shards, -0.22, 0.18) * values
    return jnp.clip(values, min=-most, max=most).astype(held_as)


def setup_inputs(seed: int = 0) -> dict:
    streams_of = jax.random.split(jax.random.key(seed), 8)
    return {
        "hidden": draw_hidden(jax.random.fold_in(streams_of[7], 71), 0),
        "query_weight": normal_values(streams_of[1], (MODEL_WIDTH, QUERY_HEADS * HEAD_WIDTH), (MODEL_WIDTH // 4) ** -0.5, 0.1875, ((1, 4),)),
        "key_matrix": normal_values(streams_of[2], (MODEL_WIDTH, KEY_VALUE_HEADS * HEAD_WIDTH), MODEL_WIDTH ** -0.5, 0.09375, ((1, 4),)),
        "value_matrix": normal_values(streams_of[3], (MODEL_WIDTH, KEY_VALUE_HEADS * HEAD_WIDTH), MODEL_WIDTH ** -0.5, 0.09375, ((1, 4),)),
        "output_weight": normal_values(streams_of[4], (QUERY_HEADS * HEAD_WIDTH, MODEL_WIDTH), (QUERY_HEADS * HEAD_WIDTH // 4) ** -0.5, 0.1875, ((0, 4),)),
        "document_bounds": draw_document_bounds(jax.random.fold_in(streams_of[7], 71), 0),
        "block_owner": draw_block_owner(jax.random.fold_in(streams_of[7], 71), 0),
    }


rope_theta = 500000.0
rope_factor = 8.0
rope_context = 8192.0
masked_score = -1e+30

def rope_inverse(head_size):
    halves = jnp.arange(head_size // 2, dtype=jnp.float32)
    inverse = 1.0 / rope_theta ** (2.0 * halves / head_size)
    wavelength = 2.0 * math.pi / inverse
    smooth = (rope_context / wavelength - 1.0) / 3.0
    blended = (1.0 - smooth) * inverse / rope_factor + smooth * inverse
    longer = jnp.where(wavelength > rope_context, inverse / rope_factor, blended)
    return jnp.where(wavelength < rope_context / 4.0, inverse, longer)

def document_of(tokens, bounds):
    inner_bounds = bounds[1:-1]
    return lax.optimization_barrier(jnp.sum((tokens[:, None] >= inner_bounds[None, :]).astype(jnp.int32), axis=1))

def position_of(tokens, bounds):
    starts = bounds[:-1]
    document_start = lax.optimization_barrier(jnp.max(jnp.where(starts[None, :] <= tokens[:, None], starts[None, :], 0), axis=1))
    return tokens - document_start

def rotate(raw_rows, tokens, bounds, head_size):
    row_count = raw_rows.shape[0]
    head_count = raw_rows.shape[1] // head_size
    angles = position_of(tokens, bounds).astype(jnp.float32)[:, None] * rope_inverse(head_size)[None, :]
    cosine = jnp.cos(angles)[:, None, :]
    sine_table = jnp.sin(angles)[:, None, :]
    heads_view = raw_rows.reshape(row_count, head_count, head_size)
    front_half = heads_view[:, :, :head_size // 2]
    back_half = heads_view[:, :, head_size // 2:]
    turned = jnp.concatenate([front_half * cosine - back_half * sine_table, back_half * cosine + front_half * sine_table], axis=2)
    return turned.reshape(row_count, head_count * head_size).astype(jnp.bfloat16)

def owner_order(block_owner, per_device):
    block_count = block_owner.shape[0]
    blocks = jnp.arange(block_count, dtype=jnp.int32)
    same_owner = block_owner[:, None] == block_owner[None, :]
    earlier = blocks[None, :] < blocks[:, None]
    owner_rank = lax.optimization_barrier(jnp.sum((same_owner & earlier).astype(jnp.int32), axis=1))
    target = block_owner * per_device + owner_rank
    return lax.optimization_barrier(jnp.sum(jnp.where(target[None, :] == blocks[:, None], blocks[None, :], 0), axis=1)).astype(jnp.int32)

def reference(hidden, query_weight, key_matrix, value_matrix, output_weight, document_bounds, block_owner):
    tokens = jnp.arange(PACKED_TOKENS, dtype=jnp.int32)
    query_raw = jnp.dot(hidden, query_weight, preferred_element_type=jnp.float32)
    key_raw = jnp.dot(hidden, key_matrix, preferred_element_type=jnp.float32)
    value_raw = jnp.dot(hidden, value_matrix, preferred_element_type=jnp.float32)
    queries = rotate(query_raw, tokens, document_bounds, HEAD_WIDTH)
    key_rows = rotate(key_raw, tokens, document_bounds, HEAD_WIDTH)
    value_rows = value_raw.astype(jnp.bfloat16)
    documents = document_of(tokens, document_bounds)
    query_heads = queries.reshape(PACKED_TOKENS, QUERY_HEADS, HEAD_WIDTH).transpose(1, 0, 2)
    per_head_keys = key_rows.reshape(PACKED_TOKENS, KEY_VALUE_HEADS, HEAD_WIDTH).transpose(1, 0, 2)
    per_head_values = value_rows.reshape(PACKED_TOKENS, KEY_VALUE_HEADS, HEAD_WIDTH).transpose(1, 0, 2)
    query_group_width = QUERY_HEADS // KEY_VALUE_HEADS
    query_block = math.gcd(PACKED_TOKENS, 1024)
    score_scale = 1.0 / math.sqrt(HEAD_WIDTH)

    def one_head(head_index):
        head_queries = query_heads[head_index]
        head_keys = per_head_keys[head_index // query_group_width]
        head_values = per_head_values[head_index // query_group_width]

        def one_block(block_index):
            first_row = block_index * query_block
            block_queries = lax.dynamic_slice_in_dim(head_queries, first_row, query_block, 0)
            block_tokens = first_row + jnp.arange(query_block, dtype=jnp.int32)
            block_documents = lax.dynamic_slice_in_dim(documents, first_row, query_block, 0)
            allowed = (block_documents[:, None] == documents[None, :]) & (tokens[None, :] <= block_tokens[:, None])
            scores = jnp.dot(block_queries, head_keys.T, preferred_element_type=jnp.float32) * score_scale
            scores = jnp.where(allowed, scores, masked_score)
            row_max = lax.optimization_barrier(jnp.max(scores, axis=1, keepdims=True))
            weights = jnp.where(allowed, jnp.exp(scores - row_max), 0.0)
            totals = lax.optimization_barrier(jnp.sum(weights, axis=1, keepdims=True))
            mixed_rows = jnp.dot(weights.astype(jnp.bfloat16), head_values, preferred_element_type=jnp.float32)
            return (mixed_rows / totals).astype(jnp.bfloat16)
        return lax.map(one_block, jnp.arange(PACKED_TOKENS // query_block, dtype=jnp.int32)).reshape(PACKED_TOKENS, HEAD_WIDTH)
    heads_out = lax.map(one_head, jnp.arange(QUERY_HEADS, dtype=jnp.int32))
    heads_out = heads_out.transpose(1, 0, 2).reshape(PACKED_TOKENS, QUERY_HEADS * HEAD_WIDTH)
    projected = jnp.dot(heads_out, output_weight, preferred_element_type=jnp.float32).astype(jnp.bfloat16)
    block_order = owner_order(block_owner, TOK_DEV // BLOCK)
    new_rows = (block_order[:, None] * BLOCK + jnp.arange(BLOCK, dtype=jnp.int32)[None, :]).reshape(-1)
    return jnp.take(projected, new_rows, axis=0)
```

```python
import functools
import math

import jax
import jax.numpy as jnp
from jax import lax
from jax.experimental import pallas as pl
from jax.experimental.pallas import tpu as pltpu
from jax.sharding import PartitionSpec as P

HEAD = 128
BLOCK = 128
CP = 32
TP = 4
ROWS = 256
WIDTH = 1024
NBLK = 64
HEADS = 8
TOKENS = 8192
PORTION = BLOCK // CP

rope_theta = 500000.0
rope_factor = 8.0
rope_context = 8192.0
masked_score = -1e30
MESH = pl.DeviceIdType.MESH


def rope_inverse(head_size):
    halves = jnp.arange(head_size // 2, dtype=jnp.float32)
    inverse = 1.0 / rope_theta ** (2.0 * halves / head_size)
    wavelength = 2.0 * math.pi / inverse
    smooth = (rope_context / wavelength - 1.0) / 3.0
    blended = (1.0 - smooth) * inverse / rope_factor + smooth * inverse
    longer = jnp.where(wavelength > rope_context, inverse / rope_factor, blended)
    return jnp.where(wavelength < rope_context / 4.0, inverse, longer)


def slots_of(block_owner):
    blocks = jnp.arange(NBLK, dtype=jnp.int32)
    same = block_owner[:, None] == block_owner[None, :]
    earlier = blocks[None, :] < blocks[:, None]
    rank = jnp.sum((same & earlier).astype(jnp.int32), axis=1)
    return block_owner * 2 + rank


def starts_of(tokens, bounds_ref):
    start = jnp.zeros_like(tokens)
    for i in range(1, 8):
        bound = bounds_ref[i]
        start = jnp.where(tokens >= bound, bound, start)
    return start


def gather_kernel(
    bounds_ref, hidden_ref, wq_ref, wk_ref, wv_ref, inverse_ref,
    k_ref, v_ref, q_ref,
    full, wq, wkv, qtmp, qsend, cosine, sine,
    w_sem, z_send, z_recv, g_send, g_recv, q_send, q_recv,
):
    me = lax.axis_index("cp")
    tp = lax.axis_index("tp")
    core = lax.rem(me, 2)
    ycoord = lax.rem(me // 2, 4)
    xcoord = me // 8
    partner = me + 1 - 2 * core
    up, down = lax.rem(tp + 1, TP), lax.rem(tp + 3, TP)

    weights = [
        pltpu.make_async_copy(wk_ref, wkv.at[:, pl.ds(0, HEAD)], w_sem.at[0]),
        pltpu.make_async_copy(wv_ref, wkv.at[:, pl.ds(HEAD, HEAD)], w_sem.at[1]),
        pltpu.make_async_copy(wq_ref, wq, w_sem.at[2]),
    ]
    for copy in weights:
        copy.start()

    barrier = pltpu.get_barrier_semaphore()

    def greet(k, carry):
        pl.semaphore_signal(
            barrier, inc=1, device_id={"cp": lax.rem(me + k, CP)}, device_id_type=MESH
        )
        return carry

    pl.semaphore_signal(barrier, inc=1, device_id={"tp": up}, device_id_type=MESH)
    pl.semaphore_signal(barrier, inc=1, device_id={"tp": down}, device_id_type=MESH)
    lax.fori_loop(1, CP, greet, 0)
    pl.semaphore_wait(barrier, CP + 1)

    def zcopy(n, source, target, owner, row, count):
        columns = pl.ds(pl.multiple_of(owner * WIDTH, WIDTH), WIDTH)
        source_ref = (
            hidden_ref.at[pl.ds(row, count), :]
            if source
            else full.at[pl.ds(row, count), columns]
        )
        return pltpu.make_async_remote_copy(
            src_ref=source_ref,
            dst_ref=full.at[pl.ds(row, count), columns],
            send_sem=z_send.at[n],
            recv_sem=z_recv.at[n],
            device_id={"tp": target},
            device_id_type=MESH,
        )

    own = {}
    for n, (row, count) in enumerate(((0, 128), (128, 64), (192, 64))):
        own[n] = (
            zcopy(2 * n, True, up, tp, row, count),
            zcopy(2 * n + 1, True, down, tp, row, count),
        )
    fwd = {
        r: (
            zcopy(6 + 2 * r, False, up, down, r * 128, 64),
            zcopy(7 + 2 * r, False, down, up, r * 128 + 64, 64),
        )
        for r in range(2)
    }
    for n in (0, 1):
        for copy in own[n]:
            copy.start()

    full[:, pl.ds(pl.multiple_of(tp * WIDTH, WIDTH), WIDTH)] = hidden_ref[...]
    inverse = inverse_ref[...]
    lanes = lax.broadcasted_iota(jnp.int32, (BLOCK, HEAD), 1)
    for r in range(2):
        tokens = me * ROWS + r * BLOCK + lax.broadcasted_iota(jnp.int32, (BLOCK, HEAD), 0)
        angle = (tokens - starts_of(tokens, bounds_ref)).astype(jnp.float32) * inverse
        turn = jnp.sin(angle)
        cosine[pl.ds(r * BLOCK, BLOCK), :] = jnp.cos(angle)
        sine[pl.ds(r * BLOCK, BLOCK), :] = jnp.where(lanes < HEAD // 2, -turn, turn)
    weights[0].wait()
    weights[1].wait()

    for copy in own[0]:
        copy.wait_recv()
    for copy in fwd[0]:
        copy.start()
    for copy in own[2]:
        copy.start()
    weights[2].wait()

    def rotate(raw, r):
        table = pl.ds(r * BLOCK, BLOCK)
        return raw * cosine[table, :] + pltpu.roll(raw, HEAD // 2, 1) * sine[table, :]

    def keys_values(r):
        raw = jnp.dot(
            full[pl.ds(r * BLOCK, BLOCK), :], wkv[...], preferred_element_type=jnp.float32
        )
        k_ref[xcoord, ycoord, core, r] = rotate(raw[:, :HEAD], r).astype(jnp.bfloat16)
        v_ref[xcoord, ycoord, core, r] = raw[:, HEAD:].astype(jnp.bfloat16)

    def queries(r):
        def pair(n, carry):
            columns = pl.ds(pl.multiple_of(n * 2 * HEAD, 2 * HEAD), 2 * HEAD)
            raw = jnp.dot(
                full[pl.ds(r * BLOCK, BLOCK), :],
                wq[:, columns],
                preferred_element_type=jnp.float32,
            )
            turned = jnp.concatenate(
                [rotate(raw[:, :HEAD], r), rotate(raw[:, HEAD:], r)], axis=1
            )
            qtmp[pl.ds(r * BLOCK, BLOCK), columns] = turned.astype(jnp.bfloat16)
            return carry

        lax.fori_loop(0, WIDTH // (2 * HEAD), pair, 0)

    def gather(which, r):
        buffer = (k_ref, v_ref)[which]
        a, b = ((xcoord, ycoord), (ycoord, xcoord))[which]
        base = (which * 2 + r) * 12

        def neighbour(along, step):
            if along == 0:
                na, nb = lax.rem(a + step, 4), b
            else:
                na, nb = a, lax.rem(b + step, 4)
            x, y = ((na, nb), (nb, na))[which]
            return (x * 4 + y) * 2 + core

        def copy(n, ref, target):
            return pltpu.make_async_remote_copy(
                src_ref=ref,
                dst_ref=ref,
                send_sem=g_send.at[base + n],
                recv_sem=g_recv.at[base + n],
                device_id={"cp": target},
                device_id_type=MESH,
            )

        def piece(at, row, count):
            rows = pl.ds(row, count)
            if which == 0:
                return buffer.at[at, b, core, r, rows]
            return buffer.at[b, at, core, r, rows]

        def line(at, first, count):
            along = pl.ds(first, count)
            if which == 0:
                return buffer.at[along, at, core, r]
            return buffer.at[at, along, core, r]

        a_next, a_prev = lax.rem(a + 1, 4), lax.rem(a + 3, 4)
        b_next, b_prev = lax.rem(b + 1, 4), lax.rem(b + 3, 4)
        b_far = lax.rem(b + 2, 4)
        return dict(
            ring1=(
                copy(0, piece(a, 0, BLOCK), neighbour(0, 1)),
                copy(1, piece(a, 0, BLOCK), neighbour(0, 3)),
            ),
            ring1_far=(
                copy(2, piece(a_prev, 0, 64), neighbour(0, 1)),
                copy(3, piece(a_next, 64, 64), neighbour(0, 3)),
            ),
            ring2=(
                copy(4, line(b, 0, 4), neighbour(1, 1)),
                copy(5, line(b, 0, 4), neighbour(1, 3)),
            ),
            ring2_far=(
                copy(6, line(b_prev, 0, 2), neighbour(1, 1)),
                copy(7, line(b_next, 2, 2), neighbour(1, 3)),
            ),
            across=(
                copy(8, line(b, 0, 4), partner),
                copy(9, line(b_prev, 0, 4), partner),
                copy(10, line(b_next, 0, 4), partner),
                copy(11, line(b_far, 0, 4), partner),
            ),
        )

    flows = {r: [gather(which, r) for which in range(2)] for r in range(2)}

    def start(r, name):
        for flow in flows[r]:
            for copy in flow[name]:
                copy.start()

    def arrived(r, name):
        for flow in flows[r]:
            for copy in flow[name]:
                copy.wait_recv()

    def across(r, which):
        for flow in flows[r]:
            for n in which:
                flow["across"][n].start()

    for copy in fwd[0]:
        copy.wait_recv()
    keys_values(0)
    start(0, "ring1")
    for n in (1, 2):
        for copy in own[n]:
            copy.wait_recv()
    for copy in fwd[1]:
        copy.start()
    queries(0)
    arrived(0, "ring1")
    start(0, "ring1_far")
    arrived(0, "ring1_far")
    start(0, "ring2")
    across(0, (0,))
    for copy in fwd[1]:
        copy.wait_recv()
    keys_values(1)
    start(1, "ring1")
    arrived(0, "ring2")
    start(0, "ring2_far")
    across(0, (1, 2))
    queries(1)
    arrived(1, "ring1")
    start(1, "ring1_far")

    out_row = lax.broadcasted_iota(jnp.int32, (ROWS, ROWS), 0)
    in_row = lax.broadcasted_iota(jnp.int32, (ROWS, ROWS), 1)
    origin = lax.rem(out_row // 4, 2) * BLOCK + (out_row // 8) * 4 + lax.rem(out_row, 4)
    pick = (in_row == origin).astype(jnp.float32).astype(jnp.bfloat16)
    ordered = jnp.dot(pick, qtmp[...], preferred_element_type=jnp.float32)
    qsend[...] = ordered.reshape(CP, 8, WIDTH).astype(jnp.bfloat16)
    q_ref[me] = qsend[me]

    def qcopy(k, target, slot):
        return pltpu.make_async_remote_copy(
            src_ref=qsend.at[target],
            dst_ref=q_ref.at[slot],
            send_sem=q_send.at[k],
            recv_sem=q_recv.at[k],
            device_id={"cp": target},
            device_id_type=MESH,
        )

    def send_queries(k, carry):
        qcopy(k, lax.rem(me + k, CP), me).start()
        return carry

    def wait_queries(k, carry):
        copy = qcopy(k, lax.rem(me + k, CP), lax.rem(me + CP - k, CP))
        copy.wait_send()
        copy.wait_recv()
        return carry

    arrived(1, "ring1_far")
    start(1, "ring2")
    across(1, (0,))
    lax.fori_loop(1, CP, send_queries, 0)
    arrived(0, "ring2_far")
    across(0, (3,))
    arrived(1, "ring2")
    start(1, "ring2_far")
    across(1, (1, 2))
    arrived(1, "ring2_far")
    across(1, (3,))
    lax.fori_loop(1, CP, wait_queries, 0)
    for r in range(2):
        arrived(r, "across")
        for flow in flows[r]:
            for name in ("ring1", "ring1_far", "ring2", "ring2_far", "across"):
                for copy in flow[name]:
                    copy.wait_send()
    for group in (*own.values(), *fwd.values()):
        for copy in group:
            copy.wait_send()


def gather_call(bounds, hidden, wq, wk, wv, inverse):
    vmem = pl.BlockSpec(memory_space=pltpu.VMEM)
    anywhere = pl.BlockSpec(memory_space=pl.ANY)
    kv = jax.ShapeDtypeStruct((4, 4, 2, 2, BLOCK, HEAD), jnp.bfloat16)
    dma = pltpu.SemaphoreType.DMA
    return pl.pallas_call(
        gather_kernel,
        out_shape=(kv, kv, jax.ShapeDtypeStruct((CP, 8, WIDTH), jnp.bfloat16)),
        in_specs=[
            pl.BlockSpec(memory_space=pltpu.SMEM), vmem, anywhere, anywhere, anywhere, vmem,
        ],
        out_specs=(vmem, vmem, vmem),
        scratch_shapes=[
            pltpu.VMEM((ROWS, TP * WIDTH), jnp.bfloat16),
            pltpu.VMEM((TP * WIDTH, WIDTH), jnp.bfloat16),
            pltpu.VMEM((TP * WIDTH, 2 * HEAD), jnp.bfloat16),
            pltpu.VMEM((ROWS, WIDTH), jnp.bfloat16),
            pltpu.VMEM((CP, 8, WIDTH), jnp.bfloat16),
            pltpu.VMEM((ROWS, HEAD), jnp.float32),
            pltpu.VMEM((ROWS, HEAD), jnp.float32),
            dma((3,)), dma((10,)), dma((10,)), dma((48,)), dma((48,)), dma((CP,)), dma((CP,)),
        ],
        compiler_params=pltpu.CompilerParams(
            collective_id=0, has_side_effects=True, vmem_limit_bytes=50 * 1024 * 1024
        ),
        name="gather_project",
    )(bounds, hidden, wq, wk, wv, inverse)


GROUP = 8
TILE = 512


def attend_kernel(bounds_ref, q_ref, k_ref, v_ref, o_ref):
    me = lax.axis_index("cp")
    rows = GROUP * PORTION
    scale = 1.0 / math.sqrt(HEAD)

    def group(g, carry):
        first = pl.multiple_of(g * rows, rows)
        q = jnp.concatenate(
            [q_ref[pl.ds(first, rows), h * HEAD : (h + 1) * HEAD] for h in range(HEADS)], axis=0
        )
        row = lax.rem(lax.broadcasted_iota(jnp.int32, (HEADS * rows, 1), 0), rows)
        tokens = (g * GROUP + row // PORTION) * BLOCK + me * PORTION + lax.rem(row, PORTION)
        starts = starts_of(tokens, bounds_ref)
        low_token = g * GROUP * BLOCK
        low = jnp.int32(0)
        for i in range(1, 8):
            low = jnp.where(low_token >= bounds_ref[i], bounds_ref[i], low)

        def tile(j, state):
            top, total, mixed = state
            at = pl.ds(pl.multiple_of(j * TILE, TILE), TILE)
            scores = lax.dot_general(
                q, k_ref[at, :], (((1,), (1,)), ((), ())), preferred_element_type=jnp.float32
            )
            keys = j * TILE + lax.broadcasted_iota(jnp.int32, (HEADS * rows, TILE), 1)
            allowed = (keys >= starts) & (keys <= tokens)
            scores = jnp.where(allowed, scores * scale, masked_score)
            new_top = jnp.maximum(top, jnp.max(scores, axis=1, keepdims=True))
            weights = jnp.where(allowed, jnp.exp(scores - new_top), 0.0)
            factor = jnp.exp(top - new_top)
            part = weights[:, :HEAD]
            for c in range(1, TILE // HEAD):
                part = part + weights[:, c * HEAD : (c + 1) * HEAD]
            total = total * factor + part
            mixed = mixed * factor + jnp.dot(
                weights.astype(jnp.bfloat16), v_ref[at, :], preferred_element_type=jnp.float32
            )
            return new_top, total, mixed

        top, total, mixed = lax.fori_loop(
            low // TILE,
            (g + 1) * (GROUP * BLOCK // TILE),
            tile,
            (
                jnp.full((HEADS * rows, 1), masked_score, jnp.float32),
                jnp.zeros((HEADS * rows, HEAD), jnp.float32),
                jnp.zeros((HEADS * rows, HEAD), jnp.float32),
            ),
        )
        out = (mixed / jnp.sum(total, axis=1, keepdims=True)).astype(jnp.bfloat16)
        for h in range(HEADS):
            o_ref[pl.ds(first, rows), h * HEAD : (h + 1) * HEAD] = out[h * rows : (h + 1) * rows]
        return carry

    lax.fori_loop(0, NBLK // GROUP, group, 0)


def attend_call(bounds, q, k, v):
    vmem = pl.BlockSpec(memory_space=pltpu.VMEM)
    return pl.pallas_call(
        attend_kernel,
        out_shape=jax.ShapeDtypeStruct((ROWS, WIDTH), jnp.bfloat16),
        in_specs=[pl.BlockSpec(memory_space=pltpu.SMEM), vmem, vmem, vmem],
        out_specs=vmem,
        compiler_params=pltpu.CompilerParams(vmem_limit_bytes=40 * 1024 * 1024),
        name="attend",
    )(bounds, q, k, v)


CHUNKS = 4
CW = WIDTH // CHUNKS


def output_kernel(
    slot_ref, heads_ref, wo_ref, out_ref,
    wo, far, near, far_in, near_in, spread, landed, own_sum,
    w_sem, z_send, z_recv, a_send, a_recv,
):
    me = lax.axis_index("cp")
    tp = lax.axis_index("tp")
    up, down, across = lax.rem(tp + 1, TP), lax.rem(tp + 3, TP), lax.rem(tp + 2, TP)

    loads = []
    for n, t in enumerate((across, up, down, tp)):
        columns = pl.ds(pl.multiple_of(t * WIDTH, WIDTH), WIDTH)
        loads.append(pltpu.make_async_copy(wo_ref.at[:, columns], wo.at[n], w_sem.at[n]))
        loads[-1].start()

    barrier = pltpu.get_barrier_semaphore()

    def greet(k, carry):
        pl.semaphore_signal(
            barrier, inc=1, device_id={"cp": lax.rem(me + k, CP)}, device_id_type=MESH
        )
        return carry

    pl.semaphore_signal(barrier, inc=1, device_id={"tp": up}, device_id_type=MESH)
    pl.semaphore_signal(barrier, inc=1, device_id={"tp": down}, device_id_type=MESH)
    lax.fori_loop(1, CP, greet, 0)

    def product(n, c):
        return jnp.dot(
            heads_ref[...], wo[n, :, c * CW : (c + 1) * CW], preferred_element_type=jnp.float32
        )

    def remote(n, src, dst, target):
        return pltpu.make_async_remote_copy(
            src_ref=src,
            dst_ref=dst,
            send_sem=z_send.at[n],
            recv_sem=z_recv.at[n],
            device_id={"tp": target},
            device_id_type=MESH,
        )

    half = ROWS // 2
    far_copies, near_copies = [], []
    for c in range(CHUNKS):
        far_copies.append(
            (
                remote(4 * c, far.at[c, pl.ds(0, half)], far_in.at[c, 0], up),
                remote(4 * c + 1, far.at[c, pl.ds(half, half)], far_in.at[c, 1], down),
            )
        )
        near_copies.append(
            (
                remote(4 * c + 2, near.at[c, 0], near_in.at[c, 0], up),
                remote(4 * c + 3, near.at[c, 1], near_in.at[c, 1], down),
            )
        )

    def send_far(c):
        far[c] = product(0, c).astype(jnp.bfloat16)
        for copy in far_copies[c]:
            copy.start()

    def send_near(c):
        to_up, to_down = product(1, c), product(2, c)
        far_copies[c][0].wait_recv()
        near[c, 0, :half] = (to_up[:half] + far_in[c, 0].astype(jnp.float32)).astype(jnp.bfloat16)
        near[c, 0, half:] = to_up[half:].astype(jnp.bfloat16)
        near_copies[c][0].start()
        far_copies[c][1].wait_recv()
        near[c, 1, :half] = to_down[:half].astype(jnp.bfloat16)
        near[c, 1, half:] = (to_down[half:] + far_in[c, 1].astype(jnp.float32)).astype(
            jnp.bfloat16
        )
        near_copies[c][1].start()

    row = lax.broadcasted_iota(jnp.int32, (ROWS, ROWS), 0)
    column = lax.broadcasted_iota(jnp.int32, (ROWS, ROWS), 1)
    to_owner = (row == slot_ref[...]).astype(jnp.float32).astype(jnp.bfloat16)
    origin = (lax.rem(row, BLOCK) // 4) * 8 + (row // BLOCK) * 4 + lax.rem(row, 4)
    to_place = (column == origin).astype(jnp.float32).astype(jnp.bfloat16)

    def acopy(c, k, target, slot):
        return pltpu.make_async_remote_copy(
            src_ref=spread.at[c, target],
            dst_ref=landed.at[c, slot],
            send_sem=a_send.at[c, k],
            recv_sem=a_recv.at[c, k],
            device_id={"cp": target},
            device_id_type=MESH,
        )

    def finish_sum(c):
        for copy in near_copies[c]:
            copy.wait_recv()
        total = (
            own_sum[c]
            + near_in[c, 0].astype(jnp.float32)
            + near_in[c, 1].astype(jnp.float32)
        ).astype(jnp.bfloat16)
        picked = jnp.dot(to_owner, total, preferred_element_type=jnp.float32)
        spread[c] = picked.reshape(CP, 8, CW).astype(jnp.bfloat16)
        landed[c, me] = spread[c, me]

        def send(k, carry):
            acopy(c, k, lax.rem(me + k, CP), me).start()
            return carry

        lax.fori_loop(1, CP, send, 0)

    def place(c):
        def wait(k, carry):
            copy = acopy(c, k, lax.rem(me + k, CP), lax.rem(me + CP - k, CP))
            copy.wait_send()
            copy.wait_recv()
            return carry

        lax.fori_loop(1, CP, wait, 0)
        rows = landed[c].astype(jnp.float32).reshape(ROWS, CW).astype(jnp.bfloat16)
        out_ref[:, c * CW : (c + 1) * CW] = jnp.dot(
            to_place, rows, preferred_element_type=jnp.float32
        ).astype(jnp.bfloat16)

    loads[0].wait()
    far[0] = product(0, 0).astype(jnp.bfloat16)
    pl.semaphore_wait(barrier, CP + 1)
    for copy in far_copies[0]:
        copy.start()
    send_far(1)
    loads[1].wait()
    loads[2].wait()
    send_near(0)
    send_far(2)
    send_near(1)
    send_far(3)
    loads[3].wait()
    own_sum[0] = product(3, 0)
    send_near(2)
    own_sum[1] = product(3, 1)
    send_near(3)
    own_sum[2] = product(3, 2)
    own_sum[3] = product(3, 3)
    for c in range(CHUNKS):
        finish_sum(c)
        if c > 0:
            place(c - 1)
    place(CHUNKS - 1)
    for c in range(CHUNKS):
        for copy in (*far_copies[c], *near_copies[c]):
            copy.wait_send()


def output_call(slot_rows, heads, wo):
    vmem = pl.BlockSpec(memory_space=pltpu.VMEM)
    dma = pltpu.SemaphoreType.DMA
    half = ROWS // 2
    bf16 = jnp.bfloat16
    return pl.pallas_call(
        output_kernel,
        out_shape=jax.ShapeDtypeStruct((ROWS, WIDTH), bf16),
        in_specs=[vmem, vmem, pl.BlockSpec(memory_space=pl.ANY)],
        out_specs=vmem,
        scratch_shapes=[
            pltpu.VMEM((TP, WIDTH, WIDTH), bf16),
            pltpu.VMEM((CHUNKS, ROWS, CW), bf16),
            pltpu.VMEM((CHUNKS, 2, ROWS, CW), bf16),
            pltpu.VMEM((CHUNKS, 2, half, CW), bf16),
            pltpu.VMEM((CHUNKS, 2, ROWS, CW), bf16),
            pltpu.VMEM((CHUNKS, CP, 8, CW), bf16),
            pltpu.VMEM((CHUNKS, CP, 8, CW), bf16),
            pltpu.VMEM((CHUNKS, ROWS, CW), jnp.float32),
            dma((4,)), dma((4 * CHUNKS,)), dma((4 * CHUNKS,)), dma((CHUNKS, CP)), dma((CHUNKS, CP)),
        ],
        compiler_params=pltpu.CompilerParams(
            collective_id=1, has_side_effects=True, vmem_limit_bytes=40 * 1024 * 1024
        ),
        name="project_out",
    )(slot_rows, heads, wo)


def local(hidden, query_weight, key_matrix, value_matrix, output_weight, bounds, block_owner):
    inverse = rope_inverse(HEAD)
    inverse = jnp.concatenate([inverse, inverse])[None, :]
    slots = slots_of(block_owner)
    slot_rows = (slots[:, None] * PORTION + jnp.arange(PORTION, dtype=jnp.int32)[None, :]).reshape(
        1, ROWS
    )
    keys, values, queries = gather_call(
        bounds, hidden, query_weight, key_matrix, value_matrix, inverse
    )
    heads = attend_call(
        bounds,
        queries.reshape(ROWS, WIDTH),
        keys.reshape(TOKENS, HEAD),
        values.reshape(TOKENS, HEAD),
    )
    return output_call(slot_rows, heads, output_weight)


def solution(mesh):
    placed = (P("cp", "tp"), P(None, "tp"), P(None, "tp"), P(None, "tp"), P("tp", None), P(), P())
    return jax.shard_map(
        local, mesh=mesh, in_specs=placed, out_specs=P("cp", "tp"), check_vma=False
    )
```

```python
import functools
import math

import jax
import jax.numpy as jnp
from jax import lax
from jax.experimental import pallas as pl
from jax.experimental.pallas import tpu as pltpu
from jax.sharding import PartitionSpec as P

HEAD = 128
BLOCK = 128
CP = 32
TP = 4
ROWS = 256
WIDTH = 1024
NBLK = 64
HEADS = 8
TOKENS = 8192
PORTION = BLOCK // CP

rope_theta = 500000.0
rope_factor = 8.0
rope_context = 8192.0
masked_score = -1e30
MESH = pl.DeviceIdType.MESH


def rope_inverse(head_size):
    halves = jnp.arange(head_size // 2, dtype=jnp.float32)
    inverse = 1.0 / rope_theta ** (2.0 * halves / head_size)
    wavelength = 2.0 * math.pi / inverse
    smooth = (rope_context / wavelength - 1.0) / 3.0
    blended = (1.0 - smooth) * inverse / rope_factor + smooth * inverse
    longer = jnp.where(wavelength > rope_context, inverse / rope_factor, blended)
    return jnp.where(wavelength < rope_context / 4.0, inverse, longer)


def slots_of(block_owner):
    blocks = jnp.arange(NBLK, dtype=jnp.int32)
    same = block_owner[:, None] == block_owner[None, :]
    earlier = blocks[None, :] < blocks[:, None]
    rank = jnp.sum((same & earlier).astype(jnp.int32), axis=1)
    return block_owner * 2 + rank


def starts_of(tokens, bounds_ref):
    start = jnp.zeros_like(tokens)
    for i in range(1, 8):
        bound = bounds_ref[i]
        start = jnp.where(tokens >= bound, bound, start)
    return start


PARTS = 4
PART = ROWS // PARTS
SPAN = 8
PENALTY = -1e30


def gather_kernel(
    bounds_ref, hidden_ref, wq_ref, wk_ref, wv_ref, inverse_ref,
    k_ref, v_ref, q_ref, mark_ref,
    full, wq, wkv, qtmp, qsend, cosine, sine,
    w_sem, z_send, z_recv, g_send, g_recv, q_send, q_recv,
):
    me = lax.axis_index("cp")
    tp = lax.axis_index("tp")
    core = lax.rem(me, 2)
    ycoord = lax.rem(me // 2, 4)
    xcoord = me // 8
    partner = me + 1 - 2 * core
    up, down = lax.rem(tp + 1, TP), lax.rem(tp + 3, TP)
    own_columns = pl.ds(pl.multiple_of(tp * WIDTH, WIDTH), WIDTH)

    bring = pltpu.make_async_copy(hidden_ref, full.at[:, own_columns], w_sem.at[3])
    weights = [
        pltpu.make_async_copy(wk_ref, wkv.at[:, pl.ds(0, HEAD)], w_sem.at[0]),
        pltpu.make_async_copy(wv_ref, wkv.at[:, pl.ds(HEAD, HEAD)], w_sem.at[1]),
        pltpu.make_async_copy(wq_ref, wq, w_sem.at[2]),
    ]
    bring.start()
    for copy in weights:
        copy.start()

    barrier = pltpu.get_barrier_semaphore()

    def greet(k, carry):
        pl.semaphore_signal(
            barrier, inc=1, device_id={"cp": lax.rem(me + k, CP)}, device_id_type=MESH
        )
        return carry

    pl.semaphore_signal(barrier, inc=1, device_id={"tp": up}, device_id_type=MESH)
    pl.semaphore_signal(barrier, inc=1, device_id={"tp": down}, device_id_type=MESH)
    lax.fori_loop(1, CP, greet, 0)
    bring.wait()
    pl.semaphore_wait(barrier, CP + 1)

    def zcopy(n, target, owner, row, count):
        columns = pl.ds(pl.multiple_of(owner * WIDTH, WIDTH), WIDTH)
        ref = full.at[pl.ds(row, count), columns]
        return pltpu.make_async_remote_copy(
            src_ref=ref,
            dst_ref=ref,
            send_sem=z_send.at[n],
            recv_sem=z_recv.at[n],
            device_id={"tp": target},
            device_id_type=MESH,
        )

    half = PART // 2
    own = [
        (
            zcopy(4 * r, up, tp, r * PART, PART),
            zcopy(4 * r + 1, down, tp, r * PART, PART),
        )
        for r in range(PARTS)
    ]
    fwd = [
        (
            zcopy(4 * r + 2, down, up, r * PART, half),
            zcopy(4 * r + 3, up, down, r * PART + half, half),
        )
        for r in range(PARTS)
    ]
    for copy in (*own[0], *own[1]):
        copy.start()

    def relay_z(r):
        for copy in own[r]:
            copy.wait_recv()
        for copy in fwd[r]:
            copy.start()
        if r + 2 < PARTS:
            for copy in own[r + 2]:
                copy.start()

    lanes = lax.broadcasted_iota(jnp.int32, (BLOCK, HEAD), 1)
    sublanes = lax.broadcasted_iota(jnp.int32, (BLOCK, HEAD), 0)
    inverse = inverse_ref[...]
    for r in range(2):
        tokens = me * ROWS + r * BLOCK + sublanes
        angle = (tokens - starts_of(tokens, bounds_ref)).astype(jnp.float32) * inverse
        turn = jnp.sin(angle)
        cosine[pl.ds(r * BLOCK, BLOCK), :] = jnp.cos(angle)
        sine[pl.ds(r * BLOCK, BLOCK), :] = jnp.where(lanes < HEAD // 2, -turn, turn)

    place = jnp.minimum(jnp.maximum(sublanes - me * PORTION, 0), PORTION)

    def mark(b, carry):
        tokens = b * BLOCK + sublanes
        document = jnp.zeros_like(tokens)
        for i in range(1, 8):
            document = jnp.where(tokens >= bounds_ref[i], i, document)
        spot = 8 + lax.rem(b, SPAN) * (PORTION + 1) + place
        hit = (lanes == document) | (lanes == spot)
        mark_ref[pl.ds(pl.multiple_of(b * BLOCK, BLOCK), BLOCK), :] = (
            hit.astype(jnp.float32).astype(jnp.bfloat16)
        )
        return carry

    lax.fori_loop(0, NBLK // 2, mark, 0)
    weights[0].wait()
    weights[1].wait()
    weights[2].wait()

    def rotate(raw, row, count):
        table = pl.ds(row, count)
        return raw * cosine[table, :] + pltpu.roll(raw, HEAD // 2, 1) * sine[table, :]

    def queries(r, n):
        columns = slice(n * 2 * HEAD, (n + 1) * 2 * HEAD)
        rows = pl.ds(r * BLOCK, BLOCK)
        raw = jnp.dot(full[rows, :], wq[:, columns], preferred_element_type=jnp.float32)
        turned = jnp.concatenate(
            [rotate(raw[:, :HEAD], r * BLOCK, BLOCK), rotate(raw[:, HEAD:], r * BLOCK, BLOCK)],
            axis=1,
        )
        qtmp[pl.ds((n // 2) * BLOCK, BLOCK), (n % 2) * 2 * HEAD : (n % 2 + 1) * 2 * HEAD] = (
            turned.astype(jnp.bfloat16)
        )

    def gather(which, r):
        buffer = (k_ref, v_ref)[which]
        a, b = ((xcoord, ycoord), (ycoord, xcoord))[which]
        base = (which * PARTS + r) * 12

        def neighbour(along, step):
            if along == 0:
                na, nb = lax.rem(a + step, 4), b
            else:
                na, nb = a, lax.rem(b + step, 4)
            x, y = ((na, nb), (nb, na))[which]
            return (x * 4 + y) * 2 + core

        def copy(n, ref, target):
            return pltpu.make_async_remote_copy(
                src_ref=ref,
                dst_ref=ref,
                send_sem=g_send.at[base + n],
                recv_sem=g_recv.at[base + n],
                device_id={"cp": target},
                device_id_type=MESH,
            )

        def piece(at, row, count):
            rows = pl.ds(row, count)
            if which == 0:
                return buffer.at[at, b, core, r, rows]
            return buffer.at[b, at, core, r, rows]

        def line(at, first, count):
            along = pl.ds(first, count)
            if which == 0:
                return buffer.at[along, at, core, r]
            return buffer.at[at, along, core, r]

        a_next, a_prev = lax.rem(a + 1, 4), lax.rem(a + 3, 4)
        b_next, b_prev = lax.rem(b + 1, 4), lax.rem(b + 3, 4)
        b_far = lax.rem(b + 2, 4)
        return dict(
            ring1=(
                copy(0, piece(a, 0, PART), neighbour(0, 1)),
                copy(1, piece(a, 0, PART), neighbour(0, 3)),
            ),
            ring1_far=(
                copy(2, piece(a_prev, 0, half), neighbour(0, 1)),
                copy(3, piece(a_next, half, half), neighbour(0, 3)),
            ),
            ring2=(
                copy(4, line(b, 0, 4), neighbour(1, 1)),
                copy(5, line(b, 0, 4), neighbour(1, 3)),
            ),
            ring2_far=(
                copy(6, line(b_prev, 0, 2), neighbour(1, 1)),
                copy(7, line(b_next, 2, 2), neighbour(1, 3)),
            ),
            across=(
                copy(8, line(b, 0, 4), partner),
                copy(9, line(b_prev, 0, 4), partner),
                copy(10, line(b_next, 0, 4), partner),
                copy(11, line(b_far, 0, 4), partner),
            ),
        )

    flows = [[gather(which, r) for which in range(2)] for r in range(PARTS)]

    def start(r, name):
        for flow in flows[r]:
            for copy in flow[name]:
                copy.start()

    def arrived(r, name):
        for flow in flows[r]:
            for copy in flow[name]:
                copy.wait_recv()

    def across(r, which):
        for flow in flows[r]:
            for n in which:
                flow["across"][n].start()

    def s0(r):
        for copy in fwd[r]:
            copy.wait_recv()
        raw = jnp.dot(
            full[pl.ds(r * PART, PART), :], wkv[...], preferred_element_type=jnp.float32
        )
        k_ref[xcoord, ycoord, core, r] = rotate(raw[:, :HEAD], r * PART, PART).astype(
            jnp.bfloat16
        )
        v_ref[xcoord, ycoord, core, r] = raw[:, HEAD:].astype(jnp.bfloat16)
        start(r, "ring1")

    def s1(r):
        arrived(r, "ring1")
        start(r, "ring1_far")

    def s2(r):
        arrived(r, "ring1_far")
        start(r, "ring2")
        across(r, (0,))

    def s3(r):
        arrived(r, "ring2")
        start(r, "ring2_far")
        across(r, (1, 2))

    def s4(r):
        arrived(r, "ring2_far")
        across(r, (3,))

    out_row = lax.broadcasted_iota(jnp.int32, (ROWS, ROWS), 0)
    in_row = lax.broadcasted_iota(jnp.int32, (ROWS, ROWS), 1)
    origin = lax.rem(out_row // 4, 2) * BLOCK + (out_row // 8) * 4 + lax.rem(out_row, 4)
    pick = (in_row == origin).astype(jnp.float32).astype(jnp.bfloat16)

    def qcopy(r, k, target, slot):
        return pltpu.make_async_remote_copy(
            src_ref=qsend.at[r, target],
            dst_ref=q_ref.at[slot, r],
            send_sem=q_send.at[r, k],
            recv_sem=q_recv.at[r, k],
            device_id={"cp": target},
            device_id_type=MESH,
        )

    def spread(r):
        ordered = jnp.dot(pick, qtmp[...], preferred_element_type=jnp.float32)
        qsend[r] = ordered.reshape(CP, 8, WIDTH // 2).astype(jnp.bfloat16)
        q_ref[me, r] = qsend[r, me]

        def send(k, carry):
            qcopy(r, k, lax.rem(me + k, CP), me).start()
            return carry

        lax.fori_loop(1, CP, send, 0)

    def spread_done(r):
        def wait(k, carry):
            copy = qcopy(r, k, lax.rem(me + k, CP), lax.rem(me + CP - k, CP))
            copy.wait_send()
            copy.wait_recv()
            return carry

        lax.fori_loop(1, CP, wait, 0)

    relay_z(0)
    lax.fori_loop(NBLK // 2, NBLK, mark, 0)
    relay_z(1)
    s0(0)
    s1(0)
    relay_z(2)
    s2(0)
    s0(1)
    queries(0, 0)
    queries(0, 1)
    s1(1)
    relay_z(3)
    s3(0)
    queries(0, 2)
    s2(1)
    s0(2)
    queries(0, 3)
    spread(0)
    s4(0)
    s0(3)
    s1(2)
    s3(1)
    queries(1, 0)
    s1(3)
    s2(2)
    queries(1, 1)
    s4(1)
    queries(1, 2)
    s2(3)
    queries(1, 3)
    spread(1)
    s3(2)
    s3(3)
    s4(2)
    s4(3)
    spread_done(0)
    spread_done(1)
    for r in range(PARTS):
        arrived(r, "across")
        for flow in flows[r]:
            for name in ("ring1", "ring1_far", "ring2", "ring2_far", "across"):
                for copy in flow[name]:
                    copy.wait_send()
    for group in (*own, *fwd):
        for copy in group:
            copy.wait_send()


def gather_call(bounds, hidden, wq, wk, wv, inverse):
    vmem = pl.BlockSpec(memory_space=pltpu.VMEM)
    hbm = pl.BlockSpec(memory_space=pltpu.HBM)
    kv = jax.ShapeDtypeStruct((4, 4, 2, PARTS, PART, HEAD), jnp.bfloat16)
    dma = pltpu.SemaphoreType.DMA
    return pl.pallas_call(
        gather_kernel,
        out_shape=(
            kv,
            kv,
            jax.ShapeDtypeStruct((CP, 2, 8, WIDTH // 2), jnp.bfloat16),
            jax.ShapeDtypeStruct((TOKENS, HEAD), jnp.bfloat16),
        ),
        in_specs=[pl.BlockSpec(memory_space=pltpu.SMEM), hbm, hbm, hbm, hbm, vmem],
        out_specs=(vmem, vmem, vmem, vmem),
        scratch_shapes=[
            pltpu.VMEM((ROWS, TP * WIDTH), jnp.bfloat16),
            pltpu.VMEM((TP * WIDTH, WIDTH), jnp.bfloat16),
            pltpu.VMEM((TP * WIDTH, 2 * HEAD), jnp.bfloat16),
            pltpu.VMEM((ROWS, WIDTH // 2), jnp.bfloat16),
            pltpu.VMEM((2, CP, 8, WIDTH // 2), jnp.bfloat16),
            pltpu.VMEM((ROWS, HEAD), jnp.float32),
            pltpu.VMEM((ROWS, HEAD), jnp.float32),
            dma((4,)), dma((4 * PARTS,)), dma((4 * PARTS,)),
            dma((24 * PARTS,)), dma((24 * PARTS,)), dma((2, CP)), dma((2, CP)),
        ],
        compiler_params=pltpu.CompilerParams(
            collective_id=0, has_side_effects=True, vmem_limit_bytes=32 * 1024 * 1024
        ),
        name="gather_project",
    )(bounds, hidden, wq, wk, wv, inverse)


TILE = SPAN * BLOCK


def attend_kernel(bounds_ref, q_ref, k_ref, v_ref, mark_ref, o_ref):
    rows = SPAN * 8
    count = 4 * rows
    factor = math.log2(math.e) / math.sqrt(HEAD)
    row = lax.rem(lax.broadcasted_iota(jnp.int32, (count, HEAD), 0), rows)
    lane = lax.broadcasted_iota(jnp.int32, (count, HEAD), 1)
    block, step = row // 8, lax.rem(row, PORTION)
    key_block, key_step = (lane - 8) // (PORTION + 1), lax.rem(lane - 8, PORTION + 1)
    later = (key_block > block) | ((key_block == block) & (key_step > step))
    later = later & (lane >= 8) & (lane < 8 + SPAN * (PORTION + 1))
    me = lax.axis_index("cp")
    ones = jnp.ones((TILE, HEAD), jnp.bfloat16)

    def group(g, carry):
        first = pl.multiple_of(g * rows, rows)
        tokens = (g * SPAN + block) * BLOCK + me * PORTION + step
        document = jnp.zeros_like(tokens)
        low = jnp.int32(0)
        for i in range(1, 8):
            document = jnp.where(tokens >= bounds_ref[i], i, document)
            low = jnp.where(g * TILE >= bounds_ref[i], bounds_ref[i], low)
        other = (lane < 8) & (lane != document)
        q = jnp.concatenate(
            [q_ref[pl.ds(first, rows), h * HEAD : (h + 1) * HEAD] for h in range(4)], axis=0
        )
        inner = jnp.where(other, PENALTY, 0.0).astype(jnp.bfloat16)
        outer = jnp.where(other | later, PENALTY, 0.0).astype(jnp.bfloat16)

        def scores_of(j, penalties):
            at = pl.ds(pl.multiple_of(j * TILE, TILE), TILE)
            return lax.dot_general(
                jnp.concatenate([q, penalties], axis=1),
                jnp.concatenate([k_ref[at, :], mark_ref[at, :]], axis=1),
                (((1,), (1,)), ((), ())),
                preferred_element_type=jnp.float32,
            ) * factor

        def mix(j, scores, top):
            at = pl.ds(pl.multiple_of(j * TILE, TILE), TILE)
            weights = jnp.exp2(scores - top).astype(jnp.bfloat16)
            return jnp.dot(
                weights,
                jnp.concatenate([v_ref[at, :], ones], axis=1),
                preferred_element_type=jnp.float32,
            )

        scores = scores_of(g, outer)
        top = jnp.max(scores, axis=1, keepdims=True)
        mixed = mix(g, scores, top)

        def tile(n, state):
            top, mixed = state
            j = g - 1 - n
            scores = scores_of(j, inner)
            new_top = jnp.maximum(top, jnp.max(scores, axis=1, keepdims=True))
            return new_top, mixed * jnp.exp2(top - new_top) + mix(j, scores, new_top)

        top, mixed = lax.fori_loop(0, g - low // TILE, tile, (top, mixed))
        out = (mixed[:, :HEAD] / mixed[:, HEAD:]).astype(jnp.bfloat16)
        for h in range(4):
            o_ref[pl.ds(first, rows), h * HEAD : (h + 1) * HEAD] = out[h * rows : (h + 1) * rows]
        return carry

    lax.fori_loop(0, NBLK // SPAN, group, 0)


def attend_call(bounds, q, k, v, marks):
    vmem = pl.BlockSpec(memory_space=pltpu.VMEM)
    return pl.pallas_call(
        attend_kernel,
        out_shape=jax.ShapeDtypeStruct((2 * ROWS, WIDTH // 2), jnp.bfloat16),
        in_specs=[pl.BlockSpec(memory_space=pltpu.SMEM), vmem, vmem, vmem, vmem],
        out_specs=vmem,
        compiler_params=pltpu.CompilerParams(vmem_limit_bytes=20 * 1024 * 1024),
        name="attend",
    )(bounds, q, k, v, marks)


CHUNKS = 4
CW = WIDTH // CHUNKS


def output_kernel(
    slot_ref, heads_ref, wo_ref, out_ref,
    heads, wo, far, near, far_in, near_in, spread, landed, own_sum,
    w_sem, z_send, z_recv, a_send, a_recv,
):
    me = lax.axis_index("cp")
    tp = lax.axis_index("tp")
    up, down, across = lax.rem(tp + 1, TP), lax.rem(tp + 3, TP), lax.rem(tp + 2, TP)

    loads = []
    for n, t in enumerate((across, up, down, tp)):
        columns = pl.ds(pl.multiple_of(t * WIDTH, WIDTH), WIDTH)
        loads.append(pltpu.make_async_copy(wo_ref.at[:, columns], wo.at[n], w_sem.at[n]))
        loads[-1].start()

    barrier = pltpu.get_barrier_semaphore()

    def greet(k, carry):
        pl.semaphore_signal(
            barrier, inc=1, device_id={"cp": lax.rem(me + k, CP)}, device_id_type=MESH
        )
        return carry

    pl.semaphore_signal(barrier, inc=1, device_id={"tp": up}, device_id_type=MESH)
    pl.semaphore_signal(barrier, inc=1, device_id={"tp": down}, device_id_type=MESH)
    lax.fori_loop(1, CP, greet, 0)

    wide_row = lax.broadcasted_iota(jnp.int32, (ROWS, 2 * ROWS), 0)
    wide_column = lax.broadcasted_iota(jnp.int32, (ROWS, 2 * ROWS), 1)
    for h in range(2):
        source = (wide_row // PORTION) * 8 + h * PORTION + lax.rem(wide_row, PORTION)
        select = (wide_column == source).astype(jnp.float32).astype(jnp.bfloat16)
        heads[:, h * (WIDTH // 2) : (h + 1) * (WIDTH // 2)] = jnp.dot(
            select, heads_ref[...], preferred_element_type=jnp.float32
        ).astype(jnp.bfloat16)

    def product(n, c):
        return jnp.dot(
            heads[...], wo[n, :, c * CW : (c + 1) * CW], preferred_element_type=jnp.float32
        )

    def remote(n, src, dst, target):
        return pltpu.make_async_remote_copy(
            src_ref=src,
            dst_ref=dst,
            send_sem=z_send.at[n],
            recv_sem=z_recv.at[n],
            device_id={"tp": target},
            device_id_type=MESH,
        )

    half = ROWS // 2
    far_copies, near_copies = [], []
    for c in range(CHUNKS):
        far_copies.append(
            (
                remote(4 * c, far.at[c, pl.ds(0, half)], far_in.at[c, 0], up),
                remote(4 * c + 1, far.at[c, pl.ds(half, half)], far_in.at[c, 1], down),
            )
        )
        near_copies.append(
            (
                remote(4 * c + 2, near.at[c, 0], near_in.at[c, 0], up),
                remote(4 * c + 3, near.at[c, 1], near_in.at[c, 1], down),
            )
        )

    def send_far(c):
        far[c] = product(0, c).astype(jnp.bfloat16)
        for copy in far_copies[c]:
            copy.start()

    def send_near(c):
        to_up, to_down = product(1, c), product(2, c)
        far_copies[c][0].wait_recv()
        near[c, 0, :half] = (to_up[:half] + far_in[c, 0].astype(jnp.float32)).astype(jnp.bfloat16)
        near[c, 0, half:] = to_up[half:].astype(jnp.bfloat16)
        near_copies[c][0].start()
        far_copies[c][1].wait_recv()
        near[c, 1, :half] = to_down[:half].astype(jnp.bfloat16)
        near[c, 1, half:] = (to_down[half:] + far_in[c, 1].astype(jnp.float32)).astype(
            jnp.bfloat16
        )
        near_copies[c][1].start()

    row = lax.broadcasted_iota(jnp.int32, (ROWS, ROWS), 0)
    column = lax.broadcasted_iota(jnp.int32, (ROWS, ROWS), 1)
    to_owner = (row == slot_ref[...]).astype(jnp.float32).astype(jnp.bfloat16)
    origin = (lax.rem(row, BLOCK) // 4) * 8 + (row // BLOCK) * 4 + lax.rem(row, 4)
    to_place = (column == origin).astype(jnp.float32).astype(jnp.bfloat16)

    def acopy(c, k, target, slot):
        return pltpu.make_async_remote_copy(
            src_ref=spread.at[c, target],
            dst_ref=landed.at[c, slot],
            send_sem=a_send.at[c, k],
            recv_sem=a_recv.at[c, k],
            device_id={"cp": target},
            device_id_type=MESH,
        )

    def finish_sum(c):
        for copy in near_copies[c]:
            copy.wait_recv()
        total = (
            own_sum[c]
            + near_in[c, 0].astype(jnp.float32)
            + near_in[c, 1].astype(jnp.float32)
        ).astype(jnp.bfloat16)
        picked = jnp.dot(to_owner, total, preferred_element_type=jnp.float32)
        spread[c] = picked.reshape(CP, 8, CW).astype(jnp.bfloat16)
        landed[c, me] = spread[c, me]

        def send(k, carry):
            acopy(c, k, lax.rem(me + k, CP), me).start()
            return carry

        lax.fori_loop(1, CP, send, 0)

    def place(c):
        def wait(k, carry):
            copy = acopy(c, k, lax.rem(me + k, CP), lax.rem(me + CP - k, CP))
            copy.wait_send()
            copy.wait_recv()
            return carry

        lax.fori_loop(1, CP, wait, 0)
        rows = landed[c].astype(jnp.float32).reshape(ROWS, CW).astype(jnp.bfloat16)
        out_ref[:, c * CW : (c + 1) * CW] = jnp.dot(
            to_place, rows, preferred_element_type=jnp.float32
        ).astype(jnp.bfloat16)

    loads[0].wait()
    far[0] = product(0, 0).astype(jnp.bfloat16)
    pl.semaphore_wait(barrier, CP + 1)
    for copy in far_copies[0]:
        copy.start()
    send_far(1)
    loads[1].wait()
    loads[2].wait()
    send_near(0)
    send_far(2)
    send_near(1)
    send_far(3)
    loads[3].wait()
    own_sum[0] = product(3, 0)
    send_near(2)
    own_sum[1] = product(3, 1)
    send_near(3)
    own_sum[2] = product(3, 2)
    own_sum[3] = product(3, 3)
    for c in range(CHUNKS):
        finish_sum(c)
        if c > 0:
            place(c - 1)
    place(CHUNKS - 1)
    for c in range(CHUNKS):
        for copy in (*far_copies[c], *near_copies[c]):
            copy.wait_send()


def output_call(slot_rows, heads, wo):
    vmem = pl.BlockSpec(memory_space=pltpu.VMEM)
    dma = pltpu.SemaphoreType.DMA
    half = ROWS // 2
    bf16 = jnp.bfloat16
    return pl.pallas_call(
        output_kernel,
        out_shape=jax.ShapeDtypeStruct((ROWS, WIDTH), bf16),
        in_specs=[vmem, vmem, pl.BlockSpec(memory_space=pltpu.HBM)],
        out_specs=vmem,
        scratch_shapes=[
            pltpu.VMEM((ROWS, WIDTH), bf16),
            pltpu.VMEM((TP, WIDTH, WIDTH), bf16),
            pltpu.VMEM((CHUNKS, ROWS, CW), bf16),
            pltpu.VMEM((CHUNKS, 2, ROWS, CW), bf16),
            pltpu.VMEM((CHUNKS, 2, half, CW), bf16),
            pltpu.VMEM((CHUNKS, 2, ROWS, CW), bf16),
            pltpu.VMEM((CHUNKS, CP, 8, CW), bf16),
            pltpu.VMEM((CHUNKS, CP, 8, CW), bf16),
            pltpu.VMEM((CHUNKS, ROWS, CW), jnp.float32),
            dma((4,)), dma((4 * CHUNKS,)), dma((4 * CHUNKS,)), dma((CHUNKS, CP)), dma((CHUNKS, CP)),
        ],
        compiler_params=pltpu.CompilerParams(
            collective_id=1, has_side_effects=True, vmem_limit_bytes=40 * 1024 * 1024
        ),
        name="project_out",
    )(slot_rows, heads, wo)


def local(hidden, query_weight, key_matrix, value_matrix, output_weight, bounds, block_owner):
    inverse = rope_inverse(HEAD)
    inverse = jnp.concatenate([inverse, inverse])[None, :]
    slots = slots_of(block_owner)
    slot_rows = (slots[:, None] * PORTION + jnp.arange(PORTION, dtype=jnp.int32)[None, :]).reshape(
        1, ROWS
    )
    hidden, query_weight, key_matrix, value_matrix, output_weight = (
        pltpu.with_memory_space_constraint(a, pltpu.HBM)
        for a in (hidden, query_weight, key_matrix, value_matrix, output_weight)
    )
    keys, values, queries, marks = gather_call(
        bounds, hidden, query_weight, key_matrix, value_matrix, inverse
    )
    heads = attend_call(
        bounds,
        queries.reshape(2 * ROWS, WIDTH // 2),
        keys.reshape(TOKENS, HEAD),
        values.reshape(TOKENS, HEAD),
        marks,
    )
    return output_call(slot_rows, heads, output_weight)


def solution(mesh):
    placed = (P("cp", "tp"), P(None, "tp"), P(None, "tp"), P(None, "tp"), P("tp", None), P(), P())
    return jax.shard_map(
        local, mesh=mesh, in_specs=placed, out_specs=P("cp", "tp"), check_vma=False
    )
```

```python
import functools
import math

import jax
import jax.numpy as jnp
from jax import lax
from jax.experimental import pallas as pl
from jax.experimental.pallas import tpu as pltpu
from jax.sharding import PartitionSpec as P

HEAD = 128
BLOCK = 128
CP = 32
TP = 4
ROWS = 256
WIDTH = 1024
NBLK = 64
HEADS = 8
TOKENS = 8192
PORTION = BLOCK // CP

rope_theta = 500000.0
rope_factor = 8.0
rope_context = 8192.0
masked_score = -1e30
MESH = pl.DeviceIdType.MESH


def rope_inverse(head_size):
    halves = jnp.arange(head_size // 2, dtype=jnp.float32)
    inverse = 1.0 / rope_theta ** (2.0 * halves / head_size)
    wavelength = 2.0 * math.pi / inverse
    smooth = (rope_context / wavelength - 1.0) / 3.0
    blended = (1.0 - smooth) * inverse / rope_factor + smooth * inverse
    longer = jnp.where(wavelength > rope_context, inverse / rope_factor, blended)
    return jnp.where(wavelength < rope_context / 4.0, inverse, longer)


def slots_of(block_owner):
    blocks = jnp.arange(NBLK, dtype=jnp.int32)
    same = block_owner[:, None] == block_owner[None, :]
    earlier = blocks[None, :] < blocks[:, None]
    rank = jnp.sum((same & earlier).astype(jnp.int32), axis=1)
    return block_owner * 2 + rank


def starts_of(tokens, bounds_ref):
    start = jnp.zeros_like(tokens)
    for i in range(1, 8):
        bound = bounds_ref[i]
        start = jnp.where(tokens >= bound, bound, start)
    return start


PARTS = 4
PART = ROWS // PARTS
RELAYED = 2
SPAN = 8
PENALTY = -1e30


def gather_kernel(
    bounds_ref, hidden_ref, wq_ref, wk_ref, wv_ref, inverse_ref,
    k_ref, v_ref, q_ref, mark_ref,
    full, wq, wkv, qtmp, qsend, cosine, sine,
    w_sem, z_send, z_recv, g_send, g_recv, q_send, q_recv,
):
    me = lax.axis_index("cp")
    tp = lax.axis_index("tp")
    core = lax.rem(me, 2)
    ycoord = lax.rem(me // 2, 4)
    xcoord = me // 8
    partner = me + 1 - 2 * core
    up, down = lax.rem(tp + 1, TP), lax.rem(tp + 3, TP)
    own_columns = pl.ds(pl.multiple_of(tp * WIDTH, WIDTH), WIDTH)

    bring = pltpu.make_async_copy(hidden_ref, full.at[:, own_columns], w_sem.at[3])
    weights = [
        pltpu.make_async_copy(wk_ref, wkv.at[:, pl.ds(0, HEAD)], w_sem.at[0]),
        pltpu.make_async_copy(wv_ref, wkv.at[:, pl.ds(HEAD, HEAD)], w_sem.at[1]),
        pltpu.make_async_copy(wq_ref, wq, w_sem.at[2]),
    ]
    bring.start()
    for copy in weights:
        copy.start()

    barrier = pltpu.get_barrier_semaphore()

    def greet(k, carry):
        pl.semaphore_signal(
            barrier, inc=1, device_id={"cp": lax.rem(me + k, CP)}, device_id_type=MESH
        )
        return carry

    pl.semaphore_signal(barrier, inc=1, device_id={"tp": up}, device_id_type=MESH)
    pl.semaphore_signal(barrier, inc=1, device_id={"tp": down}, device_id_type=MESH)
    lax.fori_loop(1, CP, greet, 0)
    bring.wait()
    pl.semaphore_wait(barrier, CP + 1)

    def zcopy(n, target, owner, row, count):
        columns = pl.ds(pl.multiple_of(owner * WIDTH, WIDTH), WIDTH)
        ref = full.at[pl.ds(row, count), columns]
        return pltpu.make_async_remote_copy(
            src_ref=ref,
            dst_ref=ref,
            send_sem=z_send.at[n],
            recv_sem=z_recv.at[n],
            device_id={"tp": target},
            device_id_type=MESH,
        )

    half = PART // 2
    own = [
        (
            zcopy(4 * r, up, tp, r * PART, PART),
            zcopy(4 * r + 1, down, tp, r * PART, PART),
        )
        for r in range(PARTS)
    ]
    fwd = [
        (
            zcopy(4 * r + 2, down, up, r * PART, half),
            zcopy(4 * r + 3, up, down, r * PART + half, half),
        )
        for r in range(PARTS)
    ]
    for copy in (*own[0], *own[1]):
        copy.start()

    def relay_z(r):
        for copy in own[r]:
            copy.wait_recv()
        for copy in fwd[r]:
            copy.start()
        if r + 2 < PARTS:
            for copy in own[r + 2]:
                copy.start()

    lanes = lax.broadcasted_iota(jnp.int32, (BLOCK, HEAD), 1)
    sublanes = lax.broadcasted_iota(jnp.int32, (BLOCK, HEAD), 0)
    inverse = inverse_ref[...]
    for r in range(2):
        tokens = me * ROWS + r * BLOCK + sublanes
        angle = (tokens - starts_of(tokens, bounds_ref)).astype(jnp.float32) * inverse
        turn = jnp.sin(angle)
        cosine[pl.ds(r * BLOCK, BLOCK), :] = jnp.cos(angle)
        sine[pl.ds(r * BLOCK, BLOCK), :] = jnp.where(lanes < HEAD // 2, -turn, turn)

    place = jnp.minimum(jnp.maximum(sublanes - me * PORTION, 0), PORTION)

    def mark(b, carry):
        tokens = b * BLOCK + sublanes
        document = jnp.zeros_like(tokens)
        for i in range(1, 8):
            document = jnp.where(tokens >= bounds_ref[i], i, document)
        spot = 8 + lax.rem(b, SPAN) * (PORTION + 1) + place
        hit = (lanes == document) | (lanes == spot)
        mark_ref[pl.ds(pl.multiple_of(b * BLOCK, BLOCK), BLOCK), :] = (
            hit.astype(jnp.float32).astype(jnp.bfloat16)
        )
        return carry

    lax.fori_loop(0, NBLK // 2, mark, 0)
    weights[0].wait()
    weights[1].wait()
    weights[2].wait()

    def rotate(raw, row, count):
        table = pl.ds(row, count)
        return raw * cosine[table, :] + pltpu.roll(raw, HEAD // 2, 1) * sine[table, :]

    def queries(r, n):
        columns = slice(n * 2 * HEAD, (n + 1) * 2 * HEAD)
        rows = pl.ds(r * BLOCK, BLOCK)
        raw = jnp.dot(full[rows, :], wq[:, columns], preferred_element_type=jnp.float32)
        turned = jnp.concatenate(
            [rotate(raw[:, :HEAD], r * BLOCK, BLOCK), rotate(raw[:, HEAD:], r * BLOCK, BLOCK)],
            axis=1,
        )
        qtmp[pl.ds((n // 2) * BLOCK, BLOCK), (n % 2) * 2 * HEAD : (n % 2 + 1) * 2 * HEAD] = (
            turned.astype(jnp.bfloat16)
        )

    def gather(which, r):
        buffer = (k_ref, v_ref)[which]
        a, b = ((xcoord, ycoord), (ycoord, xcoord))[which]
        base = (which * PARTS + r) * 12

        def neighbour(along, step):
            if along == 0:
                na, nb = lax.rem(a + step, 4), b
            else:
                na, nb = a, lax.rem(b + step, 4)
            x, y = ((na, nb), (nb, na))[which]
            return (x * 4 + y) * 2 + core

        def copy(n, ref, target):
            return pltpu.make_async_remote_copy(
                src_ref=ref,
                dst_ref=ref,
                send_sem=g_send.at[base + n],
                recv_sem=g_recv.at[base + n],
                device_id={"cp": target},
                device_id_type=MESH,
            )

        def piece(at, row, count):
            rows = pl.ds(row, count)
            if which == 0:
                return buffer.at[at, b, core, r, rows]
            return buffer.at[b, at, core, r, rows]

        def line(at, first, count):
            along = pl.ds(first, count)
            if which == 0:
                return buffer.at[along, at, core, r]
            return buffer.at[at, along, core, r]

        a_next, a_prev = lax.rem(a + 1, 4), lax.rem(a + 3, 4)
        b_next, b_prev = lax.rem(b + 1, 4), lax.rem(b + 3, 4)
        b_far = lax.rem(b + 2, 4)
        direct = r >= RELAYED
        return dict(
            ring1=(
                copy(0, piece(a, 0, PART), neighbour(0, 1)),
                copy(1, piece(a, 0, PART), neighbour(0, 3)),
            ),
            ring1_far=(copy(2, piece(a, 0, PART), neighbour(0, 2)),)
            if direct
            else (
                copy(2, piece(a_prev, 0, half), neighbour(0, 1)),
                copy(3, piece(a_next, half, half), neighbour(0, 3)),
            ),
            ring2=(
                copy(4, line(b, 0, 4), neighbour(1, 1)),
                copy(5, line(b, 0, 4), neighbour(1, 3)),
            ),
            ring2_far=(copy(6, line(b, 0, 4), neighbour(1, 2)),)
            if direct
            else (
                copy(6, line(b_prev, 0, 2), neighbour(1, 1)),
                copy(7, line(b_next, 2, 2), neighbour(1, 3)),
            ),
            across=(
                copy(8, line(b, 0, 4), partner),
                copy(9, line(b_prev, 0, 4), partner),
                copy(10, line(b_next, 0, 4), partner),
                copy(11, line(b_far, 0, 4), partner),
            ),
        )

    flows = [[gather(which, r) for which in range(2)] for r in range(PARTS)]

    def start(r, name):
        for flow in flows[r]:
            for copy in flow[name]:
                copy.start()

    def arrived(r, name):
        for flow in flows[r]:
            for copy in flow[name]:
                copy.wait_recv()

    def across(r, which):
        for flow in flows[r]:
            for n in which:
                flow["across"][n].start()

    def s0(r):
        for copy in fwd[r]:
            copy.wait_recv()
        raw = jnp.dot(
            full[pl.ds(r * PART, PART), :], wkv[...], preferred_element_type=jnp.float32
        )
        k_ref[xcoord, ycoord, core, r] = rotate(raw[:, :HEAD], r * PART, PART).astype(
            jnp.bfloat16
        )
        v_ref[xcoord, ycoord, core, r] = raw[:, HEAD:].astype(jnp.bfloat16)
        start(r, "ring1")
        if r >= RELAYED:
            start(r, "ring1_far")

    def s1(r):
        arrived(r, "ring1")
        if r < RELAYED:
            start(r, "ring1_far")

    def s2(r):
        arrived(r, "ring1_far")
        start(r, "ring2")
        if r >= RELAYED:
            start(r, "ring2_far")
        across(r, (0,))

    def s3(r):
        arrived(r, "ring2")
        if r < RELAYED:
            start(r, "ring2_far")
        across(r, (1, 2))

    def s4(r):
        arrived(r, "ring2_far")
        across(r, (3,))

    out_row = lax.broadcasted_iota(jnp.int32, (ROWS, ROWS), 0)
    in_row = lax.broadcasted_iota(jnp.int32, (ROWS, ROWS), 1)
    origin = lax.rem(out_row // 4, 2) * BLOCK + (out_row // 8) * 4 + lax.rem(out_row, 4)
    pick = (in_row == origin).astype(jnp.float32).astype(jnp.bfloat16)

    def qcopy(r, k, target, slot):
        return pltpu.make_async_remote_copy(
            src_ref=qsend.at[r, target],
            dst_ref=q_ref.at[slot, r],
            send_sem=q_send.at[r, k],
            recv_sem=q_recv.at[r, k],
            device_id={"cp": target},
            device_id_type=MESH,
        )

    def spread(r):
        ordered = jnp.dot(pick, qtmp[...], preferred_element_type=jnp.float32)
        qsend[r] = ordered.reshape(CP, 8, WIDTH // 2).astype(jnp.bfloat16)
        q_ref[me, r] = qsend[r, me]

        def send(k, carry):
            qcopy(r, k, lax.rem(me + k, CP), me).start()
            return carry

        lax.fori_loop(1, CP, send, 0)

    def spread_done(r):
        def wait(k, carry):
            copy = qcopy(r, k, lax.rem(me + k, CP), lax.rem(me + CP - k, CP))
            copy.wait_send()
            copy.wait_recv()
            return carry

        lax.fori_loop(1, CP, wait, 0)

    relay_z(0)
    lax.fori_loop(NBLK // 2, NBLK, mark, 0)
    relay_z(1)
    s0(0)
    relay_z(2)
    s1(0)
    s0(1)
    queries(0, 0)
    queries(0, 1)
    s2(0)
    relay_z(3)
    s1(1)
    s0(2)
    queries(0, 2)
    s2(1)
    s3(0)
    queries(0, 3)
    s0(3)
    spread(0)
    s1(2)
    s2(2)
    s1(3)
    s2(3)
    s3(1)
    s4(0)
    queries(1, 0)
    queries(1, 1)
    s4(1)
    queries(1, 2)
    queries(1, 3)
    spread(1)
    s3(2)
    s4(2)
    s3(3)
    s4(3)
    spread_done(0)
    spread_done(1)
    for r in range(PARTS):
        arrived(r, "across")
        for flow in flows[r]:
            for name in ("ring1", "ring1_far", "ring2", "ring2_far", "across"):
                for copy in flow[name]:
                    copy.wait_send()
    for group in (*own, *fwd):
        for copy in group:
            copy.wait_send()


def gather_call(bounds, hidden, wq, wk, wv, inverse):
    vmem = pl.BlockSpec(memory_space=pltpu.VMEM)
    hbm = pl.BlockSpec(memory_space=pltpu.HBM)
    kv = jax.ShapeDtypeStruct((4, 4, 2, PARTS, PART, HEAD), jnp.bfloat16)
    dma = pltpu.SemaphoreType.DMA
    return pl.pallas_call(
        gather_kernel,
        out_shape=(
            kv,
            kv,
            jax.ShapeDtypeStruct((CP, 2, 8, WIDTH // 2), jnp.bfloat16),
            jax.ShapeDtypeStruct((TOKENS, HEAD), jnp.bfloat16),
        ),
        in_specs=[pl.BlockSpec(memory_space=pltpu.SMEM), hbm, hbm, hbm, hbm, vmem],
        out_specs=(vmem, vmem, vmem, vmem),
        scratch_shapes=[
            pltpu.VMEM((ROWS, TP * WIDTH), jnp.bfloat16),
            pltpu.VMEM((TP * WIDTH, WIDTH), jnp.bfloat16),
            pltpu.VMEM((TP * WIDTH, 2 * HEAD), jnp.bfloat16),
            pltpu.VMEM((ROWS, WIDTH // 2), jnp.bfloat16),
            pltpu.VMEM((2, CP, 8, WIDTH // 2), jnp.bfloat16),
            pltpu.VMEM((ROWS, HEAD), jnp.float32),
            pltpu.VMEM((ROWS, HEAD), jnp.float32),
            dma((4,)), dma((4 * PARTS,)), dma((4 * PARTS,)),
            dma((24 * PARTS,)), dma((24 * PARTS,)), dma((2, CP)), dma((2, CP)),
        ],
        compiler_params=pltpu.CompilerParams(
            collective_id=0, has_side_effects=True, vmem_limit_bytes=32 * 1024 * 1024
        ),
        name="gather_project",
    )(bounds, hidden, wq, wk, wv, inverse)


TILE = SPAN * BLOCK


GROUPS = NBLK // SPAN
QROWS = 4 * SPAN * 8


def attend_kernel(
    bounds_ref, q_ref, k_ref, v_ref, mark_ref, o_ref,
    turned, asked, even, odd, mixed_ref, total_ref,
):
    rows = SPAN * 8
    factor = math.log2(math.e) / math.sqrt(HEAD)
    row = lax.rem(lax.broadcasted_iota(jnp.int32, (rows, HEAD), 0), rows)
    lane = lax.broadcasted_iota(jnp.int32, (rows, HEAD), 1)
    block, step = row // 8, lax.rem(row, PORTION)
    key_block, key_step = (lane - 8) // (PORTION + 1), lax.rem(lane - 8, PORTION + 1)
    later = (key_block > block) | ((key_block == block) & (key_step > step))
    later = later & (lane >= 8) & (lane < 8 + SPAN * (PORTION + 1))
    me = lax.axis_index("cp")
    contract_last = (((1,), (1,)), ((), ()))
    diagonal = lax.broadcasted_iota(jnp.int32, (HEAD, HEAD), 0) == lax.broadcasted_iota(
        jnp.int32, (HEAD, HEAD), 1
    )
    identity = diagonal.astype(jnp.float32).astype(jnp.bfloat16)

    def prepare(g, carry):
        at = pl.ds(pl.multiple_of(g * TILE, TILE), TILE)
        turned[:, at] = lax.dot_general(
            identity, v_ref[at, :], contract_last, preferred_element_type=jnp.float32
        ).astype(jnp.bfloat16)
        tokens = (g * SPAN + block) * BLOCK + me * PORTION + step
        document = jnp.zeros_like(tokens)
        for i in range(1, 8):
            document = jnp.where(tokens >= bounds_ref[i], i, document)
        other = (lane < 8) & (lane != document)
        inner = jnp.where(other, PENALTY, 0.0).astype(jnp.bfloat16)
        outer = jnp.where(other | later, PENALTY, 0.0).astype(jnp.bfloat16)
        first = pl.multiple_of(g * rows, rows)
        for h in range(4):
            part = q_ref[pl.ds(first, rows), h * HEAD : (h + 1) * HEAD]
            for n, penalties in enumerate((inner, outer)):
                asked[2 * g + n, h * rows : (h + 1) * rows, :HEAD] = part
                asked[2 * g + n, h * rows : (h + 1) * rows, HEAD:] = penalties
        return carry

    lax.fori_loop(0, GROUPS, prepare, 0)

    def lowest(g):
        low = jnp.int32(0)
        for i in range(1, 8):
            low = jnp.where(g * TILE >= bounds_ref[i], bounds_ref[i], low)
        return low // TILE

    def following(item):
        g, j = item
        more = j > lowest(g)
        return jnp.where(more, g, g + 1), jnp.where(more, j - 1, g + 1)

    def score(item, ref):
        g, j = item
        own = jnp.where(g == j, 1, 0)
        q = asked[2 * jnp.minimum(g, GROUPS - 1) + own]
        for part in range(2):
            size = TILE // 2
            first = jnp.minimum(j, GROUPS - 1) * TILE + part * size
            at = pl.ds(pl.multiple_of(first, size), size)
            ref[part * size : (part + 1) * size, :] = lax.dot_general(
                jnp.concatenate([k_ref[at, :], mark_ref[at, :]], axis=1),
                q,
                contract_last,
                preferred_element_type=jnp.float32,
            )

    def soften(item, ref, state):
        g, j = item
        top, total, mixed = state
        top = jnp.where(g == j, 0.5 * PENALTY, top)
        at = pl.ds(pl.multiple_of(jnp.minimum(j, GROUPS - 1) * TILE, TILE), TILE)
        new_top = jnp.maximum(top, jnp.max(ref[...], axis=0, keepdims=True))
        shrink = jnp.exp2((top - new_top) * factor)
        weights = jnp.exp2((ref[...] - new_top) * factor)
        total = total * shrink + jnp.sum(weights, axis=0, keepdims=True)
        mixed = mixed * shrink + jnp.dot(
            turned[:, at], weights.astype(jnp.bfloat16), preferred_element_type=jnp.float32
        )
        mixed_ref[g] = mixed
        total_ref[g] = total
        return new_top, total, mixed

    count = lax.fori_loop(0, GROUPS, lambda g, n: n + g + 1 - lowest(g), jnp.int32(0))
    zero = jnp.int32(0)
    score((zero, zero), even)

    def pair(n, carry):
        g, j, *state = carry
        item = (g, j)
        second = following(item)
        score(second, odd)
        state = soften(item, even, state)
        third = following(second)
        third = (jnp.minimum(third[0], GROUPS), jnp.minimum(third[1], GROUPS))
        score(third, even)
        state = soften(second, odd, state)
        return (*third, *state)

    lax.fori_loop(
        0,
        (count + 1) // 2,
        pair,
        (
            zero,
            zero,
            jnp.full((1, QROWS), 0.5 * PENALTY, jnp.float32),
            jnp.zeros((1, QROWS), jnp.float32),
            jnp.zeros((HEAD, QROWS), jnp.float32),
        ),
    )

    def finish(g, carry):
        out = (mixed_ref[g] / total_ref[g]).T.astype(jnp.bfloat16)
        first = pl.multiple_of(g * rows, rows)
        for h in range(4):
            o_ref[pl.ds(first, rows), h * HEAD : (h + 1) * HEAD] = out[h * rows : (h + 1) * rows]
        return carry

    lax.fori_loop(0, GROUPS, finish, 0)


def attend_call(bounds, q, k, v, marks):
    vmem = pl.BlockSpec(memory_space=pltpu.VMEM)
    return pl.pallas_call(
        attend_kernel,
        out_shape=jax.ShapeDtypeStruct((2 * ROWS, WIDTH // 2), jnp.bfloat16),
        in_specs=[pl.BlockSpec(memory_space=pltpu.SMEM), vmem, vmem, vmem, vmem],
        out_specs=vmem,
        scratch_shapes=[
            pltpu.VMEM((HEAD, TOKENS), jnp.bfloat16),
            pltpu.VMEM((2 * GROUPS, QROWS, 2 * HEAD), jnp.bfloat16),
            pltpu.VMEM((TILE, QROWS), jnp.float32),
            pltpu.VMEM((TILE, QROWS), jnp.float32),
            pltpu.VMEM((GROUPS + 1, HEAD, QROWS), jnp.float32),
            pltpu.VMEM((GROUPS + 1, 1, QROWS), jnp.float32),
        ],
        compiler_params=pltpu.CompilerParams(vmem_limit_bytes=28 * 1024 * 1024),
        name="attend",
    )(bounds, q, k, v, marks)


CHUNKS = 4
CW = WIDTH // CHUNKS


def output_kernel(
    slot_ref, heads_ref, wo_ref, out_ref,
    heads, wo, far, near, far_in, near_in, spread, landed, own_sum,
    w_sem, z_send, z_recv, a_send, a_recv,
):
    me = lax.axis_index("cp")
    tp = lax.axis_index("tp")
    up, down, across = lax.rem(tp + 1, TP), lax.rem(tp + 3, TP), lax.rem(tp + 2, TP)

    loads = []
    for n, t in enumerate((across, up, down, tp)):
        columns = pl.ds(pl.multiple_of(t * WIDTH, WIDTH), WIDTH)
        loads.append(pltpu.make_async_copy(wo_ref.at[:, columns], wo.at[n], w_sem.at[n]))
        loads[-1].start()

    barrier = pltpu.get_barrier_semaphore()

    def greet(k, carry):
        pl.semaphore_signal(
            barrier, inc=1, device_id={"cp": lax.rem(me + k, CP)}, device_id_type=MESH
        )
        return carry

    pl.semaphore_signal(barrier, inc=1, device_id={"tp": up}, device_id_type=MESH)
    pl.semaphore_signal(barrier, inc=1, device_id={"tp": down}, device_id_type=MESH)
    lax.fori_loop(1, CP, greet, 0)

    wide_row = lax.broadcasted_iota(jnp.int32, (ROWS, 2 * ROWS), 0)
    wide_column = lax.broadcasted_iota(jnp.int32, (ROWS, 2 * ROWS), 1)
    for h in range(2):
        source = (wide_row // PORTION) * 8 + h * PORTION + lax.rem(wide_row, PORTION)
        select = (wide_column == source).astype(jnp.float32).astype(jnp.bfloat16)
        heads[:, h * (WIDTH // 2) : (h + 1) * (WIDTH // 2)] = jnp.dot(
            select, heads_ref[...], preferred_element_type=jnp.float32
        ).astype(jnp.bfloat16)

    def product(n, c):
        return jnp.dot(
            heads[...], wo[n, :, c * CW : (c + 1) * CW], preferred_element_type=jnp.float32
        )

    def remote(n, src, dst, target):
        return pltpu.make_async_remote_copy(
            src_ref=src,
            dst_ref=dst,
            send_sem=z_send.at[n],
            recv_sem=z_recv.at[n],
            device_id={"tp": target},
            device_id_type=MESH,
        )

    half = ROWS // 2
    far_copies, near_copies = [], []
    for c in range(CHUNKS):
        far_copies.append(
            (
                remote(4 * c, far.at[c, pl.ds(0, half)], far_in.at[c, 0], up),
                remote(4 * c + 1, far.at[c, pl.ds(half, half)], far_in.at[c, 1], down),
            )
        )
        near_copies.append(
            (
                remote(4 * c + 2, near.at[c, 0], near_in.at[c, 0], up),
                remote(4 * c + 3, near.at[c, 1], near_in.at[c, 1], down),
            )
        )

    def send_far(c):
        far[c] = product(0, c).astype(jnp.bfloat16)
        for copy in far_copies[c]:
            copy.start()

    def send_near(c):
        to_up, to_down = product(1, c), product(2, c)
        far_copies[c][0].wait_recv()
        near[c, 0, :half] = (to_up[:half] + far_in[c, 0].astype(jnp.float32)).astype(jnp.bfloat16)
        near[c, 0, half:] = to_up[half:].astype(jnp.bfloat16)
        near_copies[c][0].start()
        far_copies[c][1].wait_recv()
        near[c, 1, :half] = to_down[:half].astype(jnp.bfloat16)
        near[c, 1, half:] = (to_down[half:] + far_in[c, 1].astype(jnp.float32)).astype(
            jnp.bfloat16
        )
        near_copies[c][1].start()

    row = lax.broadcasted_iota(jnp.int32, (ROWS, ROWS), 0)
    column = lax.broadcasted_iota(jnp.int32, (ROWS, ROWS), 1)
    to_owner = (row == slot_ref[...]).astype(jnp.float32).astype(jnp.bfloat16)
    origin = (lax.rem(row, BLOCK) // 4) * 8 + (row // BLOCK) * 4 + lax.rem(row, 4)
    to_place = (column == origin).astype(jnp.float32).astype(jnp.bfloat16)

    def acopy(c, k, target, slot):
        return pltpu.make_async_remote_copy(
            src_ref=spread.at[c, target],
            dst_ref=landed.at[c, slot],
            send_sem=a_send.at[c, k],
            recv_sem=a_recv.at[c, k],
            device_id={"cp": target},
            device_id_type=MESH,
        )

    def finish_sum(c):
        for copy in near_copies[c]:
            copy.wait_recv()
        total = (
            own_sum[c]
            + near_in[c, 0].astype(jnp.float32)
            + near_in[c, 1].astype(jnp.float32)
        ).astype(jnp.bfloat16)
        picked = jnp.dot(to_owner, total, preferred_element_type=jnp.float32)
        spread[c] = picked.reshape(CP, 8, CW).astype(jnp.bfloat16)
        landed[c, me] = spread[c, me]

        def send(k, carry):
            acopy(c, k, lax.rem(me + k, CP), me).start()
            return carry

        lax.fori_loop(1, CP, send, 0)

    def place(c):
        def wait(k, carry):
            copy = acopy(c, k, lax.rem(me + k, CP), lax.rem(me + CP - k, CP))
            copy.wait_send()
            copy.wait_recv()
            return carry

        lax.fori_loop(1, CP, wait, 0)
        rows = landed[c].astype(jnp.float32).reshape(ROWS, CW).astype(jnp.bfloat16)
        out_ref[:, c * CW : (c + 1) * CW] = jnp.dot(
            to_place, rows, preferred_element_type=jnp.float32
        ).astype(jnp.bfloat16)

    loads[0].wait()
    far[0] = product(0, 0).astype(jnp.bfloat16)
    pl.semaphore_wait(barrier, CP + 1)
    for copy in far_copies[0]:
        copy.start()
    send_far(1)
    loads[1].wait()
    loads[2].wait()
    send_near(0)
    send_far(2)
    send_near(1)
    send_far(3)
    loads[3].wait()
    own_sum[0] = product(3, 0)
    send_near(2)
    own_sum[1] = product(3, 1)
    send_near(3)
    own_sum[2] = product(3, 2)
    own_sum[3] = product(3, 3)
    for c in range(CHUNKS):
        finish_sum(c)
        if c > 0:
            place(c - 1)
    place(CHUNKS - 1)
    for c in range(CHUNKS):
        for copy in (*far_copies[c], *near_copies[c]):
            copy.wait_send()


def output_call(slot_rows, heads, wo):
    vmem = pl.BlockSpec(memory_space=pltpu.VMEM)
    dma = pltpu.SemaphoreType.DMA
    half = ROWS // 2
    bf16 = jnp.bfloat16
    return pl.pallas_call(
        output_kernel,
        out_shape=jax.ShapeDtypeStruct((ROWS, WIDTH), bf16),
        in_specs=[vmem, vmem, pl.BlockSpec(memory_space=pltpu.HBM)],
        out_specs=vmem,
        scratch_shapes=[
            pltpu.VMEM((ROWS, WIDTH), bf16),
            pltpu.VMEM((TP, WIDTH, WIDTH), bf16),
            pltpu.VMEM((CHUNKS, ROWS, CW), bf16),
            pltpu.VMEM((CHUNKS, 2, ROWS, CW), bf16),
            pltpu.VMEM((CHUNKS, 2, half, CW), bf16),
            pltpu.VMEM((CHUNKS, 2, ROWS, CW), bf16),
            pltpu.VMEM((CHUNKS, CP, 8, CW), bf16),
            pltpu.VMEM((CHUNKS, CP, 8, CW), bf16),
            pltpu.VMEM((CHUNKS, ROWS, CW), jnp.float32),
            dma((4,)), dma((4 * CHUNKS,)), dma((4 * CHUNKS,)), dma((CHUNKS, CP)), dma((CHUNKS, CP)),
        ],
        compiler_params=pltpu.CompilerParams(
            collective_id=1, has_side_effects=True, vmem_limit_bytes=40 * 1024 * 1024
        ),
        name="project_out",
    )(slot_rows, heads, wo)


def local(hidden, query_weight, key_matrix, value_matrix, output_weight, bounds, block_owner):
    inverse = rope_inverse(HEAD)
    inverse = jnp.concatenate([inverse, inverse])[None, :]
    slots = slots_of(block_owner)
    slot_rows = (slots[:, None] * PORTION + jnp.arange(PORTION, dtype=jnp.int32)[None, :]).reshape(
        1, ROWS
    )
    hidden, query_weight, key_matrix, value_matrix, output_weight = (
        pltpu.with_memory_space_constraint(a, pltpu.HBM)
        for a in (hidden, query_weight, key_matrix, value_matrix, output_weight)
    )
    keys, values, queries, marks = gather_call(
        bounds, hidden, query_weight, key_matrix, value_matrix, inverse
    )
    heads = attend_call(
        bounds,
        queries.reshape(2 * ROWS, WIDTH // 2),
        keys.reshape(TOKENS, HEAD),
        values.reshape(TOKENS, HEAD),
        marks,
    )
    return output_call(slot_rows, heads, output_weight)


def solution(mesh):
    placed = (P("cp", "tp"), P(None, "tp"), P(None, "tp"), P(None, "tp"), P("tp", None), P(), P())
    return jax.shard_map(
        local, mesh=mesh, in_specs=placed, out_specs=P("cp", "tp"), check_vma=False
    )
```

```python
import functools
import math

import jax
import jax.numpy as jnp
from jax import lax
from jax.experimental import pallas as pl
from jax.experimental.pallas import tpu as pltpu
from jax.sharding import PartitionSpec as P

HEAD = 128
BLOCK = 128
CP = 32
TP = 4
ROWS = 256
WIDTH = 1024
NBLK = 64
HEADS = 8
TOKENS = 8192
PORTION = BLOCK // CP

rope_theta = 500000.0
rope_factor = 8.0
rope_context = 8192.0
masked_score = -1e30
MESH = pl.DeviceIdType.MESH


def rope_inverse(head_size):
    halves = jnp.arange(head_size // 2, dtype=jnp.float32)
    inverse = 1.0 / rope_theta ** (2.0 * halves / head_size)
    wavelength = 2.0 * math.pi / inverse
    smooth = (rope_context / wavelength - 1.0) / 3.0
    blended = (1.0 - smooth) * inverse / rope_factor + smooth * inverse
    longer = jnp.where(wavelength > rope_context, inverse / rope_factor, blended)
    return jnp.where(wavelength < rope_context / 4.0, inverse, longer)


def slots_of(block_owner):
    blocks = jnp.arange(NBLK, dtype=jnp.int32)
    same = block_owner[:, None] == block_owner[None, :]
    earlier = blocks[None, :] < blocks[:, None]
    rank = jnp.sum((same & earlier).astype(jnp.int32), axis=1)
    return block_owner * 2 + rank


def starts_of(tokens, bounds_ref):
    start = jnp.zeros_like(tokens)
    for i in range(1, 8):
        bound = bounds_ref[i]
        start = jnp.where(tokens >= bound, bound, start)
    return start


SIZES = (64, 64, 64, 32, 32)
STARTS = (0, 64, 128, 192, 224)
PARTS = len(SIZES)
STRAIGHT1 = (True, False, True, True, True)
STRAIGHT2 = (True, False, False, False, True)
SPAN = 8
PENALTY = -1e30


def gather_kernel(
    bounds_ref, hidden_ref, wq_ref, wk_ref, wv_ref, inverse_ref,
    k_ref, v_ref, q_ref, mark_ref,
    full, wq, wkv, qtmp, qsend, cosine, sine,
    w_sem, z_send, z_recv, g_send, g_recv, q_send, q_recv,
):
    me = lax.axis_index("cp")
    tp = lax.axis_index("tp")
    core = lax.rem(me, 2)
    ycoord = lax.rem(me // 2, 4)
    xcoord = me // 8
    partner = me + 1 - 2 * core
    up, down = lax.rem(tp + 1, TP), lax.rem(tp + 3, TP)
    own_columns = pl.ds(pl.multiple_of(tp * WIDTH, WIDTH), WIDTH)

    bring = pltpu.make_async_copy(hidden_ref, full.at[:, own_columns], w_sem.at[3])
    weights = [
        pltpu.make_async_copy(wk_ref, wkv.at[:, pl.ds(0, HEAD)], w_sem.at[0]),
        pltpu.make_async_copy(wv_ref, wkv.at[:, pl.ds(HEAD, HEAD)], w_sem.at[1]),
        pltpu.make_async_copy(wq_ref, wq, w_sem.at[2]),
    ]
    bring.start()
    for copy in weights:
        copy.start()

    barrier = pltpu.get_barrier_semaphore()

    def greet(k, carry):
        pl.semaphore_signal(
            barrier, inc=1, device_id={"cp": lax.rem(me + k, CP)}, device_id_type=MESH
        )
        return carry

    pl.semaphore_signal(barrier, inc=1, device_id={"tp": up}, device_id_type=MESH)
    pl.semaphore_signal(barrier, inc=1, device_id={"tp": down}, device_id_type=MESH)
    lax.fori_loop(1, CP, greet, 0)
    bring.wait()
    pl.semaphore_wait(barrier, CP + 1)

    def zcopy(n, target, owner, row, count):
        columns = pl.ds(pl.multiple_of(owner * WIDTH, WIDTH), WIDTH)
        ref = full.at[pl.ds(row, count), columns]
        return pltpu.make_async_remote_copy(
            src_ref=ref,
            dst_ref=ref,
            send_sem=z_send.at[n],
            recv_sem=z_recv.at[n],
            device_id={"tp": target},
            device_id_type=MESH,
        )

    own = [
        (
            zcopy(4 * r, up, tp, STARTS[r], SIZES[r]),
            zcopy(4 * r + 1, down, tp, STARTS[r], SIZES[r]),
        )
        for r in range(PARTS)
    ]
    fwd = [
        (
            zcopy(4 * r + 2, down, up, STARTS[r], SIZES[r] // 2),
            zcopy(4 * r + 3, up, down, STARTS[r] + SIZES[r] // 2, SIZES[r] // 2),
        )
        for r in range(PARTS)
    ]
    for copy in (*own[0], *own[1]):
        copy.start()

    def relay_z(r):
        for copy in own[r]:
            copy.wait_recv()
        for copy in fwd[r]:
            copy.start()
        if r + 2 < PARTS:
            for copy in own[r + 2]:
                copy.start()

    lanes = lax.broadcasted_iota(jnp.int32, (BLOCK, HEAD), 1)
    sublanes = lax.broadcasted_iota(jnp.int32, (BLOCK, HEAD), 0)
    inverse = inverse_ref[...]
    for r in range(2):
        tokens = me * ROWS + r * BLOCK + sublanes
        angle = (tokens - starts_of(tokens, bounds_ref)).astype(jnp.float32) * inverse
        turn = jnp.sin(angle)
        cosine[pl.ds(r * BLOCK, BLOCK), :] = jnp.cos(angle)
        sine[pl.ds(r * BLOCK, BLOCK), :] = jnp.where(lanes < HEAD // 2, -turn, turn)

    place = jnp.minimum(jnp.maximum(sublanes - me * PORTION, 0), PORTION)

    def mark(b, carry):
        tokens = b * BLOCK + sublanes
        document = jnp.zeros_like(tokens)
        for i in range(1, 8):
            document = jnp.where(tokens >= bounds_ref[i], i, document)
        spot = 8 + lax.rem(b, SPAN) * (PORTION + 1) + place
        hit = (lanes == document) | (lanes == spot)
        mark_ref[pl.ds(pl.multiple_of(b * BLOCK, BLOCK), BLOCK), :] = (
            hit.astype(jnp.float32).astype(jnp.bfloat16)
        )
        return carry

    lax.fori_loop(0, NBLK // 2, mark, 0)
    weights[0].wait()
    weights[1].wait()
    weights[2].wait()

    def rotate(raw, row, count):
        table = pl.ds(row, count)
        return raw * cosine[table, :] + pltpu.roll(raw, HEAD // 2, 1) * sine[table, :]

    def queries(r, n):
        columns = slice(n * 2 * HEAD, (n + 1) * 2 * HEAD)
        rows = pl.ds(r * BLOCK, BLOCK)
        raw = jnp.dot(full[rows, :], wq[:, columns], preferred_element_type=jnp.float32)
        turned = jnp.concatenate(
            [rotate(raw[:, :HEAD], r * BLOCK, BLOCK), rotate(raw[:, HEAD:], r * BLOCK, BLOCK)],
            axis=1,
        )
        qtmp[pl.ds((n // 2) * BLOCK, BLOCK), (n % 2) * 2 * HEAD : (n % 2 + 1) * 2 * HEAD] = (
            turned.astype(jnp.bfloat16)
        )

    def gather(which, r):
        buffer = (k_ref, v_ref)[which]
        a, b = ((xcoord, ycoord), (ycoord, xcoord))[which]
        base = (which * PARTS + r) * 12

        def neighbour(along, step):
            if along == 0:
                na, nb = lax.rem(a + step, 4), b
            else:
                na, nb = a, lax.rem(b + step, 4)
            x, y = ((na, nb), (nb, na))[which]
            return (x * 4 + y) * 2 + core

        def copy(n, ref, target):
            return pltpu.make_async_remote_copy(
                src_ref=ref,
                dst_ref=ref,
                send_sem=g_send.at[base + n],
                recv_sem=g_recv.at[base + n],
                device_id={"cp": target},
                device_id_type=MESH,
            )

        def piece(at, row, count):
            rows = pl.ds(STARTS[r] + row, count)
            if which == 0:
                return buffer.at[at, b, core, rows]
            return buffer.at[b, at, core, rows]

        def line(at, first, count):
            along, rows = pl.ds(first, count), pl.ds(STARTS[r], SIZES[r])
            if which == 0:
                return buffer.at[along, at, core, rows]
            return buffer.at[at, along, core, rows]

        a_next, a_prev = lax.rem(a + 1, 4), lax.rem(a + 3, 4)
        b_next, b_prev = lax.rem(b + 1, 4), lax.rem(b + 3, 4)
        b_far = lax.rem(b + 2, 4)
        size, half = SIZES[r], SIZES[r] // 2
        return dict(
            ring1=(
                copy(0, piece(a, 0, size), neighbour(0, 1)),
                copy(1, piece(a, 0, size), neighbour(0, 3)),
            ),
            ring1_far=(copy(2, piece(a, 0, size), neighbour(0, 2)),)
            if STRAIGHT1[r]
            else (
                copy(2, piece(a_prev, 0, half), neighbour(0, 1)),
                copy(3, piece(a_next, half, half), neighbour(0, 3)),
            ),
            ring2=(
                copy(4, line(b, 0, 4), neighbour(1, 1)),
                copy(5, line(b, 0, 4), neighbour(1, 3)),
            ),
            ring2_far=(copy(6, line(b, 0, 4), neighbour(1, 2)),)
            if STRAIGHT2[r]
            else (
                copy(6, line(b_prev, 0, 2), neighbour(1, 1)),
                copy(7, line(b_next, 2, 2), neighbour(1, 3)),
            ),
            across=(
                copy(8, line(b, 0, 4), partner),
                copy(9, line(b_prev, 0, 4), partner),
                copy(10, line(b_next, 0, 4), partner),
                copy(11, line(b_far, 0, 4), partner),
            ),
        )

    flows = [[gather(which, r) for which in range(2)] for r in range(PARTS)]

    def start(r, name):
        for flow in flows[r]:
            for copy in flow[name]:
                copy.start()

    def arrived(r, name):
        for flow in flows[r]:
            for copy in flow[name]:
                copy.wait_recv()

    def across(r, which):
        for flow in flows[r]:
            for n in which:
                flow["across"][n].start()

    def s0(r):
        for copy in fwd[r]:
            copy.wait_recv()
        rows = pl.ds(STARTS[r], SIZES[r])
        raw = jnp.dot(full[rows, :], wkv[...], preferred_element_type=jnp.float32)
        k_ref[xcoord, ycoord, core, rows] = rotate(raw[:, :HEAD], STARTS[r], SIZES[r]).astype(
            jnp.bfloat16
        )
        v_ref[xcoord, ycoord, core, rows] = raw[:, HEAD:].astype(jnp.bfloat16)
        start(r, "ring1")
        if STRAIGHT1[r]:
            start(r, "ring1_far")

    def s1(r):
        arrived(r, "ring1")
        if not STRAIGHT1[r]:
            start(r, "ring1_far")

    def s2(r):
        arrived(r, "ring1_far")
        start(r, "ring2")
        if STRAIGHT2[r]:
            start(r, "ring2_far")
        across(r, (0,))

    def s3(r):
        arrived(r, "ring2")
        if not STRAIGHT2[r]:
            start(r, "ring2_far")
        across(r, (1, 2))

    def s4(r):
        arrived(r, "ring2_far")
        across(r, (3,))

    out_row = lax.broadcasted_iota(jnp.int32, (ROWS, ROWS), 0)
    in_row = lax.broadcasted_iota(jnp.int32, (ROWS, ROWS), 1)
    origin = lax.rem(out_row // 4, 2) * BLOCK + (out_row // 8) * 4 + lax.rem(out_row, 4)
    pick = (in_row == origin).astype(jnp.float32).astype(jnp.bfloat16)

    def qcopy(r, k, target, slot):
        return pltpu.make_async_remote_copy(
            src_ref=qsend.at[r, target],
            dst_ref=q_ref.at[slot, r],
            send_sem=q_send.at[r, k],
            recv_sem=q_recv.at[r, k],
            device_id={"cp": target},
            device_id_type=MESH,
        )

    def spread(r):
        ordered = jnp.dot(pick, qtmp[...], preferred_element_type=jnp.float32)
        qsend[r] = ordered.reshape(CP, 8, WIDTH // 2).astype(jnp.bfloat16)
        q_ref[me, r] = qsend[r, me]

        def send(k, carry):
            qcopy(r, k, lax.rem(me + k, CP), me).start()
            return carry

        lax.fori_loop(1, CP, send, 0)

    def spread_done(r):
        def wait(k, carry):
            copy = qcopy(r, k, lax.rem(me + k, CP), lax.rem(me + CP - k, CP))
            copy.wait_send()
            copy.wait_recv()
            return carry

        lax.fori_loop(1, CP, wait, 0)

    relay_z(0)
    lax.fori_loop(NBLK // 2, NBLK, mark, 0)
    relay_z(1)
    s0(0)
    relay_z(2)
    s1(0)
    s0(1)
    s2(0)
    queries(0, 0)
    queries(0, 1)
    relay_z(3)
    queries(0, 2)
    queries(0, 3)
    s0(2)
    s1(1)
    spread(0)
    relay_z(4)
    s0(3)
    s3(0)
    s1(2)
    s2(1)
    s4(0)
    s0(4)
    s2(2)
    queries(1, 0)
    queries(1, 1)
    queries(1, 2)
    queries(1, 3)
    s1(3)
    spread(1)
    s2(3)
    s3(1)
    s1(4)
    s2(4)
    s3(2)
    s3(3)
    s4(1)
    s3(4)
    s4(2)
    s4(4)
    s4(3)
    spread_done(0)
    spread_done(1)
    for r in range(PARTS):
        arrived(r, "across")
        for flow in flows[r]:
            for name in ("ring1", "ring1_far", "ring2", "ring2_far", "across"):
                for copy in flow[name]:
                    copy.wait_send()
    for group in (*own, *fwd):
        for copy in group:
            copy.wait_send()


def gather_call(bounds, hidden, wq, wk, wv, inverse):
    vmem = pl.BlockSpec(memory_space=pltpu.VMEM)
    hbm = pl.BlockSpec(memory_space=pltpu.HBM)
    kv = jax.ShapeDtypeStruct((4, 4, 2, ROWS, HEAD), jnp.bfloat16)
    dma = pltpu.SemaphoreType.DMA
    return pl.pallas_call(
        gather_kernel,
        out_shape=(
            kv,
            kv,
            jax.ShapeDtypeStruct((CP, 2, 8, WIDTH // 2), jnp.bfloat16),
            jax.ShapeDtypeStruct((TOKENS, HEAD), jnp.bfloat16),
        ),
        in_specs=[pl.BlockSpec(memory_space=pltpu.SMEM), hbm, hbm, hbm, hbm, vmem],
        out_specs=(vmem, vmem, vmem, vmem),
        scratch_shapes=[
            pltpu.VMEM((ROWS, TP * WIDTH), jnp.bfloat16),
            pltpu.VMEM((TP * WIDTH, WIDTH), jnp.bfloat16),
            pltpu.VMEM((TP * WIDTH, 2 * HEAD), jnp.bfloat16),
            pltpu.VMEM((ROWS, WIDTH // 2), jnp.bfloat16),
            pltpu.VMEM((2, CP, 8, WIDTH // 2), jnp.bfloat16),
            pltpu.VMEM((ROWS, HEAD), jnp.float32),
            pltpu.VMEM((ROWS, HEAD), jnp.float32),
            dma((4,)), dma((4 * PARTS,)), dma((4 * PARTS,)),
            dma((24 * PARTS,)), dma((24 * PARTS,)), dma((2, CP)), dma((2, CP)),
        ],
        compiler_params=pltpu.CompilerParams(
            collective_id=0, has_side_effects=True, vmem_limit_bytes=32 * 1024 * 1024
        ),
        name="gather_project",
    )(bounds, hidden, wq, wk, wv, inverse)


TILE = SPAN * BLOCK


GROUPS = NBLK // SPAN
QROWS = 4 * SPAN * 8
PIECE = 256


def attend_kernel(
    bounds_ref, q_ref, k_ref, v_ref, mark_ref, o_ref,
    turned, asked, even, odd, mixed_ref, total_ref,
):
    rows = SPAN * 8
    factor = math.log2(math.e) / math.sqrt(HEAD)
    row = lax.rem(lax.broadcasted_iota(jnp.int32, (rows, HEAD), 0), rows)
    lane = lax.broadcasted_iota(jnp.int32, (rows, HEAD), 1)
    block, step = row // 8, lax.rem(row, PORTION)
    key_block, key_step = (lane - 8) // (PORTION + 1), lax.rem(lane - 8, PORTION + 1)
    later = (key_block > block) | ((key_block == block) & (key_step > step))
    later = later & (lane >= 8) & (lane < 8 + SPAN * (PORTION + 1))
    me = lax.axis_index("cp")
    contract_last = (((1,), (1,)), ((), ()))
    diagonal = lax.broadcasted_iota(jnp.int32, (HEAD, HEAD), 0) == lax.broadcasted_iota(
        jnp.int32, (HEAD, HEAD), 1
    )
    identity = diagonal.astype(jnp.float32).astype(jnp.bfloat16)

    def prepare(g, carry):
        at = pl.ds(pl.multiple_of(g * TILE, TILE), TILE)
        turned[:, at] = lax.dot_general(
            identity, v_ref[at, :], contract_last, preferred_element_type=jnp.float32
        ).astype(jnp.bfloat16)
        tokens = (g * SPAN + block) * BLOCK + me * PORTION + step
        document = jnp.zeros_like(tokens)
        for i in range(1, 8):
            document = jnp.where(tokens >= bounds_ref[i], i, document)
        other = (lane < 8) & (lane != document)
        inner = jnp.where(other, PENALTY, 0.0).astype(jnp.bfloat16)
        outer = jnp.where(other | later, PENALTY, 0.0).astype(jnp.bfloat16)
        first = pl.multiple_of(g * rows, rows)
        for h in range(4):
            part = q_ref[pl.ds(first, rows), h * HEAD : (h + 1) * HEAD]
            for n, penalties in enumerate((inner, outer)):
                asked[2 * g + n, h * rows : (h + 1) * rows, :HEAD] = part
                asked[2 * g + n, h * rows : (h + 1) * rows, HEAD:] = penalties
        return carry

    lax.fori_loop(0, GROUPS, prepare, 0)

    def lowest(g):
        low = jnp.int32(0)
        for i in range(1, 8):
            low = jnp.where(g * TILE >= bounds_ref[i], bounds_ref[i], low)
        return low // TILE

    def following(item):
        g, j = item
        more = j > lowest(g)
        return jnp.where(more, g, g + 1), jnp.where(more, j - 1, g + 1)

    def score(item, ref):
        g, j = item
        own = jnp.where(g == j, 1, 0)
        q = asked[2 * jnp.minimum(g, GROUPS - 1) + own]
        for part in range(2):
            size = TILE // 2
            first = jnp.minimum(j, GROUPS - 1) * TILE + part * size
            at = pl.ds(pl.multiple_of(first, size), size)
            ref[part * size : (part + 1) * size, :] = lax.dot_general(
                jnp.concatenate([k_ref[at, :], mark_ref[at, :]], axis=1),
                q,
                contract_last,
                preferred_element_type=jnp.float32,
            )

    def soften(item, ref, state):
        g, j = item
        top, total, mixed = state
        top = jnp.where(g == j, 0.5 * PENALTY, top)
        start = jnp.minimum(j, GROUPS - 1) * TILE
        new_top = jnp.maximum(top, jnp.max(ref[...], axis=0, keepdims=True))
        shrink = jnp.exp2((top - new_top) * factor)
        total, mixed = total * shrink, mixed * shrink
        for first in range(0, TILE, PIECE):
            weights = jnp.exp2((ref[first : first + PIECE, :] - new_top) * factor)
            total = total + jnp.sum(weights, axis=0, keepdims=True)
            keys = pl.ds(pl.multiple_of(start + first, PIECE), PIECE)
            mixed = mixed + jnp.dot(
                turned[:, keys], weights.astype(jnp.bfloat16), preferred_element_type=jnp.float32
            )
        mixed_ref[g] = mixed
        total_ref[g] = total
        return new_top, total, mixed

    count = lax.fori_loop(0, GROUPS, lambda g, n: n + g + 1 - lowest(g), jnp.int32(0))
    zero = jnp.int32(0)
    score((zero, zero), even)

    def pair(n, carry):
        g, j, *state = carry
        item = (g, j)
        second = following(item)
        score(second, odd)
        state = soften(item, even, state)
        third = following(second)
        third = (jnp.minimum(third[0], GROUPS), jnp.minimum(third[1], GROUPS))
        score(third, even)
        state = soften(second, odd, state)
        return (*third, *state)

    lax.fori_loop(
        0,
        (count + 1) // 2,
        pair,
        (
            zero,
            zero,
            jnp.full((1, QROWS), 0.5 * PENALTY, jnp.float32),
            jnp.zeros((1, QROWS), jnp.float32),
            jnp.zeros((HEAD, QROWS), jnp.float32),
        ),
    )

    def finish(g, carry):
        out = (mixed_ref[g] / total_ref[g]).T.astype(jnp.bfloat16)
        first = pl.multiple_of(g * rows, rows)
        for h in range(4):
            o_ref[pl.ds(first, rows), h * HEAD : (h + 1) * HEAD] = out[h * rows : (h + 1) * rows]
        return carry

    lax.fori_loop(0, GROUPS, finish, 0)


def attend_call(bounds, q, k, v, marks):
    vmem = pl.BlockSpec(memory_space=pltpu.VMEM)
    return pl.pallas_call(
        attend_kernel,
        out_shape=jax.ShapeDtypeStruct((2 * ROWS, WIDTH // 2), jnp.bfloat16),
        in_specs=[pl.BlockSpec(memory_space=pltpu.SMEM), vmem, vmem, vmem, vmem],
        out_specs=vmem,
        scratch_shapes=[
            pltpu.VMEM((HEAD, TOKENS), jnp.bfloat16),
            pltpu.VMEM((2 * GROUPS, QROWS, 2 * HEAD), jnp.bfloat16),
            pltpu.VMEM((TILE, QROWS), jnp.float32),
            pltpu.VMEM((TILE, QROWS), jnp.float32),
            pltpu.VMEM((GROUPS + 1, HEAD, QROWS), jnp.float32),
            pltpu.VMEM((GROUPS + 1, 1, QROWS), jnp.float32),
        ],
        compiler_params=pltpu.CompilerParams(vmem_limit_bytes=28 * 1024 * 1024),
        name="attend",
    )(bounds, q, k, v, marks)


CHUNKS = (2, 2, 2, 1, 1)
FIRST = (0, 2, 4, 6, 7)
PIECES = WIDTH // HEAD


def output_kernel(
    slot_ref, heads_ref, wo_ref, out_ref,
    heads, wo, far, near, far_in, near_in, spread, landed, own_sum,
    w_sem, z_send, z_recv, a_send, a_recv,
):
    me = lax.axis_index("cp")
    tp = lax.axis_index("tp")
    up, down, across = lax.rem(tp + 1, TP), lax.rem(tp + 3, TP), lax.rem(tp + 2, TP)

    loads = []
    for n, t in enumerate((across, up, down, tp)):
        columns = pl.ds(pl.multiple_of(t * WIDTH, WIDTH), WIDTH)
        loads.append(pltpu.make_async_copy(wo_ref.at[:, columns], wo.at[n], w_sem.at[n]))
        loads[-1].start()

    barrier = pltpu.get_barrier_semaphore()

    def greet(k, carry):
        pl.semaphore_signal(
            barrier, inc=1, device_id={"cp": lax.rem(me + k, CP)}, device_id_type=MESH
        )
        return carry

    pl.semaphore_signal(barrier, inc=1, device_id={"tp": up}, device_id_type=MESH)
    pl.semaphore_signal(barrier, inc=1, device_id={"tp": down}, device_id_type=MESH)
    lax.fori_loop(1, CP, greet, 0)

    wide_row = lax.broadcasted_iota(jnp.int32, (ROWS, 2 * ROWS), 0)
    wide_column = lax.broadcasted_iota(jnp.int32, (ROWS, 2 * ROWS), 1)
    for h in range(2):
        source = (wide_row // PORTION) * 8 + h * PORTION + lax.rem(wide_row, PORTION)
        select = (wide_column == source).astype(jnp.float32).astype(jnp.bfloat16)
        heads[:, h * (WIDTH // 2) : (h + 1) * (WIDTH // 2)] = jnp.dot(
            select, heads_ref[...], preferred_element_type=jnp.float32
        ).astype(jnp.bfloat16)

    def product(n, c):
        columns = slice(FIRST[c] * HEAD, (FIRST[c] + CHUNKS[c]) * HEAD)
        return jnp.dot(heads[...], wo[n, :, columns], preferred_element_type=jnp.float32)

    def remote(n, src, dst, target):
        return pltpu.make_async_remote_copy(
            src_ref=src,
            dst_ref=dst,
            send_sem=z_send.at[n],
            recv_sem=z_recv.at[n],
            device_id={"tp": target},
            device_id_type=MESH,
        )

    half = ROWS // 2
    upper, lower = pl.ds(0, half), pl.ds(half, half)
    far_copies, near_copies = [], []
    for c, count in enumerate(CHUNKS):
        at = pl.ds(FIRST[c], count)
        far_copies.append(
            (
                remote(4 * c, far.at[0, at], far_in.at[0, at], up),
                remote(4 * c + 1, far.at[1, at], far_in.at[1, at], down),
            )
        )
        near_copies.append(
            (
                remote(4 * c + 2, near.at[0, at], near_in.at[0, at], up),
                remote(4 * c + 3, near.at[1, at], near_in.at[1, at], down),
            )
        )

    def pieces(c):
        return [(FIRST[c] + n, slice(n * HEAD, (n + 1) * HEAD)) for n in range(CHUNKS[c])]

    def make_far(c):
        value = product(0, c).astype(jnp.bfloat16)
        for at, columns in pieces(c):
            far[0, at] = value[:half, columns]
            far[1, at] = value[half:, columns]

    def send_far(c):
        for copy in far_copies[c]:
            copy.start()

    def send_near(c):
        to_up, to_down = product(1, c), product(2, c)
        far_copies[c][0].wait_recv()
        for at, columns in pieces(c):
            near[0, at, upper] = (
                to_up[:half, columns] + far_in[0, at].astype(jnp.float32)
            ).astype(jnp.bfloat16)
            near[0, at, lower] = to_up[half:, columns].astype(jnp.bfloat16)
        near_copies[c][0].start()
        far_copies[c][1].wait_recv()
        for at, columns in pieces(c):
            near[1, at, upper] = to_down[:half, columns].astype(jnp.bfloat16)
            near[1, at, lower] = (
                to_down[half:, columns] + far_in[1, at].astype(jnp.float32)
            ).astype(jnp.bfloat16)
        near_copies[c][1].start()

    def sum_own(c):
        value = product(3, c)
        for at, columns in pieces(c):
            own_sum[at] = value[:, columns]

    row = lax.broadcasted_iota(jnp.int32, (ROWS, ROWS), 0)
    column = lax.broadcasted_iota(jnp.int32, (ROWS, ROWS), 1)
    to_owner = (row == slot_ref[...]).astype(jnp.float32).astype(jnp.bfloat16)
    origin = (lax.rem(row, BLOCK) // 4) * 8 + (row // BLOCK) * 4 + lax.rem(row, 4)
    to_place = (column == origin).astype(jnp.float32).astype(jnp.bfloat16)

    def acopy(c, k, target, slot):
        at = pl.ds(FIRST[c], CHUNKS[c])
        return pltpu.make_async_remote_copy(
            src_ref=spread.at[target, at],
            dst_ref=landed.at[slot, at],
            send_sem=a_send.at[c, k],
            recv_sem=a_recv.at[c, k],
            device_id={"cp": target},
            device_id_type=MESH,
        )

    def finish_sum(c):
        for copy in near_copies[c]:
            copy.wait_recv()
        total = jnp.concatenate(
            [
                (
                    own_sum[at]
                    + near_in[0, at].astype(jnp.float32)
                    + near_in[1, at].astype(jnp.float32)
                ).astype(jnp.bfloat16)
                for at, columns in pieces(c)
            ],
            axis=1,
        )
        picked = jnp.dot(to_owner, total, preferred_element_type=jnp.float32)
        for at, columns in pieces(c):
            spread[:, at] = picked[:, columns].reshape(CP, 8, HEAD).astype(jnp.bfloat16)
            landed[me, at] = spread[me, at]

        def send(k, carry):
            acopy(c, k, lax.rem(me + k, CP), me).start()
            return carry

        lax.fori_loop(1, CP, send, 0)

    def place(c):
        def wait(k, carry):
            copy = acopy(c, k, lax.rem(me + k, CP), lax.rem(me + CP - k, CP))
            copy.wait_send()
            copy.wait_recv()
            return carry

        lax.fori_loop(1, CP, wait, 0)
        rows = jnp.concatenate(
            [
                landed[:, at].astype(jnp.float32).reshape(ROWS, HEAD).astype(jnp.bfloat16)
                for at, columns in pieces(c)
            ],
            axis=1,
        )
        out_ref[:, FIRST[c] * HEAD : (FIRST[c] + CHUNKS[c]) * HEAD] = jnp.dot(
            to_place, rows, preferred_element_type=jnp.float32
        ).astype(jnp.bfloat16)

    loads[0].wait()
    make_far(0)
    pl.semaphore_wait(barrier, CP + 1)
    send_far(0)
    make_far(1)
    send_far(1)
    make_far(2)
    send_far(2)
    loads[1].wait()
    loads[2].wait()
    send_near(0)
    make_far(3)
    send_far(3)
    send_near(1)
    make_far(4)
    send_far(4)
    send_near(2)
    loads[3].wait()
    for c in range(len(CHUNKS)):
        sum_own(c)
    send_near(3)
    finish_sum(0)
    send_near(4)
    finish_sum(1)
    finish_sum(2)
    finish_sum(3)
    finish_sum(4)
    for c in range(len(CHUNKS)):
        place(c)
    for c in range(len(CHUNKS)):
        for copy in (*far_copies[c], *near_copies[c]):
            copy.wait_send()


def output_call(slot_rows, heads, wo):
    vmem = pl.BlockSpec(memory_space=pltpu.VMEM)
    dma = pltpu.SemaphoreType.DMA
    half = ROWS // 2
    bf16 = jnp.bfloat16
    return pl.pallas_call(
        output_kernel,
        out_shape=jax.ShapeDtypeStruct((ROWS, WIDTH), bf16),
        in_specs=[vmem, vmem, pl.BlockSpec(memory_space=pltpu.HBM)],
        out_specs=vmem,
        scratch_shapes=[
            pltpu.VMEM((ROWS, WIDTH), bf16),
            pltpu.VMEM((TP, WIDTH, WIDTH), bf16),
            pltpu.VMEM((2, PIECES, half, HEAD), bf16),
            pltpu.VMEM((2, PIECES, ROWS, HEAD), bf16),
            pltpu.VMEM((2, PIECES, half, HEAD), bf16),
            pltpu.VMEM((2, PIECES, ROWS, HEAD), bf16),
            pltpu.VMEM((CP, PIECES, 8, HEAD), bf16),
            pltpu.VMEM((CP, PIECES, 8, HEAD), bf16),
            pltpu.VMEM((PIECES, ROWS, HEAD), jnp.float32),
            dma((4,)), dma((4 * len(CHUNKS),)), dma((4 * len(CHUNKS),)),
            dma((len(CHUNKS), CP)), dma((len(CHUNKS), CP)),
        ],
        compiler_params=pltpu.CompilerParams(
            collective_id=1, has_side_effects=True, vmem_limit_bytes=40 * 1024 * 1024
        ),
        name="project_out",
    )(slot_rows, heads, wo)


def local(hidden, query_weight, key_matrix, value_matrix, output_weight, bounds, block_owner):
    inverse = rope_inverse(HEAD)
    inverse = jnp.concatenate([inverse, inverse])[None, :]
    slots = slots_of(block_owner)
    slot_rows = (slots[:, None] * PORTION + jnp.arange(PORTION, dtype=jnp.int32)[None, :]).reshape(
        1, ROWS
    )
    hidden, query_weight, key_matrix, value_matrix, output_weight = (
        pltpu.with_memory_space_constraint(a, pltpu.HBM)
        for a in (hidden, query_weight, key_matrix, value_matrix, output_weight)
    )
    keys, values, queries, marks = gather_call(
        bounds, hidden, query_weight, key_matrix, value_matrix, inverse
    )
    heads = attend_call(
        bounds,
        queries.reshape(2 * ROWS, WIDTH // 2),
        keys.reshape(TOKENS, HEAD),
        values.reshape(TOKENS, HEAD),
        marks,
    )
    return output_call(slot_rows, heads, output_weight)


def solution(mesh):
    placed = (P("cp", "tp"), P(None, "tp"), P(None, "tp"), P(None, "tp"), P("tp", None), P(), P())
    return jax.shard_map(
        local, mesh=mesh, in_specs=placed, out_specs=P("cp", "tp"), check_vma=False
    )
```

```python
import functools
import math

import jax
import jax.numpy as jnp
from jax import lax
from jax.experimental import pallas as pl
from jax.experimental.pallas import tpu as pltpu
from jax.sharding import PartitionSpec as P

HEAD = 128
BLOCK = 128
CP = 32
TP = 4
ROWS = 256
WIDTH = 1024
NBLK = 64
HEADS = 8
TOKENS = 8192
PORTION = BLOCK // CP

rope_theta = 500000.0
rope_factor = 8.0
rope_context = 8192.0
masked_score = -1e30
MESH = pl.DeviceIdType.MESH


def rope_inverse(head_size):
    halves = jnp.arange(head_size // 2, dtype=jnp.float32)
    inverse = 1.0 / rope_theta ** (2.0 * halves / head_size)
    wavelength = 2.0 * math.pi / inverse
    smooth = (rope_context / wavelength - 1.0) / 3.0
    blended = (1.0 - smooth) * inverse / rope_factor + smooth * inverse
    longer = jnp.where(wavelength > rope_context, inverse / rope_factor, blended)
    return jnp.where(wavelength < rope_context / 4.0, inverse, longer)


def slots_of(block_owner):
    blocks = jnp.arange(NBLK, dtype=jnp.int32)
    same = block_owner[:, None] == block_owner[None, :]
    earlier = blocks[None, :] < blocks[:, None]
    rank = jnp.sum((same & earlier).astype(jnp.int32), axis=1)
    return block_owner * 2 + rank


def starts_of(tokens, bounds_ref):
    start = jnp.zeros_like(tokens)
    for i in range(1, 8):
        bound = bounds_ref[i]
        start = jnp.where(tokens >= bound, bound, start)
    return start


SIZES = (64, 64, 64, 32, 32)
STARTS = (0, 64, 128, 192, 224)
PARTS = len(SIZES)
STRAIGHT1 = (True, False, True, True, True)
STRAIGHT2 = (True, False, False, False, True)
SPAN = 8
PENALTY = -1e30


def gather_kernel(
    bounds_hbm, hidden_ref, wq_ref, wk_ref, wv_ref, inverse_ref,
    k_ref, v_ref, q_ref, mark_ref,
    full, wq, wkv, qtmp, qsend, cosine, sine,
    w_sem, z_send, z_recv, g_send, g_recv, q_send, q_recv, bounds_ref, met,
):
    me = lax.axis_index("cp")
    tp = lax.axis_index("tp")
    core = lax.rem(me, 2)
    ycoord = lax.rem(me // 2, 4)
    xcoord = me // 8
    partner = me + 1 - 2 * core
    up, down = lax.rem(tp + 1, TP), lax.rem(tp + 3, TP)
    own_columns = pl.ds(pl.multiple_of(tp * WIDTH, WIDTH), WIDTH)

    bring = pltpu.make_async_copy(hidden_ref, full.at[:, own_columns], w_sem.at[3])
    weights = [
        pltpu.make_async_copy(wk_ref, wkv.at[:, pl.ds(0, HEAD)], w_sem.at[0]),
        pltpu.make_async_copy(wv_ref, wkv.at[:, pl.ds(HEAD, HEAD)], w_sem.at[1]),
        pltpu.make_async_copy(wq_ref, wq, w_sem.at[2]),
    ]
    bring_bounds = pltpu.make_async_copy(bounds_hbm, bounds_ref, w_sem.at[4])
    bring.start()
    bring_bounds.start()
    for copy in weights:
        copy.start()

    barrier = pltpu.get_barrier_semaphore()

    def signal(semaphore, target):
        pl.semaphore_signal(semaphore, inc=1, device_id={"cp": target}, device_id_type=MESH)

    along_x = [(lax.rem(xcoord + n, 4) * 4 + ycoord) * 2 + core for n in (1, 2, 3)]
    along_y = [(xcoord * 4 + lax.rem(ycoord + n, 4)) * 2 + core for n in (1, 2, 3)]
    pl.semaphore_signal(barrier, inc=1, device_id={"tp": up}, device_id_type=MESH)
    pl.semaphore_signal(barrier, inc=1, device_id={"tp": down}, device_id_type=MESH)
    for target in (*along_x, *along_y, partner):
        signal(barrier, target)
    bring.wait()
    pl.semaphore_wait(barrier, 9)

    def zcopy(n, target, owner, row, count):
        columns = pl.ds(pl.multiple_of(owner * WIDTH, WIDTH), WIDTH)
        ref = full.at[pl.ds(row, count), columns]
        return pltpu.make_async_remote_copy(
            src_ref=ref,
            dst_ref=ref,
            send_sem=z_send.at[n],
            recv_sem=z_recv.at[n],
            device_id={"tp": target},
            device_id_type=MESH,
        )

    own = [
        (
            zcopy(4 * r, up, tp, STARTS[r], SIZES[r]),
            zcopy(4 * r + 1, down, tp, STARTS[r], SIZES[r]),
        )
        for r in range(PARTS)
    ]
    fwd = [
        (
            zcopy(4 * r + 2, down, up, STARTS[r], SIZES[r] // 2),
            zcopy(4 * r + 3, up, down, STARTS[r] + SIZES[r] // 2, SIZES[r] // 2),
        )
        for r in range(PARTS)
    ]
    for copy in (*own[0], *own[1]):
        copy.start()
    for target in along_x:
        signal(met.at[0], target)
    bring_bounds.wait()

    def relay_z(r):
        for copy in own[r]:
            copy.wait_recv()
        for copy in fwd[r]:
            copy.start()
        if r + 2 < PARTS:
            for copy in own[r + 2]:
                copy.start()

    lanes = lax.broadcasted_iota(jnp.int32, (BLOCK, HEAD), 1)
    sublanes = lax.broadcasted_iota(jnp.int32, (BLOCK, HEAD), 0)
    inverse = inverse_ref[...]
    for r in range(2):
        tokens = me * ROWS + r * BLOCK + sublanes
        angle = (tokens - starts_of(tokens, bounds_ref)).astype(jnp.float32) * inverse
        turn = jnp.sin(angle)
        cosine[pl.ds(r * BLOCK, BLOCK), :] = jnp.cos(angle)
        sine[pl.ds(r * BLOCK, BLOCK), :] = jnp.where(lanes < HEAD // 2, -turn, turn)

    place = jnp.minimum(jnp.maximum(sublanes - me * PORTION, 0), PORTION)

    def mark(b, carry):
        tokens = b * BLOCK + sublanes
        document = jnp.zeros_like(tokens)
        for i in range(1, 8):
            document = jnp.where(tokens >= bounds_ref[i], i, document)
        spot = 8 + lax.rem(b, SPAN) * (PORTION + 1) + place
        hit = (lanes == document) | (lanes == spot)
        mark_ref[pl.ds(pl.multiple_of(b * BLOCK, BLOCK), BLOCK), :] = (
            hit.astype(jnp.float32).astype(jnp.bfloat16)
        )
        return carry

    lax.fori_loop(0, NBLK // 2, mark, 0)
    weights[0].wait()
    weights[1].wait()
    weights[2].wait()

    def rotate(raw, row, count):
        table = pl.ds(row, count)
        return raw * cosine[table, :] + pltpu.roll(raw, HEAD // 2, 1) * sine[table, :]

    def queries(r, n):
        columns = slice(n * 2 * HEAD, (n + 1) * 2 * HEAD)
        rows = pl.ds(r * BLOCK, BLOCK)
        raw = jnp.dot(full[rows, :], wq[:, columns], preferred_element_type=jnp.float32)
        turned = jnp.concatenate(
            [rotate(raw[:, :HEAD], r * BLOCK, BLOCK), rotate(raw[:, HEAD:], r * BLOCK, BLOCK)],
            axis=1,
        )
        qtmp[pl.ds((n // 2) * BLOCK, BLOCK), (n % 2) * 2 * HEAD : (n % 2 + 1) * 2 * HEAD] = (
            turned.astype(jnp.bfloat16)
        )

    def gather(which, r):
        buffer = (k_ref, v_ref)[which]
        a, b = ((xcoord, ycoord), (ycoord, xcoord))[which]
        base = (which * PARTS + r) * 12

        def neighbour(along, step):
            if along == 0:
                na, nb = lax.rem(a + step, 4), b
            else:
                na, nb = a, lax.rem(b + step, 4)
            x, y = ((na, nb), (nb, na))[which]
            return (x * 4 + y) * 2 + core

        def copy(n, ref, target):
            return pltpu.make_async_remote_copy(
                src_ref=ref,
                dst_ref=ref,
                send_sem=g_send.at[base + n],
                recv_sem=g_recv.at[base + n],
                device_id={"cp": target},
                device_id_type=MESH,
            )

        def piece(at, row, count):
            rows = pl.ds(STARTS[r] + row, count)
            if which == 0:
                return buffer.at[at, b, core, rows]
            return buffer.at[b, at, core, rows]

        def line(at, first, count):
            along, rows = pl.ds(first, count), pl.ds(STARTS[r], SIZES[r])
            if which == 0:
                return buffer.at[along, at, core, rows]
            return buffer.at[at, along, core, rows]

        a_next, a_prev = lax.rem(a + 1, 4), lax.rem(a + 3, 4)
        b_next, b_prev = lax.rem(b + 1, 4), lax.rem(b + 3, 4)
        b_far = lax.rem(b + 2, 4)
        size, half = SIZES[r], SIZES[r] // 2
        return dict(
            ring1=(
                copy(0, piece(a, 0, size), neighbour(0, 1)),
                copy(1, piece(a, 0, size), neighbour(0, 3)),
            ),
            ring1_far=(copy(2, piece(a, 0, size), neighbour(0, 2)),)
            if STRAIGHT1[r]
            else (
                copy(2, piece(a_prev, 0, half), neighbour(0, 1)),
                copy(3, piece(a_next, half, half), neighbour(0, 3)),
            ),
            ring2=(
                copy(4, line(b, 0, 4), neighbour(1, 1)),
                copy(5, line(b, 0, 4), neighbour(1, 3)),
            ),
            ring2_far=(copy(6, line(b, 0, 4), neighbour(1, 2)),)
            if STRAIGHT2[r]
            else (
                copy(6, line(b_prev, 0, 2), neighbour(1, 1)),
                copy(7, line(b_next, 2, 2), neighbour(1, 3)),
            ),
            across=(
                copy(8, line(b, 0, 4), partner),
                copy(9, line(b_prev, 0, 4), partner),
                copy(10, line(b_next, 0, 4), partner),
                copy(11, line(b_far, 0, 4), partner),
            ),
        )

    flows = [[gather(which, r) for which in range(2)] for r in range(PARTS)]

    def start(r, name):
        for flow in flows[r]:
            for copy in flow[name]:
                copy.start()

    def arrived(r, name):
        for flow in flows[r]:
            for copy in flow[name]:
                copy.wait_recv()

    def across(r, which):
        for flow in flows[r]:
            for n in which:
                flow["across"][n].start()

    def s0(r):
        for copy in fwd[r]:
            copy.wait_recv()
        rows = pl.ds(STARTS[r], SIZES[r])
        raw = jnp.dot(full[rows, :], wkv[...], preferred_element_type=jnp.float32)
        k_ref[xcoord, ycoord, core, rows] = rotate(raw[:, :HEAD], STARTS[r], SIZES[r]).astype(
            jnp.bfloat16
        )
        v_ref[xcoord, ycoord, core, rows] = raw[:, HEAD:].astype(jnp.bfloat16)
        start(r, "ring1")
        if STRAIGHT1[r]:
            start(r, "ring1_far")

    def s1(r):
        arrived(r, "ring1")
        if not STRAIGHT1[r]:
            start(r, "ring1_far")

    def s2(r):
        arrived(r, "ring1_far")
        start(r, "ring2")
        if STRAIGHT2[r]:
            start(r, "ring2_far")
        across(r, (0,))

    def s3(r):
        arrived(r, "ring2")
        if not STRAIGHT2[r]:
            start(r, "ring2_far")
        across(r, (1, 2))

    def s4(r):
        arrived(r, "ring2_far")
        across(r, (3,))

    out_row = lax.broadcasted_iota(jnp.int32, (ROWS, ROWS), 0)
    in_row = lax.broadcasted_iota(jnp.int32, (ROWS, ROWS), 1)
    origin = lax.rem(out_row // 4, 2) * BLOCK + (out_row // 8) * 4 + lax.rem(out_row, 4)
    pick = (in_row == origin).astype(jnp.float32).astype(jnp.bfloat16)

    def qcopy(r, target, slot):
        return pltpu.make_async_remote_copy(
            src_ref=qsend.at[r, target],
            dst_ref=q_ref.at[slot, r],
            send_sem=q_send.at[r],
            recv_sem=q_recv.at[r],
            device_id={"cp": target},
            device_id_type=MESH,
        )

    def spread(r):
        ordered = jnp.dot(pick, qtmp[...], preferred_element_type=jnp.float32)
        qsend[r] = ordered.reshape(CP, 8, WIDTH // 2).astype(jnp.bfloat16)
        q_ref[me, r] = qsend[r, me]

        def send(k, carry):
            qcopy(r, lax.rem(me + k, CP), me).start()
            return carry

        lax.fori_loop(1, CP, send, 0)

    def spread_done(r):
        sent, landed = qsend.at[r, pl.ds(0, CP - 1)], q_ref.at[pl.ds(0, CP - 1), r]
        pltpu.make_async_copy(sent, sent, q_send.at[r]).wait()
        pltpu.make_async_copy(landed, landed, q_recv.at[r]).wait()

    relay_z(0)
    pl.semaphore_wait(met.at[0], 3)
    signal(met.at[1], partner)
    lax.fori_loop(NBLK // 2, NBLK, mark, 0)
    relay_z(1)
    pl.semaphore_wait(met.at[1], 1)
    s0(0)
    relay_z(2)
    s1(0)
    s0(1)
    s2(0)
    queries(0, 0)
    queries(0, 1)
    relay_z(3)
    queries(0, 2)
    queries(0, 3)
    s0(2)
    s1(1)
    spread(0)
    relay_z(4)
    s0(3)
    s3(0)
    s1(2)
    s2(1)
    s4(0)
    s0(4)
    s2(2)
    queries(1, 0)
    queries(1, 1)
    queries(1, 2)
    queries(1, 3)
    s1(3)
    spread(1)
    s2(3)
    s3(1)
    s1(4)
    s2(4)
    s3(2)
    s3(3)
    s4(1)
    s3(4)
    s4(2)
    s4(4)
    s4(3)
    spread_done(0)
    spread_done(1)
    for r in range(PARTS):
        arrived(r, "across")
        for flow in flows[r]:
            for name in ("ring1", "ring1_far", "ring2", "ring2_far", "across"):
                for copy in flow[name]:
                    copy.wait_send()
    for group in (*own, *fwd):
        for copy in group:
            copy.wait_send()


def gather_call(bounds, hidden, wq, wk, wv, inverse):
    vmem = pl.BlockSpec(memory_space=pltpu.VMEM)
    hbm = pl.BlockSpec(memory_space=pltpu.HBM)
    kv = jax.ShapeDtypeStruct((4, 4, 2, ROWS, HEAD), jnp.bfloat16)
    dma = pltpu.SemaphoreType.DMA
    return pl.pallas_call(
        gather_kernel,
        out_shape=(
            kv,
            kv,
            jax.ShapeDtypeStruct((CP, 2, 8, WIDTH // 2), jnp.bfloat16),
            jax.ShapeDtypeStruct((TOKENS, HEAD), jnp.bfloat16),
        ),
        in_specs=[hbm, hbm, hbm, hbm, hbm, vmem],
        out_specs=(vmem, vmem, vmem, vmem),
        scratch_shapes=[
            pltpu.VMEM((ROWS, TP * WIDTH), jnp.bfloat16),
            pltpu.VMEM((TP * WIDTH, WIDTH), jnp.bfloat16),
            pltpu.VMEM((TP * WIDTH, 2 * HEAD), jnp.bfloat16),
            pltpu.VMEM((ROWS, WIDTH // 2), jnp.bfloat16),
            pltpu.VMEM((2, CP, 8, WIDTH // 2), jnp.bfloat16),
            pltpu.VMEM((ROWS, HEAD), jnp.float32),
            pltpu.VMEM((ROWS, HEAD), jnp.float32),
            dma((5,)), dma((4 * PARTS,)), dma((4 * PARTS,)),
            dma((24 * PARTS,)), dma((24 * PARTS,)), dma((2,)), dma((2,)),
            pltpu.SMEM((9,), jnp.int32), pltpu.SemaphoreType.REGULAR((2,)),
        ],
        compiler_params=pltpu.CompilerParams(
            collective_id=0, has_side_effects=True, vmem_limit_bytes=32 * 1024 * 1024
        ),
        name="gather_project",
    )(bounds, hidden, wq, wk, wv, inverse)


TILE = SPAN * BLOCK


GROUPS = NBLK // SPAN
QROWS = 4 * SPAN * 8
PIECE = 256


def attend_kernel(
    bounds_ref, q_ref, k_ref, v_ref, mark_ref, o_ref,
    turned, penalty_ref, even, odd, mixed_ref, total_ref,
):
    rows = SPAN * 8
    factor = math.log2(math.e) / math.sqrt(HEAD)
    row = lax.rem(lax.broadcasted_iota(jnp.int32, (rows, HEAD), 0), rows)
    lane = lax.broadcasted_iota(jnp.int32, (rows, HEAD), 1)
    block, step = row // 8, lax.rem(row, PORTION)
    key_block, key_step = (lane - 8) // (PORTION + 1), lax.rem(lane - 8, PORTION + 1)
    later = (key_block > block) | ((key_block == block) & (key_step > step))
    later = later & (lane >= 8) & (lane < 8 + SPAN * (PORTION + 1))
    me = lax.axis_index("cp")
    contract_last = (((1,), (1,)), ((), ()))
    diagonal = lax.broadcasted_iota(jnp.int32, (HEAD, HEAD), 0) == lax.broadcasted_iota(
        jnp.int32, (HEAD, HEAD), 1
    )
    identity = diagonal.astype(jnp.float32).astype(jnp.bfloat16)

    def prepare(g, carry):
        at = pl.ds(pl.multiple_of(g * TILE, TILE), TILE)
        turned[:, at] = lax.dot_general(
            identity, v_ref[at, :], contract_last, preferred_element_type=jnp.float32
        ).astype(jnp.bfloat16)
        tokens = (g * SPAN + block) * BLOCK + me * PORTION + step
        document = jnp.zeros_like(tokens)
        for i in range(1, 8):
            document = jnp.where(tokens >= bounds_ref[i], i, document)
        other = (lane < 8) & (lane != document)
        penalty_ref[2 * g] = jnp.where(other, PENALTY, 0.0).astype(jnp.bfloat16)
        penalty_ref[2 * g + 1] = jnp.where(other | later, PENALTY, 0.0).astype(jnp.bfloat16)
        return carry

    lax.fori_loop(0, GROUPS, prepare, 0)

    def lowest(g):
        low = jnp.int32(0)
        for i in range(1, 8):
            low = jnp.where(g * TILE >= bounds_ref[i], bounds_ref[i], low)
        return low // TILE

    def following(item):
        g, j = item
        more = j > lowest(g)
        return jnp.where(more, g, g + 1), jnp.where(more, j - 1, g + 1)

    def score(item, ref):
        g, j = item
        own = jnp.where(g == j, 1, 0)
        held = jnp.minimum(g, GROUPS - 1)
        penalties = penalty_ref[2 * held + own]
        asking = pl.ds(pl.multiple_of(held * rows, rows), rows)
        q = jnp.concatenate(
            [
                jnp.concatenate([q_ref[asking, h * HEAD : (h + 1) * HEAD], penalties], axis=1)
                for h in range(4)
            ],
            axis=0,
        )
        for part in range(2):
            size = TILE // 2
            first = jnp.minimum(j, GROUPS - 1) * TILE + part * size
            at = pl.ds(pl.multiple_of(first, size), size)
            scores = lax.dot_general(
                jnp.concatenate([k_ref[at, :], mark_ref[at, :]], axis=1),
                q,
                contract_last,
                preferred_element_type=jnp.float32,
            )
            ref[part * size : (part + 1) * size, :] = scores
            top = jnp.max(scores, axis=0, keepdims=True)
            largest = top if part == 0 else jnp.maximum(largest, top)
        return largest

    def soften(item, ref, largest, state):
        g, j = item
        top, total, mixed = state
        top = jnp.where(g == j, 0.5 * PENALTY, top)
        start = jnp.minimum(j, GROUPS - 1) * TILE
        new_top = jnp.maximum(top, largest)
        shrink = jnp.exp2((top - new_top) * factor)
        total, mixed = total * shrink, mixed * shrink
        for first in range(0, TILE, PIECE):
            piece = slice(first, first + PIECE)
            weights = jnp.exp2((ref[piece, :] - new_top) * factor)
            total = total + jnp.sum(weights, axis=0, keepdims=True)
            keys = pl.ds(pl.multiple_of(start + first, PIECE), PIECE)
            mixed = mixed + jnp.dot(
                turned[:, keys], weights.astype(jnp.bfloat16), preferred_element_type=jnp.float32
            )
        mixed_ref[g] = mixed
        total_ref[g] = total
        return new_top, total, mixed

    count = lax.fori_loop(0, GROUPS, lambda g, n: n + g + 1 - lowest(g), jnp.int32(0))
    zero = jnp.int32(0)
    highest = score((zero, zero), even)

    def pair(n, carry):
        g, j, largest, *state = carry
        item = (g, j)
        second = following(item)
        second_largest = score(second, odd)
        state = soften(item, even, largest, state)
        third = following(second)
        third = (jnp.minimum(third[0], GROUPS), jnp.minimum(third[1], GROUPS))
        largest = score(third, even)
        state = soften(second, odd, second_largest, state)
        return (*third, largest, *state)

    lax.fori_loop(
        0,
        (count + 1) // 2,
        pair,
        (
            zero,
            zero,
            highest,
            jnp.full((1, QROWS), 0.5 * PENALTY, jnp.float32),
            jnp.zeros((1, QROWS), jnp.float32),
            jnp.zeros((HEAD, QROWS), jnp.float32),
        ),
    )

    def finish(g, carry):
        o_ref[g] = (mixed_ref[g] / total_ref[g]).astype(jnp.bfloat16)
        return carry

    lax.fori_loop(0, GROUPS, finish, 0)


def attend_call(bounds, q, k, v, marks):
    vmem = pl.BlockSpec(memory_space=pltpu.VMEM)
    return pl.pallas_call(
        attend_kernel,
        out_shape=jax.ShapeDtypeStruct((GROUPS, HEAD, QROWS), jnp.bfloat16),
        in_specs=[pl.BlockSpec(memory_space=pltpu.SMEM), vmem, vmem, vmem, vmem],
        out_specs=vmem,
        scratch_shapes=[
            pltpu.VMEM((HEAD, TOKENS), jnp.bfloat16),
            pltpu.VMEM((2 * GROUPS, SPAN * 8, HEAD), jnp.bfloat16),
            pltpu.VMEM((TILE, QROWS), jnp.float32),
            pltpu.VMEM((TILE, QROWS), jnp.float32),
            pltpu.VMEM((GROUPS + 1, HEAD, QROWS), jnp.float32),
            pltpu.VMEM((GROUPS + 1, 1, QROWS), jnp.float32),
        ],
        compiler_params=pltpu.CompilerParams(vmem_limit_bytes=28 * 1024 * 1024),
        name="attend",
    )(bounds, q, k, v, marks)


CHUNKS = (2, 2, 2, 1, 1)
FIRST = (0, 2, 4, 6, 7)
PIECES = WIDTH // HEAD


def output_kernel(
    slot_ref, heads_ref, wo_ref, out_ref,
    heads, wo, far, near, far_in, near_in, spread, landed, own_sum,
    w_sem, z_send, z_recv, a_send, a_recv,
):
    me = lax.axis_index("cp")
    tp = lax.axis_index("tp")
    up, down, across = lax.rem(tp + 1, TP), lax.rem(tp + 3, TP), lax.rem(tp + 2, TP)

    loads = []
    for n, t in enumerate((across, up, down, tp)):
        columns = pl.ds(pl.multiple_of(t * WIDTH, WIDTH), WIDTH)
        loads.append(pltpu.make_async_copy(wo_ref.at[:, columns], wo.at[n], w_sem.at[n]))
        loads[-1].start()

    barrier = pltpu.get_barrier_semaphore()

    def greet(k, carry):
        pl.semaphore_signal(
            barrier, inc=1, device_id={"cp": lax.rem(me + k, CP)}, device_id_type=MESH
        )
        return carry

    pl.semaphore_signal(barrier, inc=1, device_id={"tp": up}, device_id_type=MESH)
    pl.semaphore_signal(barrier, inc=1, device_id={"tp": down}, device_id_type=MESH)
    lax.fori_loop(1, CP, greet, 0)

    turned_row = lax.broadcasted_iota(jnp.int32, (QROWS, QROWS), 0)
    turned_column = lax.broadcasted_iota(jnp.int32, (QROWS, QROWS), 1)
    rows = SPAN * PORTION
    head, at_row = turned_row // rows, lax.rem(turned_row, rows)
    source = (
        lax.rem(head, 4) * 2 * rows
        + (at_row // PORTION) * 2 * PORTION
        + (head // 4) * PORTION
        + lax.rem(at_row, PORTION)
    )
    select = (turned_column == source).astype(jnp.float32).astype(jnp.bfloat16)
    for g in range(GROUPS):
        part = lax.dot_general(
            select,
            heads_ref[g],
            (((1,), (1,)), ((), ())),
            preferred_element_type=jnp.float32,
        ).astype(jnp.bfloat16)
        for h in range(HEADS):
            heads[g * rows : (g + 1) * rows, h * HEAD : (h + 1) * HEAD] = part[
                h * rows : (h + 1) * rows
            ]

    def product(n, c):
        columns = slice(FIRST[c] * HEAD, (FIRST[c] + CHUNKS[c]) * HEAD)
        return jnp.dot(heads[...], wo[n, :, columns], preferred_element_type=jnp.float32)

    def remote(n, src, dst, target):
        return pltpu.make_async_remote_copy(
            src_ref=src,
            dst_ref=dst,
            send_sem=z_send.at[n],
            recv_sem=z_recv.at[n],
            device_id={"tp": target},
            device_id_type=MESH,
        )

    half = ROWS // 2
    upper, lower = pl.ds(0, half), pl.ds(half, half)
    far_copies, near_copies = [], []
    for c, count in enumerate(CHUNKS):
        at = pl.ds(FIRST[c], count)
        far_copies.append(
            (
                remote(4 * c, far.at[0, at], far_in.at[0, at], up),
                remote(4 * c + 1, far.at[1, at], far_in.at[1, at], down),
            )
        )
        near_copies.append(
            (
                remote(4 * c + 2, near.at[0, at], near_in.at[0, at], up),
                remote(4 * c + 3, near.at[1, at], near_in.at[1, at], down),
            )
        )

    def pieces(c):
        return [(FIRST[c] + n, slice(n * HEAD, (n + 1) * HEAD)) for n in range(CHUNKS[c])]

    def make_far(c):
        value = product(0, c).astype(jnp.bfloat16)
        for at, columns in pieces(c):
            far[0, at] = value[:half, columns]
            far[1, at] = value[half:, columns]

    def send_far(c):
        for copy in far_copies[c]:
            copy.start()

    def send_near(c):
        to_up, to_down = product(1, c), product(2, c)
        far_copies[c][0].wait_recv()
        for at, columns in pieces(c):
            near[0, at, upper] = (
                to_up[:half, columns] + far_in[0, at].astype(jnp.float32)
            ).astype(jnp.bfloat16)
            near[0, at, lower] = to_up[half:, columns].astype(jnp.bfloat16)
        near_copies[c][0].start()
        far_copies[c][1].wait_recv()
        for at, columns in pieces(c):
            near[1, at, upper] = to_down[:half, columns].astype(jnp.bfloat16)
            near[1, at, lower] = (
                to_down[half:, columns] + far_in[1, at].astype(jnp.float32)
            ).astype(jnp.bfloat16)
        near_copies[c][1].start()

    def sum_own(c):
        value = product(3, c)
        for at, columns in pieces(c):
            own_sum[at] = value[:, columns]

    row = lax.broadcasted_iota(jnp.int32, (ROWS, ROWS), 0)
    column = lax.broadcasted_iota(jnp.int32, (ROWS, ROWS), 1)
    to_owner = (row == slot_ref[...]).astype(jnp.float32).astype(jnp.bfloat16)
    origin = (lax.rem(row, BLOCK) // 4) * 8 + (row // BLOCK) * 4 + lax.rem(row, 4)
    to_place = (column == origin).astype(jnp.float32).astype(jnp.bfloat16)

    def acopy(c, target, slot):
        at = pl.ds(FIRST[c], CHUNKS[c])
        return pltpu.make_async_remote_copy(
            src_ref=spread.at[target, at],
            dst_ref=landed.at[slot, at],
            send_sem=a_send.at[c],
            recv_sem=a_recv.at[c],
            device_id={"cp": target},
            device_id_type=MESH,
        )

    def finish_sum(c):
        for copy in near_copies[c]:
            copy.wait_recv()
        total = jnp.concatenate(
            [
                (
                    own_sum[at]
                    + near_in[0, at].astype(jnp.float32)
                    + near_in[1, at].astype(jnp.float32)
                ).astype(jnp.bfloat16)
                for at, columns in pieces(c)
            ],
            axis=1,
        )
        picked = jnp.dot(to_owner, total, preferred_element_type=jnp.float32)
        for at, columns in pieces(c):
            spread[:, at] = picked[:, columns].reshape(CP, 8, HEAD).astype(jnp.bfloat16)
            landed[me, at] = spread[me, at]

        def send(k, carry):
            acopy(c, lax.rem(me + k, CP), me).start()
            return carry

        lax.fori_loop(1, CP, send, 0)

    def place(c):
        everyone = landed.at[pl.ds(0, CP - 1), pl.ds(FIRST[c], CHUNKS[c])]
        pltpu.make_async_copy(everyone, everyone, a_recv.at[c]).wait()
        rows = jnp.concatenate(
            [
                landed[:, at].astype(jnp.float32).reshape(ROWS, HEAD).astype(jnp.bfloat16)
                for at, columns in pieces(c)
            ],
            axis=1,
        )
        out_ref[:, FIRST[c] * HEAD : (FIRST[c] + CHUNKS[c]) * HEAD] = jnp.dot(
            to_place, rows, preferred_element_type=jnp.float32
        ).astype(jnp.bfloat16)

    loads[0].wait()
    make_far(0)
    pl.semaphore_wait(barrier, CP + 1)
    send_far(0)
    make_far(1)
    send_far(1)
    make_far(2)
    send_far(2)
    loads[1].wait()
    loads[2].wait()
    send_near(0)
    make_far(3)
    send_far(3)
    send_near(1)
    make_far(4)
    send_far(4)
    send_near(2)
    loads[3].wait()
    for c in range(len(CHUNKS)):
        sum_own(c)
    send_near(3)
    finish_sum(0)
    send_near(4)
    finish_sum(1)
    finish_sum(2)
    finish_sum(3)
    finish_sum(4)
    for c in range(len(CHUNKS)):
        place(c)
    for c in range(len(CHUNKS)):
        for copy in (*far_copies[c], *near_copies[c]):
            copy.wait_send()
        everyone = spread.at[pl.ds(0, CP - 1), pl.ds(FIRST[c], CHUNKS[c])]
        pltpu.make_async_copy(everyone, everyone, a_send.at[c]).wait()


def output_call(slot_rows, heads, wo):
    vmem = pl.BlockSpec(memory_space=pltpu.VMEM)
    dma = pltpu.SemaphoreType.DMA
    half = ROWS // 2
    bf16 = jnp.bfloat16
    return pl.pallas_call(
        output_kernel,
        out_shape=jax.ShapeDtypeStruct((ROWS, WIDTH), bf16),
        in_specs=[vmem, vmem, pl.BlockSpec(memory_space=pltpu.HBM)],
        out_specs=vmem,
        scratch_shapes=[
            pltpu.VMEM((ROWS, WIDTH), bf16),
            pltpu.VMEM((TP, WIDTH, WIDTH), bf16),
            pltpu.VMEM((2, PIECES, half, HEAD), bf16),
            pltpu.VMEM((2, PIECES, ROWS, HEAD), bf16),
            pltpu.VMEM((2, PIECES, half, HEAD), bf16),
            pltpu.VMEM((2, PIECES, ROWS, HEAD), bf16),
            pltpu.VMEM((CP, PIECES, 8, HEAD), bf16),
            pltpu.VMEM((CP, PIECES, 8, HEAD), bf16),
            pltpu.VMEM((PIECES, ROWS, HEAD), jnp.float32),
            dma((4,)), dma((4 * len(CHUNKS),)), dma((4 * len(CHUNKS),)),
            dma((len(CHUNKS),)), dma((len(CHUNKS),)),
        ],
        compiler_params=pltpu.CompilerParams(
            collective_id=1, has_side_effects=True, vmem_limit_bytes=40 * 1024 * 1024
        ),
        name="project_out",
    )(slot_rows, heads, wo)


def local(hidden, query_weight, key_matrix, value_matrix, output_weight, bounds, block_owner):
    inverse = rope_inverse(HEAD)
    inverse = jnp.concatenate([inverse, inverse])[None, :]
    slots = slots_of(block_owner)
    slot_rows = (slots[:, None] * PORTION + jnp.arange(PORTION, dtype=jnp.int32)[None, :]).reshape(
        1, ROWS
    )
    hidden, query_weight, key_matrix, value_matrix, output_weight = (
        pltpu.with_memory_space_constraint(a, pltpu.HBM)
        for a in (hidden, query_weight, key_matrix, value_matrix, output_weight)
    )
    keys, values, queries, marks = gather_call(
        pltpu.with_memory_space_constraint(bounds, pltpu.HBM), hidden, query_weight, key_matrix, value_matrix, inverse
    )
    heads = attend_call(
        bounds,
        queries.reshape(2 * ROWS, WIDTH // 2),
        keys.reshape(TOKENS, HEAD),
        values.reshape(TOKENS, HEAD),
        marks,
    )
    return output_call(slot_rows, heads, output_weight)


def solution(mesh):
    placed = (P("cp", "tp"), P(None, "tp"), P(None, "tp"), P(None, "tp"), P("tp", None), P(), P())
    return jax.shard_map(
        local, mesh=mesh, in_specs=placed, out_specs=P("cp", "tp"), check_vma=False
    )
```

```python
import functools
import math

import jax
import jax.numpy as jnp
from jax import lax
from jax.experimental import pallas as pl
from jax.experimental.pallas import tpu as pltpu
from jax.sharding import PartitionSpec as P

HEAD = 128
BLOCK = 128
CP = 32
TP = 4
ROWS = 256
WIDTH = 1024
NBLK = 64
HEADS = 8
TOKENS = 8192
PORTION = BLOCK // CP

rope_theta = 500000.0
rope_factor = 8.0
rope_context = 8192.0
masked_score = -1e30
MESH = pl.DeviceIdType.MESH


def rope_inverse(head_size):
    halves = jnp.arange(head_size // 2, dtype=jnp.float32)
    inverse = 1.0 / rope_theta ** (2.0 * halves / head_size)
    wavelength = 2.0 * math.pi / inverse
    smooth = (rope_context / wavelength - 1.0) / 3.0
    blended = (1.0 - smooth) * inverse / rope_factor + smooth * inverse
    longer = jnp.where(wavelength > rope_context, inverse / rope_factor, blended)
    return jnp.where(wavelength < rope_context / 4.0, inverse, longer)


def slots_of(block_owner):
    blocks = jnp.arange(NBLK, dtype=jnp.int32)
    same = block_owner[:, None] == block_owner[None, :]
    earlier = blocks[None, :] < blocks[:, None]
    rank = jnp.sum((same & earlier).astype(jnp.int32), axis=1)
    return block_owner * 2 + rank


def starts_of(tokens, bounds_ref):
    start = jnp.zeros_like(tokens)
    for i in range(1, 8):
        bound = bounds_ref[i]
        start = jnp.where(tokens >= bound, bound, start)
    return start


SIZES = (64, 64, 64, 32, 32)
STARTS = (0, 64, 128, 192, 224)
PARTS = len(SIZES)
STRAIGHT1 = (True, False, True, True, True)
STRAIGHT2 = (True, False, False, False, True)
SPAN = 8
PENALTY = -1e30


def gather_kernel(
    bounds_hbm, hidden_ref, wq_ref, wk_ref, wv_ref, inverse_ref,
    k_ref, v_ref, q_ref, mark_ref,
    full, wq, wkv, qtmp, qsend, cosine, sine,
    w_sem, z_send, z_recv, g_send, g_recv, q_send, q_recv, bounds_ref, met,
):
    me = lax.axis_index("cp")
    tp = lax.axis_index("tp")
    core = lax.rem(me, 2)
    ycoord = lax.rem(me // 2, 4)
    xcoord = me // 8
    partner = me + 1 - 2 * core
    up, down = lax.rem(tp + 1, TP), lax.rem(tp + 3, TP)
    own_columns = pl.ds(pl.multiple_of(tp * WIDTH, WIDTH), WIDTH)

    bring = pltpu.make_async_copy(hidden_ref, full.at[:, own_columns], w_sem.at[3])
    weights = [
        pltpu.make_async_copy(wk_ref, wkv.at[:, pl.ds(0, HEAD)], w_sem.at[0]),
        pltpu.make_async_copy(wv_ref, wkv.at[:, pl.ds(HEAD, HEAD)], w_sem.at[1]),
        pltpu.make_async_copy(wq_ref, wq, w_sem.at[2]),
    ]
    bring_bounds = pltpu.make_async_copy(bounds_hbm, bounds_ref, w_sem.at[4])
    bring.start()
    bring_bounds.start()
    for copy in weights:
        copy.start()

    barrier = pltpu.get_barrier_semaphore()

    def signal(semaphore, target):
        pl.semaphore_signal(semaphore, inc=1, device_id={"cp": target}, device_id_type=MESH)

    along_x = [(lax.rem(xcoord + n, 4) * 4 + ycoord) * 2 + core for n in (1, 2, 3)]
    along_y = [(xcoord * 4 + lax.rem(ycoord + n, 4)) * 2 + core for n in (1, 2, 3)]
    pl.semaphore_signal(barrier, inc=1, device_id={"tp": up}, device_id_type=MESH)
    pl.semaphore_signal(barrier, inc=1, device_id={"tp": down}, device_id_type=MESH)
    for target in (*along_x, *along_y, partner):
        signal(barrier, target)
    bring.wait()
    pl.semaphore_wait(barrier, 9)

    def zcopy(n, target, owner, row, count):
        columns = pl.ds(pl.multiple_of(owner * WIDTH, WIDTH), WIDTH)
        ref = full.at[pl.ds(row, count), columns]
        return pltpu.make_async_remote_copy(
            src_ref=ref,
            dst_ref=ref,
            send_sem=z_send.at[0],
            recv_sem=z_recv.at[n],
            device_id={"tp": target},
            device_id_type=MESH,
        )

    own = [
        (
            zcopy(2 * r, up, tp, STARTS[r], SIZES[r]),
            zcopy(2 * r, down, tp, STARTS[r], SIZES[r]),
        )
        for r in range(PARTS)
    ]
    fwd = [
        (
            zcopy(2 * r + 1, down, up, STARTS[r], SIZES[r] // 2),
            zcopy(2 * r + 1, up, down, STARTS[r] + SIZES[r] // 2, SIZES[r] // 2),
        )
        for r in range(PARTS)
    ]

    def wait_for(ref, semaphore):
        pltpu.make_async_copy(ref, ref, semaphore).wait()

    def arrived_z(n, r, owners):
        wait_for(
            full.at[pl.ds(STARTS[r], SIZES[r]), pl.ds(0, owners * WIDTH)], z_recv.at[2 * r + n]
        )
    for copy in (*own[0], *own[1]):
        copy.start()
    for target in along_x:
        signal(met.at[0], target)
    bring_bounds.wait()

    def relay_z(r):
        arrived_z(0, r, 2)
        for copy in fwd[r]:
            copy.start()
        if r + 2 < PARTS:
            for copy in own[r + 2]:
                copy.start()

    lanes = lax.broadcasted_iota(jnp.int32, (BLOCK, HEAD), 1)
    sublanes = lax.broadcasted_iota(jnp.int32, (BLOCK, HEAD), 0)
    inverse = inverse_ref[...]
    for r in range(2):
        tokens = me * ROWS + r * BLOCK + sublanes
        angle = (tokens - starts_of(tokens, bounds_ref)).astype(jnp.float32) * inverse
        turn = jnp.sin(angle)
        cosine[pl.ds(r * BLOCK, BLOCK), :] = jnp.cos(angle)
        sine[pl.ds(r * BLOCK, BLOCK), :] = jnp.where(lanes < HEAD // 2, -turn, turn)

    place = jnp.minimum(jnp.maximum(sublanes - me * PORTION, 0), PORTION)

    def mark(b, carry):
        tokens = b * BLOCK + sublanes
        document = jnp.zeros_like(tokens)
        for i in range(1, 8):
            document = jnp.where(tokens >= bounds_ref[i], i, document)
        spot = 8 + lax.rem(b, SPAN) * (PORTION + 1) + place
        hit = (lanes == document) | (lanes == spot)
        mark_ref[pl.ds(pl.multiple_of(b * BLOCK, BLOCK), BLOCK), :] = (
            hit.astype(jnp.float32).astype(jnp.bfloat16)
        )
        return carry

    lax.fori_loop(0, NBLK // 2, mark, 0)
    weights[0].wait()
    weights[1].wait()
    weights[2].wait()

    def rotate(raw, row, count):
        table = pl.ds(row, count)
        return raw * cosine[table, :] + pltpu.roll(raw, HEAD // 2, 1) * sine[table, :]

    def queries(r, n):
        columns = slice(n * 2 * HEAD, (n + 1) * 2 * HEAD)
        rows = pl.ds(r * BLOCK, BLOCK)
        raw = jnp.dot(full[rows, :], wq[:, columns], preferred_element_type=jnp.float32)
        turned = jnp.concatenate(
            [rotate(raw[:, :HEAD], r * BLOCK, BLOCK), rotate(raw[:, HEAD:], r * BLOCK, BLOCK)],
            axis=1,
        )
        qtmp[pl.ds((n // 2) * BLOCK, BLOCK), (n % 2) * 2 * HEAD : (n % 2 + 1) * 2 * HEAD] = (
            turned.astype(jnp.bfloat16)
        )

    def gather(which, r):
        buffer = (k_ref, v_ref)[which]
        a, b = ((xcoord, ycoord), (ycoord, xcoord))[which]

        def neighbour(along, step):
            if along == 0:
                na, nb = lax.rem(a + step, 4), b
            else:
                na, nb = a, lax.rem(b + step, 4)
            x, y = ((na, nb), (nb, na))[which]
            return (x * 4 + y) * 2 + core

        def copy(n, ref, target):
            return pltpu.make_async_remote_copy(
                src_ref=ref,
                dst_ref=ref,
                send_sem=g_send.at[r],
                recv_sem=g_recv.at[r, n],
                device_id={"cp": target},
                device_id_type=MESH,
            )

        def piece(at, row, count):
            rows = pl.ds(STARTS[r] + row, count)
            if which == 0:
                return buffer.at[at, b, core, rows]
            return buffer.at[b, at, core, rows]

        def line(at, first, count):
            along, rows = pl.ds(first, count), pl.ds(STARTS[r], SIZES[r])
            if which == 0:
                return buffer.at[along, at, core, rows]
            return buffer.at[at, along, core, rows]

        a_next, a_prev = lax.rem(a + 1, 4), lax.rem(a + 3, 4)
        b_next, b_prev = lax.rem(b + 1, 4), lax.rem(b + 3, 4)
        b_far = lax.rem(b + 2, 4)
        size, half = SIZES[r], SIZES[r] // 2
        return dict(
            ring1=(
                copy(0, piece(a, 0, size), neighbour(0, 1)),
                copy(0, piece(a, 0, size), neighbour(0, 3)),
            ),
            ring1_far=(copy(1, piece(a, 0, size), neighbour(0, 2)),)
            if STRAIGHT1[r]
            else (
                copy(1, piece(a_prev, 0, half), neighbour(0, 1)),
                copy(1, piece(a_next, half, half), neighbour(0, 3)),
            ),
            ring2=(
                copy(2, line(b, 0, 4), neighbour(1, 1)),
                copy(2, line(b, 0, 4), neighbour(1, 3)),
            ),
            ring2_far=(copy(3, line(b, 0, 4), neighbour(1, 2)),)
            if STRAIGHT2[r]
            else (
                copy(3, line(b_prev, 0, 2), neighbour(1, 1)),
                copy(3, line(b_next, 2, 2), neighbour(1, 3)),
            ),
            across=(
                copy(4, line(b, 0, 4), partner),
                copy(4, line(b_prev, 0, 4), partner),
                copy(4, line(b_next, 0, 4), partner),
                copy(4, line(b_far, 0, 4), partner),
            ),
        )

    flows = [[gather(which, r) for which in range(2)] for r in range(PARTS)]

    def start(r, name):
        for flow in flows[r]:
            for copy in flow[name]:
                copy.start()

    def arrived(r, name):
        rows = pl.ds(STARTS[r], SIZES[r])
        n, ref = {
            "ring1": (0, k_ref.at[0, :, core, rows]),
            "ring1_far": (1, k_ref.at[0, pl.ds(0, 2), core, rows]),
            "ring2": (2, k_ref.at[:, :, core, rows]),
            "ring2_far": (3, k_ref.at[pl.ds(0, 2), :, core, rows]),
            "across": (4, k_ref.at[:, :, :, rows]),
        }[name]
        wait_for(ref, g_recv.at[r, n])

    def across(r, which):
        for flow in flows[r]:
            for n in which:
                flow["across"][n].start()

    def s0(r):
        arrived_z(1, r, 1)
        rows = pl.ds(STARTS[r], SIZES[r])
        raw = jnp.dot(full[rows, :], wkv[...], preferred_element_type=jnp.float32)
        k_ref[xcoord, ycoord, core, rows] = rotate(raw[:, :HEAD], STARTS[r], SIZES[r]).astype(
            jnp.bfloat16
        )
        v_ref[xcoord, ycoord, core, rows] = raw[:, HEAD:].astype(jnp.bfloat16)
        start(r, "ring1")
        if STRAIGHT1[r]:
            start(r, "ring1_far")

    def s1(r):
        arrived(r, "ring1")
        if not STRAIGHT1[r]:
            start(r, "ring1_far")

    def s2(r):
        arrived(r, "ring1_far")
        start(r, "ring2")
        if STRAIGHT2[r]:
            start(r, "ring2_far")
        across(r, (0,))

    def s3(r):
        arrived(r, "ring2")
        if not STRAIGHT2[r]:
            start(r, "ring2_far")
        across(r, (1, 2))

    def s4(r):
        arrived(r, "ring2_far")
        across(r, (3,))

    out_row = lax.broadcasted_iota(jnp.int32, (ROWS, ROWS), 0)
    in_row = lax.broadcasted_iota(jnp.int32, (ROWS, ROWS), 1)
    origin = lax.rem(out_row // 4, 2) * BLOCK + (out_row // 8) * 4 + lax.rem(out_row, 4)
    pick = (in_row == origin).astype(jnp.float32).astype(jnp.bfloat16)

    def qcopy(r, target, slot):
        return pltpu.make_async_remote_copy(
            src_ref=qsend.at[r, target],
            dst_ref=q_ref.at[slot, r],
            send_sem=q_send.at[r],
            recv_sem=q_recv.at[r],
            device_id={"cp": target},
            device_id_type=MESH,
        )

    def spread(r):
        ordered = jnp.dot(pick, qtmp[...], preferred_element_type=jnp.float32)
        qsend[r] = ordered.reshape(CP, 8, WIDTH // 2).astype(jnp.bfloat16)
        q_ref[me, r] = qsend[r, me]

        def send(k, carry):
            qcopy(r, lax.rem(me + k, CP), me).start()
            return carry

        lax.fori_loop(1, CP, send, 0)

    def spread_done(r):
        sent, landed = qsend.at[r, pl.ds(0, CP - 1)], q_ref.at[pl.ds(0, CP - 1), r]
        pltpu.make_async_copy(sent, sent, q_send.at[r]).wait()
        pltpu.make_async_copy(landed, landed, q_recv.at[r]).wait()

    relay_z(0)
    pl.semaphore_wait(met.at[0], 3)
    signal(met.at[1], partner)
    lax.fori_loop(NBLK // 2, NBLK, mark, 0)
    relay_z(1)
    pl.semaphore_wait(met.at[1], 1)
    s0(0)
    relay_z(2)
    s1(0)
    s0(1)
    s2(0)
    queries(0, 0)
    queries(0, 1)
    relay_z(3)
    queries(0, 2)
    queries(0, 3)
    s0(2)
    s1(1)
    spread(0)
    relay_z(4)
    s0(3)
    s3(0)
    s1(2)
    s2(1)
    s4(0)
    s0(4)
    s2(2)
    queries(1, 0)
    queries(1, 1)
    queries(1, 2)
    queries(1, 3)
    s1(3)
    spread(1)
    s2(3)
    s3(1)
    s1(4)
    s2(4)
    s3(2)
    s3(3)
    s4(1)
    s3(4)
    s4(2)
    s4(4)
    s4(3)
    spread_done(0)
    spread_done(1)
    for r in range(PARTS):
        arrived(r, "across")
        wait_for(mark_ref.at[pl.ds(0, 62 * SIZES[r])], g_send.at[r])
    wait_for(full.at[:, pl.ds(0, 3 * WIDTH)], z_send.at[0])


def gather_call(bounds, hidden, wq, wk, wv, inverse):
    vmem = pl.BlockSpec(memory_space=pltpu.VMEM)
    hbm = pl.BlockSpec(memory_space=pltpu.HBM)
    kv = jax.ShapeDtypeStruct((4, 4, 2, ROWS, HEAD), jnp.bfloat16)
    dma = pltpu.SemaphoreType.DMA
    return pl.pallas_call(
        gather_kernel,
        out_shape=(
            kv,
            kv,
            jax.ShapeDtypeStruct((CP, 2, 8, WIDTH // 2), jnp.bfloat16),
            jax.ShapeDtypeStruct((TOKENS, HEAD), jnp.bfloat16),
        ),
        in_specs=[hbm, hbm, hbm, hbm, hbm, vmem],
        out_specs=(vmem, vmem, vmem, vmem),
        scratch_shapes=[
            pltpu.VMEM((ROWS, TP * WIDTH), jnp.bfloat16),
            pltpu.VMEM((TP * WIDTH, WIDTH), jnp.bfloat16),
            pltpu.VMEM((TP * WIDTH, 2 * HEAD), jnp.bfloat16),
            pltpu.VMEM((ROWS, WIDTH // 2), jnp.bfloat16),
            pltpu.VMEM((2, CP, 8, WIDTH // 2), jnp.bfloat16),
            pltpu.VMEM((ROWS, HEAD), jnp.float32),
            pltpu.VMEM((ROWS, HEAD), jnp.float32),
            dma((5,)), dma((1,)), dma((2 * PARTS,)),
            dma((PARTS,)), dma((PARTS, 5)), dma((2,)), dma((2,)),
            pltpu.SMEM((9,), jnp.int32), pltpu.SemaphoreType.REGULAR((2,)),
        ],
        compiler_params=pltpu.CompilerParams(
            collective_id=0, has_side_effects=True, vmem_limit_bytes=32 * 1024 * 1024
        ),
        name="gather_project",
    )(bounds, hidden, wq, wk, wv, inverse)


TILE = SPAN * BLOCK


GROUPS = NBLK // SPAN
QROWS = 4 * SPAN * 8
PIECE = 256


def attend_kernel(
    bounds_ref, q_ref, k_ref, v_ref, mark_ref, o_ref,
    turned, penalty_ref, even, odd, mixed_ref, total_ref,
):
    rows = SPAN * 8
    factor = math.log2(math.e) / math.sqrt(HEAD)
    row = lax.rem(lax.broadcasted_iota(jnp.int32, (rows, HEAD), 0), rows)
    lane = lax.broadcasted_iota(jnp.int32, (rows, HEAD), 1)
    block, step = row // 8, lax.rem(row, PORTION)
    key_block, key_step = (lane - 8) // (PORTION + 1), lax.rem(lane - 8, PORTION + 1)
    later = (key_block > block) | ((key_block == block) & (key_step > step))
    later = later & (lane >= 8) & (lane < 8 + SPAN * (PORTION + 1))
    me = lax.axis_index("cp")
    contract_last = (((1,), (1,)), ((), ()))
    diagonal = lax.broadcasted_iota(jnp.int32, (HEAD, HEAD), 0) == lax.broadcasted_iota(
        jnp.int32, (HEAD, HEAD), 1
    )
    identity = diagonal.astype(jnp.float32).astype(jnp.bfloat16)

    def prepare(g, carry):
        at = pl.ds(pl.multiple_of(g * TILE, TILE), TILE)
        turned[:, at] = lax.dot_general(
            identity, v_ref[at, :], contract_last, preferred_element_type=jnp.float32
        ).astype(jnp.bfloat16)
        tokens = (g * SPAN + block) * BLOCK + me * PORTION + step
        document = jnp.zeros_like(tokens)
        for i in range(1, 8):
            document = jnp.where(tokens >= bounds_ref[i], i, document)
        other = (lane < 8) & (lane != document)
        penalty_ref[2 * g] = jnp.where(other, PENALTY, 0.0).astype(jnp.bfloat16)
        penalty_ref[2 * g + 1] = jnp.where(other | later, PENALTY, 0.0).astype(jnp.bfloat16)
        return carry

    lax.fori_loop(0, GROUPS, prepare, 0)

    def lowest(g):
        low = jnp.int32(0)
        for i in range(1, 8):
            low = jnp.where(g * TILE >= bounds_ref[i], bounds_ref[i], low)
        return low // TILE

    def following(item):
        g, j = item
        more = j > lowest(g)
        return jnp.where(more, g, g + 1), jnp.where(more, j - 1, g + 1)

    def score(item, ref):
        g, j = item
        own = jnp.where(g == j, 1, 0)
        held = jnp.minimum(g, GROUPS - 1)
        penalties = penalty_ref[2 * held + own]
        asking = pl.ds(pl.multiple_of(held * rows, rows), rows)
        q = jnp.concatenate(
            [
                jnp.concatenate([q_ref[asking, h * HEAD : (h + 1) * HEAD], penalties], axis=1)
                for h in range(4)
            ],
            axis=0,
        )
        for part in range(2):
            size = TILE // 2
            first = jnp.minimum(j, GROUPS - 1) * TILE + part * size
            at = pl.ds(pl.multiple_of(first, size), size)
            scores = lax.dot_general(
                jnp.concatenate([k_ref[at, :], mark_ref[at, :]], axis=1),
                q,
                contract_last,
                preferred_element_type=jnp.float32,
            )
            ref[part * size : (part + 1) * size, :] = scores
            top = jnp.max(scores, axis=0, keepdims=True)
            largest = top if part == 0 else jnp.maximum(largest, top)
        return largest

    def soften(item, ref, largest, state):
        g, j = item
        top, total, mixed = state
        top = jnp.where(g == j, 0.5 * PENALTY, top)
        start = jnp.minimum(j, GROUPS - 1) * TILE
        new_top = jnp.maximum(top, largest)
        shrink = jnp.exp2((top - new_top) * factor)
        total, mixed = total * shrink, mixed * shrink
        for first in range(0, TILE, PIECE):
            piece = slice(first, first + PIECE)
            weights = jnp.exp2((ref[piece, :] - new_top) * factor)
            total = total + jnp.sum(weights, axis=0, keepdims=True)
            keys = pl.ds(pl.multiple_of(start + first, PIECE), PIECE)
            mixed = mixed + jnp.dot(
                turned[:, keys], weights.astype(jnp.bfloat16), preferred_element_type=jnp.float32
            )
        mixed_ref[g] = mixed
        total_ref[g] = total
        return new_top, total, mixed

    count = lax.fori_loop(0, GROUPS, lambda g, n: n + g + 1 - lowest(g), jnp.int32(0))
    zero = jnp.int32(0)
    highest = score((zero, zero), even)

    def pair(n, carry):
        g, j, largest, *state = carry
        item = (g, j)
        second = following(item)
        second_largest = score(second, odd)
        state = soften(item, even, largest, state)
        third = following(second)
        third = (jnp.minimum(third[0], GROUPS), jnp.minimum(third[1], GROUPS))
        largest = score(third, even)
        state = soften(second, odd, second_largest, state)
        return (*third, largest, *state)

    lax.fori_loop(
        0,
        (count + 1) // 2,
        pair,
        (
            zero,
            zero,
            highest,
            jnp.full((1, QROWS), 0.5 * PENALTY, jnp.float32),
            jnp.zeros((1, QROWS), jnp.float32),
            jnp.zeros((HEAD, QROWS), jnp.float32),
        ),
    )

    def finish(g, carry):
        o_ref[g] = (mixed_ref[g] / total_ref[g]).astype(jnp.bfloat16)
        return carry

    lax.fori_loop(0, GROUPS, finish, 0)


def attend_call(bounds, q, k, v, marks):
    vmem = pl.BlockSpec(memory_space=pltpu.VMEM)
    return pl.pallas_call(
        attend_kernel,
        out_shape=jax.ShapeDtypeStruct((GROUPS, HEAD, QROWS), jnp.bfloat16),
        in_specs=[pl.BlockSpec(memory_space=pltpu.SMEM), vmem, vmem, vmem, vmem],
        out_specs=vmem,
        scratch_shapes=[
            pltpu.VMEM((HEAD, TOKENS), jnp.bfloat16),
            pltpu.VMEM((2 * GROUPS, SPAN * 8, HEAD), jnp.bfloat16),
            pltpu.VMEM((TILE, QROWS), jnp.float32),
            pltpu.VMEM((TILE, QROWS), jnp.float32),
            pltpu.VMEM((GROUPS + 1, HEAD, QROWS), jnp.float32),
            pltpu.VMEM((GROUPS + 1, 1, QROWS), jnp.float32),
        ],
        compiler_params=pltpu.CompilerParams(vmem_limit_bytes=28 * 1024 * 1024),
        name="attend",
    )(bounds, q, k, v, marks)


CHUNKS = (2, 2, 2, 1, 1)
FIRST = (0, 2, 4, 6, 7)
PIECES = WIDTH // HEAD


def output_kernel(
    slot_ref, heads_ref, wo_ref, out_ref,
    heads, wo, far, near, far_in, near_in, spread, landed, own_sum,
    w_sem, z_send, z_recv, a_send, a_recv,
):
    me = lax.axis_index("cp")
    tp = lax.axis_index("tp")
    up, down, across = lax.rem(tp + 1, TP), lax.rem(tp + 3, TP), lax.rem(tp + 2, TP)

    loads = []
    for n, t in enumerate((across, up, down, tp)):
        columns = pl.ds(pl.multiple_of(t * WIDTH, WIDTH), WIDTH)
        loads.append(pltpu.make_async_copy(wo_ref.at[:, columns], wo.at[n], w_sem.at[n]))
        loads[-1].start()

    barrier = pltpu.get_barrier_semaphore()

    def greet(k, carry):
        pl.semaphore_signal(
            barrier, inc=1, device_id={"cp": lax.rem(me + k, CP)}, device_id_type=MESH
        )
        return carry

    pl.semaphore_signal(barrier, inc=1, device_id={"tp": up}, device_id_type=MESH)
    pl.semaphore_signal(barrier, inc=1, device_id={"tp": down}, device_id_type=MESH)
    lax.fori_loop(1, CP, greet, 0)

    turned_row = lax.broadcasted_iota(jnp.int32, (QROWS, QROWS), 0)
    turned_column = lax.broadcasted_iota(jnp.int32, (QROWS, QROWS), 1)
    rows = SPAN * PORTION
    head, at_row = turned_row // rows, lax.rem(turned_row, rows)
    source = (
        lax.rem(head, 4) * 2 * rows
        + (at_row // PORTION) * 2 * PORTION
        + (head // 4) * PORTION
        + lax.rem(at_row, PORTION)
    )
    select = (turned_column == source).astype(jnp.float32).astype(jnp.bfloat16)
    for g in range(GROUPS):
        part = lax.dot_general(
            select,
            heads_ref[g],
            (((1,), (1,)), ((), ())),
            preferred_element_type=jnp.float32,
        ).astype(jnp.bfloat16)
        for h in range(HEADS):
            heads[g * rows : (g + 1) * rows, h * HEAD : (h + 1) * HEAD] = part[
                h * rows : (h + 1) * rows
            ]

    def product(n, c):
        columns = slice(FIRST[c] * HEAD, (FIRST[c] + CHUNKS[c]) * HEAD)
        return jnp.dot(heads[...], wo[n, :, columns], preferred_element_type=jnp.float32)

    def remote(n, src, dst, target):
        return pltpu.make_async_remote_copy(
            src_ref=src,
            dst_ref=dst,
            send_sem=z_send.at[0],
            recv_sem=z_recv.at[n],
            device_id={"tp": target},
            device_id_type=MESH,
        )

    half = ROWS // 2
    upper, lower = pl.ds(0, half), pl.ds(half, half)
    far_copies, near_copies = [], []
    for c, count in enumerate(CHUNKS):
        at = pl.ds(FIRST[c], count)
        far_copies.append(
            (
                remote(3 * c, far.at[0, at], far_in.at[0, at], up),
                remote(3 * c + 1, far.at[1, at], far_in.at[1, at], down),
            )
        )
        near_copies.append(
            (
                remote(3 * c + 2, near.at[0, at], near_in.at[0, at], up),
                remote(3 * c + 2, near.at[1, at], near_in.at[1, at], down),
            )
        )

    def pieces(c):
        return [(FIRST[c] + n, slice(n * HEAD, (n + 1) * HEAD)) for n in range(CHUNKS[c])]

    def make_far(c):
        value = product(0, c).astype(jnp.bfloat16)
        for at, columns in pieces(c):
            far[0, at] = value[:half, columns]
            far[1, at] = value[half:, columns]

    def send_far(c):
        for copy in far_copies[c]:
            copy.start()

    def send_near(c):
        to_up, to_down = product(1, c), product(2, c)
        far_copies[c][0].wait_recv()
        for at, columns in pieces(c):
            near[0, at, upper] = (
                to_up[:half, columns] + far_in[0, at].astype(jnp.float32)
            ).astype(jnp.bfloat16)
            near[0, at, lower] = to_up[half:, columns].astype(jnp.bfloat16)
        near_copies[c][0].start()
        far_copies[c][1].wait_recv()
        for at, columns in pieces(c):
            near[1, at, upper] = to_down[:half, columns].astype(jnp.bfloat16)
            near[1, at, lower] = (
                to_down[half:, columns] + far_in[1, at].astype(jnp.float32)
            ).astype(jnp.bfloat16)
        near_copies[c][1].start()

    def sum_own(c):
        value = product(3, c)
        for at, columns in pieces(c):
            own_sum[at] = value[:, columns]

    row = lax.broadcasted_iota(jnp.int32, (ROWS, ROWS), 0)
    column = lax.broadcasted_iota(jnp.int32, (ROWS, ROWS), 1)
    to_owner = (row == slot_ref[...]).astype(jnp.float32).astype(jnp.bfloat16)
    origin = (lax.rem(row, BLOCK) // 4) * 8 + (row // BLOCK) * 4 + lax.rem(row, 4)
    to_place = (column == origin).astype(jnp.float32).astype(jnp.bfloat16)

    def acopy(c, target, slot):
        at = pl.ds(FIRST[c], CHUNKS[c])
        return pltpu.make_async_remote_copy(
            src_ref=spread.at[target, at],
            dst_ref=landed.at[slot, at],
            send_sem=a_send.at[c],
            recv_sem=a_recv.at[c],
            device_id={"cp": target},
            device_id_type=MESH,
        )

    def finish_sum(c):
        both = near_in.at[:, pl.ds(FIRST[c], CHUNKS[c])]
        pltpu.make_async_copy(both, both, z_recv.at[3 * c + 2]).wait()
        total = jnp.concatenate(
            [
                (
                    own_sum[at]
                    + near_in[0, at].astype(jnp.float32)
                    + near_in[1, at].astype(jnp.float32)
                ).astype(jnp.bfloat16)
                for at, columns in pieces(c)
            ],
            axis=1,
        )
        picked = jnp.dot(to_owner, total, preferred_element_type=jnp.float32)
        for at, columns in pieces(c):
            spread[:, at] = picked[:, columns].reshape(CP, 8, HEAD).astype(jnp.bfloat16)
            landed[me, at] = spread[me, at]

        def send(k, carry):
            acopy(c, lax.rem(me + k, CP), me).start()
            return carry

        lax.fori_loop(1, CP, send, 0)

    def place(c):
        everyone = landed.at[pl.ds(0, CP - 1), pl.ds(FIRST[c], CHUNKS[c])]
        pltpu.make_async_copy(everyone, everyone, a_recv.at[c]).wait()
        rows = jnp.concatenate(
            [
                landed[:, at].astype(jnp.float32).reshape(ROWS, HEAD).astype(jnp.bfloat16)
                for at, columns in pieces(c)
            ],
            axis=1,
        )
        out_ref[:, FIRST[c] * HEAD : (FIRST[c] + CHUNKS[c]) * HEAD] = jnp.dot(
            to_place, rows, preferred_element_type=jnp.float32
        ).astype(jnp.bfloat16)

    loads[0].wait()
    make_far(0)
    pl.semaphore_wait(barrier, CP + 1)
    send_far(0)
    make_far(1)
    send_far(1)
    make_far(2)
    send_far(2)
    loads[1].wait()
    loads[2].wait()
    send_near(0)
    make_far(3)
    send_far(3)
    send_near(1)
    make_far(4)
    send_far(4)
    send_near(2)
    loads[3].wait()
    for c in range(len(CHUNKS)):
        sum_own(c)
    send_near(3)
    finish_sum(0)
    send_near(4)
    finish_sum(1)
    finish_sum(2)
    finish_sum(3)
    finish_sum(4)
    for c in range(len(CHUNKS)):
        place(c)
    for c in range(len(CHUNKS)):
        everyone = spread.at[pl.ds(0, CP - 1), pl.ds(FIRST[c], CHUNKS[c])]
        pltpu.make_async_copy(everyone, everyone, a_send.at[c]).wait()
    sent = wo.at[0, pl.ds(0, 3 * ROWS)]
    pltpu.make_async_copy(sent, sent, z_send.at[0]).wait()


def output_call(slot_rows, heads, wo):
    vmem = pl.BlockSpec(memory_space=pltpu.VMEM)
    dma = pltpu.SemaphoreType.DMA
    half = ROWS // 2
    bf16 = jnp.bfloat16
    return pl.pallas_call(
        output_kernel,
        out_shape=jax.ShapeDtypeStruct((ROWS, WIDTH), bf16),
        in_specs=[vmem, vmem, pl.BlockSpec(memory_space=pltpu.HBM)],
        out_specs=vmem,
        scratch_shapes=[
            pltpu.VMEM((ROWS, WIDTH), bf16),
            pltpu.VMEM((TP, WIDTH, WIDTH), bf16),
            pltpu.VMEM((2, PIECES, half, HEAD), bf16),
            pltpu.VMEM((2, PIECES, ROWS, HEAD), bf16),
            pltpu.VMEM((2, PIECES, half, HEAD), bf16),
            pltpu.VMEM((2, PIECES, ROWS, HEAD), bf16),
            pltpu.VMEM((CP, PIECES, 8, HEAD), bf16),
            pltpu.VMEM((CP, PIECES, 8, HEAD), bf16),
            pltpu.VMEM((PIECES, ROWS, HEAD), jnp.float32),
            dma((4,)), dma((1,)), dma((3 * len(CHUNKS),)),
            dma((len(CHUNKS),)), dma((len(CHUNKS),)),
        ],
        compiler_params=pltpu.CompilerParams(
            collective_id=1, has_side_effects=True, vmem_limit_bytes=40 * 1024 * 1024
        ),
        name="project_out",
    )(slot_rows, heads, wo)


def local(hidden, query_weight, key_matrix, value_matrix, output_weight, bounds, block_owner):
    inverse = rope_inverse(HEAD)
    inverse = jnp.concatenate([inverse, inverse])[None, :]
    slots = slots_of(block_owner)
    slot_rows = (slots[:, None] * PORTION + jnp.arange(PORTION, dtype=jnp.int32)[None, :]).reshape(
        1, ROWS
    )
    hidden, query_weight, key_matrix, value_matrix, output_weight = (
        pltpu.with_memory_space_constraint(a, pltpu.HBM)
        for a in (hidden, query_weight, key_matrix, value_matrix, output_weight)
    )
    keys, values, queries, marks = gather_call(
        pltpu.with_memory_space_constraint(bounds, pltpu.HBM), hidden, query_weight, key_matrix, value_matrix, inverse
    )
    heads = attend_call(
        bounds,
        queries.reshape(2 * ROWS, WIDTH // 2),
        keys.reshape(TOKENS, HEAD),
        values.reshape(TOKENS, HEAD),
        marks,
    )
    return output_call(slot_rows, heads, output_weight)


def solution(mesh):
    placed = (P("cp", "tp"), P(None, "tp"), P(None, "tp"), P(None, "tp"), P("tp", None), P(), P())
    return jax.shard_map(
        local, mesh=mesh, in_specs=placed, out_specs=P("cp", "tp"), check_vma=False
    )
```

```python
import functools
import math

import jax
import jax.numpy as jnp
from jax import lax
from jax.experimental import pallas as pl
from jax.experimental.pallas import tpu as pltpu
from jax.sharding import PartitionSpec as P

HEAD = 128
BLOCK = 128
CP = 32
TP = 4
ROWS = 256
WIDTH = 1024
NBLK = 64
HEADS = 8
TOKENS = 8192
PORTION = BLOCK // CP

rope_theta = 500000.0
rope_factor = 8.0
rope_context = 8192.0
masked_score = -1e30
MESH = pl.DeviceIdType.MESH


def rope_inverse(head_size):
    halves = jnp.arange(head_size // 2, dtype=jnp.float32)
    inverse = 1.0 / rope_theta ** (2.0 * halves / head_size)
    wavelength = 2.0 * math.pi / inverse
    smooth = (rope_context / wavelength - 1.0) / 3.0
    blended = (1.0 - smooth) * inverse / rope_factor + smooth * inverse
    longer = jnp.where(wavelength > rope_context, inverse / rope_factor, blended)
    return jnp.where(wavelength < rope_context / 4.0, inverse, longer)


def slots_of(block_owner):
    blocks = jnp.arange(NBLK, dtype=jnp.int32)
    same = block_owner[:, None] == block_owner[None, :]
    earlier = blocks[None, :] < blocks[:, None]
    rank = jnp.sum((same & earlier).astype(jnp.int32), axis=1)
    return block_owner * 2 + rank


def starts_of(tokens, bounds_ref):
    start = jnp.zeros_like(tokens)
    for i in range(1, 8):
        bound = bounds_ref[i]
        start = jnp.where(tokens >= bound, bound, start)
    return start


SIZES = (64, 64, 64, 32, 32)
STARTS = (0, 64, 128, 192, 224)
PARTS = len(SIZES)
STRAIGHT1 = (True, False, True, True, True)
STRAIGHT2 = (True, False, False, False, True)
SPAN = 8
PENALTY = -1e30


def gather_kernel(
    bounds_hbm, hidden_ref, wq_ref, wk_ref, wv_ref, inverse_ref,
    k_ref, v_ref, q_ref, mark_ref,
    full, wq, wkv, qtmp, qsend, cosine, sine,
    w_sem, z_send, z_recv, g_send, g_recv, q_send, q_recv, bounds_ref, met,
):
    me = lax.axis_index("cp")
    tp = lax.axis_index("tp")
    core = lax.rem(me, 2)
    ycoord = lax.rem(me // 2, 4)
    xcoord = me // 8
    partner = me + 1 - 2 * core
    up, down = lax.rem(tp + 1, TP), lax.rem(tp + 3, TP)
    own_columns = pl.ds(pl.multiple_of(tp * WIDTH, WIDTH), WIDTH)

    bring = pltpu.make_async_copy(hidden_ref, full.at[:, own_columns], w_sem.at[3])
    weights = [
        pltpu.make_async_copy(wk_ref, wkv.at[:, pl.ds(0, HEAD)], w_sem.at[0]),
        pltpu.make_async_copy(wv_ref, wkv.at[:, pl.ds(HEAD, HEAD)], w_sem.at[1]),
        pltpu.make_async_copy(wq_ref, wq, w_sem.at[2]),
    ]
    bring_bounds = pltpu.make_async_copy(bounds_hbm, bounds_ref, w_sem.at[4])
    bring.start()
    bring_bounds.start()
    for copy in weights:
        copy.start()

    barrier = pltpu.get_barrier_semaphore()

    def signal(semaphore, target):
        pl.semaphore_signal(semaphore, inc=1, device_id={"cp": target}, device_id_type=MESH)

    along_x = [(lax.rem(xcoord + n, 4) * 4 + ycoord) * 2 + core for n in (1, 2, 3)]
    along_y = [(xcoord * 4 + lax.rem(ycoord + n, 4)) * 2 + core for n in (1, 2, 3)]
    pl.semaphore_signal(barrier, inc=1, device_id={"tp": up}, device_id_type=MESH)
    pl.semaphore_signal(barrier, inc=1, device_id={"tp": down}, device_id_type=MESH)
    for target in (*along_x, *along_y, partner):
        signal(barrier, target)
    bring.wait()
    pl.semaphore_wait(barrier, 9)

    def zcopy(n, target, owner, row, count):
        columns = pl.ds(pl.multiple_of(owner * WIDTH, WIDTH), WIDTH)
        ref = full.at[pl.ds(row, count), columns]
        return pltpu.make_async_remote_copy(
            src_ref=ref,
            dst_ref=ref,
            send_sem=z_send.at[0],
            recv_sem=z_recv.at[n],
            device_id={"tp": target},
            device_id_type=MESH,
        )

    own = [
        (
            zcopy(2 * r, up, tp, STARTS[r], SIZES[r]),
            zcopy(2 * r, down, tp, STARTS[r], SIZES[r]),
        )
        for r in range(PARTS)
    ]
    fwd = [
        (
            zcopy(2 * r + 1, down, up, STARTS[r], SIZES[r] // 2),
            zcopy(2 * r + 1, up, down, STARTS[r] + SIZES[r] // 2, SIZES[r] // 2),
        )
        for r in range(PARTS)
    ]

    def wait_for(ref, semaphore):
        pltpu.make_async_copy(ref, ref, semaphore).wait()

    def arrived_z(n, r, owners):
        wait_for(
            full.at[pl.ds(STARTS[r], SIZES[r]), pl.ds(0, owners * WIDTH)], z_recv.at[2 * r + n]
        )
    for copy in (*own[0], *own[1]):
        copy.start()
    for target in along_x:
        signal(met.at[0], target)
    bring_bounds.wait()

    def relay_z(r):
        arrived_z(0, r, 2)
        for copy in fwd[r]:
            copy.start()
        if r + 2 < PARTS:
            for copy in own[r + 2]:
                copy.start()

    lanes = lax.broadcasted_iota(jnp.int32, (BLOCK, HEAD), 1)
    sublanes = lax.broadcasted_iota(jnp.int32, (BLOCK, HEAD), 0)
    inverse = inverse_ref[...]
    for r in range(2):
        tokens = me * ROWS + r * BLOCK + sublanes
        angle = (tokens - starts_of(tokens, bounds_ref)).astype(jnp.float32) * inverse
        turn = jnp.sin(angle)
        cosine[pl.ds(r * BLOCK, BLOCK), :] = jnp.cos(angle)
        sine[pl.ds(r * BLOCK, BLOCK), :] = jnp.where(lanes < HEAD // 2, -turn, turn)

    place = jnp.minimum(jnp.maximum(sublanes - me * PORTION, 0), PORTION)

    def mark(b, carry):
        tokens = b * BLOCK + sublanes
        document = jnp.zeros_like(tokens)
        for i in range(1, 8):
            document = jnp.where(tokens >= bounds_ref[i], i, document)
        spot = 8 + lax.rem(b, SPAN) * (PORTION + 1) + place
        hit = (lanes == document) | (lanes == spot)
        mark_ref[pl.ds(pl.multiple_of(b * BLOCK, BLOCK), BLOCK), :] = (
            hit.astype(jnp.float32).astype(jnp.bfloat16)
        )
        return carry

    lax.fori_loop(0, NBLK // 2, mark, 0)
    weights[0].wait()
    weights[1].wait()
    weights[2].wait()

    def rotate(raw, row, count):
        table = pl.ds(row, count)
        return raw * cosine[table, :] + pltpu.roll(raw, HEAD // 2, 1) * sine[table, :]

    def queries(r, n):
        columns = slice(n * 2 * HEAD, (n + 1) * 2 * HEAD)
        rows = pl.ds(r * BLOCK, BLOCK)
        raw = jnp.dot(full[rows, :], wq[:, columns], preferred_element_type=jnp.float32)
        turned = jnp.concatenate(
            [rotate(raw[:, :HEAD], r * BLOCK, BLOCK), rotate(raw[:, HEAD:], r * BLOCK, BLOCK)],
            axis=1,
        )
        qtmp[pl.ds((n // 2) * BLOCK, BLOCK), (n % 2) * 2 * HEAD : (n % 2 + 1) * 2 * HEAD] = (
            turned.astype(jnp.bfloat16)
        )

    def gather(which, r):
        buffer = (k_ref, v_ref)[which]
        a, b = ((xcoord, ycoord), (ycoord, xcoord))[which]

        def neighbour(along, step):
            if along == 0:
                na, nb = lax.rem(a + step, 4), b
            else:
                na, nb = a, lax.rem(b + step, 4)
            x, y = ((na, nb), (nb, na))[which]
            return (x * 4 + y) * 2 + core

        def copy(n, ref, target):
            return pltpu.make_async_remote_copy(
                src_ref=ref,
                dst_ref=ref,
                send_sem=g_send.at[r],
                recv_sem=g_recv.at[r, n],
                device_id={"cp": target},
                device_id_type=MESH,
            )

        def piece(at, row, count):
            rows = pl.ds(STARTS[r] + row, count)
            if which == 0:
                return buffer.at[at, b, core, rows]
            return buffer.at[b, at, core, rows]

        def line(at, first, count):
            along, rows = pl.ds(first, count), pl.ds(STARTS[r], SIZES[r])
            if which == 0:
                return buffer.at[along, at, core, rows]
            return buffer.at[at, along, core, rows]

        a_next, a_prev = lax.rem(a + 1, 4), lax.rem(a + 3, 4)
        b_next, b_prev = lax.rem(b + 1, 4), lax.rem(b + 3, 4)
        b_far = lax.rem(b + 2, 4)
        size, half = SIZES[r], SIZES[r] // 2
        return dict(
            ring1=(
                copy(0, piece(a, 0, size), neighbour(0, 1)),
                copy(0, piece(a, 0, size), neighbour(0, 3)),
            ),
            ring1_far=(copy(1, piece(a, 0, size), neighbour(0, 2)),)
            if STRAIGHT1[r]
            else (
                copy(1, piece(a_prev, 0, half), neighbour(0, 1)),
                copy(1, piece(a_next, half, half), neighbour(0, 3)),
            ),
            ring2=(
                copy(2, line(b, 0, 4), neighbour(1, 1)),
                copy(2, line(b, 0, 4), neighbour(1, 3)),
            ),
            ring2_far=(copy(3, line(b, 0, 4), neighbour(1, 2)),)
            if STRAIGHT2[r]
            else (
                copy(3, line(b_prev, 0, 2), neighbour(1, 1)),
                copy(3, line(b_next, 2, 2), neighbour(1, 3)),
            ),
            across=(
                copy(4, line(b, 0, 4), partner),
                copy(4, line(b_prev, 0, 4), partner),
                copy(4, line(b_next, 0, 4), partner),
                copy(4, line(b_far, 0, 4), partner),
            ),
        )

    flows = [[gather(which, r) for which in range(2)] for r in range(PARTS)]

    def start(r, name):
        for flow in flows[r]:
            for copy in flow[name]:
                copy.start()

    def arrived(r, name):
        rows = pl.ds(STARTS[r], SIZES[r])
        n, ref = {
            "ring1": (0, k_ref.at[0, :, core, rows]),
            "ring1_far": (1, k_ref.at[0, pl.ds(0, 2), core, rows]),
            "ring2": (2, k_ref.at[:, :, core, rows]),
            "ring2_far": (3, k_ref.at[pl.ds(0, 2), :, core, rows]),
            "across": (4, k_ref.at[:, :, :, rows]),
        }[name]
        wait_for(ref, g_recv.at[r, n])

    def across(r, which):
        for flow in flows[r]:
            for n in which:
                flow["across"][n].start()

    def s0(r):
        arrived_z(1, r, 1)
        rows = pl.ds(STARTS[r], SIZES[r])
        raw = jnp.dot(full[rows, :], wkv[...], preferred_element_type=jnp.float32)
        k_ref[xcoord, ycoord, core, rows] = rotate(raw[:, :HEAD], STARTS[r], SIZES[r]).astype(
            jnp.bfloat16
        )
        v_ref[xcoord, ycoord, core, rows] = raw[:, HEAD:].astype(jnp.bfloat16)
        start(r, "ring1")
        if STRAIGHT1[r]:
            start(r, "ring1_far")

    def s1(r):
        arrived(r, "ring1")
        if not STRAIGHT1[r]:
            start(r, "ring1_far")

    def s2(r):
        arrived(r, "ring1_far")
        start(r, "ring2")
        if STRAIGHT2[r]:
            start(r, "ring2_far")
        across(r, (0,))

    def s3(r):
        arrived(r, "ring2")
        if not STRAIGHT2[r]:
            start(r, "ring2_far")
        across(r, (1, 2))

    def s4(r):
        arrived(r, "ring2_far")
        across(r, (3,))

    out_row = lax.broadcasted_iota(jnp.int32, (ROWS, ROWS), 0)
    in_row = lax.broadcasted_iota(jnp.int32, (ROWS, ROWS), 1)
    origin = lax.rem(out_row // 4, 2) * BLOCK + (out_row // 8) * 4 + lax.rem(out_row, 4)
    pick = (in_row == origin).astype(jnp.float32).astype(jnp.bfloat16)

    def qcopy(r, target, slot):
        return pltpu.make_async_remote_copy(
            src_ref=qsend.at[r, target],
            dst_ref=q_ref.at[slot, r],
            send_sem=q_send.at[r],
            recv_sem=q_recv.at[r],
            device_id={"cp": target},
            device_id_type=MESH,
        )

    def spread(r):
        ordered = jnp.dot(pick, qtmp[...], preferred_element_type=jnp.float32)
        qsend[r] = ordered.reshape(CP, 8, WIDTH // 2).astype(jnp.bfloat16)
        q_ref[me, r] = qsend[r, me]

        def send(k, carry):
            qcopy(r, lax.rem(me + k, CP), me).start()
            return carry

        lax.fori_loop(1, CP, send, 0)

    def spread_done(r):
        sent, landed = qsend.at[r, pl.ds(0, CP - 1)], q_ref.at[pl.ds(0, CP - 1), r]
        pltpu.make_async_copy(sent, sent, q_send.at[r]).wait()
        pltpu.make_async_copy(landed, landed, q_recv.at[r]).wait()

    relay_z(0)
    pl.semaphore_wait(met.at[0], 3)
    signal(met.at[1], partner)
    lax.fori_loop(NBLK // 2, NBLK, mark, 0)
    relay_z(1)
    pl.semaphore_wait(met.at[1], 1)
    s0(0)
    relay_z(2)
    s1(0)
    s0(1)
    s2(0)
    queries(0, 0)
    queries(0, 1)
    relay_z(3)
    queries(0, 2)
    queries(0, 3)
    s0(2)
    s1(1)
    spread(0)
    relay_z(4)
    s0(3)
    s3(0)
    s1(2)
    s2(1)
    s4(0)
    s0(4)
    s2(2)
    queries(1, 0)
    queries(1, 1)
    queries(1, 2)
    queries(1, 3)
    s1(3)
    spread(1)
    s2(3)
    s3(1)
    s1(4)
    s2(4)
    s3(2)
    s3(3)
    s4(1)
    s3(4)
    s4(2)
    s4(4)
    s4(3)
    spread_done(0)
    spread_done(1)
    for r in range(PARTS):
        arrived(r, "across")
        wait_for(mark_ref.at[pl.ds(0, 62 * SIZES[r])], g_send.at[r])
    wait_for(full.at[:, pl.ds(0, 3 * WIDTH)], z_send.at[0])


def gather_call(bounds, hidden, wq, wk, wv, inverse):
    vmem = pl.BlockSpec(memory_space=pltpu.VMEM)
    hbm = pl.BlockSpec(memory_space=pltpu.HBM)
    kv = jax.ShapeDtypeStruct((4, 4, 2, ROWS, HEAD), jnp.bfloat16)
    dma = pltpu.SemaphoreType.DMA
    return pl.pallas_call(
        gather_kernel,
        out_shape=(
            kv,
            kv,
            jax.ShapeDtypeStruct((CP, 2, 8, WIDTH // 2), jnp.bfloat16),
            jax.ShapeDtypeStruct((TOKENS, HEAD), jnp.bfloat16),
        ),
        in_specs=[hbm, hbm, hbm, hbm, hbm, vmem],
        out_specs=(vmem, vmem, vmem, vmem),
        scratch_shapes=[
            pltpu.VMEM((ROWS, TP * WIDTH), jnp.bfloat16),
            pltpu.VMEM((TP * WIDTH, WIDTH), jnp.bfloat16),
            pltpu.VMEM((TP * WIDTH, 2 * HEAD), jnp.bfloat16),
            pltpu.VMEM((ROWS, WIDTH // 2), jnp.bfloat16),
            pltpu.VMEM((2, CP, 8, WIDTH // 2), jnp.bfloat16),
            pltpu.VMEM((ROWS, HEAD), jnp.float32),
            pltpu.VMEM((ROWS, HEAD), jnp.float32),
            dma((5,)), dma((1,)), dma((2 * PARTS,)),
            dma((PARTS,)), dma((PARTS, 5)), dma((2,)), dma((2,)),
            pltpu.SMEM((9,), jnp.int32), pltpu.SemaphoreType.REGULAR((2,)),
        ],
        compiler_params=pltpu.CompilerParams(
            collective_id=0, has_side_effects=True, vmem_limit_bytes=32 * 1024 * 1024
        ),
        name="gather_project",
    )(bounds, hidden, wq, wk, wv, inverse)


TILE = SPAN * BLOCK


GROUPS = NBLK // SPAN
QROWS = 4 * SPAN * 8
PIECE = 256


def attend_kernel(
    bounds_ref, q_ref, k_ref, v_ref, mark_ref, o_ref,
    turned, penalty_ref, even, odd, even_soft, odd_soft, mixed_ref, total_ref,
):
    rows = SPAN * 8
    factor = math.log2(math.e) / math.sqrt(HEAD)
    row = lax.rem(lax.broadcasted_iota(jnp.int32, (rows, HEAD), 0), rows)
    lane = lax.broadcasted_iota(jnp.int32, (rows, HEAD), 1)
    block, step = row // 8, lax.rem(row, PORTION)
    key_block, key_step = (lane - 8) // (PORTION + 1), lax.rem(lane - 8, PORTION + 1)
    later = (key_block > block) | ((key_block == block) & (key_step > step))
    later = later & (lane >= 8) & (lane < 8 + SPAN * (PORTION + 1))
    me = lax.axis_index("cp")
    contract_last = (((1,), (1,)), ((), ()))
    diagonal = lax.broadcasted_iota(jnp.int32, (HEAD, HEAD), 0) == lax.broadcasted_iota(
        jnp.int32, (HEAD, HEAD), 1
    )
    identity = diagonal.astype(jnp.float32).astype(jnp.bfloat16)

    def prepare(g, carry):
        at = pl.ds(pl.multiple_of(g * TILE, TILE), TILE)
        turned[:, at] = lax.dot_general(
            identity, v_ref[at, :], contract_last, preferred_element_type=jnp.float32
        ).astype(jnp.bfloat16)
        tokens = (g * SPAN + block) * BLOCK + me * PORTION + step
        document = jnp.zeros_like(tokens)
        for i in range(1, 8):
            document = jnp.where(tokens >= bounds_ref[i], i, document)
        other = (lane < 8) & (lane != document)
        penalty_ref[2 * g] = jnp.where(other, PENALTY, 0.0).astype(jnp.bfloat16)
        penalty_ref[2 * g + 1] = jnp.where(other | later, PENALTY, 0.0).astype(jnp.bfloat16)
        return carry

    lax.fori_loop(0, GROUPS, prepare, 0)

    def lowest(g):
        low = jnp.int32(0)
        for i in range(1, 8):
            low = jnp.where(g * TILE >= bounds_ref[i], bounds_ref[i], low)
        return low // TILE

    def following(item):
        g, j = item
        more = j > lowest(g)
        return jnp.where(more, g, g + 1), jnp.where(more, j - 1, g + 1)

    def score(item, ref):
        g, j = item
        own = jnp.where(g == j, 1, 0)
        held = jnp.minimum(g, GROUPS - 1)
        penalties = penalty_ref[2 * held + own]
        asking = pl.ds(pl.multiple_of(held * rows, rows), rows)
        q = jnp.concatenate(
            [
                jnp.concatenate([q_ref[asking, h * HEAD : (h + 1) * HEAD], penalties], axis=1)
                for h in range(4)
            ],
            axis=0,
        )
        for part in range(2):
            size = TILE // 2
            first = jnp.minimum(j, GROUPS - 1) * TILE + part * size
            at = pl.ds(pl.multiple_of(first, size), size)
            scores = lax.dot_general(
                jnp.concatenate([k_ref[at, :], mark_ref[at, :]], axis=1),
                q,
                contract_last,
                preferred_element_type=jnp.float32,
            )
            ref[part * size : (part + 1) * size, :] = scores
            top = jnp.max(scores, axis=0, keepdims=True)
            largest = top if part == 0 else jnp.maximum(largest, top)
        return largest

    def soften(item, ref, soft, largest, top, total):
        g, j = item
        top = jnp.where(g == j, 0.5 * PENALTY, top)
        new_top = jnp.maximum(top, largest)
        shrink = jnp.exp2((top - new_top) * factor)
        total = total * shrink
        for first in range(0, TILE, PIECE):
            piece = slice(first, first + PIECE)
            weights = jnp.exp2((ref[piece, :] - new_top) * factor)
            total = total + jnp.sum(weights, axis=0, keepdims=True)
            soft[piece, :] = weights.astype(jnp.bfloat16)
        total_ref[g] = total
        return new_top, total, shrink

    def blend(item, soft, shrink, mixed):
        g, j = item
        first = pl.multiple_of(jnp.minimum(j, GROUPS - 1) * TILE, TILE)
        mixed = mixed * shrink + jnp.dot(
            turned[:, pl.ds(first, TILE)], soft[...], preferred_element_type=jnp.float32
        )
        mixed_ref[g] = mixed
        return mixed

    count = lax.fori_loop(0, GROUPS, lambda g, n: n + g + 1 - lowest(g), jnp.int32(0))
    zero = jnp.int32(0)
    highest = score((zero, zero), even)
    odd_soft[...] = jnp.zeros_like(odd_soft)

    def pair(n, carry):
        g, j, largest, last_g, last_j, last_shrink, top, total, mixed = carry
        item = (g, j)
        second = following(item)
        second_largest = score(second, odd)
        mixed = blend((last_g, last_j), odd_soft, last_shrink, mixed)
        top, total, shrink = soften(item, even, even_soft, largest, top, total)
        third = following(second)
        third = (jnp.minimum(third[0], GROUPS), jnp.minimum(third[1], GROUPS))
        largest = score(third, even)
        mixed = blend(item, even_soft, shrink, mixed)
        top, total, shrink = soften(second, odd, odd_soft, second_largest, top, total)
        return (*third, largest, *second, shrink, top, total, mixed)

    row_of = functools.partial(jnp.full, (1, QROWS), dtype=jnp.float32)
    carry = lax.fori_loop(
        0,
        (count + 1) // 2,
        pair,
        (
            zero,
            zero,
            highest,
            jnp.int32(GROUPS),
            zero,
            row_of(0.0),
            row_of(0.5 * PENALTY),
            row_of(0.0),
            jnp.zeros((HEAD, QROWS), jnp.float32),
        ),
    )
    blend(carry[3:5], odd_soft, carry[5], carry[8])

    def finish(g, carry):
        o_ref[g] = (mixed_ref[g] / total_ref[g]).astype(jnp.bfloat16)
        return carry

    lax.fori_loop(0, GROUPS, finish, 0)


def attend_call(bounds, q, k, v, marks):
    vmem = pl.BlockSpec(memory_space=pltpu.VMEM)
    return pl.pallas_call(
        attend_kernel,
        out_shape=jax.ShapeDtypeStruct((GROUPS, HEAD, QROWS), jnp.bfloat16),
        in_specs=[pl.BlockSpec(memory_space=pltpu.SMEM), vmem, vmem, vmem, vmem],
        out_specs=vmem,
        scratch_shapes=[
            pltpu.VMEM((HEAD, TOKENS), jnp.bfloat16),
            pltpu.VMEM((2 * GROUPS, SPAN * 8, HEAD), jnp.bfloat16),
            pltpu.VMEM((TILE, QROWS), jnp.float32),
            pltpu.VMEM((TILE, QROWS), jnp.float32),
            pltpu.VMEM((TILE, QROWS), jnp.bfloat16),
            pltpu.VMEM((TILE, QROWS), jnp.bfloat16),
            pltpu.VMEM((GROUPS + 1, HEAD, QROWS), jnp.float32),
            pltpu.VMEM((GROUPS + 1, 1, QROWS), jnp.float32),
        ],
        compiler_params=pltpu.CompilerParams(vmem_limit_bytes=28 * 1024 * 1024),
        name="attend",
    )(bounds, q, k, v, marks)


CHUNKS = (2, 2, 2, 1, 1)
FIRST = (0, 2, 4, 6, 7)
PIECES = WIDTH // HEAD


def output_kernel(
    slot_ref, heads_ref, wo_ref, out_ref,
    heads, wo, far, near, far_in, near_in, spread, landed, own_sum,
    w_sem, z_send, z_recv, a_send, a_recv,
):
    me = lax.axis_index("cp")
    tp = lax.axis_index("tp")
    up, down, across = lax.rem(tp + 1, TP), lax.rem(tp + 3, TP), lax.rem(tp + 2, TP)

    loads = []
    for n, t in enumerate((across, up, down, tp)):
        columns = pl.ds(pl.multiple_of(t * WIDTH, WIDTH), WIDTH)
        loads.append(pltpu.make_async_copy(wo_ref.at[:, columns], wo.at[n], w_sem.at[n]))
        loads[-1].start()

    barrier = pltpu.get_barrier_semaphore()

    def greet(k, carry):
        pl.semaphore_signal(
            barrier, inc=1, device_id={"cp": lax.rem(me + k, CP)}, device_id_type=MESH
        )
        return carry

    pl.semaphore_signal(barrier, inc=1, device_id={"tp": up}, device_id_type=MESH)
    pl.semaphore_signal(barrier, inc=1, device_id={"tp": down}, device_id_type=MESH)
    lax.fori_loop(1, CP, greet, 0)

    turned_row = lax.broadcasted_iota(jnp.int32, (QROWS, QROWS), 0)
    turned_column = lax.broadcasted_iota(jnp.int32, (QROWS, QROWS), 1)
    rows = SPAN * PORTION
    head, at_row = turned_row // rows, lax.rem(turned_row, rows)
    source = (
        lax.rem(head, 4) * 2 * rows
        + (at_row // PORTION) * 2 * PORTION
        + (head // 4) * PORTION
        + lax.rem(at_row, PORTION)
    )
    select = (turned_column == source).astype(jnp.float32).astype(jnp.bfloat16)
    for g in range(GROUPS):
        part = lax.dot_general(
            select,
            heads_ref[g],
            (((1,), (1,)), ((), ())),
            preferred_element_type=jnp.float32,
        ).astype(jnp.bfloat16)
        for h in range(HEADS):
            heads[g * rows : (g + 1) * rows, h * HEAD : (h + 1) * HEAD] = part[
                h * rows : (h + 1) * rows
            ]

    def product(n, c):
        columns = slice(FIRST[c] * HEAD, (FIRST[c] + CHUNKS[c]) * HEAD)
        return jnp.dot(heads[...], wo[n, :, columns], preferred_element_type=jnp.float32)

    def remote(n, src, dst, target):
        return pltpu.make_async_remote_copy(
            src_ref=src,
            dst_ref=dst,
            send_sem=z_send.at[0],
            recv_sem=z_recv.at[n],
            device_id={"tp": target},
            device_id_type=MESH,
        )

    half = ROWS // 2
    upper, lower = pl.ds(0, half), pl.ds(half, half)
    far_copies, near_copies = [], []
    for c, count in enumerate(CHUNKS):
        at = pl.ds(FIRST[c], count)
        far_copies.append(
            (
                remote(3 * c, far.at[0, at], far_in.at[0, at], up),
                remote(3 * c + 1, far.at[1, at], far_in.at[1, at], down),
            )
        )
        near_copies.append(
            (
                remote(3 * c + 2, near.at[0, at], near_in.at[0, at], up),
                remote(3 * c + 2, near.at[1, at], near_in.at[1, at], down),
            )
        )

    def pieces(c):
        return [(FIRST[c] + n, slice(n * HEAD, (n + 1) * HEAD)) for n in range(CHUNKS[c])]

    def make_far(c):
        value = product(0, c).astype(jnp.bfloat16)
        for at, columns in pieces(c):
            far[0, at] = value[:half, columns]
            far[1, at] = value[half:, columns]

    def send_far(c):
        for copy in far_copies[c]:
            copy.start()

    def send_near(c):
        to_up, to_down = product(1, c), product(2, c)
        far_copies[c][0].wait_recv()
        for at, columns in pieces(c):
            near[0, at, upper] = (
                to_up[:half, columns] + far_in[0, at].astype(jnp.float32)
            ).astype(jnp.bfloat16)
            near[0, at, lower] = to_up[half:, columns].astype(jnp.bfloat16)
        near_copies[c][0].start()
        far_copies[c][1].wait_recv()
        for at, columns in pieces(c):
            near[1, at, upper] = to_down[:half, columns].astype(jnp.bfloat16)
            near[1, at, lower] = (
                to_down[half:, columns] + far_in[1, at].astype(jnp.float32)
            ).astype(jnp.bfloat16)
        near_copies[c][1].start()

    def sum_own(c):
        value = product(3, c)
        for at, columns in pieces(c):
            own_sum[at] = value[:, columns]

    row = lax.broadcasted_iota(jnp.int32, (ROWS, ROWS), 0)
    column = lax.broadcasted_iota(jnp.int32, (ROWS, ROWS), 1)
    to_owner = (row == slot_ref[...]).astype(jnp.float32).astype(jnp.bfloat16)
    origin = (lax.rem(row, BLOCK) // 4) * 8 + (row // BLOCK) * 4 + lax.rem(row, 4)
    to_place = (column == origin).astype(jnp.float32).astype(jnp.bfloat16)

    def acopy(c, target, slot):
        at = pl.ds(FIRST[c], CHUNKS[c])
        return pltpu.make_async_remote_copy(
            src_ref=spread.at[target, at],
            dst_ref=landed.at[slot, at],
            send_sem=a_send.at[c],
            recv_sem=a_recv.at[c],
            device_id={"cp": target},
            device_id_type=MESH,
        )

    def finish_sum(c):
        both = near_in.at[:, pl.ds(FIRST[c], CHUNKS[c])]
        pltpu.make_async_copy(both, both, z_recv.at[3 * c + 2]).wait()
        total = jnp.concatenate(
            [
                (
                    own_sum[at]
                    + near_in[0, at].astype(jnp.float32)
                    + near_in[1, at].astype(jnp.float32)
                ).astype(jnp.bfloat16)
                for at, columns in pieces(c)
            ],
            axis=1,
        )
        picked = jnp.dot(to_owner, total, preferred_element_type=jnp.float32)
        for at, columns in pieces(c):
            spread[:, at] = picked[:, columns].reshape(CP, 8, HEAD).astype(jnp.bfloat16)
            landed[me, at] = spread[me, at]

        def send(k, carry):
            acopy(c, lax.rem(me + k, CP), me).start()
            return carry

        lax.fori_loop(1, CP, send, 0)

    def place(c):
        everyone = landed.at[pl.ds(0, CP - 1), pl.ds(FIRST[c], CHUNKS[c])]
        pltpu.make_async_copy(everyone, everyone, a_recv.at[c]).wait()
        rows = jnp.concatenate(
            [
                landed[:, at].astype(jnp.float32).reshape(ROWS, HEAD).astype(jnp.bfloat16)
                for at, columns in pieces(c)
            ],
            axis=1,
        )
        out_ref[:, FIRST[c] * HEAD : (FIRST[c] + CHUNKS[c]) * HEAD] = jnp.dot(
            to_place, rows, preferred_element_type=jnp.float32
        ).astype(jnp.bfloat16)

    loads[0].wait()
    make_far(0)
    pl.semaphore_wait(barrier, CP + 1)
    send_far(0)
    make_far(1)
    send_far(1)
    make_far(2)
    send_far(2)
    loads[1].wait()
    loads[2].wait()
    send_near(0)
    make_far(3)
    send_far(3)
    send_near(1)
    make_far(4)
    send_far(4)
    send_near(2)
    loads[3].wait()
    for c in range(len(CHUNKS)):
        sum_own(c)
    send_near(3)
    finish_sum(0)
    send_near(4)
    finish_sum(1)
    finish_sum(2)
    finish_sum(3)
    finish_sum(4)
    for c in range(len(CHUNKS)):
        place(c)
    for c in range(len(CHUNKS)):
        everyone = spread.at[pl.ds(0, CP - 1), pl.ds(FIRST[c], CHUNKS[c])]
        pltpu.make_async_copy(everyone, everyone, a_send.at[c]).wait()
    sent = wo.at[0, pl.ds(0, 3 * ROWS)]
    pltpu.make_async_copy(sent, sent, z_send.at[0]).wait()


def output_call(slot_rows, heads, wo):
    vmem = pl.BlockSpec(memory_space=pltpu.VMEM)
    dma = pltpu.SemaphoreType.DMA
    half = ROWS // 2
    bf16 = jnp.bfloat16
    return pl.pallas_call(
        output_kernel,
        out_shape=jax.ShapeDtypeStruct((ROWS, WIDTH), bf16),
        in_specs=[vmem, vmem, pl.BlockSpec(memory_space=pltpu.HBM)],
        out_specs=vmem,
        scratch_shapes=[
            pltpu.VMEM((ROWS, WIDTH), bf16),
            pltpu.VMEM((TP, WIDTH, WIDTH), bf16),
            pltpu.VMEM((2, PIECES, half, HEAD), bf16),
            pltpu.VMEM((2, PIECES, ROWS, HEAD), bf16),
            pltpu.VMEM((2, PIECES, half, HEAD), bf16),
            pltpu.VMEM((2, PIECES, ROWS, HEAD), bf16),
            pltpu.VMEM((CP, PIECES, 8, HEAD), bf16),
            pltpu.VMEM((CP, PIECES, 8, HEAD), bf16),
            pltpu.VMEM((PIECES, ROWS, HEAD), jnp.float32),
            dma((4,)), dma((1,)), dma((3 * len(CHUNKS),)),
            dma((len(CHUNKS),)), dma((len(CHUNKS),)),
        ],
        compiler_params=pltpu.CompilerParams(
            collective_id=1, has_side_effects=True, vmem_limit_bytes=40 * 1024 * 1024
        ),
        name="project_out",
    )(slot_rows, heads, wo)


def local(hidden, query_weight, key_matrix, value_matrix, output_weight, bounds, block_owner):
    inverse = rope_inverse(HEAD)
    inverse = jnp.concatenate([inverse, inverse])[None, :]
    slots = slots_of(block_owner)
    slot_rows = (slots[:, None] * PORTION + jnp.arange(PORTION, dtype=jnp.int32)[None, :]).reshape(
        1, ROWS
    )
    hidden, query_weight, key_matrix, value_matrix, output_weight = (
        pltpu.with_memory_space_constraint(a, pltpu.HBM)
        for a in (hidden, query_weight, key_matrix, value_matrix, output_weight)
    )
    keys, values, queries, marks = gather_call(
        pltpu.with_memory_space_constraint(bounds, pltpu.HBM), hidden, query_weight, key_matrix, value_matrix, inverse
    )
    heads = attend_call(
        bounds,
        queries.reshape(2 * ROWS, WIDTH // 2),
        keys.reshape(TOKENS, HEAD),
        values.reshape(TOKENS, HEAD),
        marks,
    )
    return output_call(slot_rows, heads, output_weight)


def solution(mesh):
    placed = (P("cp", "tp"), P(None, "tp"), P(None, "tp"), P(None, "tp"), P("tp", None), P(), P())
    return jax.shard_map(
        local, mesh=mesh, in_specs=placed, out_specs=P("cp", "tp"), check_vma=False
    )
```

```python
import functools
import math

import jax
import jax.numpy as jnp
from jax import lax
from jax.experimental import pallas as pl
from jax.experimental.pallas import tpu as pltpu
from jax.sharding import PartitionSpec as P

HEAD = 128
BLOCK = 128
CP = 32
TP = 4
ROWS = 256
WIDTH = 1024
NBLK = 64
HEADS = 8
TOKENS = 8192
PORTION = BLOCK // CP

rope_theta = 500000.0
rope_factor = 8.0
rope_context = 8192.0
masked_score = -1e30
MESH = pl.DeviceIdType.MESH


def rope_inverse(head_size):
    halves = jnp.arange(head_size // 2, dtype=jnp.float32)
    inverse = 1.0 / rope_theta ** (2.0 * halves / head_size)
    wavelength = 2.0 * math.pi / inverse
    smooth = (rope_context / wavelength - 1.0) / 3.0
    blended = (1.0 - smooth) * inverse / rope_factor + smooth * inverse
    longer = jnp.where(wavelength > rope_context, inverse / rope_factor, blended)
    return jnp.where(wavelength < rope_context / 4.0, inverse, longer)


def slots_of(block_owner):
    blocks = jnp.arange(NBLK, dtype=jnp.int32)
    same = block_owner[:, None] == block_owner[None, :]
    earlier = blocks[None, :] < blocks[:, None]
    rank = jnp.sum((same & earlier).astype(jnp.int32), axis=1)
    return block_owner * 2 + rank


def starts_of(tokens, bounds_ref):
    start = jnp.zeros_like(tokens)
    for i in range(1, 8):
        bound = bounds_ref[i]
        start = jnp.where(tokens >= bound, bound, start)
    return start


def to_others(me, send):
    core, ycoord, xcoord = lax.rem(me, 2), lax.rem(me // 2, 4), me // 8

    def offset(n):
        return 2 - n + 3 * (n // 2) - 2 * (n // 3)

    def step(n, carry):
        chip = lax.rem(xcoord + offset(n // 4), 4) * 4 + lax.rem(ycoord + offset(lax.rem(n, 4)), 4)
        send(chip * 2 + core)
        send(chip * 2 + 1 - core)
        return carry

    lax.fori_loop(0, 15, step, 0)
    send(me + 1 - 2 * core)


SIZES = (64, 64, 64, 32, 32)
STARTS = (0, 64, 128, 192, 224)
PARTS = len(SIZES)
STRAIGHT1 = (True, False, True, True, True)
STRAIGHT2 = (True, False, False, False, True)
SPAN = 8
PENALTY = -1e30


def gather_kernel(
    bounds_hbm, hidden_ref, wq_ref, wk_ref, wv_ref, inverse_ref,
    k_ref, v_ref, q_ref, mark_ref,
    full, wq, wkv, qtmp, qsend, cosine, sine,
    w_sem, z_send, z_recv, g_send, g_recv, q_send, q_recv, bounds_ref, met,
):
    me = lax.axis_index("cp")
    tp = lax.axis_index("tp")
    core = lax.rem(me, 2)
    ycoord = lax.rem(me // 2, 4)
    xcoord = me // 8
    partner = me + 1 - 2 * core
    up, down = lax.rem(tp + 1, TP), lax.rem(tp + 3, TP)
    own_columns = pl.ds(pl.multiple_of(tp * WIDTH, WIDTH), WIDTH)

    bring = pltpu.make_async_copy(hidden_ref, full.at[:, own_columns], w_sem.at[3])
    weights = [
        pltpu.make_async_copy(wk_ref, wkv.at[:, pl.ds(0, HEAD)], w_sem.at[0]),
        pltpu.make_async_copy(wv_ref, wkv.at[:, pl.ds(HEAD, HEAD)], w_sem.at[1]),
        pltpu.make_async_copy(wq_ref, wq, w_sem.at[2]),
    ]
    bring_bounds = pltpu.make_async_copy(bounds_hbm, bounds_ref, w_sem.at[4])
    bring.start()
    bring_bounds.start()
    for copy in weights:
        copy.start()

    barrier = pltpu.get_barrier_semaphore()

    def signal(semaphore, target):
        pl.semaphore_signal(semaphore, inc=1, device_id={"cp": target}, device_id_type=MESH)

    along_x = [(lax.rem(xcoord + n, 4) * 4 + ycoord) * 2 + core for n in (1, 2, 3)]
    along_y = [(xcoord * 4 + lax.rem(ycoord + n, 4)) * 2 + core for n in (1, 2, 3)]
    pl.semaphore_signal(barrier, inc=1, device_id={"tp": up}, device_id_type=MESH)
    pl.semaphore_signal(barrier, inc=1, device_id={"tp": down}, device_id_type=MESH)
    for target in (*along_x, *along_y, partner):
        signal(barrier, target)
    bring.wait()
    pl.semaphore_wait(barrier, 9)

    def zcopy(n, target, owner, row, count):
        columns = pl.ds(pl.multiple_of(owner * WIDTH, WIDTH), WIDTH)
        ref = full.at[pl.ds(row, count), columns]
        return pltpu.make_async_remote_copy(
            src_ref=ref,
            dst_ref=ref,
            send_sem=z_send.at[0],
            recv_sem=z_recv.at[n],
            device_id={"tp": target},
            device_id_type=MESH,
        )

    own = [
        (
            zcopy(2 * r, up, tp, STARTS[r], SIZES[r]),
            zcopy(2 * r, down, tp, STARTS[r], SIZES[r]),
        )
        for r in range(PARTS)
    ]
    fwd = [
        (
            zcopy(2 * r + 1, down, up, STARTS[r], SIZES[r] // 2),
            zcopy(2 * r + 1, up, down, STARTS[r] + SIZES[r] // 2, SIZES[r] // 2),
        )
        for r in range(PARTS)
    ]

    def wait_for(ref, semaphore):
        pltpu.make_async_copy(ref, ref, semaphore).wait()

    def arrived_z(n, r, owners):
        wait_for(
            full.at[pl.ds(STARTS[r], SIZES[r]), pl.ds(0, owners * WIDTH)], z_recv.at[2 * r + n]
        )
    for copy in (*own[0], *own[1]):
        copy.start()
    for target in along_x:
        signal(met.at[0], target)
    bring_bounds.wait()

    def relay_z(r):
        arrived_z(0, r, 2)
        for copy in fwd[r]:
            copy.start()
        if r + 2 < PARTS:
            for copy in own[r + 2]:
                copy.start()

    lanes = lax.broadcasted_iota(jnp.int32, (BLOCK, HEAD), 1)
    sublanes = lax.broadcasted_iota(jnp.int32, (BLOCK, HEAD), 0)
    inverse = inverse_ref[...]
    for r in range(2):
        tokens = me * ROWS + r * BLOCK + sublanes
        angle = (tokens - starts_of(tokens, bounds_ref)).astype(jnp.float32) * inverse
        turn = jnp.sin(angle)
        cosine[pl.ds(r * BLOCK, BLOCK), :] = jnp.cos(angle)
        sine[pl.ds(r * BLOCK, BLOCK), :] = jnp.where(lanes < HEAD // 2, -turn, turn)

    place = jnp.minimum(jnp.maximum(sublanes - me * PORTION, 0), PORTION)

    def mark(b, carry):
        tokens = b * BLOCK + sublanes
        document = jnp.zeros_like(tokens)
        for i in range(1, 8):
            document = jnp.where(tokens >= bounds_ref[i], i, document)
        spot = 8 + lax.rem(b, SPAN) * (PORTION + 1) + place
        hit = (lanes == document) | (lanes == spot)
        mark_ref[pl.ds(pl.multiple_of(b * BLOCK, BLOCK), BLOCK), :] = (
            hit.astype(jnp.float32).astype(jnp.bfloat16)
        )
        return carry

    lax.fori_loop(0, NBLK // 2, mark, 0)
    weights[0].wait()
    weights[1].wait()
    weights[2].wait()

    def rotate(raw, row, count):
        table = pl.ds(row, count)
        return raw * cosine[table, :] + pltpu.roll(raw, HEAD // 2, 1) * sine[table, :]

    def queries(r, n):
        columns = slice(n * 2 * HEAD, (n + 1) * 2 * HEAD)
        rows = pl.ds(r * BLOCK, BLOCK)
        raw = jnp.dot(full[rows, :], wq[:, columns], preferred_element_type=jnp.float32)
        turned = jnp.concatenate(
            [rotate(raw[:, :HEAD], r * BLOCK, BLOCK), rotate(raw[:, HEAD:], r * BLOCK, BLOCK)],
            axis=1,
        )
        qtmp[pl.ds((n // 2) * BLOCK, BLOCK), (n % 2) * 2 * HEAD : (n % 2 + 1) * 2 * HEAD] = (
            turned.astype(jnp.bfloat16)
        )

    def gather(which, r):
        buffer = (k_ref, v_ref)[which]
        a, b = ((xcoord, ycoord), (ycoord, xcoord))[which]

        def neighbour(along, step):
            if along == 0:
                na, nb = lax.rem(a + step, 4), b
            else:
                na, nb = a, lax.rem(b + step, 4)
            x, y = ((na, nb), (nb, na))[which]
            return (x * 4 + y) * 2 + core

        def copy(n, ref, target):
            return pltpu.make_async_remote_copy(
                src_ref=ref,
                dst_ref=ref,
                send_sem=g_send.at[r],
                recv_sem=g_recv.at[r, n],
                device_id={"cp": target},
                device_id_type=MESH,
            )

        def piece(at, row, count):
            rows = pl.ds(STARTS[r] + row, count)
            if which == 0:
                return buffer.at[at, b, core, rows]
            return buffer.at[b, at, core, rows]

        def line(at, first, count):
            along, rows = pl.ds(first, count), pl.ds(STARTS[r], SIZES[r])
            if which == 0:
                return buffer.at[along, at, core, rows]
            return buffer.at[at, along, core, rows]

        a_next, a_prev = lax.rem(a + 1, 4), lax.rem(a + 3, 4)
        b_next, b_prev = lax.rem(b + 1, 4), lax.rem(b + 3, 4)
        b_far = lax.rem(b + 2, 4)
        size, half = SIZES[r], SIZES[r] // 2
        return dict(
            ring1=(
                copy(0, piece(a, 0, size), neighbour(0, 1)),
                copy(0, piece(a, 0, size), neighbour(0, 3)),
            ),
            ring1_far=(copy(1, piece(a, 0, size), neighbour(0, 2)),)
            if STRAIGHT1[r]
            else (
                copy(1, piece(a_prev, 0, half), neighbour(0, 1)),
                copy(1, piece(a_next, half, half), neighbour(0, 3)),
            ),
            ring2=(
                copy(2, line(b, 0, 4), neighbour(1, 1)),
                copy(2, line(b, 0, 4), neighbour(1, 3)),
            ),
            ring2_far=(copy(3, line(b, 0, 4), neighbour(1, 2)),)
            if STRAIGHT2[r]
            else (
                copy(3, line(b_prev, 0, 2), neighbour(1, 1)),
                copy(3, line(b_next, 2, 2), neighbour(1, 3)),
            ),
            across=(
                copy(4, line(b, 0, 4), partner),
                copy(4, line(b_prev, 0, 4), partner),
                copy(4, line(b_next, 0, 4), partner),
                copy(4, line(b_far, 0, 4), partner),
            ),
        )

    flows = [[gather(which, r) for which in range(2)] for r in range(PARTS)]

    def start(r, name):
        for flow in flows[r]:
            for copy in flow[name]:
                copy.start()

    def arrived(r, name):
        rows = pl.ds(STARTS[r], SIZES[r])
        n, ref = {
            "ring1": (0, k_ref.at[0, :, core, rows]),
            "ring1_far": (1, k_ref.at[0, pl.ds(0, 2), core, rows]),
            "ring2": (2, k_ref.at[:, :, core, rows]),
            "ring2_far": (3, k_ref.at[pl.ds(0, 2), :, core, rows]),
            "across": (4, k_ref.at[:, :, :, rows]),
        }[name]
        wait_for(ref, g_recv.at[r, n])

    def across(r, which):
        for flow in flows[r]:
            for n in which:
                flow["across"][n].start()

    def s0(r):
        arrived_z(1, r, 1)
        rows = pl.ds(STARTS[r], SIZES[r])
        raw = jnp.dot(full[rows, :], wkv[...], preferred_element_type=jnp.float32)
        k_ref[xcoord, ycoord, core, rows] = rotate(raw[:, :HEAD], STARTS[r], SIZES[r]).astype(
            jnp.bfloat16
        )
        v_ref[xcoord, ycoord, core, rows] = raw[:, HEAD:].astype(jnp.bfloat16)
        start(r, "ring1")
        if STRAIGHT1[r]:
            start(r, "ring1_far")

    def s1(r):
        arrived(r, "ring1")
        if not STRAIGHT1[r]:
            start(r, "ring1_far")

    def s2(r):
        arrived(r, "ring1_far")
        start(r, "ring2")
        if STRAIGHT2[r]:
            start(r, "ring2_far")
        across(r, (0,))

    def s3(r):
        arrived(r, "ring2")
        if not STRAIGHT2[r]:
            start(r, "ring2_far")
        across(r, (1, 2))

    def s4(r):
        arrived(r, "ring2_far")
        across(r, (3,))

    out_row = lax.broadcasted_iota(jnp.int32, (ROWS, ROWS), 0)
    in_row = lax.broadcasted_iota(jnp.int32, (ROWS, ROWS), 1)
    origin = lax.rem(out_row // 4, 2) * BLOCK + (out_row // 8) * 4 + lax.rem(out_row, 4)
    pick = (in_row == origin).astype(jnp.float32).astype(jnp.bfloat16)

    def qcopy(r, target, slot):
        return pltpu.make_async_remote_copy(
            src_ref=qsend.at[r, target],
            dst_ref=q_ref.at[slot, r],
            send_sem=q_send.at[r],
            recv_sem=q_recv.at[r],
            device_id={"cp": target},
            device_id_type=MESH,
        )

    def spread(r):
        ordered = jnp.dot(pick, qtmp[...], preferred_element_type=jnp.float32)
        qsend[r] = ordered.reshape(CP, 8, WIDTH // 2).astype(jnp.bfloat16)
        q_ref[me, r] = qsend[r, me]

        to_others(me, lambda target: qcopy(r, target, me).start())

    def spread_done(r):
        sent, landed = qsend.at[r, pl.ds(0, CP - 1)], q_ref.at[pl.ds(0, CP - 1), r]
        pltpu.make_async_copy(sent, sent, q_send.at[r]).wait()
        pltpu.make_async_copy(landed, landed, q_recv.at[r]).wait()

    relay_z(0)
    pl.semaphore_wait(met.at[0], 3)
    signal(met.at[1], partner)
    lax.fori_loop(NBLK // 2, NBLK, mark, 0)
    relay_z(1)
    pl.semaphore_wait(met.at[1], 1)
    s0(0)
    relay_z(2)
    s1(0)
    s0(1)
    s2(0)
    queries(0, 0)
    queries(0, 1)
    relay_z(3)
    queries(0, 2)
    queries(0, 3)
    s0(2)
    s1(1)
    spread(0)
    relay_z(4)
    s0(3)
    s3(0)
    s1(2)
    s2(1)
    s4(0)
    s0(4)
    s2(2)
    queries(1, 0)
    queries(1, 1)
    queries(1, 2)
    queries(1, 3)
    s1(3)
    spread(1)
    s2(3)
    s3(1)
    s1(4)
    s2(4)
    s3(2)
    s3(3)
    s4(1)
    s3(4)
    s4(2)
    s4(4)
    s4(3)
    spread_done(0)
    spread_done(1)
    for r in range(PARTS):
        arrived(r, "across")
        wait_for(mark_ref.at[pl.ds(0, 62 * SIZES[r])], g_send.at[r])
    wait_for(full.at[:, pl.ds(0, 3 * WIDTH)], z_send.at[0])


def gather_call(bounds, hidden, wq, wk, wv, inverse):
    vmem = pl.BlockSpec(memory_space=pltpu.VMEM)
    hbm = pl.BlockSpec(memory_space=pltpu.HBM)
    kv = jax.ShapeDtypeStruct((4, 4, 2, ROWS, HEAD), jnp.bfloat16)
    dma = pltpu.SemaphoreType.DMA
    return pl.pallas_call(
        gather_kernel,
        out_shape=(
            kv,
            kv,
            jax.ShapeDtypeStruct((CP, 2, 8, WIDTH // 2), jnp.bfloat16),
            jax.ShapeDtypeStruct((TOKENS, HEAD), jnp.bfloat16),
        ),
        in_specs=[hbm, hbm, hbm, hbm, hbm, vmem],
        out_specs=(vmem, vmem, vmem, vmem),
        scratch_shapes=[
            pltpu.VMEM((ROWS, TP * WIDTH), jnp.bfloat16),
            pltpu.VMEM((TP * WIDTH, WIDTH), jnp.bfloat16),
            pltpu.VMEM((TP * WIDTH, 2 * HEAD), jnp.bfloat16),
            pltpu.VMEM((ROWS, WIDTH // 2), jnp.bfloat16),
            pltpu.VMEM((2, CP, 8, WIDTH // 2), jnp.bfloat16),
            pltpu.VMEM((ROWS, HEAD), jnp.float32),
            pltpu.VMEM((ROWS, HEAD), jnp.float32),
            dma((5,)), dma((1,)), dma((2 * PARTS,)),
            dma((PARTS,)), dma((PARTS, 5)), dma((2,)), dma((2,)),
            pltpu.SMEM((9,), jnp.int32), pltpu.SemaphoreType.REGULAR((2,)),
        ],
        compiler_params=pltpu.CompilerParams(
            collective_id=0, has_side_effects=True, vmem_limit_bytes=32 * 1024 * 1024
        ),
        name="gather_project",
    )(bounds, hidden, wq, wk, wv, inverse)


TILE = SPAN * BLOCK


GROUPS = NBLK // SPAN
QROWS = 4 * SPAN * 8
PIECE = 256


def attend_kernel(
    bounds_ref, q_ref, k_ref, v_ref, mark_ref, o_ref,
    turned, penalty_ref, even, odd, mixed_ref, total_ref,
):
    rows = SPAN * 8
    factor = math.log2(math.e) / math.sqrt(HEAD)
    row = lax.rem(lax.broadcasted_iota(jnp.int32, (rows, HEAD), 0), rows)
    lane = lax.broadcasted_iota(jnp.int32, (rows, HEAD), 1)
    block, step = row // 8, lax.rem(row, PORTION)
    key_block, key_step = (lane - 8) // (PORTION + 1), lax.rem(lane - 8, PORTION + 1)
    later = (key_block > block) | ((key_block == block) & (key_step > step))
    later = later & (lane >= 8) & (lane < 8 + SPAN * (PORTION + 1))
    me = lax.axis_index("cp")
    contract_last = (((1,), (1,)), ((), ()))
    diagonal = lax.broadcasted_iota(jnp.int32, (HEAD, HEAD), 0) == lax.broadcasted_iota(
        jnp.int32, (HEAD, HEAD), 1
    )
    identity = diagonal.astype(jnp.float32).astype(jnp.bfloat16)

    def prepare(g, carry):
        at = pl.ds(pl.multiple_of(g * TILE, TILE), TILE)
        turned[:, at] = lax.dot_general(
            identity, v_ref[at, :], contract_last, preferred_element_type=jnp.float32
        ).astype(jnp.bfloat16)
        tokens = (g * SPAN + block) * BLOCK + me * PORTION + step
        document = jnp.zeros_like(tokens)
        for i in range(1, 8):
            document = jnp.where(tokens >= bounds_ref[i], i, document)
        other = (lane < 8) & (lane != document)
        penalty_ref[2 * g] = jnp.where(other, PENALTY, 0.0).astype(jnp.bfloat16)
        penalty_ref[2 * g + 1] = jnp.where(other | later, PENALTY, 0.0).astype(jnp.bfloat16)
        return carry

    lax.fori_loop(0, GROUPS, prepare, 0)

    def lowest(g):
        low = jnp.int32(0)
        for i in range(1, 8):
            low = jnp.where(g * TILE >= bounds_ref[i], bounds_ref[i], low)
        return low // TILE

    def following(item):
        g, j = item
        more = j > lowest(g)
        return jnp.where(more, g, g + 1), jnp.where(more, j - 1, g + 1)

    def score(item, ref):
        g, j = item
        own = jnp.where(g == j, 1, 0)
        held = jnp.minimum(g, GROUPS - 1)
        penalties = penalty_ref[2 * held + own]
        asking = pl.ds(pl.multiple_of(held * rows, rows), rows)
        q = jnp.concatenate(
            [
                jnp.concatenate([q_ref[asking, h * HEAD : (h + 1) * HEAD], penalties], axis=1)
                for h in range(4)
            ],
            axis=0,
        )
        for part in range(2):
            size = TILE // 2
            first = jnp.minimum(j, GROUPS - 1) * TILE + part * size
            at = pl.ds(pl.multiple_of(first, size), size)
            scores = lax.dot_general(
                jnp.concatenate([k_ref[at, :], mark_ref[at, :]], axis=1),
                q,
                contract_last,
                preferred_element_type=jnp.float32,
            )
            ref[part * size : (part + 1) * size, :] = scores
            top = jnp.max(scores, axis=0, keepdims=True)
            largest = top if part == 0 else jnp.maximum(largest, top)
        return largest

    def soften(item, ref, largest, state):
        g, j = item
        top, total, mixed = state
        top = jnp.where(g == j, 0.5 * PENALTY, top)
        start = jnp.minimum(j, GROUPS - 1) * TILE
        new_top = jnp.maximum(top, largest)
        shrink = jnp.exp2((top - new_top) * factor)
        total, mixed = total * shrink, mixed * shrink
        for first in range(0, TILE, PIECE):
            piece = slice(first, first + PIECE)
            weights = jnp.exp2((ref[piece, :] - new_top) * factor)
            total = total + jnp.sum(weights, axis=0, keepdims=True)
            keys = pl.ds(pl.multiple_of(start + first, PIECE), PIECE)
            mixed = mixed + jnp.dot(
                turned[:, keys], weights.astype(jnp.bfloat16), preferred_element_type=jnp.float32
            )
        mixed_ref[g] = mixed
        total_ref[g] = total
        return new_top, total, mixed

    count = lax.fori_loop(0, GROUPS, lambda g, n: n + g + 1 - lowest(g), jnp.int32(0))
    zero = jnp.int32(0)
    highest = score((zero, zero), even)

    def pair(n, carry):
        g, j, largest, *state = carry
        item = (g, j)
        second = following(item)
        second_largest = score(second, odd)
        state = soften(item, even, largest, state)
        third = following(second)
        third = (jnp.minimum(third[0], GROUPS), jnp.minimum(third[1], GROUPS))
        largest = score(third, even)
        state = soften(second, odd, second_largest, state)
        return (*third, largest, *state)

    lax.fori_loop(
        0,
        (count + 1) // 2,
        pair,
        (
            zero,
            zero,
            highest,
            jnp.full((1, QROWS), 0.5 * PENALTY, jnp.float32),
            jnp.zeros((1, QROWS), jnp.float32),
            jnp.zeros((HEAD, QROWS), jnp.float32),
        ),
    )

    def finish(g, carry):
        o_ref[g] = (mixed_ref[g] / total_ref[g]).astype(jnp.bfloat16)
        return carry

    lax.fori_loop(0, GROUPS, finish, 0)


def attend_call(bounds, q, k, v, marks):
    vmem = pl.BlockSpec(memory_space=pltpu.VMEM)
    return pl.pallas_call(
        attend_kernel,
        out_shape=jax.ShapeDtypeStruct((GROUPS, HEAD, QROWS), jnp.bfloat16),
        in_specs=[pl.BlockSpec(memory_space=pltpu.SMEM), vmem, vmem, vmem, vmem],
        out_specs=vmem,
        scratch_shapes=[
            pltpu.VMEM((HEAD, TOKENS), jnp.bfloat16),
            pltpu.VMEM((2 * GROUPS, SPAN * 8, HEAD), jnp.bfloat16),
            pltpu.VMEM((TILE, QROWS), jnp.float32),
            pltpu.VMEM((TILE, QROWS), jnp.float32),
            pltpu.VMEM((GROUPS + 1, HEAD, QROWS), jnp.float32),
            pltpu.VMEM((GROUPS + 1, 1, QROWS), jnp.float32),
        ],
        compiler_params=pltpu.CompilerParams(vmem_limit_bytes=28 * 1024 * 1024),
        name="attend",
    )(bounds, q, k, v, marks)


CHUNKS = (2, 2, 2, 1, 1)
FIRST = (0, 2, 4, 6, 7)
PIECES = WIDTH // HEAD


def output_kernel(
    slot_ref, heads_ref, wo_ref, out_ref,
    heads, wo, far, near, far_in, near_in, spread, landed, own_sum,
    w_sem, z_send, z_recv, a_send, a_recv,
):
    me = lax.axis_index("cp")
    tp = lax.axis_index("tp")
    up, down, across = lax.rem(tp + 1, TP), lax.rem(tp + 3, TP), lax.rem(tp + 2, TP)

    loads = []
    for n, t in enumerate((across, up, down, tp)):
        columns = pl.ds(pl.multiple_of(t * WIDTH, WIDTH), WIDTH)
        loads.append(pltpu.make_async_copy(wo_ref.at[:, columns], wo.at[n], w_sem.at[n]))
        loads[-1].start()

    barrier = pltpu.get_barrier_semaphore()

    def greet(k, carry):
        pl.semaphore_signal(
            barrier, inc=1, device_id={"cp": lax.rem(me + k, CP)}, device_id_type=MESH
        )
        return carry

    pl.semaphore_signal(barrier, inc=1, device_id={"tp": up}, device_id_type=MESH)
    pl.semaphore_signal(barrier, inc=1, device_id={"tp": down}, device_id_type=MESH)
    lax.fori_loop(1, CP, greet, 0)

    turned_row = lax.broadcasted_iota(jnp.int32, (QROWS, QROWS), 0)
    turned_column = lax.broadcasted_iota(jnp.int32, (QROWS, QROWS), 1)
    rows = SPAN * PORTION
    head, at_row = turned_row // rows, lax.rem(turned_row, rows)
    source = (
        lax.rem(head, 4) * 2 * rows
        + (at_row // PORTION) * 2 * PORTION
        + (head // 4) * PORTION
        + lax.rem(at_row, PORTION)
    )
    select = (turned_column == source).astype(jnp.float32).astype(jnp.bfloat16)
    for g in range(GROUPS):
        part = lax.dot_general(
            select,
            heads_ref[g],
            (((1,), (1,)), ((), ())),
            preferred_element_type=jnp.float32,
        ).astype(jnp.bfloat16)
        for h in range(HEADS):
            heads[g * rows : (g + 1) * rows, h * HEAD : (h + 1) * HEAD] = part[
                h * rows : (h + 1) * rows
            ]

    def product(n, c):
        columns = slice(FIRST[c] * HEAD, (FIRST[c] + CHUNKS[c]) * HEAD)
        return jnp.dot(heads[...], wo[n, :, columns], preferred_element_type=jnp.float32)

    def remote(n, src, dst, target):
        return pltpu.make_async_remote_copy(
            src_ref=src,
            dst_ref=dst,
            send_sem=z_send.at[0],
            recv_sem=z_recv.at[n],
            device_id={"tp": target},
            device_id_type=MESH,
        )

    half = ROWS // 2
    upper, lower = pl.ds(0, half), pl.ds(half, half)
    far_copies, near_copies = [], []
    for c, count in enumerate(CHUNKS):
        at = pl.ds(FIRST[c], count)
        far_copies.append(
            (
                remote(3 * c, far.at[0, at], far_in.at[0, at], up),
                remote(3 * c + 1, far.at[1, at], far_in.at[1, at], down),
            )
        )
        near_copies.append(
            (
                remote(3 * c + 2, near.at[0, at], near_in.at[0, at], up),
                remote(3 * c + 2, near.at[1, at], near_in.at[1, at], down),
            )
        )

    def pieces(c):
        return [(FIRST[c] + n, slice(n * HEAD, (n + 1) * HEAD)) for n in range(CHUNKS[c])]

    def make_far(c):
        value = product(0, c).astype(jnp.bfloat16)
        for at, columns in pieces(c):
            far[0, at] = value[:half, columns]
            far[1, at] = value[half:, columns]

    def send_far(c):
        for copy in far_copies[c]:
            copy.start()

    def send_near(c):
        to_up, to_down = product(1, c), product(2, c)
        far_copies[c][0].wait_recv()
        for at, columns in pieces(c):
            near[0, at, upper] = (
                to_up[:half, columns] + far_in[0, at].astype(jnp.float32)
            ).astype(jnp.bfloat16)
            near[0, at, lower] = to_up[half:, columns].astype(jnp.bfloat16)
        near_copies[c][0].start()
        far_copies[c][1].wait_recv()
        for at, columns in pieces(c):
            near[1, at, upper] = to_down[:half, columns].astype(jnp.bfloat16)
            near[1, at, lower] = (
                to_down[half:, columns] + far_in[1, at].astype(jnp.float32)
            ).astype(jnp.bfloat16)
        near_copies[c][1].start()

    def sum_own(c):
        value = product(3, c)
        for at, columns in pieces(c):
            own_sum[at] = value[:, columns]

    row = lax.broadcasted_iota(jnp.int32, (ROWS, ROWS), 0)
    column = lax.broadcasted_iota(jnp.int32, (ROWS, ROWS), 1)
    to_owner = (row == slot_ref[...]).astype(jnp.float32).astype(jnp.bfloat16)
    origin = (lax.rem(row, BLOCK) // 4) * 8 + (row // BLOCK) * 4 + lax.rem(row, 4)
    to_place = (column == origin).astype(jnp.float32).astype(jnp.bfloat16)

    def acopy(c, target, slot):
        at = pl.ds(FIRST[c], CHUNKS[c])
        return pltpu.make_async_remote_copy(
            src_ref=spread.at[target, at],
            dst_ref=landed.at[slot, at],
            send_sem=a_send.at[c],
            recv_sem=a_recv.at[c],
            device_id={"cp": target},
            device_id_type=MESH,
        )

    def finish_sum(c):
        both = near_in.at[:, pl.ds(FIRST[c], CHUNKS[c])]
        pltpu.make_async_copy(both, both, z_recv.at[3 * c + 2]).wait()
        total = jnp.concatenate(
            [
                (
                    own_sum[at]
                    + near_in[0, at].astype(jnp.float32)
                    + near_in[1, at].astype(jnp.float32)
                ).astype(jnp.bfloat16)
                for at, columns in pieces(c)
            ],
            axis=1,
        )
        picked = jnp.dot(to_owner, total, preferred_element_type=jnp.float32)
        for at, columns in pieces(c):
            spread[:, at] = picked[:, columns].reshape(CP, 8, HEAD).astype(jnp.bfloat16)
            landed[me, at] = spread[me, at]

        to_others(me, lambda target: acopy(c, target, me).start())

    def place(c):
        everyone = landed.at[pl.ds(0, CP - 1), pl.ds(FIRST[c], CHUNKS[c])]
        pltpu.make_async_copy(everyone, everyone, a_recv.at[c]).wait()
        rows = jnp.concatenate(
            [
                landed[:, at].astype(jnp.float32).reshape(ROWS, HEAD).astype(jnp.bfloat16)
                for at, columns in pieces(c)
            ],
            axis=1,
        )
        out_ref[:, FIRST[c] * HEAD : (FIRST[c] + CHUNKS[c]) * HEAD] = jnp.dot(
            to_place, rows, preferred_element_type=jnp.float32
        ).astype(jnp.bfloat16)

    loads[0].wait()
    make_far(0)
    pl.semaphore_wait(barrier, CP + 1)
    send_far(0)
    make_far(1)
    send_far(1)
    make_far(2)
    send_far(2)
    loads[1].wait()
    loads[2].wait()
    send_near(0)
    make_far(3)
    send_far(3)
    send_near(1)
    make_far(4)
    send_far(4)
    send_near(2)
    loads[3].wait()
    for c in range(len(CHUNKS)):
        sum_own(c)
    send_near(3)
    finish_sum(0)
    send_near(4)
    finish_sum(1)
    finish_sum(2)
    finish_sum(3)
    finish_sum(4)
    for c in range(len(CHUNKS)):
        place(c)
    for c in range(len(CHUNKS)):
        everyone = spread.at[pl.ds(0, CP - 1), pl.ds(FIRST[c], CHUNKS[c])]
        pltpu.make_async_copy(everyone, everyone, a_send.at[c]).wait()
    sent = wo.at[0, pl.ds(0, 3 * ROWS)]
    pltpu.make_async_copy(sent, sent, z_send.at[0]).wait()


def output_call(slot_rows, heads, wo):
    vmem = pl.BlockSpec(memory_space=pltpu.VMEM)
    dma = pltpu.SemaphoreType.DMA
    half = ROWS // 2
    bf16 = jnp.bfloat16
    return pl.pallas_call(
        output_kernel,
        out_shape=jax.ShapeDtypeStruct((ROWS, WIDTH), bf16),
        in_specs=[vmem, vmem, pl.BlockSpec(memory_space=pltpu.HBM)],
        out_specs=vmem,
        scratch_shapes=[
            pltpu.VMEM((ROWS, WIDTH), bf16),
            pltpu.VMEM((TP, WIDTH, WIDTH), bf16),
            pltpu.VMEM((2, PIECES, half, HEAD), bf16),
            pltpu.VMEM((2, PIECES, ROWS, HEAD), bf16),
            pltpu.VMEM((2, PIECES, half, HEAD), bf16),
            pltpu.VMEM((2, PIECES, ROWS, HEAD), bf16),
            pltpu.VMEM((CP, PIECES, 8, HEAD), bf16),
            pltpu.VMEM((CP, PIECES, 8, HEAD), bf16),
            pltpu.VMEM((PIECES, ROWS, HEAD), jnp.float32),
            dma((4,)), dma((1,)), dma((3 * len(CHUNKS),)),
            dma((len(CHUNKS),)), dma((len(CHUNKS),)),
        ],
        compiler_params=pltpu.CompilerParams(
            collective_id=1, has_side_effects=True, vmem_limit_bytes=40 * 1024 * 1024
        ),
        name="project_out",
    )(slot_rows, heads, wo)


def local(hidden, query_weight, key_matrix, value_matrix, output_weight, bounds, block_owner):
    inverse = rope_inverse(HEAD)
    inverse = jnp.concatenate([inverse, inverse])[None, :]
    slots = slots_of(block_owner)
    slot_rows = (slots[:, None] * PORTION + jnp.arange(PORTION, dtype=jnp.int32)[None, :]).reshape(
        1, ROWS
    )
    hidden, query_weight, key_matrix, value_matrix, output_weight = (
        pltpu.with_memory_space_constraint(a, pltpu.HBM)
        for a in (hidden, query_weight, key_matrix, value_matrix, output_weight)
    )
    keys, values, queries, marks = gather_call(
        pltpu.with_memory_space_constraint(bounds, pltpu.HBM), hidden, query_weight, key_matrix, value_matrix, inverse
    )
    heads = attend_call(
        bounds,
        queries.reshape(2 * ROWS, WIDTH // 2),
        keys.reshape(TOKENS, HEAD),
        values.reshape(TOKENS, HEAD),
        marks,
    )
    return output_call(slot_rows, heads, output_weight)


def solution(mesh):
    placed = (P("cp", "tp"), P(None, "tp"), P(None, "tp"), P(None, "tp"), P("tp", None), P(), P())
    return jax.shard_map(
        local, mesh=mesh, in_specs=placed, out_specs=P("cp", "tp"), check_vma=False
    )
```

```python
import functools
import math

import jax
import jax.numpy as jnp
from jax import lax
from jax.experimental import pallas as pl
from jax.experimental.pallas import tpu as pltpu
from jax.sharding import PartitionSpec as P

HEAD = 128
BLOCK = 128
CP = 32
TP = 4
ROWS = 256
WIDTH = 1024
NBLK = 64
HEADS = 8
TOKENS = 8192
PORTION = BLOCK // CP

rope_theta = 500000.0
rope_factor = 8.0
rope_context = 8192.0
masked_score = -1e30
MESH = pl.DeviceIdType.MESH


def rope_inverse(head_size):
    halves = jnp.arange(head_size // 2, dtype=jnp.float32)
    inverse = 1.0 / rope_theta ** (2.0 * halves / head_size)
    wavelength = 2.0 * math.pi / inverse
    smooth = (rope_context / wavelength - 1.0) / 3.0
    blended = (1.0 - smooth) * inverse / rope_factor + smooth * inverse
    longer = jnp.where(wavelength > rope_context, inverse / rope_factor, blended)
    return jnp.where(wavelength < rope_context / 4.0, inverse, longer)


def starts_of(tokens, bounds_ref):
    start = jnp.zeros_like(tokens)
    for i in range(1, 8):
        bound = bounds_ref[i]
        start = jnp.where(tokens >= bound, bound, start)
    return start


SIZES = (64, 64, 64, 32, 32)
STARTS = (0, 64, 128, 192, 224)
PARTS = len(SIZES)
STRAIGHT1 = (True, False, True, True, True)
STRAIGHT2 = (True, False, False, False, True)
SPAN = 8
PENALTY = -1e30


def gather_kernel(
    bounds_hbm, owner_hbm, hidden_ref, wq_ref, wk_ref, wv_ref, inverse_ref,
    k_ref, v_ref, q_ref, mark_ref, slot_ref,
    full, wq, wkv, qtmp, qsend, cosine, sine,
    w_sem, z_send, z_recv, g_send, g_recv, q_send, q_recv, bounds_ref, owner_ref, met,
):
    me = lax.axis_index("cp")
    tp = lax.axis_index("tp")
    core = lax.rem(me, 2)
    ycoord = lax.rem(me // 2, 4)
    xcoord = me // 8
    partner = me + 1 - 2 * core
    up, down = lax.rem(tp + 1, TP), lax.rem(tp + 3, TP)
    own_columns = pl.ds(pl.multiple_of(tp * WIDTH, WIDTH), WIDTH)

    bring = pltpu.make_async_copy(hidden_ref, full.at[:, own_columns], w_sem.at[3])
    weights = [
        pltpu.make_async_copy(wk_ref, wkv.at[:, pl.ds(0, HEAD)], w_sem.at[0]),
        pltpu.make_async_copy(wv_ref, wkv.at[:, pl.ds(HEAD, HEAD)], w_sem.at[1]),
        pltpu.make_async_copy(wq_ref, wq, w_sem.at[2]),
    ]
    bring_bounds = pltpu.make_async_copy(bounds_hbm, bounds_ref, w_sem.at[4])
    bring_owner = pltpu.make_async_copy(owner_hbm, owner_ref, w_sem.at[5])
    bring.start()
    bring_bounds.start()
    bring_owner.start()
    for copy in weights:
        copy.start()

    barrier = pltpu.get_barrier_semaphore()

    def signal(semaphore, target):
        pl.semaphore_signal(semaphore, inc=1, device_id={"cp": target}, device_id_type=MESH)

    along_x = [(lax.rem(xcoord + n, 4) * 4 + ycoord) * 2 + core for n in (1, 2, 3)]
    along_y = [(xcoord * 4 + lax.rem(ycoord + n, 4)) * 2 + core for n in (1, 2, 3)]
    pl.semaphore_signal(barrier, inc=1, device_id={"tp": up}, device_id_type=MESH)
    pl.semaphore_signal(barrier, inc=1, device_id={"tp": down}, device_id_type=MESH)
    for target in (*along_x, *along_y, partner):
        signal(barrier, target)
    bring.wait()
    pl.semaphore_wait(barrier, 9)

    def zcopy(n, target, owner, row, count):
        columns = pl.ds(pl.multiple_of(owner * WIDTH, WIDTH), WIDTH)
        ref = full.at[pl.ds(row, count), columns]
        return pltpu.make_async_remote_copy(
            src_ref=ref,
            dst_ref=ref,
            send_sem=z_send.at[0],
            recv_sem=z_recv.at[n],
            device_id={"tp": target},
            device_id_type=MESH,
        )

    own = [
        (
            zcopy(2 * r, up, tp, STARTS[r], SIZES[r]),
            zcopy(2 * r, down, tp, STARTS[r], SIZES[r]),
        )
        for r in range(PARTS)
    ]
    fwd = [
        (
            zcopy(2 * r + 1, down, up, STARTS[r], SIZES[r] // 2),
            zcopy(2 * r + 1, up, down, STARTS[r] + SIZES[r] // 2, SIZES[r] // 2),
        )
        for r in range(PARTS)
    ]

    def wait_for(ref, semaphore):
        pltpu.make_async_copy(ref, ref, semaphore).wait()

    def arrived_z(n, r, owners):
        wait_for(
            full.at[pl.ds(STARTS[r], SIZES[r]), pl.ds(0, owners * WIDTH)], z_recv.at[2 * r + n]
        )
    for copy in (*own[0], *own[1]):
        copy.start()
    for target in along_x:
        signal(met.at[0], target)
    bring_bounds.wait()

    def relay_z(r):
        arrived_z(0, r, 2)
        for copy in fwd[r]:
            copy.start()
        if r + 2 < PARTS:
            for copy in own[r + 2]:
                copy.start()

    lanes = lax.broadcasted_iota(jnp.int32, (BLOCK, HEAD), 1)
    sublanes = lax.broadcasted_iota(jnp.int32, (BLOCK, HEAD), 0)
    inverse = inverse_ref[...]
    for r in range(2):
        tokens = me * ROWS + r * BLOCK + sublanes
        angle = (tokens - starts_of(tokens, bounds_ref)).astype(jnp.float32) * inverse
        turn = jnp.sin(angle)
        cosine[pl.ds(r * BLOCK, BLOCK), :] = jnp.cos(angle)
        sine[pl.ds(r * BLOCK, BLOCK), :] = jnp.where(lanes < HEAD // 2, -turn, turn)

    place = jnp.minimum(jnp.maximum(sublanes - me * PORTION, 0), PORTION)

    def mark(b, carry):
        tokens = b * BLOCK + sublanes
        document = jnp.zeros_like(tokens)
        for i in range(1, 8):
            document = jnp.where(tokens >= bounds_ref[i], i, document)
        spot = 8 + lax.rem(b, SPAN) * (PORTION + 1) + place
        hit = (lanes == document) | (lanes == spot)
        mark_ref[pl.ds(pl.multiple_of(b * BLOCK, BLOCK), BLOCK), :] = (
            hit.astype(jnp.float32).astype(jnp.bfloat16)
        )
        return carry

    lax.fori_loop(0, NBLK // 2, mark, 0)
    weights[0].wait()
    weights[1].wait()
    weights[2].wait()

    def slots():
        spot = lax.broadcasted_iota(jnp.int32, (8, ROWS), 1)
        block = spot // PORTION
        owner = jnp.zeros_like(spot)
        for b in range(NBLK):
            owner = jnp.where(block == b, owner_ref[b], owner)
        rank = jnp.zeros_like(spot)
        for b in range(NBLK - 1):
            rank = rank + ((block > b) & (owner == owner_ref[b])).astype(jnp.int32)
        place = (owner * 2 + rank) * PORTION + lax.rem(spot, PORTION)
        slot_ref[...] = place

    def rotate(raw, row, count):
        table = pl.ds(row, count)
        return raw * cosine[table, :] + pltpu.roll(raw, HEAD // 2, 1) * sine[table, :]

    def queries(r, n):
        columns = slice(n * 2 * HEAD, (n + 1) * 2 * HEAD)
        rows = pl.ds(r * BLOCK, BLOCK)
        raw = jnp.dot(full[rows, :], wq[:, columns], preferred_element_type=jnp.float32)
        turned = jnp.concatenate(
            [rotate(raw[:, :HEAD], r * BLOCK, BLOCK), rotate(raw[:, HEAD:], r * BLOCK, BLOCK)],
            axis=1,
        )
        qtmp[pl.ds((n // 2) * BLOCK, BLOCK), (n % 2) * 2 * HEAD : (n % 2 + 1) * 2 * HEAD] = (
            turned.astype(jnp.bfloat16)
        )

    def gather(which, r):
        buffer = (k_ref, v_ref)[which]
        a, b = ((xcoord, ycoord), (ycoord, xcoord))[which]

        def neighbour(along, step):
            if along == 0:
                na, nb = lax.rem(a + step, 4), b
            else:
                na, nb = a, lax.rem(b + step, 4)
            x, y = ((na, nb), (nb, na))[which]
            return (x * 4 + y) * 2 + core

        def copy(n, ref, target):
            return pltpu.make_async_remote_copy(
                src_ref=ref,
                dst_ref=ref,
                send_sem=g_send.at[r],
                recv_sem=g_recv.at[r, n],
                device_id={"cp": target},
                device_id_type=MESH,
            )

        def piece(at, row, count):
            rows = pl.ds(STARTS[r] + row, count)
            if which == 0:
                return buffer.at[at, b, core, rows]
            return buffer.at[b, at, core, rows]

        def line(at, first, count):
            along, rows = pl.ds(first, count), pl.ds(STARTS[r], SIZES[r])
            if which == 0:
                return buffer.at[along, at, core, rows]
            return buffer.at[at, along, core, rows]

        a_next, a_prev = lax.rem(a + 1, 4), lax.rem(a + 3, 4)
        b_next, b_prev = lax.rem(b + 1, 4), lax.rem(b + 3, 4)
        b_far = lax.rem(b + 2, 4)
        size, half = SIZES[r], SIZES[r] // 2
        return dict(
            ring1=(
                copy(0, piece(a, 0, size), neighbour(0, 1)),
                copy(0, piece(a, 0, size), neighbour(0, 3)),
            ),
            ring1_far=(copy(1, piece(a, 0, size), neighbour(0, 2)),)
            if STRAIGHT1[r]
            else (
                copy(1, piece(a_prev, 0, half), neighbour(0, 1)),
                copy(1, piece(a_next, half, half), neighbour(0, 3)),
            ),
            ring2=(
                copy(2, line(b, 0, 4), neighbour(1, 1)),
                copy(2, line(b, 0, 4), neighbour(1, 3)),
            ),
            ring2_far=(copy(3, line(b, 0, 4), neighbour(1, 2)),)
            if STRAIGHT2[r]
            else (
                copy(3, line(b_prev, 0, 2), neighbour(1, 1)),
                copy(3, line(b_next, 2, 2), neighbour(1, 3)),
            ),
            across=(
                copy(4, line(b, 0, 4), partner),
                copy(4, line(b_prev, 0, 4), partner),
                copy(4, line(b_next, 0, 4), partner),
                copy(4, line(b_far, 0, 4), partner),
            ),
        )

    flows = [[gather(which, r) for which in range(2)] for r in range(PARTS)]

    def start(r, name):
        for flow in flows[r]:
            for copy in flow[name]:
                copy.start()

    def arrived(r, name):
        rows = pl.ds(STARTS[r], SIZES[r])
        n, ref = {
            "ring1": (0, k_ref.at[0, :, core, rows]),
            "ring1_far": (1, k_ref.at[0, pl.ds(0, 2), core, rows]),
            "ring2": (2, k_ref.at[:, :, core, rows]),
            "ring2_far": (3, k_ref.at[pl.ds(0, 2), :, core, rows]),
            "across": (4, k_ref.at[:, :, :, rows]),
        }[name]
        wait_for(ref, g_recv.at[r, n])

    def across(r, which):
        for flow in flows[r]:
            for n in which:
                flow["across"][n].start()

    def s0(r):
        arrived_z(1, r, 1)
        rows = pl.ds(STARTS[r], SIZES[r])
        raw = jnp.dot(full[rows, :], wkv[...], preferred_element_type=jnp.float32)
        k_ref[xcoord, ycoord, core, rows] = rotate(raw[:, :HEAD], STARTS[r], SIZES[r]).astype(
            jnp.bfloat16
        )
        v_ref[xcoord, ycoord, core, rows] = raw[:, HEAD:].astype(jnp.bfloat16)
        start(r, "ring1")
        if STRAIGHT1[r]:
            start(r, "ring1_far")

    def s1(r):
        arrived(r, "ring1")
        if not STRAIGHT1[r]:
            start(r, "ring1_far")

    def s2(r):
        arrived(r, "ring1_far")
        start(r, "ring2")
        if STRAIGHT2[r]:
            start(r, "ring2_far")
        across(r, (0,))

    def s3(r):
        arrived(r, "ring2")
        if not STRAIGHT2[r]:
            start(r, "ring2_far")
        across(r, (1, 2))

    def s4(r):
        arrived(r, "ring2_far")
        across(r, (3,))

    out_row = lax.broadcasted_iota(jnp.int32, (ROWS, ROWS), 0)
    in_row = lax.broadcasted_iota(jnp.int32, (ROWS, ROWS), 1)
    origin = lax.rem(out_row // 4, 2) * BLOCK + (out_row // 8) * 4 + lax.rem(out_row, 4)
    pick = (in_row == origin).astype(jnp.float32).astype(jnp.bfloat16)

    def qcopy(r, target, slot):
        return pltpu.make_async_remote_copy(
            src_ref=qsend.at[r, target],
            dst_ref=q_ref.at[slot, r],
            send_sem=q_send.at[r],
            recv_sem=q_recv.at[r],
            device_id={"cp": target},
            device_id_type=MESH,
        )

    def spread(r):
        ordered = jnp.dot(pick, qtmp[...], preferred_element_type=jnp.float32)
        qsend[r] = ordered.reshape(CP, 8, WIDTH // 2).astype(jnp.bfloat16)
        q_ref[me, r] = qsend[r, me]

        def send(k, carry):
            qcopy(r, lax.rem(me + k, CP), me).start()
            return carry

        lax.fori_loop(1, CP, send, 0)

    def spread_done(r):
        sent, landed = qsend.at[r, pl.ds(0, CP - 1)], q_ref.at[pl.ds(0, CP - 1), r]
        pltpu.make_async_copy(sent, sent, q_send.at[r]).wait()
        pltpu.make_async_copy(landed, landed, q_recv.at[r]).wait()

    relay_z(0)
    pl.semaphore_wait(met.at[0], 3)
    signal(met.at[1], partner)
    bring_owner.wait()
    slots()
    lax.fori_loop(NBLK // 2, NBLK, mark, 0)
    relay_z(1)
    pl.semaphore_wait(met.at[1], 1)
    s0(0)
    relay_z(2)
    s1(0)
    s0(1)
    s2(0)
    queries(0, 0)
    queries(0, 1)
    relay_z(3)
    queries(0, 2)
    queries(0, 3)
    s0(2)
    s1(1)
    spread(0)
    relay_z(4)
    s0(3)
    s3(0)
    s1(2)
    s2(1)
    s4(0)
    s0(4)
    s2(2)
    queries(1, 0)
    queries(1, 1)
    queries(1, 2)
    queries(1, 3)
    s1(3)
    spread(1)
    s2(3)
    s3(1)
    s1(4)
    s2(4)
    s3(2)
    s3(3)
    s4(1)
    s3(4)
    s4(2)
    s4(4)
    s4(3)
    spread_done(0)
    spread_done(1)
    for r in range(PARTS):
        arrived(r, "across")
        wait_for(mark_ref.at[pl.ds(0, 62 * SIZES[r])], g_send.at[r])
    wait_for(full.at[:, pl.ds(0, 3 * WIDTH)], z_send.at[0])


def gather_call(bounds, owner, hidden, wq, wk, wv, inverse):
    vmem = pl.BlockSpec(memory_space=pltpu.VMEM)
    hbm = pl.BlockSpec(memory_space=pltpu.HBM)
    kv = jax.ShapeDtypeStruct((4, 4, 2, ROWS, HEAD), jnp.bfloat16)
    dma = pltpu.SemaphoreType.DMA
    return pl.pallas_call(
        gather_kernel,
        out_shape=(
            kv,
            kv,
            jax.ShapeDtypeStruct((CP, 2, 8, WIDTH // 2), jnp.bfloat16),
            jax.ShapeDtypeStruct((TOKENS, HEAD), jnp.bfloat16),
            jax.ShapeDtypeStruct((8, ROWS), jnp.int32),
        ),
        in_specs=[hbm, hbm, hbm, hbm, hbm, hbm, vmem],
        out_specs=(vmem, vmem, vmem, vmem, vmem),
        scratch_shapes=[
            pltpu.VMEM((ROWS, TP * WIDTH), jnp.bfloat16),
            pltpu.VMEM((TP * WIDTH, WIDTH), jnp.bfloat16),
            pltpu.VMEM((TP * WIDTH, 2 * HEAD), jnp.bfloat16),
            pltpu.VMEM((ROWS, WIDTH // 2), jnp.bfloat16),
            pltpu.VMEM((2, CP, 8, WIDTH // 2), jnp.bfloat16),
            pltpu.VMEM((ROWS, HEAD), jnp.float32),
            pltpu.VMEM((ROWS, HEAD), jnp.float32),
            dma((6,)), dma((1,)), dma((2 * PARTS,)),
            dma((PARTS,)), dma((PARTS, 5)), dma((2,)), dma((2,)),
            pltpu.SMEM((9,), jnp.int32), pltpu.SMEM((NBLK,), jnp.int32),
            pltpu.SemaphoreType.REGULAR((2,)),
        ],
        compiler_params=pltpu.CompilerParams(
            collective_id=0, has_side_effects=True, vmem_limit_bytes=32 * 1024 * 1024
        ),
        name="gather_project",
    )(bounds, owner, hidden, wq, wk, wv, inverse)


TILE = SPAN * BLOCK


GROUPS = NBLK // SPAN
QROWS = 4 * SPAN * 8
PIECE = 256


def attend_kernel(
    bounds_ref, q_ref, k_ref, v_ref, mark_ref, o_ref,
    turned, penalty_ref, even, odd, mixed_ref, total_ref,
):
    rows = SPAN * 8
    factor = math.log2(math.e) / math.sqrt(HEAD)
    row = lax.rem(lax.broadcasted_iota(jnp.int32, (rows, HEAD), 0), rows)
    lane = lax.broadcasted_iota(jnp.int32, (rows, HEAD), 1)
    block, step = row // 8, lax.rem(row, PORTION)
    key_block, key_step = (lane - 8) // (PORTION + 1), lax.rem(lane - 8, PORTION + 1)
    later = (key_block > block) | ((key_block == block) & (key_step > step))
    later = later & (lane >= 8) & (lane < 8 + SPAN * (PORTION + 1))
    me = lax.axis_index("cp")
    contract_last = (((1,), (1,)), ((), ()))
    diagonal = lax.broadcasted_iota(jnp.int32, (HEAD, HEAD), 0) == lax.broadcasted_iota(
        jnp.int32, (HEAD, HEAD), 1
    )
    identity = diagonal.astype(jnp.float32).astype(jnp.bfloat16)

    def prepare(g, carry):
        at = pl.ds(pl.multiple_of(g * TILE, TILE), TILE)
        turned[:, at] = lax.dot_general(
            identity, v_ref[at, :], contract_last, preferred_element_type=jnp.float32
        ).astype(jnp.bfloat16)
        tokens = (g * SPAN + block) * BLOCK + me * PORTION + step
        document = jnp.zeros_like(tokens)
        for i in range(1, 8):
            document = jnp.where(tokens >= bounds_ref[i], i, document)
        other = (lane < 8) & (lane != document)
        penalty_ref[2 * g] = jnp.where(other, PENALTY, 0.0).astype(jnp.bfloat16)
        penalty_ref[2 * g + 1] = jnp.where(other | later, PENALTY, 0.0).astype(jnp.bfloat16)
        return carry

    lax.fori_loop(0, GROUPS, prepare, 0)

    def lowest(g):
        low = jnp.int32(0)
        for i in range(1, 8):
            low = jnp.where(g * TILE >= bounds_ref[i], bounds_ref[i], low)
        return low // TILE

    def following(item):
        g, j = item
        more = j > lowest(g)
        return jnp.where(more, g, g + 1), jnp.where(more, j - 1, g + 1)

    def score(item, ref):
        g, j = item
        own = jnp.where(g == j, 1, 0)
        held = jnp.minimum(g, GROUPS - 1)
        penalties = penalty_ref[2 * held + own]
        asking = pl.ds(pl.multiple_of(held * rows, rows), rows)
        q = jnp.concatenate(
            [
                jnp.concatenate([q_ref[asking, h * HEAD : (h + 1) * HEAD], penalties], axis=1)
                for h in range(4)
            ],
            axis=0,
        )
        for part in range(2):
            size = TILE // 2
            first = jnp.minimum(j, GROUPS - 1) * TILE + part * size
            at = pl.ds(pl.multiple_of(first, size), size)
            scores = lax.dot_general(
                jnp.concatenate([k_ref[at, :], mark_ref[at, :]], axis=1),
                q,
                contract_last,
                preferred_element_type=jnp.float32,
            )
            ref[part * size : (part + 1) * size, :] = scores
            top = jnp.max(scores, axis=0, keepdims=True)
            largest = top if part == 0 else jnp.maximum(largest, top)
        return largest

    def soften(item, ref, largest, state):
        g, j = item
        top, total, mixed = state
        top = jnp.where(g == j, 0.5 * PENALTY, top)
        start = jnp.minimum(j, GROUPS - 1) * TILE
        new_top = jnp.maximum(top, largest)
        shrink = jnp.exp2((top - new_top) * factor)
        total, mixed = total * shrink, mixed * shrink
        for first in range(0, TILE, PIECE):
            piece = slice(first, first + PIECE)
            weights = jnp.exp2((ref[piece, :] - new_top) * factor)
            total = total + jnp.sum(weights, axis=0, keepdims=True)
            keys = pl.ds(pl.multiple_of(start + first, PIECE), PIECE)
            mixed = mixed + jnp.dot(
                turned[:, keys], weights.astype(jnp.bfloat16), preferred_element_type=jnp.float32
            )
        mixed_ref[g] = mixed
        total_ref[g] = total
        return new_top, total, mixed

    count = lax.fori_loop(0, GROUPS, lambda g, n: n + g + 1 - lowest(g), jnp.int32(0))
    zero = jnp.int32(0)
    highest = score((zero, zero), even)

    def pair(n, carry):
        g, j, largest, *state = carry
        item = (g, j)
        second = following(item)
        second_largest = score(second, odd)
        state = soften(item, even, largest, state)
        third = following(second)
        third = (jnp.minimum(third[0], GROUPS), jnp.minimum(third[1], GROUPS))
        largest = score(third, even)
        state = soften(second, odd, second_largest, state)
        return (*third, largest, *state)

    lax.fori_loop(
        0,
        (count + 1) // 2,
        pair,
        (
            zero,
            zero,
            highest,
            jnp.full((1, QROWS), 0.5 * PENALTY, jnp.float32),
            jnp.zeros((1, QROWS), jnp.float32),
            jnp.zeros((HEAD, QROWS), jnp.float32),
        ),
    )

    def finish(g, carry):
        o_ref[g] = (mixed_ref[g] / total_ref[g]).astype(jnp.bfloat16)
        return carry

    lax.fori_loop(0, GROUPS, finish, 0)


def attend_call(bounds, q, k, v, marks):
    vmem = pl.BlockSpec(memory_space=pltpu.VMEM)
    return pl.pallas_call(
        attend_kernel,
        out_shape=jax.ShapeDtypeStruct((GROUPS, HEAD, QROWS), jnp.bfloat16),
        in_specs=[pl.BlockSpec(memory_space=pltpu.SMEM), vmem, vmem, vmem, vmem],
        out_specs=vmem,
        scratch_shapes=[
            pltpu.VMEM((HEAD, TOKENS), jnp.bfloat16),
            pltpu.VMEM((2 * GROUPS, SPAN * 8, HEAD), jnp.bfloat16),
            pltpu.VMEM((TILE, QROWS), jnp.float32),
            pltpu.VMEM((TILE, QROWS), jnp.float32),
            pltpu.VMEM((GROUPS + 1, HEAD, QROWS), jnp.float32),
            pltpu.VMEM((GROUPS + 1, 1, QROWS), jnp.float32),
        ],
        compiler_params=pltpu.CompilerParams(vmem_limit_bytes=28 * 1024 * 1024),
        name="attend",
    )(bounds, q, k, v, marks)


CHUNKS = (2, 2, 2, 1, 1)
FIRST = (0, 2, 4, 6, 7)
PIECES = WIDTH // HEAD


def output_kernel(
    slot_ref, heads_ref, wo_ref, out_ref,
    heads, wo, far, near, far_in, near_in, spread, landed, own_sum,
    w_sem, z_send, z_recv, a_send, a_recv, met,
):
    me = lax.axis_index("cp")
    tp = lax.axis_index("tp")
    up, down, across = lax.rem(tp + 1, TP), lax.rem(tp + 3, TP), lax.rem(tp + 2, TP)

    loads = []
    for n, t in enumerate((across, up, down, tp)):
        columns = pl.ds(pl.multiple_of(t * WIDTH, WIDTH), WIDTH)
        loads.append(pltpu.make_async_copy(wo_ref.at[:, columns], wo.at[n], w_sem.at[n]))
        loads[-1].start()

    barrier = pltpu.get_barrier_semaphore()

    core, ycoord, xcoord = lax.rem(me, 2), lax.rem(me // 2, 4), me // 8
    partner = me + 1 - 2 * core

    def signal(semaphore, target):
        pl.semaphore_signal(semaphore, inc=1, device_id={"cp": target}, device_id_type=MESH)

    along_x = [(lax.rem(xcoord + n, 4) * 4 + ycoord) * 2 + core for n in (1, 2, 3)]
    along_y = [(xcoord * 4 + lax.rem(ycoord + n, 4)) * 2 + core for n in (1, 2, 3)]
    pl.semaphore_signal(barrier, inc=1, device_id={"tp": up}, device_id_type=MESH)
    pl.semaphore_signal(barrier, inc=1, device_id={"tp": down}, device_id_type=MESH)
    for target in (*along_x, *along_y, partner):
        signal(barrier, target)

    turned_row = lax.broadcasted_iota(jnp.int32, (QROWS, QROWS), 0)
    turned_column = lax.broadcasted_iota(jnp.int32, (QROWS, QROWS), 1)
    rows = SPAN * PORTION
    head, at_row = turned_row // rows, lax.rem(turned_row, rows)
    source = (
        lax.rem(head, 4) * 2 * rows
        + (at_row // PORTION) * 2 * PORTION
        + (head // 4) * PORTION
        + lax.rem(at_row, PORTION)
    )
    select = (turned_column == source).astype(jnp.float32).astype(jnp.bfloat16)
    for g in range(GROUPS):
        part = lax.dot_general(
            select,
            heads_ref[g],
            (((1,), (1,)), ((), ())),
            preferred_element_type=jnp.float32,
        ).astype(jnp.bfloat16)
        for h in range(HEADS):
            heads[g * rows : (g + 1) * rows, h * HEAD : (h + 1) * HEAD] = part[
                h * rows : (h + 1) * rows
            ]

    def product(n, c):
        columns = slice(FIRST[c] * HEAD, (FIRST[c] + CHUNKS[c]) * HEAD)
        return jnp.dot(heads[...], wo[n, :, columns], preferred_element_type=jnp.float32)

    def remote(n, src, dst, target):
        return pltpu.make_async_remote_copy(
            src_ref=src,
            dst_ref=dst,
            send_sem=z_send.at[0],
            recv_sem=z_recv.at[n],
            device_id={"tp": target},
            device_id_type=MESH,
        )

    half = ROWS // 2
    upper, lower = pl.ds(0, half), pl.ds(half, half)
    far_copies, near_copies = [], []
    for c, count in enumerate(CHUNKS):
        at = pl.ds(FIRST[c], count)
        far_copies.append(
            (
                remote(3 * c, far.at[0, at], far_in.at[0, at], up),
                remote(3 * c + 1, far.at[1, at], far_in.at[1, at], down),
            )
        )
        near_copies.append(
            (
                remote(3 * c + 2, near.at[0, at], near_in.at[0, at], up),
                remote(3 * c + 2, near.at[1, at], near_in.at[1, at], down),
            )
        )

    def pieces(c):
        return [(FIRST[c] + n, slice(n * HEAD, (n + 1) * HEAD)) for n in range(CHUNKS[c])]

    def make_far(c):
        value = product(0, c).astype(jnp.bfloat16)
        for at, columns in pieces(c):
            far[0, at] = value[:half, columns]
            far[1, at] = value[half:, columns]

    def send_far(c):
        for copy in far_copies[c]:
            copy.start()

    def send_near(c):
        to_up, to_down = product(1, c), product(2, c)
        far_copies[c][0].wait_recv()
        for at, columns in pieces(c):
            near[0, at, upper] = (
                to_up[:half, columns] + far_in[0, at].astype(jnp.float32)
            ).astype(jnp.bfloat16)
            near[0, at, lower] = to_up[half:, columns].astype(jnp.bfloat16)
        near_copies[c][0].start()
        far_copies[c][1].wait_recv()
        for at, columns in pieces(c):
            near[1, at, upper] = to_down[:half, columns].astype(jnp.bfloat16)
            near[1, at, lower] = (
                to_down[half:, columns] + far_in[1, at].astype(jnp.float32)
            ).astype(jnp.bfloat16)
        near_copies[c][1].start()

    def sum_own(c):
        value = product(3, c)
        for at, columns in pieces(c):
            own_sum[at] = value[:, columns]

    row = lax.broadcasted_iota(jnp.int32, (ROWS, ROWS), 0)
    column = lax.broadcasted_iota(jnp.int32, (ROWS, ROWS), 1)
    to_owner = (row == slot_ref[0:1, :]).astype(jnp.float32).astype(jnp.bfloat16)
    origin = (lax.rem(row, BLOCK) // 4) * 8 + (row // BLOCK) * 4 + lax.rem(row, 4)
    to_place = (column == origin).astype(jnp.float32).astype(jnp.bfloat16)

    def acopy(c, target, slot):
        at = pl.ds(FIRST[c], CHUNKS[c])
        return pltpu.make_async_remote_copy(
            src_ref=spread.at[target, at],
            dst_ref=landed.at[slot, at],
            send_sem=a_send.at[c],
            recv_sem=a_recv.at[c],
            device_id={"cp": target},
            device_id_type=MESH,
        )

    def finish_sum(c):
        both = near_in.at[:, pl.ds(FIRST[c], CHUNKS[c])]
        pltpu.make_async_copy(both, both, z_recv.at[3 * c + 2]).wait()
        total = jnp.concatenate(
            [
                (
                    own_sum[at]
                    + near_in[0, at].astype(jnp.float32)
                    + near_in[1, at].astype(jnp.float32)
                ).astype(jnp.bfloat16)
                for at, columns in pieces(c)
            ],
            axis=1,
        )
        picked = jnp.dot(to_owner, total, preferred_element_type=jnp.float32)
        for at, columns in pieces(c):
            spread[:, at] = picked[:, columns].reshape(CP, 8, HEAD).astype(jnp.bfloat16)
            landed[me, at] = spread[me, at]

        def send(k, carry):
            acopy(c, lax.rem(me + k, CP), me).start()
            return carry

        lax.fori_loop(1, CP, send, 0)

    def place(c):
        everyone = landed.at[pl.ds(0, CP - 1), pl.ds(FIRST[c], CHUNKS[c])]
        pltpu.make_async_copy(everyone, everyone, a_recv.at[c]).wait()
        rows = jnp.concatenate(
            [
                landed[:, at].astype(jnp.float32).reshape(ROWS, HEAD).astype(jnp.bfloat16)
                for at, columns in pieces(c)
            ],
            axis=1,
        )
        out_ref[:, FIRST[c] * HEAD : (FIRST[c] + CHUNKS[c]) * HEAD] = jnp.dot(
            to_place, rows, preferred_element_type=jnp.float32
        ).astype(jnp.bfloat16)

    loads[0].wait()
    make_far(0)
    pl.semaphore_wait(barrier, 9)
    send_far(0)
    for target in along_x:
        signal(met.at[0], target)
    make_far(1)
    send_far(1)
    make_far(2)
    send_far(2)
    loads[1].wait()
    loads[2].wait()
    send_near(0)
    pl.semaphore_wait(met.at[0], 3)
    signal(met.at[1], partner)
    make_far(3)
    send_far(3)
    send_near(1)
    make_far(4)
    send_far(4)
    send_near(2)
    loads[3].wait()
    for c in range(len(CHUNKS)):
        sum_own(c)
    send_near(3)
    pl.semaphore_wait(met.at[1], 1)
    finish_sum(0)
    send_near(4)
    finish_sum(1)
    finish_sum(2)
    finish_sum(3)
    finish_sum(4)
    for c in range(len(CHUNKS)):
        place(c)
    for c in range(len(CHUNKS)):
        everyone = spread.at[pl.ds(0, CP - 1), pl.ds(FIRST[c], CHUNKS[c])]
        pltpu.make_async_copy(everyone, everyone, a_send.at[c]).wait()
    sent = wo.at[0, pl.ds(0, 3 * ROWS)]
    pltpu.make_async_copy(sent, sent, z_send.at[0]).wait()


def output_call(slot_rows, heads, wo):
    vmem = pl.BlockSpec(memory_space=pltpu.VMEM)
    dma = pltpu.SemaphoreType.DMA
    half = ROWS // 2
    bf16 = jnp.bfloat16
    return pl.pallas_call(
        output_kernel,
        out_shape=jax.ShapeDtypeStruct((ROWS, WIDTH), bf16),
        in_specs=[vmem, vmem, pl.BlockSpec(memory_space=pltpu.HBM)],
        out_specs=vmem,
        scratch_shapes=[
            pltpu.VMEM((ROWS, WIDTH), bf16),
            pltpu.VMEM((TP, WIDTH, WIDTH), bf16),
            pltpu.VMEM((2, PIECES, half, HEAD), bf16),
            pltpu.VMEM((2, PIECES, ROWS, HEAD), bf16),
            pltpu.VMEM((2, PIECES, half, HEAD), bf16),
            pltpu.VMEM((2, PIECES, ROWS, HEAD), bf16),
            pltpu.VMEM((CP, PIECES, 8, HEAD), bf16),
            pltpu.VMEM((CP, PIECES, 8, HEAD), bf16),
            pltpu.VMEM((PIECES, ROWS, HEAD), jnp.float32),
            dma((4,)), dma((1,)), dma((3 * len(CHUNKS),)),
            dma((len(CHUNKS),)), dma((len(CHUNKS),)), pltpu.SemaphoreType.REGULAR((2,)),
        ],
        compiler_params=pltpu.CompilerParams(
            collective_id=1, has_side_effects=True, vmem_limit_bytes=40 * 1024 * 1024
        ),
        name="project_out",
    )(slot_rows, heads, wo)


def local(hidden, query_weight, key_matrix, value_matrix, output_weight, bounds, block_owner):
    inverse = rope_inverse(HEAD)
    inverse = jnp.concatenate([inverse, inverse])[None, :]
    hidden, query_weight, key_matrix, value_matrix, output_weight = (
        pltpu.with_memory_space_constraint(a, pltpu.HBM)
        for a in (hidden, query_weight, key_matrix, value_matrix, output_weight)
    )
    keys, values, queries, marks, slot_rows = gather_call(
        pltpu.with_memory_space_constraint(bounds, pltpu.HBM),
        pltpu.with_memory_space_constraint(block_owner, pltpu.HBM), hidden, query_weight, key_matrix, value_matrix, inverse
    )
    heads = attend_call(
        bounds,
        queries.reshape(2 * ROWS, WIDTH // 2),
        keys.reshape(TOKENS, HEAD),
        values.reshape(TOKENS, HEAD),
        marks,
    )
    return output_call(slot_rows, heads, output_weight)


def solution(mesh):
    placed = (P("cp", "tp"), P(None, "tp"), P(None, "tp"), P(None, "tp"), P("tp", None), P(), P())
    return jax.shard_map(
        local, mesh=mesh, in_specs=placed, out_specs=P("cp", "tp"), check_vma=False
    )
```

```python
import functools
import math

import jax
import jax.numpy as jnp
from jax import lax
from jax.experimental import pallas as pl
from jax.experimental.pallas import tpu as pltpu
from jax.sharding import PartitionSpec as P

HEAD = 128
BLOCK = 128
CP = 32
TP = 4
ROWS = 256
WIDTH = 1024
NBLK = 64
HEADS = 8
TOKENS = 8192
PORTION = BLOCK // CP

rope_theta = 500000.0
rope_factor = 8.0
rope_context = 8192.0
masked_score = -1e30
MESH = pl.DeviceIdType.MESH


def rope_inverse(head_size):
    halves = jnp.arange(head_size // 2, dtype=jnp.float32)
    inverse = 1.0 / rope_theta ** (2.0 * halves / head_size)
    wavelength = 2.0 * math.pi / inverse
    smooth = (rope_context / wavelength - 1.0) / 3.0
    blended = (1.0 - smooth) * inverse / rope_factor + smooth * inverse
    longer = jnp.where(wavelength > rope_context, inverse / rope_factor, blended)
    return jnp.where(wavelength < rope_context / 4.0, inverse, longer)


def starts_of(tokens, bounds_ref):
    start = jnp.zeros_like(tokens)
    for i in range(1, 8):
        bound = bounds_ref[i]
        start = jnp.where(tokens >= bound, bound, start)
    return start


SIZES = (64, 64, 64, 32, 32)
STARTS = (0, 64, 128, 192, 224)
PARTS = len(SIZES)
STRAIGHT1 = (True, False, True, True, True)
STRAIGHT2 = (True, False, False, False, True)
SPAN = 8
PENALTY = -1e30


def gather_kernel(
    bounds_hbm, owner_hbm, hidden_ref, wq_ref, wk_ref, wv_ref, inverse_ref,
    k_ref, v_ref, q_ref, mark_ref, slot_ref,
    full, wq, wkv, qtmp, qsend, cosine, sine,
    w_sem, z_send, z_recv, g_send, g_recv, q_send, q_recv, bounds_ref, owner_ref, met,
):
    me = lax.axis_index("cp")
    tp = lax.axis_index("tp")
    core = lax.rem(me, 2)
    ycoord = lax.rem(me // 2, 4)
    xcoord = me // 8
    partner = me + 1 - 2 * core
    up, down = lax.rem(tp + 1, TP), lax.rem(tp + 3, TP)
    own_columns = pl.ds(pl.multiple_of(tp * WIDTH, WIDTH), WIDTH)

    bring = pltpu.make_async_copy(hidden_ref, full.at[:, own_columns], w_sem.at[3])
    weights = [
        pltpu.make_async_copy(wk_ref, wkv.at[:, pl.ds(0, HEAD)], w_sem.at[0]),
        pltpu.make_async_copy(wv_ref, wkv.at[:, pl.ds(HEAD, HEAD)], w_sem.at[1]),
        pltpu.make_async_copy(wq_ref, wq, w_sem.at[2]),
    ]
    bring_bounds = pltpu.make_async_copy(bounds_hbm, bounds_ref, w_sem.at[4])
    bring_owner = pltpu.make_async_copy(owner_hbm, owner_ref, w_sem.at[5])
    bring.start()
    bring_bounds.start()
    bring_owner.start()
    for copy in weights:
        copy.start()

    barrier = pltpu.get_barrier_semaphore()

    def signal(semaphore, target):
        pl.semaphore_signal(semaphore, inc=1, device_id={"cp": target}, device_id_type=MESH)

    along_x = [(lax.rem(xcoord + n, 4) * 4 + ycoord) * 2 + core for n in (1, 2, 3)]
    along_y = [(xcoord * 4 + lax.rem(ycoord + n, 4)) * 2 + core for n in (1, 2, 3)]
    pl.semaphore_signal(barrier, inc=1, device_id={"tp": up}, device_id_type=MESH)
    pl.semaphore_signal(barrier, inc=1, device_id={"tp": down}, device_id_type=MESH)
    for target in (*along_x, *along_y, partner):
        signal(barrier, target)
    bring.wait()
    pl.semaphore_wait(barrier, 9)

    def zcopy(n, target, owner, row, count):
        columns = pl.ds(pl.multiple_of(owner * WIDTH, WIDTH), WIDTH)
        ref = full.at[pl.ds(row, count), columns]
        return pltpu.make_async_remote_copy(
            src_ref=ref,
            dst_ref=ref,
            send_sem=z_send.at[0],
            recv_sem=z_recv.at[n],
            device_id={"tp": target},
            device_id_type=MESH,
        )

    own = [
        (
            zcopy(2 * r, up, tp, STARTS[r], SIZES[r]),
            zcopy(2 * r, down, tp, STARTS[r], SIZES[r]),
        )
        for r in range(PARTS)
    ]
    fwd = [
        (
            zcopy(2 * r + 1, down, up, STARTS[r], SIZES[r] // 2),
            zcopy(2 * r + 1, up, down, STARTS[r] + SIZES[r] // 2, SIZES[r] // 2),
        )
        for r in range(PARTS)
    ]

    def wait_for(ref, semaphore):
        pltpu.make_async_copy(ref, ref, semaphore).wait()

    def arrived_z(n, r, owners):
        wait_for(
            full.at[pl.ds(STARTS[r], SIZES[r]), pl.ds(0, owners * WIDTH)], z_recv.at[2 * r + n]
        )
    for copy in (*own[0], *own[1]):
        copy.start()
    for target in along_x:
        signal(met.at[0], target)
    bring_bounds.wait()

    def relay_z(r):
        arrived_z(0, r, 2)
        for copy in fwd[r]:
            copy.start()
        if r + 2 < PARTS:
            for copy in own[r + 2]:
                copy.start()

    lanes = lax.broadcasted_iota(jnp.int32, (BLOCK, HEAD), 1)
    sublanes = lax.broadcasted_iota(jnp.int32, (BLOCK, HEAD), 0)
    inverse = inverse_ref[...]
    for r in range(2):
        tokens = me * ROWS + r * BLOCK + sublanes
        angle = (tokens - starts_of(tokens, bounds_ref)).astype(jnp.float32) * inverse
        turn = jnp.sin(angle)
        cosine[pl.ds(r * BLOCK, BLOCK), :] = jnp.cos(angle)
        sine[pl.ds(r * BLOCK, BLOCK), :] = jnp.where(lanes < HEAD // 2, -turn, turn)

    place = jnp.minimum(jnp.maximum(sublanes - me * PORTION, 0), PORTION)

    def mark(b, carry):
        tokens = b * BLOCK + sublanes
        document = jnp.zeros_like(tokens)
        for i in range(1, 8):
            document = jnp.where(tokens >= bounds_ref[i], i, document)
        spot = 8 + lax.rem(b, SPAN) * (PORTION + 1) + place
        hit = (lanes == document) | (lanes == spot)
        mark_ref[pl.ds(pl.multiple_of(b * BLOCK, BLOCK), BLOCK), :] = (
            hit.astype(jnp.float32).astype(jnp.bfloat16)
        )
        return carry

    lax.fori_loop(0, NBLK // 2, mark, 0)
    weights[0].wait()
    weights[1].wait()
    weights[2].wait()

    def slots():
        spot = lax.broadcasted_iota(jnp.int32, (8, ROWS), 1)
        block = spot // PORTION
        owner = jnp.zeros_like(spot)
        for b in range(NBLK):
            owner = jnp.where(block == b, owner_ref[b], owner)
        rank = jnp.zeros_like(spot)
        for b in range(NBLK - 1):
            rank = rank + ((block > b) & (owner == owner_ref[b])).astype(jnp.int32)
        place = (owner * 2 + rank) * PORTION + lax.rem(spot, PORTION)
        slot_ref[...] = place

    def rotate(raw, row, count):
        table = pl.ds(row, count)
        return raw * cosine[table, :] + pltpu.roll(raw, HEAD // 2, 1) * sine[table, :]

    def queries(r, n):
        columns = slice(n * 2 * HEAD, (n + 1) * 2 * HEAD)
        rows = pl.ds(r * BLOCK, BLOCK)
        raw = jnp.dot(full[rows, :], wq[:, columns], preferred_element_type=jnp.float32)
        turned = jnp.concatenate(
            [rotate(raw[:, :HEAD], r * BLOCK, BLOCK), rotate(raw[:, HEAD:], r * BLOCK, BLOCK)],
            axis=1,
        )
        qtmp[pl.ds((n // 2) * BLOCK, BLOCK), (n % 2) * 2 * HEAD : (n % 2 + 1) * 2 * HEAD] = (
            turned.astype(jnp.bfloat16)
        )

    def gather(which, r):
        buffer = (k_ref, v_ref)[which]
        a, b = ((xcoord, ycoord), (ycoord, xcoord))[which]

        def neighbour(along, step):
            if along == 0:
                na, nb = lax.rem(a + step, 4), b
            else:
                na, nb = a, lax.rem(b + step, 4)
            x, y = ((na, nb), (nb, na))[which]
            return (x * 4 + y) * 2 + core

        def copy(n, ref, target):
            return pltpu.make_async_remote_copy(
                src_ref=ref,
                dst_ref=ref,
                send_sem=g_send.at[r],
                recv_sem=g_recv.at[r, n],
                device_id={"cp": target},
                device_id_type=MESH,
            )

        def piece(at, row, count):
            rows = pl.ds(STARTS[r] + row, count)
            if which == 0:
                return buffer.at[at, b, core, rows]
            return buffer.at[b, at, core, rows]

        def line(at, first, count):
            along, rows = pl.ds(first, count), pl.ds(STARTS[r], SIZES[r])
            if which == 0:
                return buffer.at[along, at, core, rows]
            return buffer.at[at, along, core, rows]

        a_next, a_prev = lax.rem(a + 1, 4), lax.rem(a + 3, 4)
        b_next, b_prev = lax.rem(b + 1, 4), lax.rem(b + 3, 4)
        b_far = lax.rem(b + 2, 4)
        size, half = SIZES[r], SIZES[r] // 2
        return dict(
            ring1=(
                copy(0, piece(a, 0, size), neighbour(0, 1)),
                copy(0, piece(a, 0, size), neighbour(0, 3)),
            ),
            ring1_far=(copy(1, piece(a, 0, size), neighbour(0, 2)),)
            if STRAIGHT1[r]
            else (
                copy(1, piece(a_prev, 0, half), neighbour(0, 1)),
                copy(1, piece(a_next, half, half), neighbour(0, 3)),
            ),
            ring2=(
                copy(2, line(b, 0, 4), neighbour(1, 1)),
                copy(2, line(b, 0, 4), neighbour(1, 3)),
            ),
            ring2_far=(copy(3, line(b, 0, 4), neighbour(1, 2)),)
            if STRAIGHT2[r]
            else (
                copy(3, line(b_prev, 0, 2), neighbour(1, 1)),
                copy(3, line(b_next, 2, 2), neighbour(1, 3)),
            ),
            across=(
                copy(4, line(b, 0, 4), partner),
                copy(4, line(b_prev, 0, 4), partner),
                copy(4, line(b_next, 0, 4), partner),
                copy(4, line(b_far, 0, 4), partner),
            ),
        )

    flows = [[gather(which, r) for which in range(2)] for r in range(PARTS)]

    def start(r, name):
        for flow in flows[r]:
            for copy in flow[name]:
                copy.start()

    def arrived(r, name):
        rows = pl.ds(STARTS[r], SIZES[r])
        n, ref = {
            "ring1": (0, k_ref.at[0, :, core, rows]),
            "ring1_far": (1, k_ref.at[0, pl.ds(0, 2), core, rows]),
            "ring2": (2, k_ref.at[:, :, core, rows]),
            "ring2_far": (3, k_ref.at[pl.ds(0, 2), :, core, rows]),
            "across": (4, k_ref.at[:, :, :, rows]),
        }[name]
        wait_for(ref, g_recv.at[r, n])

    def across(r, which):
        for flow in flows[r]:
            for n in which:
                flow["across"][n].start()

    def s0(r):
        arrived_z(1, r, 1)
        rows = pl.ds(STARTS[r], SIZES[r])
        raw = jnp.dot(full[rows, :], wkv[...], preferred_element_type=jnp.float32)
        k_ref[xcoord, ycoord, core, rows] = rotate(raw[:, :HEAD], STARTS[r], SIZES[r]).astype(
            jnp.bfloat16
        )
        v_ref[xcoord, ycoord, core, rows] = raw[:, HEAD:].astype(jnp.bfloat16)
        start(r, "ring1")
        if STRAIGHT1[r]:
            start(r, "ring1_far")

    def s1(r):
        arrived(r, "ring1")
        if not STRAIGHT1[r]:
            start(r, "ring1_far")

    def s2(r):
        arrived(r, "ring1_far")
        start(r, "ring2")
        if STRAIGHT2[r]:
            start(r, "ring2_far")
        across(r, (0,))

    def s3(r):
        arrived(r, "ring2")
        if not STRAIGHT2[r]:
            start(r, "ring2_far")
        across(r, (1, 2))

    def s4(r):
        arrived(r, "ring2_far")
        across(r, (3,))

    out_row = lax.broadcasted_iota(jnp.int32, (ROWS, ROWS), 0)
    in_row = lax.broadcasted_iota(jnp.int32, (ROWS, ROWS), 1)
    origin = lax.rem(out_row // 4, 2) * BLOCK + (out_row // 8) * 4 + lax.rem(out_row, 4)
    pick = (in_row == origin).astype(jnp.float32).astype(jnp.bfloat16)

    def qcopy(r, target, slot):
        return pltpu.make_async_remote_copy(
            src_ref=qsend.at[r, target],
            dst_ref=q_ref.at[slot, r],
            send_sem=q_send.at[r],
            recv_sem=q_recv.at[r],
            device_id={"cp": target},
            device_id_type=MESH,
        )

    def spread(r):
        ordered = jnp.dot(pick, qtmp[...], preferred_element_type=jnp.float32)
        qsend[r] = ordered.reshape(CP, 8, WIDTH // 2).astype(jnp.bfloat16)
        q_ref[me, r] = qsend[r, me]

        def send(k, carry):
            qcopy(r, lax.rem(me + k, CP), me).start()
            return carry

        lax.fori_loop(1, CP, send, 0)

    def spread_done(r):
        sent, landed = qsend.at[r, pl.ds(0, CP - 1)], q_ref.at[pl.ds(0, CP - 1), r]
        pltpu.make_async_copy(sent, sent, q_send.at[r]).wait()
        pltpu.make_async_copy(landed, landed, q_recv.at[r]).wait()

    relay_z(0)
    pl.semaphore_wait(met.at[0], 3)
    signal(met.at[1], partner)
    bring_owner.wait()
    slots()
    lax.fori_loop(NBLK // 2, NBLK, mark, 0)
    relay_z(1)
    pl.semaphore_wait(met.at[1], 1)
    s0(0)
    relay_z(2)
    s1(0)
    s0(1)
    s2(0)
    queries(0, 0)
    queries(0, 1)
    relay_z(3)
    queries(0, 2)
    queries(0, 3)
    s0(2)
    s1(1)
    spread(0)
    relay_z(4)
    s0(3)
    s3(0)
    s1(2)
    s2(1)
    s4(0)
    s0(4)
    s2(2)
    queries(1, 0)
    queries(1, 1)
    queries(1, 2)
    queries(1, 3)
    s1(3)
    s2(3)
    s3(1)
    s1(4)
    s2(4)
    spread(1)
    s3(2)
    s3(3)
    s4(1)
    s3(4)
    s4(2)
    s4(4)
    s4(3)
    spread_done(0)
    spread_done(1)
    for r in range(PARTS):
        arrived(r, "across")
        wait_for(mark_ref.at[pl.ds(0, 62 * SIZES[r])], g_send.at[r])
    wait_for(full.at[:, pl.ds(0, 3 * WIDTH)], z_send.at[0])


def gather_call(bounds, owner, hidden, wq, wk, wv, inverse):
    vmem = pl.BlockSpec(memory_space=pltpu.VMEM)
    hbm = pl.BlockSpec(memory_space=pltpu.HBM)
    kv = jax.ShapeDtypeStruct((4, 4, 2, ROWS, HEAD), jnp.bfloat16)
    dma = pltpu.SemaphoreType.DMA
    return pl.pallas_call(
        gather_kernel,
        out_shape=(
            kv,
            kv,
            jax.ShapeDtypeStruct((CP, 2, 8, WIDTH // 2), jnp.bfloat16),
            jax.ShapeDtypeStruct((TOKENS, HEAD), jnp.bfloat16),
            jax.ShapeDtypeStruct((8, ROWS), jnp.int32),
        ),
        in_specs=[hbm, hbm, hbm, hbm, hbm, hbm, vmem],
        out_specs=(vmem, vmem, vmem, vmem, vmem),
        scratch_shapes=[
            pltpu.VMEM((ROWS, TP * WIDTH), jnp.bfloat16),
            pltpu.VMEM((TP * WIDTH, WIDTH), jnp.bfloat16),
            pltpu.VMEM((TP * WIDTH, 2 * HEAD), jnp.bfloat16),
            pltpu.VMEM((ROWS, WIDTH // 2), jnp.bfloat16),
            pltpu.VMEM((2, CP, 8, WIDTH // 2), jnp.bfloat16),
            pltpu.VMEM((ROWS, HEAD), jnp.float32),
            pltpu.VMEM((ROWS, HEAD), jnp.float32),
            dma((6,)), dma((1,)), dma((2 * PARTS,)),
            dma((PARTS,)), dma((PARTS, 5)), dma((2,)), dma((2,)),
            pltpu.SMEM((9,), jnp.int32), pltpu.SMEM((NBLK,), jnp.int32),
            pltpu.SemaphoreType.REGULAR((2,)),
        ],
        compiler_params=pltpu.CompilerParams(
            collective_id=0, has_side_effects=True, vmem_limit_bytes=32 * 1024 * 1024
        ),
        name="gather_project",
    )(bounds, owner, hidden, wq, wk, wv, inverse)


TILE = SPAN * BLOCK


GROUPS = NBLK // SPAN
QROWS = 4 * SPAN * 8
PIECE = 256


def attend_kernel(
    bounds_ref, q_ref, k_ref, v_ref, mark_ref, o_ref,
    turned, penalty_ref, even, odd, mixed_ref, total_ref,
):
    rows = SPAN * 8
    factor = math.log2(math.e) / math.sqrt(HEAD)
    row = lax.rem(lax.broadcasted_iota(jnp.int32, (rows, HEAD), 0), rows)
    lane = lax.broadcasted_iota(jnp.int32, (rows, HEAD), 1)
    block, step = row // 8, lax.rem(row, PORTION)
    key_block, key_step = (lane - 8) // (PORTION + 1), lax.rem(lane - 8, PORTION + 1)
    later = (key_block > block) | ((key_block == block) & (key_step > step))
    later = later & (lane >= 8) & (lane < 8 + SPAN * (PORTION + 1))
    me = lax.axis_index("cp")
    contract_last = (((1,), (1,)), ((), ()))
    diagonal = lax.broadcasted_iota(jnp.int32, (HEAD, HEAD), 0) == lax.broadcasted_iota(
        jnp.int32, (HEAD, HEAD), 1
    )
    identity = diagonal.astype(jnp.float32).astype(jnp.bfloat16)

    def prepare(g, carry):
        at = pl.ds(pl.multiple_of(g * TILE, TILE), TILE)
        turned[:, at] = lax.dot_general(
            identity, v_ref[at, :], contract_last, preferred_element_type=jnp.float32
        ).astype(jnp.bfloat16)
        tokens = (g * SPAN + block) * BLOCK + me * PORTION + step
        document = jnp.zeros_like(tokens)
        for i in range(1, 8):
            document = jnp.where(tokens >= bounds_ref[i], i, document)
        other = (lane < 8) & (lane != document)
        penalty_ref[2 * g] = jnp.where(other, PENALTY, 0.0).astype(jnp.bfloat16)
        penalty_ref[2 * g + 1] = jnp.where(other | later, PENALTY, 0.0).astype(jnp.bfloat16)
        return carry

    lax.fori_loop(0, GROUPS, prepare, 0)

    def lowest(g):
        low = jnp.int32(0)
        for i in range(1, 8):
            low = jnp.where(g * TILE >= bounds_ref[i], bounds_ref[i], low)
        return low // TILE

    def following(item):
        g, j = item
        more = j > lowest(g)
        return jnp.where(more, g, g + 1), jnp.where(more, j - 1, g + 1)

    def score(item, ref):
        g, j = item
        own = jnp.where(g == j, 1, 0)
        held = jnp.minimum(g, GROUPS - 1)
        penalties = penalty_ref[2 * held + own]
        asking = pl.ds(pl.multiple_of(held * rows, rows), rows)
        q = jnp.concatenate(
            [
                jnp.concatenate([q_ref[asking, h * HEAD : (h + 1) * HEAD], penalties], axis=1)
                for h in range(4)
            ],
            axis=0,
        )
        for part in range(2):
            size = TILE // 2
            first = jnp.minimum(j, GROUPS - 1) * TILE + part * size
            at = pl.ds(pl.multiple_of(first, size), size)
            scores = lax.dot_general(
                jnp.concatenate([k_ref[at, :], mark_ref[at, :]], axis=1),
                q,
                contract_last,
                preferred_element_type=jnp.float32,
            )
            ref[part * size : (part + 1) * size, :] = scores
            top = jnp.max(scores, axis=0, keepdims=True)
            largest = top if part == 0 else jnp.maximum(largest, top)
        return largest

    def soften(item, ref, largest, state):
        g, j = item
        top, total, mixed = state
        top = jnp.where(g == j, 0.5 * PENALTY, top)
        start = jnp.minimum(j, GROUPS - 1) * TILE
        new_top = jnp.maximum(top, largest)
        shrink = jnp.exp2((top - new_top) * factor)
        total, mixed = total * shrink, mixed * shrink
        for first in range(0, TILE, PIECE):
            piece = slice(first, first + PIECE)
            weights = jnp.exp2((ref[piece, :] - new_top) * factor)
            total = total + jnp.sum(weights, axis=0, keepdims=True)
            keys = pl.ds(pl.multiple_of(start + first, PIECE), PIECE)
            mixed = mixed + jnp.dot(
                turned[:, keys], weights.astype(jnp.bfloat16), preferred_element_type=jnp.float32
            )
        mixed_ref[g] = mixed
        total_ref[g] = total
        return new_top, total, mixed

    count = lax.fori_loop(0, GROUPS, lambda g, n: n + g + 1 - lowest(g), jnp.int32(0))
    zero = jnp.int32(0)
    highest = score((zero, zero), even)

    def pair(n, carry):
        g, j, largest, *state = carry
        item = (g, j)
        second = following(item)
        second_largest = score(second, odd)
        state = soften(item, even, largest, state)
        third = following(second)
        third = (jnp.minimum(third[0], GROUPS), jnp.minimum(third[1], GROUPS))
        largest = score(third, even)
        state = soften(second, odd, second_largest, state)
        return (*third, largest, *state)

    lax.fori_loop(
        0,
        (count + 1) // 2,
        pair,
        (
            zero,
            zero,
            highest,
            jnp.full((1, QROWS), 0.5 * PENALTY, jnp.float32),
            jnp.zeros((1, QROWS), jnp.float32),
            jnp.zeros((HEAD, QROWS), jnp.float32),
        ),
    )

    def finish(g, carry):
        o_ref[g] = (mixed_ref[g] / total_ref[g]).astype(jnp.bfloat16)
        return carry

    lax.fori_loop(0, GROUPS, finish, 0)


def attend_call(bounds, q, k, v, marks):
    vmem = pl.BlockSpec(memory_space=pltpu.VMEM)
    return pl.pallas_call(
        attend_kernel,
        out_shape=jax.ShapeDtypeStruct((GROUPS, HEAD, QROWS), jnp.bfloat16),
        in_specs=[pl.BlockSpec(memory_space=pltpu.SMEM), vmem, vmem, vmem, vmem],
        out_specs=vmem,
        scratch_shapes=[
            pltpu.VMEM((HEAD, TOKENS), jnp.bfloat16),
            pltpu.VMEM((2 * GROUPS, SPAN * 8, HEAD), jnp.bfloat16),
            pltpu.VMEM((TILE, QROWS), jnp.float32),
            pltpu.VMEM((TILE, QROWS), jnp.float32),
            pltpu.VMEM((GROUPS + 1, HEAD, QROWS), jnp.float32),
            pltpu.VMEM((GROUPS + 1, 1, QROWS), jnp.float32),
        ],
        compiler_params=pltpu.CompilerParams(vmem_limit_bytes=28 * 1024 * 1024),
        name="attend",
    )(bounds, q, k, v, marks)


CHUNKS = (2, 2, 2, 1, 1)
FIRST = (0, 2, 4, 6, 7)
PIECES = WIDTH // HEAD


def output_kernel(
    slot_ref, heads_ref, wo_ref, out_ref,
    heads, wo, far, near, far_in, near_in, spread, landed, own_sum,
    w_sem, z_send, z_recv, a_send, a_recv, met,
):
    me = lax.axis_index("cp")
    tp = lax.axis_index("tp")
    up, down, across = lax.rem(tp + 1, TP), lax.rem(tp + 3, TP), lax.rem(tp + 2, TP)

    loads = []
    for n, t in enumerate((across, up, down, tp)):
        columns = pl.ds(pl.multiple_of(t * WIDTH, WIDTH), WIDTH)
        loads.append(pltpu.make_async_copy(wo_ref.at[:, columns], wo.at[n], w_sem.at[n]))
        loads[-1].start()

    barrier = pltpu.get_barrier_semaphore()

    core, ycoord, xcoord = lax.rem(me, 2), lax.rem(me // 2, 4), me // 8
    partner = me + 1 - 2 * core

    def signal(semaphore, target):
        pl.semaphore_signal(semaphore, inc=1, device_id={"cp": target}, device_id_type=MESH)

    along_x = [(lax.rem(xcoord + n, 4) * 4 + ycoord) * 2 + core for n in (1, 2, 3)]
    along_y = [(xcoord * 4 + lax.rem(ycoord + n, 4)) * 2 + core for n in (1, 2, 3)]
    pl.semaphore_signal(barrier, inc=1, device_id={"tp": up}, device_id_type=MESH)
    pl.semaphore_signal(barrier, inc=1, device_id={"tp": down}, device_id_type=MESH)
    for target in (*along_x, *along_y, partner):
        signal(barrier, target)

    turned_row = lax.broadcasted_iota(jnp.int32, (QROWS, QROWS), 0)
    turned_column = lax.broadcasted_iota(jnp.int32, (QROWS, QROWS), 1)
    rows = SPAN * PORTION
    head, at_row = turned_row // rows, lax.rem(turned_row, rows)
    source = (
        lax.rem(head, 4) * 2 * rows
        + (at_row // PORTION) * 2 * PORTION
        + (head // 4) * PORTION
        + lax.rem(at_row, PORTION)
    )
    select = (turned_column == source).astype(jnp.float32).astype(jnp.bfloat16)
    for g in range(GROUPS):
        part = lax.dot_general(
            select,
            heads_ref[g],
            (((1,), (1,)), ((), ())),
            preferred_element_type=jnp.float32,
        ).astype(jnp.bfloat16)
        for h in range(HEADS):
            heads[g * rows : (g + 1) * rows, h * HEAD : (h + 1) * HEAD] = part[
                h * rows : (h + 1) * rows
            ]

    def product(n, c):
        columns = slice(FIRST[c] * HEAD, (FIRST[c] + CHUNKS[c]) * HEAD)
        return jnp.dot(heads[...], wo[n, :, columns], preferred_element_type=jnp.float32)

    def remote(n, src, dst, target):
        return pltpu.make_async_remote_copy(
            src_ref=src,
            dst_ref=dst,
            send_sem=z_send.at[0],
            recv_sem=z_recv.at[n],
            device_id={"tp": target},
            device_id_type=MESH,
        )

    half = ROWS // 2
    upper, lower = pl.ds(0, half), pl.ds(half, half)
    far_copies, near_copies = [], []
    for c, count in enumerate(CHUNKS):
        at = pl.ds(FIRST[c], count)
        far_copies.append(
            (
                remote(3 * c, far.at[0, at], far_in.at[0, at], up),
                remote(3 * c + 1, far.at[1, at], far_in.at[1, at], down),
            )
        )
        near_copies.append(
            (
                remote(3 * c + 2, near.at[0, at], near_in.at[0, at], up),
                remote(3 * c + 2, near.at[1, at], near_in.at[1, at], down),
            )
        )

    def pieces(c):
        return [(FIRST[c] + n, slice(n * HEAD, (n + 1) * HEAD)) for n in range(CHUNKS[c])]

    def make_far(c):
        value = product(0, c).astype(jnp.bfloat16)
        for at, columns in pieces(c):
            far[0, at] = value[:half, columns]
            far[1, at] = value[half:, columns]

    def send_far(c):
        for copy in far_copies[c]:
            copy.start()

    def send_near(c):
        to_up, to_down = product(1, c), product(2, c)
        far_copies[c][0].wait_recv()
        for at, columns in pieces(c):
            near[0, at, upper] = (
                to_up[:half, columns] + far_in[0, at].astype(jnp.float32)
            ).astype(jnp.bfloat16)
            near[0, at, lower] = to_up[half:, columns].astype(jnp.bfloat16)
        near_copies[c][0].start()
        far_copies[c][1].wait_recv()
        for at, columns in pieces(c):
            near[1, at, upper] = to_down[:half, columns].astype(jnp.bfloat16)
            near[1, at, lower] = (
                to_down[half:, columns] + far_in[1, at].astype(jnp.float32)
            ).astype(jnp.bfloat16)
        near_copies[c][1].start()

    def sum_own(c):
        value = product(3, c)
        for at, columns in pieces(c):
            own_sum[at] = value[:, columns]

    row = lax.broadcasted_iota(jnp.int32, (ROWS, ROWS), 0)
    column = lax.broadcasted_iota(jnp.int32, (ROWS, ROWS), 1)
    to_owner = (row == slot_ref[0:1, :]).astype(jnp.float32).astype(jnp.bfloat16)
    origin = (lax.rem(row, BLOCK) // 4) * 8 + (row // BLOCK) * 4 + lax.rem(row, 4)
    to_place = (column == origin).astype(jnp.float32).astype(jnp.bfloat16)

    def acopy(c, target, slot):
        at = pl.ds(FIRST[c], CHUNKS[c])
        return pltpu.make_async_remote_copy(
            src_ref=spread.at[target, at],
            dst_ref=landed.at[slot, at],
            send_sem=a_send.at[c],
            recv_sem=a_recv.at[c],
            device_id={"cp": target},
            device_id_type=MESH,
        )

    def finish_sum(c):
        both = near_in.at[:, pl.ds(FIRST[c], CHUNKS[c])]
        pltpu.make_async_copy(both, both, z_recv.at[3 * c + 2]).wait()
        total = jnp.concatenate(
            [
                (
                    own_sum[at]
                    + near_in[0, at].astype(jnp.float32)
                    + near_in[1, at].astype(jnp.float32)
                ).astype(jnp.bfloat16)
                for at, columns in pieces(c)
            ],
            axis=1,
        )
        picked = jnp.dot(to_owner, total, preferred_element_type=jnp.float32)
        for at, columns in pieces(c):
            spread[:, at] = picked[:, columns].reshape(CP, 8, HEAD).astype(jnp.bfloat16)
            landed[me, at] = spread[me, at]

        def send(k, carry):
            acopy(c, lax.rem(me + k, CP), me).start()
            return carry

        lax.fori_loop(1, CP, send, 0)

    def place(c):
        everyone = landed.at[pl.ds(0, CP - 1), pl.ds(FIRST[c], CHUNKS[c])]
        pltpu.make_async_copy(everyone, everyone, a_recv.at[c]).wait()
        rows = jnp.concatenate(
            [
                landed[:, at].astype(jnp.float32).reshape(ROWS, HEAD).astype(jnp.bfloat16)
                for at, columns in pieces(c)
            ],
            axis=1,
        )
        out_ref[:, FIRST[c] * HEAD : (FIRST[c] + CHUNKS[c]) * HEAD] = jnp.dot(
            to_place, rows, preferred_element_type=jnp.float32
        ).astype(jnp.bfloat16)

    loads[0].wait()
    make_far(0)
    pl.semaphore_wait(barrier, 9)
    send_far(0)
    for target in along_x:
        signal(met.at[0], target)
    make_far(1)
    send_far(1)
    make_far(2)
    send_far(2)
    loads[1].wait()
    loads[2].wait()
    send_near(0)
    pl.semaphore_wait(met.at[0], 3)
    signal(met.at[1], partner)
    make_far(3)
    send_far(3)
    send_near(1)
    make_far(4)
    send_far(4)
    send_near(2)
    loads[3].wait()
    for c in range(len(CHUNKS)):
        sum_own(c)
    send_near(3)
    pl.semaphore_wait(met.at[1], 1)
    finish_sum(0)
    send_near(4)
    finish_sum(1)
    finish_sum(2)
    finish_sum(3)
    finish_sum(4)
    for c in range(len(CHUNKS)):
        place(c)
    for c in range(len(CHUNKS)):
        everyone = spread.at[pl.ds(0, CP - 1), pl.ds(FIRST[c], CHUNKS[c])]
        pltpu.make_async_copy(everyone, everyone, a_send.at[c]).wait()
    sent = wo.at[0, pl.ds(0, 3 * ROWS)]
    pltpu.make_async_copy(sent, sent, z_send.at[0]).wait()


def output_call(slot_rows, heads, wo):
    vmem = pl.BlockSpec(memory_space=pltpu.VMEM)
    dma = pltpu.SemaphoreType.DMA
    half = ROWS // 2
    bf16 = jnp.bfloat16
    return pl.pallas_call(
        output_kernel,
        out_shape=jax.ShapeDtypeStruct((ROWS, WIDTH), bf16),
        in_specs=[vmem, vmem, pl.BlockSpec(memory_space=pltpu.HBM)],
        out_specs=vmem,
        scratch_shapes=[
            pltpu.VMEM((ROWS, WIDTH), bf16),
            pltpu.VMEM((TP, WIDTH, WIDTH), bf16),
            pltpu.VMEM((2, PIECES, half, HEAD), bf16),
            pltpu.VMEM((2, PIECES, ROWS, HEAD), bf16),
            pltpu.VMEM((2, PIECES, half, HEAD), bf16),
            pltpu.VMEM((2, PIECES, ROWS, HEAD), bf16),
            pltpu.VMEM((CP, PIECES, 8, HEAD), bf16),
            pltpu.VMEM((CP, PIECES, 8, HEAD), bf16),
            pltpu.VMEM((PIECES, ROWS, HEAD), jnp.float32),
            dma((4,)), dma((1,)), dma((3 * len(CHUNKS),)),
            dma((len(CHUNKS),)), dma((len(CHUNKS),)), pltpu.SemaphoreType.REGULAR((2,)),
        ],
        compiler_params=pltpu.CompilerParams(
            collective_id=1, has_side_effects=True, vmem_limit_bytes=40 * 1024 * 1024
        ),
        name="project_out",
    )(slot_rows, heads, wo)


def local(hidden, query_weight, key_matrix, value_matrix, output_weight, bounds, block_owner):
    inverse = rope_inverse(HEAD)
    inverse = jnp.concatenate([inverse, inverse])[None, :]
    hidden, query_weight, key_matrix, value_matrix, output_weight = (
        pltpu.with_memory_space_constraint(a, pltpu.HBM)
        for a in (hidden, query_weight, key_matrix, value_matrix, output_weight)
    )
    keys, values, queries, marks, slot_rows = gather_call(
        pltpu.with_memory_space_constraint(bounds, pltpu.HBM),
        pltpu.with_memory_space_constraint(block_owner, pltpu.HBM), hidden, query_weight, key_matrix, value_matrix, inverse
    )
    heads = attend_call(
        bounds,
        queries.reshape(2 * ROWS, WIDTH // 2),
        keys.reshape(TOKENS, HEAD),
        values.reshape(TOKENS, HEAD),
        marks,
    )
    return output_call(slot_rows, heads, output_weight)


def solution(mesh):
    placed = (P("cp", "tp"), P(None, "tp"), P(None, "tp"), P(None, "tp"), P("tp", None), P(), P())
    return jax.shard_map(
        local, mesh=mesh, in_specs=placed, out_specs=P("cp", "tp"), check_vma=False
    )
```

```python
import functools
import math

import jax
import jax.numpy as jnp
from jax import lax
from jax.experimental import pallas as pl
from jax.experimental.pallas import tpu as pltpu
from jax.sharding import PartitionSpec as P

HEAD = 128
BLOCK = 128
CP = 32
TP = 4
ROWS = 256
WIDTH = 1024
NBLK = 64
HEADS = 8
TOKENS = 8192
PORTION = BLOCK // CP

rope_theta = 500000.0
rope_factor = 8.0
rope_context = 8192.0
masked_score = -1e30
MESH = pl.DeviceIdType.MESH


def rope_inverse(head_size):
    halves = jnp.arange(head_size // 2, dtype=jnp.float32)
    inverse = 1.0 / rope_theta ** (2.0 * halves / head_size)
    wavelength = 2.0 * math.pi / inverse
    smooth = (rope_context / wavelength - 1.0) / 3.0
    blended = (1.0 - smooth) * inverse / rope_factor + smooth * inverse
    longer = jnp.where(wavelength > rope_context, inverse / rope_factor, blended)
    return jnp.where(wavelength < rope_context / 4.0, inverse, longer)


def starts_of(tokens, bounds_ref):
    start = jnp.zeros_like(tokens)
    for i in range(1, 8):
        bound = bounds_ref[i]
        start = jnp.where(tokens >= bound, bound, start)
    return start


SIZES = (64, 64, 64, 32, 32)
STARTS = (0, 64, 128, 192, 224)
PARTS = len(SIZES)
STRAIGHT1 = (True, False, True, True, True)
STRAIGHT2 = (True, False, False, False, True)
SPAN = 8
PENALTY = -1e30


def gather_kernel(
    bounds_hbm, owner_hbm, hidden_ref, wq_ref, wk_ref, wv_ref, inverse_ref,
    k_ref, v_ref, q_ref, mark_ref, slot_ref,
    full, wq, wkv, qtmp, qsend, cosine, sine,
    w_sem, z_send, z_recv, g_send, g_recv, q_send, q_recv, bounds_ref, owner_ref, met,
):
    me = lax.axis_index("cp")
    tp = lax.axis_index("tp")
    core = lax.rem(me, 2)
    ycoord = lax.rem(me // 2, 4)
    xcoord = me // 8
    partner = me + 1 - 2 * core
    up, down = lax.rem(tp + 1, TP), lax.rem(tp + 3, TP)
    own_columns = pl.ds(pl.multiple_of(tp * WIDTH, WIDTH), WIDTH)

    bring = pltpu.make_async_copy(hidden_ref, full.at[:, own_columns], w_sem.at[3])
    weights = [
        pltpu.make_async_copy(wk_ref, wkv.at[:, pl.ds(0, HEAD)], w_sem.at[0]),
        pltpu.make_async_copy(wv_ref, wkv.at[:, pl.ds(HEAD, HEAD)], w_sem.at[1]),
        pltpu.make_async_copy(wq_ref, wq, w_sem.at[2]),
    ]
    bring_bounds = pltpu.make_async_copy(bounds_hbm, bounds_ref, w_sem.at[4])
    bring_owner = pltpu.make_async_copy(owner_hbm, owner_ref, w_sem.at[5])
    bring.start()
    bring_bounds.start()
    bring_owner.start()
    for copy in weights:
        copy.start()

    barrier = pltpu.get_barrier_semaphore()

    def signal(semaphore, target):
        pl.semaphore_signal(semaphore, inc=1, device_id={"cp": target}, device_id_type=MESH)

    along_x = [(lax.rem(xcoord + n, 4) * 4 + ycoord) * 2 + core for n in (1, 2, 3)]
    along_y = [(xcoord * 4 + lax.rem(ycoord + n, 4)) * 2 + core for n in (1, 2, 3)]
    pl.semaphore_signal(barrier, inc=1, device_id={"tp": up}, device_id_type=MESH)
    pl.semaphore_signal(barrier, inc=1, device_id={"tp": down}, device_id_type=MESH)
    for target in (*along_x, *along_y, partner):
        signal(barrier, target)
    bring.wait()
    pl.semaphore_wait(barrier, 9)

    def zcopy(n, target, owner, row, count):
        columns = pl.ds(pl.multiple_of(owner * WIDTH, WIDTH), WIDTH)
        ref = full.at[pl.ds(row, count), columns]
        return pltpu.make_async_remote_copy(
            src_ref=ref,
            dst_ref=ref,
            send_sem=z_send.at[0],
            recv_sem=z_recv.at[n],
            device_id={"tp": target},
            device_id_type=MESH,
        )

    own = [
        (
            zcopy(2 * r, up, tp, STARTS[r], SIZES[r]),
            zcopy(2 * r, down, tp, STARTS[r], SIZES[r]),
        )
        for r in range(PARTS)
    ]
    fwd = [
        (
            zcopy(2 * r + 1, down, up, STARTS[r], SIZES[r] // 2),
            zcopy(2 * r + 1, up, down, STARTS[r] + SIZES[r] // 2, SIZES[r] // 2),
        )
        for r in range(PARTS)
    ]

    def wait_for(ref, semaphore):
        pltpu.make_async_copy(ref, ref, semaphore).wait()

    def arrived_z(n, r, owners):
        wait_for(
            full.at[pl.ds(STARTS[r], SIZES[r]), pl.ds(0, owners * WIDTH)], z_recv.at[2 * r + n]
        )
    for copy in (*own[0], *own[1]):
        copy.start()
    for target in along_x:
        signal(met.at[0], target)
    bring_bounds.wait()

    def relay_z(r):
        arrived_z(0, r, 2)
        for copy in fwd[r]:
            copy.start()
        if r + 2 < PARTS:
            for copy in own[r + 2]:
                copy.start()

    lanes = lax.broadcasted_iota(jnp.int32, (BLOCK, HEAD), 1)
    sublanes = lax.broadcasted_iota(jnp.int32, (BLOCK, HEAD), 0)
    inverse = inverse_ref[...]
    for r in range(2):
        tokens = me * ROWS + r * BLOCK + sublanes
        angle = (tokens - starts_of(tokens, bounds_ref)).astype(jnp.float32) * inverse
        turn = jnp.sin(angle)
        cosine[pl.ds(r * BLOCK, BLOCK), :] = jnp.cos(angle)
        sine[pl.ds(r * BLOCK, BLOCK), :] = jnp.where(lanes < HEAD // 2, -turn, turn)

    place = jnp.minimum(jnp.maximum(sublanes - me * PORTION, 0), PORTION)

    def mark(b, carry):
        tokens = b * BLOCK + sublanes
        document = jnp.zeros_like(tokens)
        for i in range(1, 8):
            document = jnp.where(tokens >= bounds_ref[i], i, document)
        spot = 8 + lax.rem(b, SPAN) * (PORTION + 1) + place
        hit = (lanes == document) | (lanes == spot)
        mark_ref[pl.ds(pl.multiple_of(b * BLOCK, BLOCK), BLOCK), :] = (
            hit.astype(jnp.float32).astype(jnp.bfloat16)
        )
        return carry

    lax.fori_loop(0, NBLK // 2, mark, 0)
    weights[0].wait()
    weights[1].wait()
    weights[2].wait()

    def slots():
        spot = lax.broadcasted_iota(jnp.int32, (8, ROWS), 1)
        block = spot // PORTION
        owner = jnp.zeros_like(spot)
        for b in range(NBLK):
            owner = jnp.where(block == b, owner_ref[b], owner)
        rank = jnp.zeros_like(spot)
        for b in range(NBLK - 1):
            rank = rank + ((block > b) & (owner == owner_ref[b])).astype(jnp.int32)
        place = (owner * 2 + rank) * PORTION + lax.rem(spot, PORTION)
        slot_ref[...] = place

    def rotate(raw, row, count):
        table = pl.ds(row, count)
        return raw * cosine[table, :] + pltpu.roll(raw, HEAD // 2, 1) * sine[table, :]

    def queries(r, n):
        columns = slice(n * 2 * HEAD, (n + 1) * 2 * HEAD)
        rows = pl.ds(r * BLOCK, BLOCK)
        raw = jnp.dot(full[rows, :], wq[:, columns], preferred_element_type=jnp.float32)
        turned = jnp.concatenate(
            [rotate(raw[:, :HEAD], r * BLOCK, BLOCK), rotate(raw[:, HEAD:], r * BLOCK, BLOCK)],
            axis=1,
        )
        qtmp[pl.ds((n // 2) * BLOCK, BLOCK), (n % 2) * 2 * HEAD : (n % 2 + 1) * 2 * HEAD] = (
            turned.astype(jnp.bfloat16)
        )

    def gather(which, r):
        buffer = (k_ref, v_ref)[which]
        a, b = ((xcoord, ycoord), (ycoord, xcoord))[which]

        def neighbour(along, step):
            if along == 0:
                na, nb = lax.rem(a + step, 4), b
            else:
                na, nb = a, lax.rem(b + step, 4)
            x, y = ((na, nb), (nb, na))[which]
            return (x * 4 + y) * 2 + core

        def copy(n, ref, target):
            return pltpu.make_async_remote_copy(
                src_ref=ref,
                dst_ref=ref,
                send_sem=g_send.at[r],
                recv_sem=g_recv.at[r, n],
                device_id={"cp": target},
                device_id_type=MESH,
            )

        def piece(at, row, count):
            rows = pl.ds(STARTS[r] + row, count)
            if which == 0:
                return buffer.at[at, b, core, rows]
            return buffer.at[b, at, core, rows]

        def line(at, first, count):
            along, rows = pl.ds(first, count), pl.ds(STARTS[r], SIZES[r])
            if which == 0:
                return buffer.at[along, at, core, rows]
            return buffer.at[at, along, core, rows]

        a_next, a_prev = lax.rem(a + 1, 4), lax.rem(a + 3, 4)
        b_next, b_prev = lax.rem(b + 1, 4), lax.rem(b + 3, 4)
        b_far = lax.rem(b + 2, 4)
        size, half = SIZES[r], SIZES[r] // 2
        return dict(
            ring1=(
                copy(0, piece(a, 0, size), neighbour(0, 1)),
                copy(0, piece(a, 0, size), neighbour(0, 3)),
            ),
            ring1_far=(copy(1, piece(a, 0, size), neighbour(0, 2)),)
            if STRAIGHT1[r]
            else (
                copy(1, piece(a_prev, 0, half), neighbour(0, 1)),
                copy(1, piece(a_next, half, half), neighbour(0, 3)),
            ),
            ring2=(
                copy(2, line(b, 0, 4), neighbour(1, 1)),
                copy(2, line(b, 0, 4), neighbour(1, 3)),
            ),
            ring2_far=(copy(3, line(b, 0, 4), neighbour(1, 2)),)
            if STRAIGHT2[r]
            else (
                copy(3, line(b_prev, 0, 2), neighbour(1, 1)),
                copy(3, line(b_next, 2, 2), neighbour(1, 3)),
            ),
            across=(
                copy(4, line(b, 0, 4), partner),
                copy(4, line(b_prev, 0, 4), partner),
                copy(4, line(b_next, 0, 4), partner),
                copy(4, line(b_far, 0, 4), partner),
            ),
        )

    flows = [[gather(which, r) for which in range(2)] for r in range(PARTS)]

    def start(r, name):
        for flow in flows[r]:
            for copy in flow[name]:
                copy.start()

    def arrived(r, name):
        rows = pl.ds(STARTS[r], SIZES[r])
        n, ref = {
            "ring1": (0, k_ref.at[0, :, core, rows]),
            "ring1_far": (1, k_ref.at[0, pl.ds(0, 2), core, rows]),
            "ring2": (2, k_ref.at[:, :, core, rows]),
            "ring2_far": (3, k_ref.at[pl.ds(0, 2), :, core, rows]),
            "across": (4, k_ref.at[:, :, :, rows]),
        }[name]
        wait_for(ref, g_recv.at[r, n])

    def across(r, which):
        for flow in flows[r]:
            for n in which:
                flow["across"][n].start()

    def s0(r):
        arrived_z(1, r, 1)
        rows = pl.ds(STARTS[r], SIZES[r])
        raw = jnp.dot(full[rows, :], wkv[...], preferred_element_type=jnp.float32)
        k_ref[xcoord, ycoord, core, rows] = rotate(raw[:, :HEAD], STARTS[r], SIZES[r]).astype(
            jnp.bfloat16
        )
        v_ref[xcoord, ycoord, core, rows] = raw[:, HEAD:].astype(jnp.bfloat16)
        start(r, "ring1")
        if STRAIGHT1[r]:
            start(r, "ring1_far")

    def s1(r):
        arrived(r, "ring1")
        if not STRAIGHT1[r]:
            start(r, "ring1_far")

    def s2(r):
        arrived(r, "ring1_far")
        start(r, "ring2")
        if STRAIGHT2[r]:
            start(r, "ring2_far")
        across(r, (0,))

    def s3(r):
        arrived(r, "ring2")
        if not STRAIGHT2[r]:
            start(r, "ring2_far")
        across(r, (1, 2))

    def s4(r):
        arrived(r, "ring2_far")
        across(r, (3,))

    out_row = lax.broadcasted_iota(jnp.int32, (ROWS, ROWS), 0)
    in_row = lax.broadcasted_iota(jnp.int32, (ROWS, ROWS), 1)
    origin = lax.rem(out_row // 4, 2) * BLOCK + (out_row // 8) * 4 + lax.rem(out_row, 4)
    pick = (in_row == origin).astype(jnp.float32).astype(jnp.bfloat16)

    def qcopy(r, target, slot):
        return pltpu.make_async_remote_copy(
            src_ref=qsend.at[r, target],
            dst_ref=q_ref.at[slot, r],
            send_sem=q_send.at[r],
            recv_sem=q_recv.at[r],
            device_id={"cp": target},
            device_id_type=MESH,
        )

    def spread(r):
        ordered = jnp.dot(pick, qtmp[...], preferred_element_type=jnp.float32)
        qsend[r] = ordered.reshape(CP, 8, WIDTH // 2).astype(jnp.bfloat16)
        q_ref[me, r] = qsend[r, me]

        def send(k, carry):
            qcopy(r, lax.rem(me + k, CP), me).start()
            return carry

        lax.fori_loop(1, CP, send, 0)

    def spread_done(r):
        sent, landed = qsend.at[r, pl.ds(0, CP - 1)], q_ref.at[pl.ds(0, CP - 1), r]
        pltpu.make_async_copy(sent, sent, q_send.at[r]).wait()
        pltpu.make_async_copy(landed, landed, q_recv.at[r]).wait()

    relay_z(0)
    pl.semaphore_wait(met.at[0], 3)
    signal(met.at[1], partner)
    bring_owner.wait()
    slots()
    lax.fori_loop(NBLK // 2, NBLK, mark, 0)
    relay_z(1)
    pl.semaphore_wait(met.at[1], 1)
    s0(0)
    relay_z(2)
    s1(0)
    s0(1)
    s2(0)
    queries(0, 0)
    queries(0, 1)
    relay_z(3)
    queries(0, 2)
    queries(0, 3)
    s0(2)
    s1(1)
    spread(0)
    relay_z(4)
    s0(3)
    s3(0)
    s1(2)
    s2(1)
    s4(0)
    s0(4)
    s2(2)
    queries(1, 0)
    queries(1, 1)
    queries(1, 2)
    queries(1, 3)
    s1(3)
    s2(3)
    s3(1)
    s1(4)
    s2(4)
    s3(2)
    spread(1)
    s3(3)
    s4(1)
    s3(4)
    s4(2)
    s4(4)
    s4(3)
    spread_done(0)
    spread_done(1)
    for r in range(PARTS):
        arrived(r, "across")
        wait_for(mark_ref.at[pl.ds(0, 62 * SIZES[r])], g_send.at[r])
    wait_for(full.at[:, pl.ds(0, 3 * WIDTH)], z_send.at[0])


def gather_call(bounds, owner, hidden, wq, wk, wv, inverse):
    vmem = pl.BlockSpec(memory_space=pltpu.VMEM)
    hbm = pl.BlockSpec(memory_space=pltpu.HBM)
    kv = jax.ShapeDtypeStruct((4, 4, 2, ROWS, HEAD), jnp.bfloat16)
    dma = pltpu.SemaphoreType.DMA
    return pl.pallas_call(
        gather_kernel,
        out_shape=(
            kv,
            kv,
            jax.ShapeDtypeStruct((CP, 2, 8, WIDTH // 2), jnp.bfloat16),
            jax.ShapeDtypeStruct((TOKENS, HEAD), jnp.bfloat16),
            jax.ShapeDtypeStruct((8, ROWS), jnp.int32),
        ),
        in_specs=[hbm, hbm, hbm, hbm, hbm, hbm, vmem],
        out_specs=(vmem, vmem, vmem, vmem, vmem),
        scratch_shapes=[
            pltpu.VMEM((ROWS, TP * WIDTH), jnp.bfloat16),
            pltpu.VMEM((TP * WIDTH, WIDTH), jnp.bfloat16),
            pltpu.VMEM((TP * WIDTH, 2 * HEAD), jnp.bfloat16),
            pltpu.VMEM((ROWS, WIDTH // 2), jnp.bfloat16),
            pltpu.VMEM((2, CP, 8, WIDTH // 2), jnp.bfloat16),
            pltpu.VMEM((ROWS, HEAD), jnp.float32),
            pltpu.VMEM((ROWS, HEAD), jnp.float32),
            dma((6,)), dma((1,)), dma((2 * PARTS,)),
            dma((PARTS,)), dma((PARTS, 5)), dma((2,)), dma((2,)),
            pltpu.SMEM((9,), jnp.int32), pltpu.SMEM((NBLK,), jnp.int32),
            pltpu.SemaphoreType.REGULAR((2,)),
        ],
        compiler_params=pltpu.CompilerParams(
            collective_id=0, has_side_effects=True, vmem_limit_bytes=32 * 1024 * 1024
        ),
        name="gather_project",
    )(bounds, owner, hidden, wq, wk, wv, inverse)


TILE = SPAN * BLOCK


GROUPS = NBLK // SPAN
QROWS = 4 * SPAN * 8
PIECE = 256


def attend_kernel(
    bounds_ref, q_ref, k_ref, v_ref, mark_ref, o_ref,
    turned, penalty_ref, even, odd, mixed_ref, total_ref,
):
    rows = SPAN * 8
    factor = math.log2(math.e) / math.sqrt(HEAD)
    row = lax.rem(lax.broadcasted_iota(jnp.int32, (rows, HEAD), 0), rows)
    lane = lax.broadcasted_iota(jnp.int32, (rows, HEAD), 1)
    block, step = row // 8, lax.rem(row, PORTION)
    key_block, key_step = (lane - 8) // (PORTION + 1), lax.rem(lane - 8, PORTION + 1)
    later = (key_block > block) | ((key_block == block) & (key_step > step))
    later = later & (lane >= 8) & (lane < 8 + SPAN * (PORTION + 1))
    me = lax.axis_index("cp")
    contract_last = (((1,), (1,)), ((), ()))
    diagonal = lax.broadcasted_iota(jnp.int32, (HEAD, HEAD), 0) == lax.broadcasted_iota(
        jnp.int32, (HEAD, HEAD), 1
    )
    identity = diagonal.astype(jnp.float32).astype(jnp.bfloat16)

    def prepare(g, carry):
        at = pl.ds(pl.multiple_of(g * TILE, TILE), TILE)
        turned[:, at] = lax.dot_general(
            identity, v_ref[at, :], contract_last, preferred_element_type=jnp.float32
        ).astype(jnp.bfloat16)
        tokens = (g * SPAN + block) * BLOCK + me * PORTION + step
        document = jnp.zeros_like(tokens)
        for i in range(1, 8):
            document = jnp.where(tokens >= bounds_ref[i], i, document)
        other = (lane < 8) & (lane != document)
        penalty_ref[2 * g] = jnp.where(other, PENALTY, 0.0).astype(jnp.bfloat16)
        penalty_ref[2 * g + 1] = jnp.where(other | later, PENALTY, 0.0).astype(jnp.bfloat16)
        return carry

    lax.fori_loop(0, GROUPS, prepare, 0)

    def lowest(g):
        low = jnp.int32(0)
        for i in range(1, 8):
            low = jnp.where(g * TILE >= bounds_ref[i], bounds_ref[i], low)
        return low // TILE

    def following(item):
        g, j = item
        more = j > lowest(g)
        return jnp.where(more, g, g + 1), jnp.where(more, j - 1, g + 1)

    def score(item, ref):
        g, j = item
        own = jnp.where(g == j, 1, 0)
        held = jnp.minimum(g, GROUPS - 1)
        penalties = penalty_ref[2 * held + own]
        asking = pl.ds(pl.multiple_of(held * rows, rows), rows)
        q = jnp.concatenate(
            [
                jnp.concatenate([q_ref[asking, h * HEAD : (h + 1) * HEAD], penalties], axis=1)
                for h in range(4)
            ],
            axis=0,
        )
        for part in range(2):
            size = TILE // 2
            first = jnp.minimum(j, GROUPS - 1) * TILE + part * size
            at = pl.ds(pl.multiple_of(first, size), size)
            scores = lax.dot_general(
                jnp.concatenate([k_ref[at, :], mark_ref[at, :]], axis=1),
                q,
                contract_last,
                preferred_element_type=jnp.float32,
            )
            ref[part * size : (part + 1) * size, :] = scores
            top = jnp.max(scores, axis=0, keepdims=True)
            largest = top if part == 0 else jnp.maximum(largest, top)
        return largest

    def soften(item, ref, largest, state):
        g, j = item
        top, total, mixed = state
        top = jnp.where(g == j, 0.5 * PENALTY, top)
        start = jnp.minimum(j, GROUPS - 1) * TILE
        new_top = jnp.maximum(top, largest)
        shrink = jnp.exp2((top - new_top) * factor)
        total, mixed = total * shrink, mixed * shrink
        for first in range(0, TILE, PIECE):
            piece = slice(first, first + PIECE)
            weights = jnp.exp2((ref[piece, :] - new_top) * factor)
            total = total + jnp.sum(weights, axis=0, keepdims=True)
            keys = pl.ds(pl.multiple_of(start + first, PIECE), PIECE)
            mixed = mixed + jnp.dot(
                turned[:, keys], weights.astype(jnp.bfloat16), preferred_element_type=jnp.float32
            )
        mixed_ref[g] = mixed
        total_ref[g] = total
        return new_top, total, mixed

    count = lax.fori_loop(0, GROUPS, lambda g, n: n + g + 1 - lowest(g), jnp.int32(0))
    zero = jnp.int32(0)
    highest = score((zero, zero), even)

    def pair(n, carry):
        g, j, largest, *state = carry
        item = (g, j)
        second = following(item)
        second_largest = score(second, odd)
        state = soften(item, even, largest, state)
        third = following(second)
        third = (jnp.minimum(third[0], GROUPS), jnp.minimum(third[1], GROUPS))
        largest = score(third, even)
        state = soften(second, odd, second_largest, state)
        return (*third, largest, *state)

    lax.fori_loop(
        0,
        (count + 1) // 2,
        pair,
        (
            zero,
            zero,
            highest,
            jnp.full((1, QROWS), 0.5 * PENALTY, jnp.float32),
            jnp.zeros((1, QROWS), jnp.float32),
            jnp.zeros((HEAD, QROWS), jnp.float32),
        ),
    )

    def finish(g, carry):
        o_ref[g] = (mixed_ref[g] / total_ref[g]).astype(jnp.bfloat16)
        return carry

    lax.fori_loop(0, GROUPS, finish, 0)


def attend_call(bounds, q, k, v, marks):
    vmem = pl.BlockSpec(memory_space=pltpu.VMEM)
    return pl.pallas_call(
        attend_kernel,
        out_shape=jax.ShapeDtypeStruct((GROUPS, HEAD, QROWS), jnp.bfloat16),
        in_specs=[pl.BlockSpec(memory_space=pltpu.SMEM), vmem, vmem, vmem, vmem],
        out_specs=vmem,
        scratch_shapes=[
            pltpu.VMEM((HEAD, TOKENS), jnp.bfloat16),
            pltpu.VMEM((2 * GROUPS, SPAN * 8, HEAD), jnp.bfloat16),
            pltpu.VMEM((TILE, QROWS), jnp.float32),
            pltpu.VMEM((TILE, QROWS), jnp.float32),
            pltpu.VMEM((GROUPS + 1, HEAD, QROWS), jnp.float32),
            pltpu.VMEM((GROUPS + 1, 1, QROWS), jnp.float32),
        ],
        compiler_params=pltpu.CompilerParams(vmem_limit_bytes=28 * 1024 * 1024),
        name="attend",
    )(bounds, q, k, v, marks)


CHUNKS = (2, 2, 2, 1, 1)
FIRST = (0, 2, 4, 6, 7)
PIECES = WIDTH // HEAD


def output_kernel(
    slot_ref, heads_ref, wo_ref, out_ref,
    heads, wo, far, near, far_in, near_in, spread, landed, own_sum,
    w_sem, z_send, z_recv, a_send, a_recv, met,
):
    me = lax.axis_index("cp")
    tp = lax.axis_index("tp")
    up, down, across = lax.rem(tp + 1, TP), lax.rem(tp + 3, TP), lax.rem(tp + 2, TP)

    loads = []
    for n, t in enumerate((across, up, down, tp)):
        columns = pl.ds(pl.multiple_of(t * WIDTH, WIDTH), WIDTH)
        loads.append(pltpu.make_async_copy(wo_ref.at[:, columns], wo.at[n], w_sem.at[n]))
        loads[-1].start()

    barrier = pltpu.get_barrier_semaphore()

    core, ycoord, xcoord = lax.rem(me, 2), lax.rem(me // 2, 4), me // 8
    partner = me + 1 - 2 * core

    def signal(semaphore, target):
        pl.semaphore_signal(semaphore, inc=1, device_id={"cp": target}, device_id_type=MESH)

    along_x = [(lax.rem(xcoord + n, 4) * 4 + ycoord) * 2 + core for n in (1, 2, 3)]
    along_y = [(xcoord * 4 + lax.rem(ycoord + n, 4)) * 2 + core for n in (1, 2, 3)]
    pl.semaphore_signal(barrier, inc=1, device_id={"tp": up}, device_id_type=MESH)
    pl.semaphore_signal(barrier, inc=1, device_id={"tp": down}, device_id_type=MESH)
    for target in (*along_x, *along_y, partner):
        signal(barrier, target)

    turned_row = lax.broadcasted_iota(jnp.int32, (QROWS, QROWS), 0)
    turned_column = lax.broadcasted_iota(jnp.int32, (QROWS, QROWS), 1)
    rows = SPAN * PORTION
    head, at_row = turned_row // rows, lax.rem(turned_row, rows)
    source = (
        lax.rem(head, 4) * 2 * rows
        + (at_row // PORTION) * 2 * PORTION
        + (head // 4) * PORTION
        + lax.rem(at_row, PORTION)
    )
    select = (turned_column == source).astype(jnp.float32).astype(jnp.bfloat16)
    for g in range(GROUPS):
        part = lax.dot_general(
            select,
            heads_ref[g],
            (((1,), (1,)), ((), ())),
            preferred_element_type=jnp.float32,
        ).astype(jnp.bfloat16)
        for h in range(HEADS):
            heads[g * rows : (g + 1) * rows, h * HEAD : (h + 1) * HEAD] = part[
                h * rows : (h + 1) * rows
            ]

    def product(n, c):
        columns = slice(FIRST[c] * HEAD, (FIRST[c] + CHUNKS[c]) * HEAD)
        return jnp.dot(heads[...], wo[n, :, columns], preferred_element_type=jnp.float32)

    def remote(n, src, dst, target):
        return pltpu.make_async_remote_copy(
            src_ref=src,
            dst_ref=dst,
            send_sem=z_send.at[0],
            recv_sem=z_recv.at[n],
            device_id={"tp": target},
            device_id_type=MESH,
        )

    half = ROWS // 2
    upper, lower = pl.ds(0, half), pl.ds(half, half)
    far_copies, near_copies = [], []
    for c, count in enumerate(CHUNKS):
        at = pl.ds(FIRST[c], count)
        far_copies.append(
            (
                remote(3 * c, far.at[0, at], far_in.at[0, at], up),
                remote(3 * c + 1, far.at[1, at], far_in.at[1, at], down),
            )
        )
        near_copies.append(
            (
                remote(3 * c + 2, near.at[0, at], near_in.at[0, at], up),
                remote(3 * c + 2, near.at[1, at], near_in.at[1, at], down),
            )
        )

    def pieces(c):
        return [(FIRST[c] + n, slice(n * HEAD, (n + 1) * HEAD)) for n in range(CHUNKS[c])]

    def make_far(c):
        value = product(0, c).astype(jnp.bfloat16)
        for at, columns in pieces(c):
            far[0, at] = value[:half, columns]
            far[1, at] = value[half:, columns]

    def send_far(c):
        for copy in far_copies[c]:
            copy.start()

    def send_near(c):
        to_up, to_down = product(1, c), product(2, c)
        far_copies[c][0].wait_recv()
        for at, columns in pieces(c):
            near[0, at, upper] = (
                to_up[:half, columns] + far_in[0, at].astype(jnp.float32)
            ).astype(jnp.bfloat16)
            near[0, at, lower] = to_up[half:, columns].astype(jnp.bfloat16)
        near_copies[c][0].start()
        far_copies[c][1].wait_recv()
        for at, columns in pieces(c):
            near[1, at, upper] = to_down[:half, columns].astype(jnp.bfloat16)
            near[1, at, lower] = (
                to_down[half:, columns] + far_in[1, at].astype(jnp.float32)
            ).astype(jnp.bfloat16)
        near_copies[c][1].start()

    def sum_own(c):
        value = product(3, c)
        for at, columns in pieces(c):
            own_sum[at] = value[:, columns]

    row = lax.broadcasted_iota(jnp.int32, (ROWS, ROWS), 0)
    column = lax.broadcasted_iota(jnp.int32, (ROWS, ROWS), 1)
    to_owner = (row == slot_ref[0:1, :]).astype(jnp.float32).astype(jnp.bfloat16)
    origin = (lax.rem(row, BLOCK) // 4) * 8 + (row // BLOCK) * 4 + lax.rem(row, 4)
    to_place = (column == origin).astype(jnp.float32).astype(jnp.bfloat16)

    def acopy(c, target, slot):
        at = pl.ds(FIRST[c], CHUNKS[c])
        return pltpu.make_async_remote_copy(
            src_ref=spread.at[target, at],
            dst_ref=landed.at[slot, at],
            send_sem=a_send.at[c],
            recv_sem=a_recv.at[c],
            device_id={"cp": target},
            device_id_type=MESH,
        )

    def finish_sum(c):
        both = near_in.at[:, pl.ds(FIRST[c], CHUNKS[c])]
        pltpu.make_async_copy(both, both, z_recv.at[3 * c + 2]).wait()
        total = jnp.concatenate(
            [
                (
                    own_sum[at]
                    + near_in[0, at].astype(jnp.float32)
                    + near_in[1, at].astype(jnp.float32)
                ).astype(jnp.bfloat16)
                for at, columns in pieces(c)
            ],
            axis=1,
        )
        picked = jnp.dot(to_owner, total, preferred_element_type=jnp.float32)
        for at, columns in pieces(c):
            spread[:, at] = picked[:, columns].reshape(CP, 8, HEAD).astype(jnp.bfloat16)
            landed[me, at] = spread[me, at]

        def send(k, carry):
            acopy(c, lax.rem(me + k, CP), me).start()
            return carry

        lax.fori_loop(1, CP, send, 0)

    def place(c):
        everyone = landed.at[pl.ds(0, CP - 1), pl.ds(FIRST[c], CHUNKS[c])]
        pltpu.make_async_copy(everyone, everyone, a_recv.at[c]).wait()
        rows = jnp.concatenate(
            [
                landed[:, at].astype(jnp.float32).reshape(ROWS, HEAD).astype(jnp.bfloat16)
                for at, columns in pieces(c)
            ],
            axis=1,
        )
        out_ref[:, FIRST[c] * HEAD : (FIRST[c] + CHUNKS[c]) * HEAD] = jnp.dot(
            to_place, rows, preferred_element_type=jnp.float32
        ).astype(jnp.bfloat16)

    loads[0].wait()
    make_far(0)
    pl.semaphore_wait(barrier, 9)
    send_far(0)
    for target in along_x:
        signal(met.at[0], target)
    make_far(1)
    send_far(1)
    make_far(2)
    send_far(2)
    loads[1].wait()
    loads[2].wait()
    send_near(0)
    pl.semaphore_wait(met.at[0], 3)
    signal(met.at[1], partner)
    make_far(3)
    send_far(3)
    send_near(1)
    make_far(4)
    send_far(4)
    send_near(2)
    loads[3].wait()
    for c in range(len(CHUNKS)):
        sum_own(c)
    send_near(3)
    pl.semaphore_wait(met.at[1], 1)
    finish_sum(0)
    send_near(4)
    finish_sum(1)
    finish_sum(2)
    finish_sum(3)
    finish_sum(4)
    for c in range(len(CHUNKS)):
        place(c)
    for c in range(len(CHUNKS)):
        everyone = spread.at[pl.ds(0, CP - 1), pl.ds(FIRST[c], CHUNKS[c])]
        pltpu.make_async_copy(everyone, everyone, a_send.at[c]).wait()
    sent = wo.at[0, pl.ds(0, 3 * ROWS)]
    pltpu.make_async_copy(sent, sent, z_send.at[0]).wait()


def output_call(slot_rows, heads, wo):
    vmem = pl.BlockSpec(memory_space=pltpu.VMEM)
    dma = pltpu.SemaphoreType.DMA
    half = ROWS // 2
    bf16 = jnp.bfloat16
    return pl.pallas_call(
        output_kernel,
        out_shape=jax.ShapeDtypeStruct((ROWS, WIDTH), bf16),
        in_specs=[vmem, vmem, pl.BlockSpec(memory_space=pltpu.HBM)],
        out_specs=vmem,
        scratch_shapes=[
            pltpu.VMEM((ROWS, WIDTH), bf16),
            pltpu.VMEM((TP, WIDTH, WIDTH), bf16),
            pltpu.VMEM((2, PIECES, half, HEAD), bf16),
            pltpu.VMEM((2, PIECES, ROWS, HEAD), bf16),
            pltpu.VMEM((2, PIECES, half, HEAD), bf16),
            pltpu.VMEM((2, PIECES, ROWS, HEAD), bf16),
            pltpu.VMEM((CP, PIECES, 8, HEAD), bf16),
            pltpu.VMEM((CP, PIECES, 8, HEAD), bf16),
            pltpu.VMEM((PIECES, ROWS, HEAD), jnp.float32),
            dma((4,)), dma((1,)), dma((3 * len(CHUNKS),)),
            dma((len(CHUNKS),)), dma((len(CHUNKS),)), pltpu.SemaphoreType.REGULAR((2,)),
        ],
        compiler_params=pltpu.CompilerParams(
            collective_id=1, has_side_effects=True, vmem_limit_bytes=40 * 1024 * 1024
        ),
        name="project_out",
    )(slot_rows, heads, wo)


def local(hidden, query_weight, key_matrix, value_matrix, output_weight, bounds, block_owner):
    inverse = rope_inverse(HEAD)
    inverse = jnp.concatenate([inverse, inverse])[None, :]
    hidden, query_weight, key_matrix, value_matrix, output_weight = (
        pltpu.with_memory_space_constraint(a, pltpu.HBM)
        for a in (hidden, query_weight, key_matrix, value_matrix, output_weight)
    )
    keys, values, queries, marks, slot_rows = gather_call(
        pltpu.with_memory_space_constraint(bounds, pltpu.HBM),
        pltpu.with_memory_space_constraint(block_owner, pltpu.HBM), hidden, query_weight, key_matrix, value_matrix, inverse
    )
    heads = attend_call(
        bounds,
        queries.reshape(2 * ROWS, WIDTH // 2),
        keys.reshape(TOKENS, HEAD),
        values.reshape(TOKENS, HEAD),
        marks,
    )
    return output_call(slot_rows, heads, output_weight)


def solution(mesh):
    placed = (P("cp", "tp"), P(None, "tp"), P(None, "tp"), P(None, "tp"), P("tp", None), P(), P())
    return jax.shard_map(
        local, mesh=mesh, in_specs=placed, out_specs=P("cp", "tp"), check_vma=False
    )
```

```python
import functools
import math

import jax
import jax.numpy as jnp
from jax import lax
from jax.experimental import pallas as pl
from jax.experimental.pallas import tpu as pltpu
from jax.sharding import PartitionSpec as P

HEAD = 128
BLOCK = 128
CP = 32
TP = 4
ROWS = 256
WIDTH = 1024
NBLK = 64
HEADS = 8
TOKENS = 8192
PORTION = BLOCK // CP

rope_theta = 500000.0
rope_factor = 8.0
rope_context = 8192.0
masked_score = -1e30
MESH = pl.DeviceIdType.MESH


def rope_inverse(head_size):
    halves = jnp.arange(head_size // 2, dtype=jnp.float32)
    inverse = 1.0 / rope_theta ** (2.0 * halves / head_size)
    wavelength = 2.0 * math.pi / inverse
    smooth = (rope_context / wavelength - 1.0) / 3.0
    blended = (1.0 - smooth) * inverse / rope_factor + smooth * inverse
    longer = jnp.where(wavelength > rope_context, inverse / rope_factor, blended)
    return jnp.where(wavelength < rope_context / 4.0, inverse, longer)


def starts_of(tokens, bounds_ref):
    start = jnp.zeros_like(tokens)
    for i in range(1, 8):
        bound = bounds_ref[i]
        start = jnp.where(tokens >= bound, bound, start)
    return start


SIZES = (64, 64, 64, 32, 32)
STARTS = (0, 64, 128, 192, 224)
PARTS = len(SIZES)
STRAIGHT1 = (True, False, True, True, True)
STRAIGHT2 = (True, False, False, False, True)
SPAN = 8
PENALTY = -1e30


def gather_kernel(
    bounds_hbm, owner_hbm, hidden_ref, wq_ref, wk_ref, wv_ref, inverse_ref,
    k_ref, v_ref, q_ref, mark_ref, slot_ref,
    full, wq, wkv, qtmp, qsend, cosine, sine,
    w_sem, z_send, z_recv, g_send, g_recv, q_send, q_recv, bounds_ref, owner_ref, met,
):
    me = lax.axis_index("cp")
    tp = lax.axis_index("tp")
    core = lax.rem(me, 2)
    ycoord = lax.rem(me // 2, 4)
    xcoord = me // 8
    partner = me + 1 - 2 * core
    up, down = lax.rem(tp + 1, TP), lax.rem(tp + 3, TP)
    own_columns = pl.ds(pl.multiple_of(tp * WIDTH, WIDTH), WIDTH)

    bring = pltpu.make_async_copy(hidden_ref, full.at[:, own_columns], w_sem.at[3])
    weights = [
        pltpu.make_async_copy(wk_ref, wkv.at[:, pl.ds(0, HEAD)], w_sem.at[0]),
        pltpu.make_async_copy(wv_ref, wkv.at[:, pl.ds(HEAD, HEAD)], w_sem.at[1]),
        pltpu.make_async_copy(wq_ref, wq, w_sem.at[2]),
    ]
    bring_bounds = pltpu.make_async_copy(bounds_hbm, bounds_ref, w_sem.at[4])
    bring_owner = pltpu.make_async_copy(owner_hbm, owner_ref, w_sem.at[5])
    bring.start()
    bring_bounds.start()
    bring_owner.start()
    for copy in weights:
        copy.start()

    barrier = pltpu.get_barrier_semaphore()

    def signal(semaphore, target):
        pl.semaphore_signal(semaphore, inc=1, device_id={"cp": target}, device_id_type=MESH)

    along_x = [(lax.rem(xcoord + n, 4) * 4 + ycoord) * 2 + core for n in (1, 2, 3)]
    along_y = [(xcoord * 4 + lax.rem(ycoord + n, 4)) * 2 + core for n in (1, 2, 3)]
    pl.semaphore_signal(barrier, inc=1, device_id={"tp": up}, device_id_type=MESH)
    pl.semaphore_signal(barrier, inc=1, device_id={"tp": down}, device_id_type=MESH)
    for target in (*along_x, *along_y, partner):
        signal(barrier, target)
    bring.wait()
    pl.semaphore_wait(barrier, 9)

    def zcopy(n, target, owner, row, count):
        columns = pl.ds(pl.multiple_of(owner * WIDTH, WIDTH), WIDTH)
        ref = full.at[pl.ds(row, count), columns]
        return pltpu.make_async_remote_copy(
            src_ref=ref,
            dst_ref=ref,
            send_sem=z_send.at[0],
            recv_sem=z_recv.at[n],
            device_id={"tp": target},
            device_id_type=MESH,
        )

    own = [
        (
            zcopy(2 * r, up, tp, STARTS[r], SIZES[r]),
            zcopy(2 * r, down, tp, STARTS[r], SIZES[r]),
        )
        for r in range(PARTS)
    ]
    fwd = [
        (
            zcopy(2 * r + 1, down, up, STARTS[r], SIZES[r] // 2),
            zcopy(2 * r + 1, up, down, STARTS[r] + SIZES[r] // 2, SIZES[r] // 2),
        )
        for r in range(PARTS)
    ]

    def wait_for(ref, semaphore):
        pltpu.make_async_copy(ref, ref, semaphore).wait()

    def arrived_z(n, r, owners):
        wait_for(
            full.at[pl.ds(STARTS[r], SIZES[r]), pl.ds(0, owners * WIDTH)], z_recv.at[2 * r + n]
        )
    for copy in (*own[0], *own[1]):
        copy.start()
    for target in along_x:
        signal(met.at[0], target)
    bring_bounds.wait()

    def relay_z(r):
        arrived_z(0, r, 2)
        for copy in fwd[r]:
            copy.start()
        if r + 2 < PARTS:
            for copy in own[r + 2]:
                copy.start()

    lanes = lax.broadcasted_iota(jnp.int32, (BLOCK, HEAD), 1)
    sublanes = lax.broadcasted_iota(jnp.int32, (BLOCK, HEAD), 0)
    inverse = inverse_ref[...]
    for r in range(2):
        tokens = me * ROWS + r * BLOCK + sublanes
        angle = (tokens - starts_of(tokens, bounds_ref)).astype(jnp.float32) * inverse
        turn = jnp.sin(angle)
        cosine[pl.ds(r * BLOCK, BLOCK), :] = jnp.cos(angle)
        sine[pl.ds(r * BLOCK, BLOCK), :] = jnp.where(lanes < HEAD // 2, -turn, turn)

    place = jnp.minimum(jnp.maximum(sublanes - me * PORTION, 0), PORTION)

    def mark(b, carry):
        tokens = b * BLOCK + sublanes
        document = jnp.zeros_like(tokens)
        for i in range(1, 8):
            document = jnp.where(tokens >= bounds_ref[i], i, document)
        spot = 8 + lax.rem(b, SPAN) * (PORTION + 1) + place
        hit = (lanes == document) | (lanes == spot)
        mark_ref[pl.ds(pl.multiple_of(b * BLOCK, BLOCK), BLOCK), :] = (
            hit.astype(jnp.float32).astype(jnp.bfloat16)
        )
        return carry

    lax.fori_loop(0, NBLK // 2, mark, 0)
    weights[0].wait()
    weights[1].wait()
    weights[2].wait()

    def slots():
        spot = lax.broadcasted_iota(jnp.int32, (8, ROWS), 1)
        block = spot // PORTION
        owner = jnp.zeros_like(spot)
        for b in range(NBLK):
            owner = jnp.where(block == b, owner_ref[b], owner)
        rank = jnp.zeros_like(spot)
        for b in range(NBLK - 1):
            rank = rank + ((block > b) & (owner == owner_ref[b])).astype(jnp.int32)
        place = (owner * 2 + rank) * PORTION + lax.rem(spot, PORTION)
        slot_ref[...] = place

    def rotate(raw, row, count):
        table = pl.ds(row, count)
        return raw * cosine[table, :] + pltpu.roll(raw, HEAD // 2, 1) * sine[table, :]

    def queries(r, n):
        columns = slice(n * 2 * HEAD, (n + 1) * 2 * HEAD)
        rows = pl.ds(r * BLOCK, BLOCK)
        raw = jnp.dot(full[rows, :], wq[:, columns], preferred_element_type=jnp.float32)
        turned = jnp.concatenate(
            [rotate(raw[:, :HEAD], r * BLOCK, BLOCK), rotate(raw[:, HEAD:], r * BLOCK, BLOCK)],
            axis=1,
        )
        qtmp[pl.ds((n // 2) * BLOCK, BLOCK), (n % 2) * 2 * HEAD : (n % 2 + 1) * 2 * HEAD] = (
            turned.astype(jnp.bfloat16)
        )

    def gather(which, r):
        buffer = (k_ref, v_ref)[which]
        a, b = ((xcoord, ycoord), (ycoord, xcoord))[which]

        def neighbour(along, step):
            if along == 0:
                na, nb = lax.rem(a + step, 4), b
            else:
                na, nb = a, lax.rem(b + step, 4)
            x, y = ((na, nb), (nb, na))[which]
            return (x * 4 + y) * 2 + core

        def copy(n, ref, target):
            return pltpu.make_async_remote_copy(
                src_ref=ref,
                dst_ref=ref,
                send_sem=g_send.at[r],
                recv_sem=g_recv.at[r, n],
                device_id={"cp": target},
                device_id_type=MESH,
            )

        def piece(at, row, count):
            rows = pl.ds(STARTS[r] + row, count)
            if which == 0:
                return buffer.at[at, b, core, rows]
            return buffer.at[b, at, core, rows]

        def line(at, first, count):
            along, rows = pl.ds(first, count), pl.ds(STARTS[r], SIZES[r])
            if which == 0:
                return buffer.at[along, at, core, rows]
            return buffer.at[at, along, core, rows]

        a_next, a_prev = lax.rem(a + 1, 4), lax.rem(a + 3, 4)
        b_next, b_prev = lax.rem(b + 1, 4), lax.rem(b + 3, 4)
        b_far = lax.rem(b + 2, 4)
        size, half = SIZES[r], SIZES[r] // 2
        return dict(
            ring1=(
                copy(0, piece(a, 0, size), neighbour(0, 1)),
                copy(0, piece(a, 0, size), neighbour(0, 3)),
            ),
            ring1_far=(copy(1, piece(a, 0, size), neighbour(0, 2)),)
            if STRAIGHT1[r]
            else (
                copy(1, piece(a_prev, 0, half), neighbour(0, 1)),
                copy(1, piece(a_next, half, half), neighbour(0, 3)),
            ),
            ring2=(
                copy(2, line(b, 0, 4), neighbour(1, 1)),
                copy(2, line(b, 0, 4), neighbour(1, 3)),
            ),
            ring2_far=(copy(3, line(b, 0, 4), neighbour(1, 2)),)
            if STRAIGHT2[r]
            else (
                copy(3, line(b_prev, 0, 2), neighbour(1, 1)),
                copy(3, line(b_next, 2, 2), neighbour(1, 3)),
            ),
            across=(
                copy(4, line(b, 0, 4), partner),
                copy(4, line(b_prev, 0, 4), partner),
                copy(4, line(b_next, 0, 4), partner),
                copy(4, line(b_far, 0, 4), partner),
            ),
        )

    flows = [[gather(which, r) for which in range(2)] for r in range(PARTS)]

    def start(r, name):
        for flow in flows[r]:
            for copy in flow[name]:
                copy.start()

    def arrived(r, name):
        rows = pl.ds(STARTS[r], SIZES[r])
        n, ref = {
            "ring1": (0, k_ref.at[0, :, core, rows]),
            "ring1_far": (1, k_ref.at[0, pl.ds(0, 2), core, rows]),
            "ring2": (2, k_ref.at[:, :, core, rows]),
            "ring2_far": (3, k_ref.at[pl.ds(0, 2), :, core, rows]),
            "across": (4, k_ref.at[:, :, :, rows]),
        }[name]
        wait_for(ref, g_recv.at[r, n])

    def across(r, which):
        for flow in flows[r]:
            for n in which:
                flow["across"][n].start()

    def s0(r):
        arrived_z(1, r, 1)
        rows = pl.ds(STARTS[r], SIZES[r])
        raw = jnp.dot(full[rows, :], wkv[...], preferred_element_type=jnp.float32)
        k_ref[xcoord, ycoord, core, rows] = rotate(raw[:, :HEAD], STARTS[r], SIZES[r]).astype(
            jnp.bfloat16
        )
        v_ref[xcoord, ycoord, core, rows] = raw[:, HEAD:].astype(jnp.bfloat16)
        start(r, "ring1")
        if STRAIGHT1[r]:
            start(r, "ring1_far")

    def s1(r):
        arrived(r, "ring1")
        if not STRAIGHT1[r]:
            start(r, "ring1_far")

    def s2(r):
        arrived(r, "ring1_far")
        start(r, "ring2")
        if STRAIGHT2[r]:
            start(r, "ring2_far")
        across(r, (0,))

    def s3(r):
        arrived(r, "ring2")
        if not STRAIGHT2[r]:
            start(r, "ring2_far")
        across(r, (1, 2))

    def s4(r):
        arrived(r, "ring2_far")
        across(r, (3,))

    out_row = lax.broadcasted_iota(jnp.int32, (ROWS, ROWS), 0)
    in_row = lax.broadcasted_iota(jnp.int32, (ROWS, ROWS), 1)
    origin = lax.rem(out_row // 4, 2) * BLOCK + (out_row // 8) * 4 + lax.rem(out_row, 4)
    pick = (in_row == origin).astype(jnp.float32).astype(jnp.bfloat16)

    def qcopy(r, target, slot):
        return pltpu.make_async_remote_copy(
            src_ref=qsend.at[r, target],
            dst_ref=q_ref.at[slot, r],
            send_sem=q_send.at[r],
            recv_sem=q_recv.at[r],
            device_id={"cp": target},
            device_id_type=MESH,
        )

    def spread(r):
        ordered = jnp.dot(pick, qtmp[...], preferred_element_type=jnp.float32)
        qsend[r] = ordered.reshape(CP, 8, WIDTH // 2).astype(jnp.bfloat16)
        q_ref[me, r] = qsend[r, me]

        def send(k, carry):
            qcopy(r, lax.rem(me + k, CP), me).start()
            return carry

        lax.fori_loop(1, CP, send, 0)

    def spread_done(r):
        sent, landed = qsend.at[r, pl.ds(0, CP - 1)], q_ref.at[pl.ds(0, CP - 1), r]
        pltpu.make_async_copy(sent, sent, q_send.at[r]).wait()
        pltpu.make_async_copy(landed, landed, q_recv.at[r]).wait()

    relay_z(0)
    pl.semaphore_wait(met.at[0], 3)
    signal(met.at[1], partner)
    bring_owner.wait()
    slots()
    lax.fori_loop(NBLK // 2, NBLK, mark, 0)
    relay_z(1)
    pl.semaphore_wait(met.at[1], 1)
    s0(0)
    relay_z(2)
    s1(0)
    s0(1)
    s2(0)
    queries(0, 0)
    queries(0, 1)
    relay_z(3)
    queries(0, 2)
    queries(0, 3)
    s0(2)
    s1(1)
    relay_z(4)
    spread(0)
    s0(3)
    s3(0)
    s1(2)
    s2(1)
    s4(0)
    s0(4)
    s2(2)
    queries(1, 0)
    queries(1, 1)
    queries(1, 2)
    queries(1, 3)
    s1(3)
    s2(3)
    s3(1)
    s1(4)
    s2(4)
    spread(1)
    s3(2)
    s3(3)
    s4(1)
    s3(4)
    s4(2)
    s4(4)
    s4(3)
    spread_done(0)
    spread_done(1)
    for r in range(PARTS):
        arrived(r, "across")
        wait_for(mark_ref.at[pl.ds(0, 62 * SIZES[r])], g_send.at[r])
    wait_for(full.at[:, pl.ds(0, 3 * WIDTH)], z_send.at[0])


def gather_call(bounds, owner, hidden, wq, wk, wv, inverse):
    vmem = pl.BlockSpec(memory_space=pltpu.VMEM)
    hbm = pl.BlockSpec(memory_space=pltpu.HBM)
    kv = jax.ShapeDtypeStruct((4, 4, 2, ROWS, HEAD), jnp.bfloat16)
    dma = pltpu.SemaphoreType.DMA
    return pl.pallas_call(
        gather_kernel,
        out_shape=(
            kv,
            kv,
            jax.ShapeDtypeStruct((CP, 2, 8, WIDTH // 2), jnp.bfloat16),
            jax.ShapeDtypeStruct((TOKENS, HEAD), jnp.bfloat16),
            jax.ShapeDtypeStruct((8, ROWS), jnp.int32),
        ),
        in_specs=[hbm, hbm, hbm, hbm, hbm, hbm, vmem],
        out_specs=(vmem, vmem, vmem, vmem, vmem),
        scratch_shapes=[
            pltpu.VMEM((ROWS, TP * WIDTH), jnp.bfloat16),
            pltpu.VMEM((TP * WIDTH, WIDTH), jnp.bfloat16),
            pltpu.VMEM((TP * WIDTH, 2 * HEAD), jnp.bfloat16),
            pltpu.VMEM((ROWS, WIDTH // 2), jnp.bfloat16),
            pltpu.VMEM((2, CP, 8, WIDTH // 2), jnp.bfloat16),
            pltpu.VMEM((ROWS, HEAD), jnp.float32),
            pltpu.VMEM((ROWS, HEAD), jnp.float32),
            dma((6,)), dma((1,)), dma((2 * PARTS,)),
            dma((PARTS,)), dma((PARTS, 5)), dma((2,)), dma((2,)),
            pltpu.SMEM((9,), jnp.int32), pltpu.SMEM((NBLK,), jnp.int32),
            pltpu.SemaphoreType.REGULAR((2,)),
        ],
        compiler_params=pltpu.CompilerParams(
            collective_id=0, has_side_effects=True, vmem_limit_bytes=32 * 1024 * 1024
        ),
        name="gather_project",
    )(bounds, owner, hidden, wq, wk, wv, inverse)


TILE = SPAN * BLOCK


GROUPS = NBLK // SPAN
QROWS = 4 * SPAN * 8
PIECE = 256


def attend_kernel(
    bounds_ref, q_ref, k_ref, v_ref, mark_ref, o_ref,
    turned, penalty_ref, even, odd, mixed_ref, total_ref,
):
    rows = SPAN * 8
    factor = math.log2(math.e) / math.sqrt(HEAD)
    row = lax.rem(lax.broadcasted_iota(jnp.int32, (rows, HEAD), 0), rows)
    lane = lax.broadcasted_iota(jnp.int32, (rows, HEAD), 1)
    block, step = row // 8, lax.rem(row, PORTION)
    key_block, key_step = (lane - 8) // (PORTION + 1), lax.rem(lane - 8, PORTION + 1)
    later = (key_block > block) | ((key_block == block) & (key_step > step))
    later = later & (lane >= 8) & (lane < 8 + SPAN * (PORTION + 1))
    me = lax.axis_index("cp")
    contract_last = (((1,), (1,)), ((), ()))
    diagonal = lax.broadcasted_iota(jnp.int32, (HEAD, HEAD), 0) == lax.broadcasted_iota(
        jnp.int32, (HEAD, HEAD), 1
    )
    identity = diagonal.astype(jnp.float32).astype(jnp.bfloat16)

    def prepare(g, carry):
        at = pl.ds(pl.multiple_of(g * TILE, TILE), TILE)
        turned[:, at] = lax.dot_general(
            identity, v_ref[at, :], contract_last, preferred_element_type=jnp.float32
        ).astype(jnp.bfloat16)
        tokens = (g * SPAN + block) * BLOCK + me * PORTION + step
        document = jnp.zeros_like(tokens)
        for i in range(1, 8):
            document = jnp.where(tokens >= bounds_ref[i], i, document)
        other = (lane < 8) & (lane != document)
        penalty_ref[2 * g] = jnp.where(other, PENALTY, 0.0).astype(jnp.bfloat16)
        penalty_ref[2 * g + 1] = jnp.where(other | later, PENALTY, 0.0).astype(jnp.bfloat16)
        return carry

    lax.fori_loop(0, GROUPS, prepare, 0)

    def lowest(g):
        low = jnp.int32(0)
        for i in range(1, 8):
            low = jnp.where(g * TILE >= bounds_ref[i], bounds_ref[i], low)
        return low // TILE

    def following(item):
        g, j = item
        more = j > lowest(g)
        return jnp.where(more, g, g + 1), jnp.where(more, j - 1, g + 1)

    def score(item, ref):
        g, j = item
        own = jnp.where(g == j, 1, 0)
        held = jnp.minimum(g, GROUPS - 1)
        penalties = penalty_ref[2 * held + own]
        asking = pl.ds(pl.multiple_of(held * rows, rows), rows)
        q = jnp.concatenate(
            [
                jnp.concatenate([q_ref[asking, h * HEAD : (h + 1) * HEAD], penalties], axis=1)
                for h in range(4)
            ],
            axis=0,
        )
        for part in range(2):
            size = TILE // 2
            first = jnp.minimum(j, GROUPS - 1) * TILE + part * size
            at = pl.ds(pl.multiple_of(first, size), size)
            scores = lax.dot_general(
                jnp.concatenate([k_ref[at, :], mark_ref[at, :]], axis=1),
                q,
                contract_last,
                preferred_element_type=jnp.float32,
            )
            ref[part * size : (part + 1) * size, :] = scores
            top = jnp.max(scores, axis=0, keepdims=True)
            largest = top if part == 0 else jnp.maximum(largest, top)
        return largest

    def soften(item, ref, largest, state):
        g, j = item
        top, total, mixed = state
        top = jnp.where(g == j, 0.5 * PENALTY, top)
        start = jnp.minimum(j, GROUPS - 1) * TILE
        new_top = jnp.maximum(top, largest)
        shrink = jnp.exp2((top - new_top) * factor)
        total, mixed = total * shrink, mixed * shrink
        for first in range(0, TILE, PIECE):
            piece = slice(first, first + PIECE)
            weights = jnp.exp2((ref[piece, :] - new_top) * factor)
            total = total + jnp.sum(weights, axis=0, keepdims=True)
            keys = pl.ds(pl.multiple_of(start + first, PIECE), PIECE)
            mixed = mixed + jnp.dot(
                turned[:, keys], weights.astype(jnp.bfloat16), preferred_element_type=jnp.float32
            )
        mixed_ref[g] = mixed
        total_ref[g] = total
        return new_top, total, mixed

    count = lax.fori_loop(0, GROUPS, lambda g, n: n + g + 1 - lowest(g), jnp.int32(0))
    zero = jnp.int32(0)
    highest = score((zero, zero), even)

    def pair(n, carry):
        g, j, largest, *state = carry
        item = (g, j)
        second = following(item)
        second_largest = score(second, odd)
        state = soften(item, even, largest, state)
        third = following(second)
        third = (jnp.minimum(third[0], GROUPS), jnp.minimum(third[1], GROUPS))
        largest = score(third, even)
        state = soften(second, odd, second_largest, state)
        return (*third, largest, *state)

    lax.fori_loop(
        0,
        (count + 1) // 2,
        pair,
        (
            zero,
            zero,
            highest,
            jnp.full((1, QROWS), 0.5 * PENALTY, jnp.float32),
            jnp.zeros((1, QROWS), jnp.float32),
            jnp.zeros((HEAD, QROWS), jnp.float32),
        ),
    )

    def finish(g, carry):
        o_ref[g] = (mixed_ref[g] / total_ref[g]).astype(jnp.bfloat16)
        return carry

    lax.fori_loop(0, GROUPS, finish, 0)


def attend_call(bounds, q, k, v, marks):
    vmem = pl.BlockSpec(memory_space=pltpu.VMEM)
    return pl.pallas_call(
        attend_kernel,
        out_shape=jax.ShapeDtypeStruct((GROUPS, HEAD, QROWS), jnp.bfloat16),
        in_specs=[pl.BlockSpec(memory_space=pltpu.SMEM), vmem, vmem, vmem, vmem],
        out_specs=vmem,
        scratch_shapes=[
            pltpu.VMEM((HEAD, TOKENS), jnp.bfloat16),
            pltpu.VMEM((2 * GROUPS, SPAN * 8, HEAD), jnp.bfloat16),
            pltpu.VMEM((TILE, QROWS), jnp.float32),
            pltpu.VMEM((TILE, QROWS), jnp.float32),
            pltpu.VMEM((GROUPS + 1, HEAD, QROWS), jnp.float32),
            pltpu.VMEM((GROUPS + 1, 1, QROWS), jnp.float32),
        ],
        compiler_params=pltpu.CompilerParams(vmem_limit_bytes=28 * 1024 * 1024),
        name="attend",
    )(bounds, q, k, v, marks)


CHUNKS = (2, 2, 2, 1, 1)
FIRST = (0, 2, 4, 6, 7)
PIECES = WIDTH // HEAD


def output_kernel(
    slot_ref, heads_ref, wo_ref, out_ref,
    heads, wo, far, near, far_in, near_in, spread, landed, own_sum,
    w_sem, z_send, z_recv, a_send, a_recv, met,
):
    me = lax.axis_index("cp")
    tp = lax.axis_index("tp")
    up, down, across = lax.rem(tp + 1, TP), lax.rem(tp + 3, TP), lax.rem(tp + 2, TP)

    loads = []
    for n, t in enumerate((across, up, down, tp)):
        columns = pl.ds(pl.multiple_of(t * WIDTH, WIDTH), WIDTH)
        loads.append(pltpu.make_async_copy(wo_ref.at[:, columns], wo.at[n], w_sem.at[n]))
        loads[-1].start()

    barrier = pltpu.get_barrier_semaphore()

    core, ycoord, xcoord = lax.rem(me, 2), lax.rem(me // 2, 4), me // 8
    partner = me + 1 - 2 * core

    def signal(semaphore, target):
        pl.semaphore_signal(semaphore, inc=1, device_id={"cp": target}, device_id_type=MESH)

    along_x = [(lax.rem(xcoord + n, 4) * 4 + ycoord) * 2 + core for n in (1, 2, 3)]
    along_y = [(xcoord * 4 + lax.rem(ycoord + n, 4)) * 2 + core for n in (1, 2, 3)]
    pl.semaphore_signal(barrier, inc=1, device_id={"tp": up}, device_id_type=MESH)
    pl.semaphore_signal(barrier, inc=1, device_id={"tp": down}, device_id_type=MESH)
    for target in (*along_x, *along_y, partner):
        signal(barrier, target)

    turned_row = lax.broadcasted_iota(jnp.int32, (QROWS, QROWS), 0)
    turned_column = lax.broadcasted_iota(jnp.int32, (QROWS, QROWS), 1)
    rows = SPAN * PORTION
    head, at_row = turned_row // rows, lax.rem(turned_row, rows)
    source = (
        lax.rem(head, 4) * 2 * rows
        + (at_row // PORTION) * 2 * PORTION
        + (head // 4) * PORTION
        + lax.rem(at_row, PORTION)
    )
    select = (turned_column == source).astype(jnp.float32).astype(jnp.bfloat16)
    for g in range(GROUPS):
        part = lax.dot_general(
            select,
            heads_ref[g],
            (((1,), (1,)), ((), ())),
            preferred_element_type=jnp.float32,
        ).astype(jnp.bfloat16)
        for h in range(HEADS):
            heads[g * rows : (g + 1) * rows, h * HEAD : (h + 1) * HEAD] = part[
                h * rows : (h + 1) * rows
            ]

    def product(n, c):
        columns = slice(FIRST[c] * HEAD, (FIRST[c] + CHUNKS[c]) * HEAD)
        return jnp.dot(heads[...], wo[n, :, columns], preferred_element_type=jnp.float32)

    def remote(n, src, dst, target):
        return pltpu.make_async_remote_copy(
            src_ref=src,
            dst_ref=dst,
            send_sem=z_send.at[0],
            recv_sem=z_recv.at[n],
            device_id={"tp": target},
            device_id_type=MESH,
        )

    half = ROWS // 2
    upper, lower = pl.ds(0, half), pl.ds(half, half)
    far_copies, near_copies = [], []
    for c, count in enumerate(CHUNKS):
        at = pl.ds(FIRST[c], count)
        far_copies.append(
            (
                remote(3 * c, far.at[0, at], far_in.at[0, at], up),
                remote(3 * c + 1, far.at[1, at], far_in.at[1, at], down),
            )
        )
        near_copies.append(
            (
                remote(3 * c + 2, near.at[0, at], near_in.at[0, at], up),
                remote(3 * c + 2, near.at[1, at], near_in.at[1, at], down),
            )
        )

    def pieces(c):
        return [(FIRST[c] + n, slice(n * HEAD, (n + 1) * HEAD)) for n in range(CHUNKS[c])]

    def make_far(c):
        value = product(0, c).astype(jnp.bfloat16)
        for at, columns in pieces(c):
            far[0, at] = value[:half, columns]
            far[1, at] = value[half:, columns]

    def send_far(c):
        for copy in far_copies[c]:
            copy.start()

    def send_near(c):
        to_up, to_down = product(1, c), product(2, c)
        far_copies[c][0].wait_recv()
        for at, columns in pieces(c):
            near[0, at, upper] = (
                to_up[:half, columns] + far_in[0, at].astype(jnp.float32)
            ).astype(jnp.bfloat16)
            near[0, at, lower] = to_up[half:, columns].astype(jnp.bfloat16)
        near_copies[c][0].start()
        far_copies[c][1].wait_recv()
        for at, columns in pieces(c):
            near[1, at, upper] = to_down[:half, columns].astype(jnp.bfloat16)
            near[1, at, lower] = (
                to_down[half:, columns] + far_in[1, at].astype(jnp.float32)
            ).astype(jnp.bfloat16)
        near_copies[c][1].start()

    def sum_own(c):
        value = product(3, c)
        for at, columns in pieces(c):
            own_sum[at] = value[:, columns]

    row = lax.broadcasted_iota(jnp.int32, (ROWS, ROWS), 0)
    column = lax.broadcasted_iota(jnp.int32, (ROWS, ROWS), 1)
    to_owner = (row == slot_ref[0:1, :]).astype(jnp.float32).astype(jnp.bfloat16)
    origin = (lax.rem(row, BLOCK) // 4) * 8 + (row // BLOCK) * 4 + lax.rem(row, 4)
    to_place = (column == origin).astype(jnp.float32).astype(jnp.bfloat16)

    def acopy(c, target, slot):
        at = pl.ds(FIRST[c], CHUNKS[c])
        return pltpu.make_async_remote_copy(
            src_ref=spread.at[target, at],
            dst_ref=landed.at[slot, at],
            send_sem=a_send.at[c],
            recv_sem=a_recv.at[c],
            device_id={"cp": target},
            device_id_type=MESH,
        )

    def finish_sum(c):
        both = near_in.at[:, pl.ds(FIRST[c], CHUNKS[c])]
        pltpu.make_async_copy(both, both, z_recv.at[3 * c + 2]).wait()
        total = jnp.concatenate(
            [
                (
                    own_sum[at]
                    + near_in[0, at].astype(jnp.float32)
                    + near_in[1, at].astype(jnp.float32)
                ).astype(jnp.bfloat16)
                for at, columns in pieces(c)
            ],
            axis=1,
        )
        picked = jnp.dot(to_owner, total, preferred_element_type=jnp.float32)
        for at, columns in pieces(c):
            spread[:, at] = picked[:, columns].reshape(CP, 8, HEAD).astype(jnp.bfloat16)
            landed[me, at] = spread[me, at]

        def send(k, carry):
            acopy(c, lax.rem(me + k, CP), me).start()
            return carry

        lax.fori_loop(1, CP, send, 0)

    def place(c):
        everyone = landed.at[pl.ds(0, CP - 1), pl.ds(FIRST[c], CHUNKS[c])]
        pltpu.make_async_copy(everyone, everyone, a_recv.at[c]).wait()
        rows = jnp.concatenate(
            [
                landed[:, at].astype(jnp.float32).reshape(ROWS, HEAD).astype(jnp.bfloat16)
                for at, columns in pieces(c)
            ],
            axis=1,
        )
        out_ref[:, FIRST[c] * HEAD : (FIRST[c] + CHUNKS[c]) * HEAD] = jnp.dot(
            to_place, rows, preferred_element_type=jnp.float32
        ).astype(jnp.bfloat16)

    loads[0].wait()
    make_far(0)
    pl.semaphore_wait(barrier, 9)
    send_far(0)
    for target in along_x:
        signal(met.at[0], target)
    make_far(1)
    send_far(1)
    make_far(2)
    send_far(2)
    loads[1].wait()
    loads[2].wait()
    send_near(0)
    pl.semaphore_wait(met.at[0], 3)
    signal(met.at[1], partner)
    make_far(3)
    send_far(3)
    send_near(1)
    make_far(4)
    send_far(4)
    send_near(2)
    loads[3].wait()
    for c in range(len(CHUNKS)):
        sum_own(c)
    send_near(3)
    pl.semaphore_wait(met.at[1], 1)
    finish_sum(0)
    send_near(4)
    finish_sum(1)
    finish_sum(2)
    finish_sum(3)
    finish_sum(4)
    for c in range(len(CHUNKS)):
        place(c)
    for c in range(len(CHUNKS)):
        everyone = spread.at[pl.ds(0, CP - 1), pl.ds(FIRST[c], CHUNKS[c])]
        pltpu.make_async_copy(everyone, everyone, a_send.at[c]).wait()
    sent = wo.at[0, pl.ds(0, 3 * ROWS)]
    pltpu.make_async_copy(sent, sent, z_send.at[0]).wait()


def output_call(slot_rows, heads, wo):
    vmem = pl.BlockSpec(memory_space=pltpu.VMEM)
    dma = pltpu.SemaphoreType.DMA
    half = ROWS // 2
    bf16 = jnp.bfloat16
    return pl.pallas_call(
        output_kernel,
        out_shape=jax.ShapeDtypeStruct((ROWS, WIDTH), bf16),
        in_specs=[vmem, vmem, pl.BlockSpec(memory_space=pltpu.HBM)],
        out_specs=vmem,
        scratch_shapes=[
            pltpu.VMEM((ROWS, WIDTH), bf16),
            pltpu.VMEM((TP, WIDTH, WIDTH), bf16),
            pltpu.VMEM((2, PIECES, half, HEAD), bf16),
            pltpu.VMEM((2, PIECES, ROWS, HEAD), bf16),
            pltpu.VMEM((2, PIECES, half, HEAD), bf16),
            pltpu.VMEM((2, PIECES, ROWS, HEAD), bf16),
            pltpu.VMEM((CP, PIECES, 8, HEAD), bf16),
            pltpu.VMEM((CP, PIECES, 8, HEAD), bf16),
            pltpu.VMEM((PIECES, ROWS, HEAD), jnp.float32),
            dma((4,)), dma((1,)), dma((3 * len(CHUNKS),)),
            dma((len(CHUNKS),)), dma((len(CHUNKS),)), pltpu.SemaphoreType.REGULAR((2,)),
        ],
        compiler_params=pltpu.CompilerParams(
            collective_id=1, has_side_effects=True, vmem_limit_bytes=40 * 1024 * 1024
        ),
        name="project_out",
    )(slot_rows, heads, wo)


def local(hidden, query_weight, key_matrix, value_matrix, output_weight, bounds, block_owner):
    inverse = rope_inverse(HEAD)
    inverse = jnp.concatenate([inverse, inverse])[None, :]
    hidden, query_weight, key_matrix, value_matrix, output_weight = (
        pltpu.with_memory_space_constraint(a, pltpu.HBM)
        for a in (hidden, query_weight, key_matrix, value_matrix, output_weight)
    )
    keys, values, queries, marks, slot_rows = gather_call(
        pltpu.with_memory_space_constraint(bounds, pltpu.HBM),
        pltpu.with_memory_space_constraint(block_owner, pltpu.HBM), hidden, query_weight, key_matrix, value_matrix, inverse
    )
    heads = attend_call(
        bounds,
        queries.reshape(2 * ROWS, WIDTH // 2),
        keys.reshape(TOKENS, HEAD),
        values.reshape(TOKENS, HEAD),
        marks,
    )
    return output_call(slot_rows, heads, output_weight)


def solution(mesh):
    placed = (P("cp", "tp"), P(None, "tp"), P(None, "tp"), P(None, "tp"), P("tp", None), P(), P())
    return jax.shard_map(
        local, mesh=mesh, in_specs=placed, out_specs=P("cp", "tp"), check_vma=False
    )
```
